32 devices in a mesh: wide: 16 (over z, x, core), narrow: 2 (over y).
Axes of the slice: x: 2, y: 2, z: 4, core: 2. Of those that a mesh axis runs over, the one named last changes fastest.
Arguments:
- right_side: float32 [3, 256, 32, 128], P(None, 'wide', 'narrow'), may hold values from -8 to 8
- occupancy: int32 [256, 32, 128], P('wide', 'narrow'), may hold values from 0 to 1, as said below
- region: int32 [256, 32, 128], P('wide', 'narrow'), may hold values from 0 to 3
- coarse_inverse: float32 [384, 384], P(('wide', 'narrow')), as said below
Outputs:
- solution_field: float32 [3, 256, 32, 128], P(None, 'wide', 'narrow')
- residual: float32 [3, 256, 32, 128], P(None, 'wide', 'narrow')
The draws below stay inside these ranges and needn't reach their ends.
Inputs may be any that keep to these rules, and one draw needn't show every extreme that they name: `occupancy`: each subdomain has its own bone fraction between 0.15 and 0.9. `coarse_inverse`: symmetric positive definite.
All inputs are finite; a program needn't handle non-finite values.
Results may differ from the reference program's by a relative error of at most 0.00021.
Values sent between devices are 32-bit elements; how exact they have to be, the bound alone decides.
A program may use at most 64 MiB of HBM per device.

```python
import jax
import jax.numpy as jnp
from jax import lax

CX = 16
CY = 16
CZ = 128
NREG = 4
ITERS = 2
NX = 256
NY = 32
NZ = 128
NCOARSE = 384
N_WIDE = 16
N_NARROW = 2


def draw_occupancy(key, part):
    first, second = jax.random.split(key)
    wide_count = NX // CX
    narrow_count = NY // CY
    percent = jax.random.randint(first, (wide_count, narrow_count), 15, 91)
    level = jnp.repeat(jnp.repeat(percent, CX, axis=0), CY, axis=1)[:, :, None]
    bits = jax.random.randint(second, (NX, NY, NZ), 0, 100)
    return (bits < level).astype(jnp.int32)


def draw_coarse_inverse(key, part):
    first, second = jax.random.split(jax.random.fold_in(key, 7), 2)
    count = NCOARSE
    factor = jax.random.normal(first, (count, count), jnp.float32)
    gram = jnp.dot(factor, factor.T) / count
    gram = 0.5 * (gram + gram.T)
    diag = jax.random.uniform(second, (count,), jnp.float32, 0.5, 1.5)
    whole = gram + jnp.diag(diag)
    scale = 0.05 * jnp.sqrt(jnp.float32(NREG) / jnp.float32(CX * CY * CZ))
    return (whole * scale).astype(jnp.float32)


def with_ends(values, rng, low, top_value):
    dims = values.shape
    spot = [jax.random.randint(jax.random.fold_in(rng, axis), (), 0, dims[axis]) for axis in range(len(dims))]
    values = values.at[tuple(spot)].set(low)
    longest = dims.index(max(dims))
    spot[longest] = (spot[longest] + 1) % dims[longest]
    return values.at[tuple(spot)].set(top_value)


def level_of(stream_key, extent, shards, smallest, largest):
    factor_of = 1.0
    for dim, parts in shards:
        steps = jax.random.uniform(jax.random.fold_in(jax.random.fold_in(stream_key, 6), dim), (parts,), jnp.float32, smallest / len(shards), largest / len(shards))
        factor_of = factor_of * jnp.repeat(jnp.exp(steps), extent[dim] // parts).reshape((-1,) + (1,) * (len(extent) - 1 - dim))
    return factor_of


def centred(rng, shape, width, most, pieces=(), dtype=jnp.bfloat16):
    values = jax.random.normal(rng, shape, jnp.float32) * width
    if len(pieces) > 0:
        values = level_of(rng, shape, pieces, -0.22, 0.18) * values
    return jnp.clip(values, min=-most, max=most).astype(dtype)


def setup_inputs(seed: int = 0) -> dict:
    key_of = jax.random.split(jax.random.key(seed), 5)
    return {
        "right_side": centred(key_of[0], (3, NX, NY, NZ), 1.0, 8.0, ((1, 16), (2, 2)), jnp.float32),
        "occupancy": draw_occupancy(jax.random.fold_in(key_of[4], 71), 0),
        "region": with_ends(jax.random.randint(key_of[2], (NX, NY, NZ), 0, NREG), jax.random.fold_in(key_of[2], 1), 0, NREG - 1).astype(jnp.int32),
        "coarse_inverse": draw_coarse_inverse(jax.random.fold_in(key_of[4], 71), 0),
    }


bone_stiff = 1.0
soft_stiff = 0.1


def neighbours(padded):
    return [padded[..., 2:, 1:-1, 1:-1], padded[..., :-2, 1:-1, 1:-1],
            padded[..., 1:-1, 2:, 1:-1], padded[..., 1:-1, :-2, 1:-1],
            padded[..., 1:-1, 1:-1, 2:], padded[..., 1:-1, 1:-1, :-2]]


def reference(right_side, occupancy, region, coarse_inverse):
    stiff = soft_stiff + (bone_stiff - soft_stiff) * occupancy.astype(jnp.float32)
    faces = [0.5 * (stiff + other) for other in neighbours(jnp.pad(stiff, 1))]
    diagonal = sum(faces) + 0.5 * stiff
    wide_count = N_WIDE
    narrow_count = N_NARROW

    def operate(field):
        padded = jnp.pad(field, ((0, 0), (1, 1), (1, 1), (1, 1)))
        result = 0.25 * stiff * (field + jnp.sum(field, axis=0, keepdims=True))
        for face, other in zip(faces, neighbours(padded)):
            result = result + face * (field - other)
        return result

    selects = [(region == g).astype(jnp.float32).reshape(wide_count, CX, narrow_count, CY, CZ) for g in range(NREG)]

    def precondition(resid):
        blocks = resid.reshape(3, wide_count, CX, narrow_count, CY, CZ)
        coarse = jnp.stack([jnp.einsum('cwxnyz,wxnyz->wnc', blocks, s, precision=lax.Precision.HIGHEST) for s in selects], axis=2).reshape(-1)
        answer = jnp.dot(coarse_inverse, coarse, precision=lax.Precision.HIGHEST).reshape(wide_count, narrow_count, NREG, 3)
        spread = jnp.zeros_like(blocks)
        for g in range(NREG):
            spread = spread + jnp.einsum('wxnyz,wnc->cwxnyz', selects[g], answer[:, :, g, :], precision=lax.Precision.HIGHEST)
        return resid / diagonal + spread.reshape(resid.shape)

    solution = jnp.zeros_like(right_side)
    resid = right_side
    precond = precondition(resid)
    direction = precond
    rz_now = jnp.sum(resid * precond)
    for step in range(ITERS):
        image = operate(direction)
        alpha = rz_now / jnp.sum(direction * image)
        solution = solution + alpha * direction
        resid = resid - alpha * image
        precond = precondition(resid)
        rz_next = jnp.sum(resid * precond)
        direction = precond + (rz_next / rz_now) * direction
        rz_now = rz_next
    return solution, resid
```

```python
import functools

import jax
import jax.numpy as jnp
from jax import lax
from jax.experimental import pallas as pl
from jax.experimental.pallas import tpu as pltpu
from jax.sharding import PartitionSpec as P

LANES = 128
SUB = 8
UNROLL = 16
looped = functools.partial(lax.fori_loop, unroll=UNROLL)
MESH = pl.DeviceIdType.MESH
bone_stiff = 1.0
soft_stiff = 0.1


def group_of(n):
    return max(d for d in range(1, n + 1) if n % d == 0 and d * d <= n)


def kernel(nw, nn, r_hbm, occ_hbm, reg_hbm, ci_hbm,
           z0_v, z1_v, r_v, az_v, y_v, sc_v,
            occ_v, reg_v, c_v, k_p, kx, kym, kyp, kzm, kzp, dg, invd,
           z_p, v_p, zy, vy,
           ix_in, iy_send, iy_in, c_in, wx_send, wx_in, wy_send, wy_in,
           row_send, rows, load_sem, hs_send, hs_recv, ag_send, ag_recv, ready):
    X, Y, Z = occ_v.shape
    ncr, NC = c_v.shape
    G = ncr // 3
    ND = nw * nn
    wi = lax.axis_index("wide")
    ni = lax.axis_index("narrow")
    me = wi * nn + ni
    f32 = jnp.float32

    GP = group_of(nw) * nn
    NG = ND // GP
    grp, pos = me // GP, lax.rem(me, GP)

    loads = [pltpu.make_async_copy(s, d, load_sem.at[i]) for i, (s, d) in enumerate(
        ((reg_hbm, reg_v), (r_hbm, r_v), (occ_hbm, occ_v), (ci_hbm, c_v)))]
    for l in loads:
        l.start()

    def peer(i):
        t = lax.rem(me + i, ND)
        return (t // nn, lax.rem(t, nn))

    barrier = pltpu.get_barrier_semaphore()

    def at(t):
        return (t // nn, lax.rem(t, nn))

    def greet(t, _):
        pl.semaphore_signal(barrier, inc=1, device_id=at(t), device_id_type=MESH)
        return 0

    lax.fori_loop(me + 1, ND, greet, 0)

    def kind_of(low, high):
        apart = high // GP - low // GP
        k = jnp.where(lax.rem(high, GP) == lax.rem(low, GP), apart, NG + 1)
        k = jnp.where(high - low == nn, NG, k)
        return jnp.where(apart == 0, 0, k)

    def wait_for(sem, count):
        @pl.when(count > 0)
        def _():
            pl.semaphore_wait(sem, count)

    def tell(i, _):
        t = me - 1 - i
        pl.semaphore_signal(ready.at[kind_of(t, me)], inc=1, device_id=at(t), device_id_type=MESH)
        return 0

    has_beside = jnp.logical_and(wi < nw - 1, kind_of(me, me + nn) == NG)

    has = (wi > 0, wi < nw - 1, ni > 0, ni < nn - 1)
    to = ((wi - 1, ni), (wi + 1, ni), (wi, ni - 1), (wi, ni + 1))

    for d in range(4):
        @pl.when(jnp.logical_not(has[d]))
        def _():
            c_in[d] = jnp.zeros((ncr, NC), f32)
            for p in range(2):
                if d < 2:
                    wx_in[p, d] = jnp.zeros((3, Y, Z), f32)
                else:
                    wy_in[p, d - 2] = jnp.zeros((3, X, Z), f32)
            if d < 2:
                ix_in[d] = jnp.zeros((2, Y, Z), jnp.int32)
            else:
                iy_in[d - 2] = jnp.zeros((2, X, Z), jnp.int32)

    def pack_ints(x, _):
        iy_send[0, 0, pl.ds(x, 1), :] = occ_v[x, 0:1, :]
        iy_send[1, 0, pl.ds(x, 1), :] = occ_v[x, Y - 1:Y, :]
        iy_send[0, 1, pl.ds(x, 1), :] = reg_v[x, 0:1, :]
        iy_send[1, 1, pl.ds(x, 1), :] = reg_v[x, Y - 1:Y, :]
        return 0

    def fold(a):
        return jnp.sum(a.reshape(Y // SUB, SUB, Z), axis=0)

    def zero_acc(n):
        return tuple(jnp.zeros((SUB, Z), f32) for _ in range(n))

    def add_rc(acc, reg, u):
        out = list(acc)
        for g in range(G):
            m = reg == g
            for c in range(3):
                out[g * 3 + c] = acc[g * 3 + c] + fold(jnp.where(m, u[c], 0.0))
        return tuple(out)

    base = (me * ncr) % LANES

    def make_row(p, acc, first):
        a = jnp.concatenate([jnp.sum(b, axis=0, keepdims=True) for b in acc], axis=0)
        col = jnp.sum(a, axis=1, keepdims=True)
        n = len(acc)
        k = lax.broadcasted_iota(jnp.int32, (n, LANES), 0)
        lane = lax.broadcasted_iota(jnp.int32, (n, LANES), 1)
        target = (base + first + k) & (LANES - 1)
        row = jnp.sum(jnp.where(lane == target, col, 0.0), axis=0, keepdims=True)
        row_send[p, 0:1, :] = row
        rows[p, pl.ds(me, 1), :] = row

    def group_start():
        def send(i, _):
            pltpu.make_async_remote_copy(
                src_ref=row_send.at[0, pl.ds(0, 1)], dst_ref=rows.at[0, pl.ds(me, 1)],
                send_sem=ag_send.at[0], recv_sem=ag_recv.at[0],
                device_id=at(grp * GP + lax.rem(pos + i, GP)), device_id_type=MESH).start()
            return 0
        lax.fori_loop(1, GP, send, 0, unroll=GP <= 64)

    def group_wait(sem):
        part = rows.at[0, pl.ds(0, GP - 1)]
        pltpu.make_async_copy(part, part, sem.at[0]).wait()

    def across_start():
        mine = rows.at[0, pl.ds(pl.multiple_of(grp * GP, GP), GP)]
        for k in range(1, NG):
            for up in (True, False):
                @pl.when(grp + k < NG if up else grp >= k)
                def _():
                    if up and k * GP != nn:
                        pl.semaphore_wait(ready.at[k], 1)
                    pltpu.make_async_remote_copy(
                        src_ref=mine, dst_ref=mine,
                        send_sem=ag_send.at[3], recv_sem=ag_recv.at[3],
                        device_id=at(me + (k * GP if up else -k * GP)), device_id_type=MESH).start()

    def across_wait(sem):
        part = rows.at[0, pl.ds(0, ND - GP)]
        pltpu.make_async_copy(part, part, sem.at[3]).wait()

    def gather_start(p):
        def send(i, _):
            pltpu.make_async_remote_copy(
                src_ref=row_send.at[p, pl.ds(0, 1)], dst_ref=rows.at[p, pl.ds(me, 1)],
                send_sem=ag_send.at[p], recv_sem=ag_recv.at[p],
                device_id=peer(i), device_id_type=MESH).start()
            return 0
        lax.fori_loop(1, ND, send, 0, unroll=ND <= 64)

    def gather_wait(p, sem):
        part = rows.at[p, pl.ds(0, ND - 1)]
        pltpu.make_async_copy(part, part, sem.at[p]).wait()

    def coarse_vector(p):
        tiles = []
        for t in range(NC // LANES):
            lo = (LANES * t) // ncr // SUB * SUB
            hi = min(ND, -(-(-(-(LANES * (t + 1)) // ncr)) // SUB) * SUB)
            d = lax.broadcasted_iota(jnp.int32, (hi - lo, LANES), 0) + lo
            j = lax.broadcasted_iota(jnp.int32, (hi - lo, LANES), 1) + LANES * t
            m = (j >= d * ncr) & (j < d * ncr + ncr)
            tiles.append(jnp.sum(jnp.where(m, rows[p, lo:hi, :], 0.0), axis=0, keepdims=True))
        return tiles

    def total(p, s):
        d = lax.broadcasted_iota(jnp.int32, (ND, LANES), 0)
        lane = lax.broadcasted_iota(jnp.int32, (ND, LANES), 1)
        m = lane == ((d * ncr + ncr + s) & (LANES - 1))
        v = jnp.sum(jnp.where(m, rows[p], 0.0), axis=0, keepdims=True)
        return jnp.sum(v, axis=1, keepdims=True)

    def answers(tiles, ref):
        s = ref[:, 0:LANES] * tiles[0]
        for t in range(1, len(tiles)):
            s = s + ref[:, t * LANES:(t + 1) * LANES] * tiles[t]
        q = jnp.sum(s, axis=1, keepdims=True)
        return [q[i:i + 1, :] for i in range(ncr)]

    def spread(reg, q):
        masks = [reg == g for g in range(G)]
        out = []
        for c in range(3):
            s = jnp.zeros(reg.shape, f32)
            for g in range(G):
                s = jnp.where(masks[g], q[g * 3 + c], s)
            out.append(s)
        return out

    def halo(slot, d, src, dst):
        return pltpu.make_async_remote_copy(
            src_ref=src, dst_ref=dst, send_sem=hs_send.at[slot, d],
            recv_sem=hs_recv.at[slot, d ^ 1], device_id=to[d], device_id_type=MESH)

    def copies(kind, d):
        e = d ^ 1
        if kind == 0:
            if d < 2:
                x = 0 if d == 0 else X - 1
                return [halo(0, d, occ_v.at[x], ix_in.at[e, 0]),
                        halo(1, d, reg_v.at[x], ix_in.at[e, 1])]
            return [halo(0, d, iy_send.at[d - 2, 0], iy_in.at[e - 2, 0]),
                    halo(1, d, iy_send.at[d - 2, 1], iy_in.at[e - 2, 1])]
        if kind == 1:
            return [halo(2, d, c_v, c_in.at[e])]
        p = kind - 2
        if d < 2:
            return [halo(3 + p, d, wx_send.at[p, d], wx_in.at[p, e])]
        return [halo(3 + p, d, wy_send.at[p, d - 2], wy_in.at[p, e - 2])]

    def halo_start(kind):
        for d in range(4):
            @pl.when(has[d])
            def _():
                for c in copies(kind, d):
                    c.start()

    def halo_wait(kind):
        for d in range(4):
            @pl.when(has[d])
            def _():
                for c in copies(kind, d ^ 1):
                    c.wait_recv()

    def halo_done(kind):
        for d in range(4):
            @pl.when(has[d])
            def _():
                for c in copies(kind, d):
                    c.wait_send()

    loads[0].wait()
    loads[1].wait()
    acc = looped(0, X, lambda x, a: add_rc(a, reg_v[x], [r_v[c, x] for c in range(3)]),
                        zero_acc(ncr))
    make_row(0, acc, 0)

    wait_for(barrier, me)
    lax.fori_loop(0, me, tell, 0)
    wait_for(ready.at[0], GP - 1 - pos)
    group_start()
    loads[2].wait()
    looped(0, X, pack_ints, 0)

    @pl.when(has_beside)
    def _():
        pl.semaphore_wait(ready.at[NG], 1)

    halo_start(0)
    loads[3].wait()
    halo_start(1)
    group_wait(ag_recv)
    across_start()

    def stiff_of(o):
        return soft_stiff + (bone_stiff - soft_stiff) * o.astype(f32)

    def own_k(x, _):
        k_p[x + 1] = stiff_of(occ_v[x])
        return 0

    looped(0, X, own_k, 0)
    halo_wait(0)
    for d in range(2):
        @pl.when(has[d])
        def _():
            k_p[0 if d == 0 else X + 1] = stiff_of(ix_in[d, 0])

        @pl.when(jnp.logical_not(has[d]))
        def _():
            k_p[0 if d == 0 else X + 1] = jnp.zeros((Y, Z), f32)

    row_id = lax.broadcasted_iota(jnp.int32, (Y, Z), 0)
    lane_id = lax.broadcasted_iota(jnp.int32, (Y, Z), 1)
    side_lo = jnp.where(has[2], 1.0, 0.0).astype(f32)
    side_hi = jnp.where(has[3], 1.0, 0.0).astype(f32)

    def yshift(u, lo, hi):
        down = jnp.where(row_id == 0, lo, pltpu.roll(u, 1, 0))
        up = jnp.where(row_id == Y - 1, hi, pltpu.roll(u, Y - 1, 0))
        return down, up

    def save_faces(p, x, w):
        for c in range(3):
            wy_send[p, 0, c, pl.ds(x, 1), :] = w[c][0:1, :]
            wy_send[p, 1, c, pl.ds(x, 1), :] = w[c][Y - 1:Y, :]

    def coefficients(x, _):
        k = k_p[x + 1]
        lo = stiff_of(iy_in[0, 0, pl.ds(x, 1), :]) * side_lo
        hi = stiff_of(iy_in[1, 0, pl.ds(x, 1), :]) * side_hi
        down, up = yshift(k, lo, hi)
        back = jnp.where(lane_id == 0, 0.0, pltpu.roll(k, 1, 1))
        ahead = jnp.where(lane_id == Z - 1, 0.0, pltpu.roll(k, Z - 1, 1))
        xm = 0.5 * (k + k_p[x])
        xp = 0.5 * (k + k_p[x + 2])
        ym = 0.5 * (k + down)
        yp = 0.5 * (k + up)
        zm = 0.5 * (k + back)
        zp = 0.5 * (k + ahead)
        diag = xm + xp + ym + yp + zm + zp + 0.5 * k
        inv = 1.0 / diag
        kx[x] = xm
        kx[x + 1] = xp
        kym[x] = ym
        kyp[x] = yp
        kzm[x] = jnp.where(lane_id == 0, 0.0, zm)
        kzp[x] = jnp.where(lane_id == Z - 1, 0.0, zp)
        dg[x] = diag - 0.25 * k
        invd[x] = inv
        w = [r_v[c, x] * inv for c in range(3)]
        for c in range(3):
            z_p[c, x + 1] = w[c]
        save_faces(0, x, w)
        return 0

    looped(0, X, coefficients, 0)
    for c in range(3):
        wx_send[0, 0, c] = z_p[c, 1]
        wx_send[0, 1, c] = z_p[c, X]
    halo_start(2)

    def edges(p, qs, pad, side):
        for d in range(2):
            s = spread(ix_in[d, 1], qs[d])
            for c in range(3):
                pad[c, 0 if d == 0 else X + 1] = wx_in[p, d, c] + s[c]
        for d in range(2):
            s = spread(iy_in[d, 1], qs[2 + d])
            for c in range(3):
                side[d, c] = wy_in[p, d, c] + s[c]

    def operate(pad, side, x):
        k = k_p[x + 1]
        u = [pad[c, x + 1] for c in range(3)]
        k4 = 0.25 * k * (u[0] + u[1] + u[2])
        out = []
        for c in range(3):
            down, up = yshift(u[c], side[0, c, pl.ds(x, 1), :], side[1, c, pl.ds(x, 1), :])
            a = dg[x] * u[c] + k4
            a = a - (kx[x] * pad[c, x] + kx[x + 1] * pad[c, x + 2])
            a = a - (kym[x] * down + kyp[x] * up)
            a = a - (kzm[x] * pltpu.roll(u[c], 1, 1) + kzp[x] * pltpu.roll(u[c], Z - 1, 1))
            out.append(a)
        return u, out

    across_wait(ag_recv)
    halo_wait(1)
    tiles = coarse_vector(0)
    q = answers(tiles, c_v)
    qs = [answers(tiles, c_in.at[d]) for d in range(4)]

    def add_spread(x, _):
        s = spread(reg_v[x], q)
        for c in range(3):
            z = z_p[c, x + 1] + s[c]
            z_p[c, x + 1] = z
            z0_v[c, x] = z
        return 0

    looped(0, X, add_spread, 0)
    halo_wait(2)
    edges(0, qs, z_p, zy)

    def dots(a, b):
        return fold(a[0] * b[0] + a[1] * b[1] + a[2] * b[2])

    def first(x, carry):
        u, a = operate(z_p, zy, x)
        r = [r_v[c, x] for c in range(3)]
        w = []
        for c in range(3):
            y_v[c, x] = a[c]
            w.append(a[c] * invd[x])
            v_p[c, x + 1] = w[c]
        save_faces(1, x, w)
        acc = add_rc(carry[:ncr], reg_v[x], a)
        return acc + (carry[ncr] + dots(r, u), carry[ncr + 1] + dots(a, u))

    acc = looped(0, X, first, zero_acc(ncr + 2))
    make_row(1, acc, 0)
    rest = ND - 1 - me - (GP - 1 - pos) - (NG - 1 - grp)
    if GP != nn:
        rest = rest - jnp.where(has_beside, 1, 0)
    wait_for(ready.at[NG + 1], rest)
    gather_start(1)
    for c in range(3):
        wx_send[1, 0, c] = v_p[c, 1]
        wx_send[1, 1, c] = v_p[c, X]
    halo_start(3)
    halo_wait(3)
    gather_wait(1, ag_recv)
    tiles = coarse_vector(1)
    q = answers(tiles, c_v)
    qs = [answers(tiles, c_in.at[d]) for d in range(4)]
    rz0 = total(1, 0)
    alpha0 = rz0 / total(1, 1)

    def add_spread_v(x, _):
        s = spread(reg_v[x], q)
        for c in range(3):
            v_p[c, x + 1] = v_p[c, x + 1] + s[c]
        return 0

    looped(0, X, add_spread_v, 0)
    edges(1, qs, v_p, vy)

    def second(x, carry):
        u, a = operate(v_p, vy, x)
        r, z, az = [], [], []
        for c in range(3):
            y = y_v[c, x]
            r.append(r_v[c, x] - alpha0 * y)
            z.append(z_p[c, x + 1] - alpha0 * u[c])
            az.append(y - alpha0 * a[c])
            r_v[c, x] = r[c]
            z1_v[c, x] = z[c]
            az_v[c, x] = az[c]
        return (carry[0] + dots(r, z), carry[1] + dots(az, z))

    acc = looped(0, X, second, zero_acc(2))
    make_row(2, acc, ncr)
    gather_start(2)
    gather_wait(2, ag_recv)
    rz1 = total(2, 0)
    beta = rz1 / rz0
    alpha1 = rz1 / (total(2, 1) - beta * rz1 / alpha0)
    along = alpha0 + alpha1 * beta
    a1b = alpha1 * beta

    sc_v[0:1, :] = jnp.broadcast_to(along, (1, LANES))
    sc_v[1:2, :] = jnp.broadcast_to(alpha1, (1, LANES))
    sc_v[2:3, :] = jnp.broadcast_to(a1b, (1, LANES))
    for kind in range(4):
        halo_done(kind)
    group_wait(ag_send)
    across_wait(ag_send)
    for p in range(1, 3):
        gather_wait(p, ag_send)


def finish(z0_v, z1_v, r_v, az_v, y_v, sc_v, x_out, res_out, xb, rb, sem):
    along = sc_v[0:1, 0:1]
    alpha1 = sc_v[1:2, 0:1]
    a1b = sc_v[2:3, 0:1]
    X = z0_v.shape[1]
    copies = []
    for c in range(3):
        for x in range(X):
            xb[c, x] = along * z0_v[c, x] + alpha1 * z1_v[c, x]
            rb[c, x] = r_v[c, x] - alpha1 * az_v[c, x] - a1b * y_v[c, x]
        for n, (src, dst) in enumerate(((xb, x_out), (rb, res_out))):
            copies.append(pltpu.make_async_copy(src.at[c], dst.at[c], sem.at[n, c]))
            copies[-1].start()
    for copy in copies:
        copy.wait()


def local(nw, nn, right_side, occupancy, region, coarse_inverse):
    _, X, Y, Z = right_side.shape
    ncr, NC = coarse_inverse.shape
    ND = nw * nn
    f32, i32 = jnp.float32, jnp.int32
    V = pltpu.VMEM
    field, pad, scal = (3, X, Y, Z), (3, X + 2, Y, Z), (X, Y, Z)
    scratch = [
        V(scal, i32), V(scal, i32), V((ncr, NC), f32),
        V((X + 2, Y, Z), f32), V((X + 1, Y, Z), f32),
        V(scal, f32), V(scal, f32), V(scal, f32), V(scal, f32), V(scal, f32), V(scal, f32),
        V(pad, f32), V(pad, f32),
        V((2, 3, X, Z), f32), V((2, 3, X, Z), f32),
        V((2, 2, Y, Z), i32), V((2, 2, X, Z), i32), V((2, 2, X, Z), i32),
        V((4, ncr, NC), f32),
        V((2, 2, 3, Y, Z), f32), V((2, 2, 3, Y, Z), f32),
        V((2, 2, 3, X, Z), f32), V((2, 2, 3, X, Z), f32),
        V((3, SUB, LANES), f32), V((3, ND, LANES), f32),
        pltpu.SemaphoreType.DMA((4,)),
        pltpu.SemaphoreType.DMA((5, 4)), pltpu.SemaphoreType.DMA((5, 4)),
        pltpu.SemaphoreType.DMA((4,)), pltpu.SemaphoreType.DMA((4,)),
        pltpu.SemaphoreType.REGULAR((nw // group_of(nw) + 2,)),
    ]
    parts = pl.pallas_call(
        functools.partial(kernel, nw, nn),
        out_shape=(V(field, f32),) * 5 + (V((SUB, LANES), f32),),
        in_specs=[pl.BlockSpec(memory_space=pltpu.HBM)] * 4,
        out_specs=(pl.BlockSpec(memory_space=pltpu.VMEM),) * 6,
        scratch_shapes=scratch,
        compiler_params=pltpu.CompilerParams(collective_id=0, has_side_effects=True, vmem_limit_bytes=32 * 1024 * 1024),
    )(*[pltpu.with_memory_space_constraint(a, pltpu.HBM) for a in (right_side, occupancy, region, coarse_inverse)])
    return pl.pallas_call(
        finish,
        out_shape=(jax.ShapeDtypeStruct(field, f32),) * 2,
        in_specs=[pl.BlockSpec(memory_space=pltpu.VMEM)] * 6,
        out_specs=(pl.BlockSpec(memory_space=pltpu.HBM),) * 2,
        scratch_shapes=[V(field, f32), V(field, f32), pltpu.SemaphoreType.DMA((2, 3))],
        compiler_params=pltpu.CompilerParams(vmem_limit_bytes=16 * 1024 * 1024),
    )(*parts)


def solution(mesh):
    return jax.shard_map(
        functools.partial(local, mesh.shape["wide"], mesh.shape["narrow"]),
        mesh=mesh,
        in_specs=(
            P(None, "wide", "narrow", None),
            P("wide", "narrow", None),
            P("wide", "narrow", None),
            P(("wide", "narrow"), None),
        ),
        out_specs=(P(None, "wide", "narrow", None), P(None, "wide", "narrow", None)),
        check_vma=False,
    )
```

```python
import functools

import jax
import jax.numpy as jnp
from jax import lax
from jax.experimental import pallas as pl
from jax.experimental.pallas import tpu as pltpu
from jax.sharding import PartitionSpec as P

LANES = 128
SUB = 8
UNROLL = 16
looped = functools.partial(lax.fori_loop, unroll=UNROLL)
MESH = pl.DeviceIdType.MESH
bone_stiff = 1.0
soft_stiff = 0.1


def kernel_wide(nw, nn, r_hbm, occ_hbm, reg_hbm, ci_hbm,
           z0_v, z1_v, r_v, az_v, y_v, sc_v,
            occ_v, reg_v, c_v, k_p, kx, kym, kyp, kzm, kzp, dg, invd,
           z_p, v_p, zy, vy,
           ix_in, iy_send, iy_in, c_in, wx_send, wx_in, wy_send, wy_in,
           row_send, rows, load_sem, hs_send, hs_recv, ag_send, ag_recv):
    X, Y, Z = occ_v.shape
    ncr, NC = c_v.shape
    G = ncr // 3
    ND = nw * nn
    wi = lax.axis_index("wide")
    ni = lax.axis_index("narrow")
    me = wi * nn + ni
    f32 = jnp.float32

    loads = [pltpu.make_async_copy(s, d, load_sem.at[i]) for i, (s, d) in enumerate(
        ((occ_hbm, occ_v), (reg_hbm, reg_v), (r_hbm, r_v), (ci_hbm, c_v)))]
    for l in loads:
        l.start()

    def peer(i):
        t = lax.rem(me + i, ND)
        return (t // nn, lax.rem(t, nn))

    barrier = pltpu.get_barrier_semaphore()

    def greet(i, _):
        pl.semaphore_signal(barrier, inc=1, device_id=peer(i), device_id_type=MESH)
        return 0

    lax.fori_loop(1, ND, greet, 0, unroll=ND <= 64)

    has = (wi > 0, wi < nw - 1, ni > 0, ni < nn - 1)
    to = ((wi - 1, ni), (wi + 1, ni), (wi, ni - 1), (wi, ni + 1))

    for d in range(4):
        @pl.when(jnp.logical_not(has[d]))
        def _():
            c_in[d] = jnp.zeros((ncr, NC), f32)
            for p in range(2):
                if d < 2:
                    wx_in[p, d] = jnp.zeros((3, Y, Z), f32)
                else:
                    wy_in[p, d - 2] = jnp.zeros((3, X, Z), f32)
            if d < 2:
                ix_in[d] = jnp.zeros((2, Y, Z), jnp.int32)
            else:
                iy_in[d - 2] = jnp.zeros((2, X, Z), jnp.int32)

    loads[0].wait()
    loads[1].wait()

    def pack_ints(x, _):
        iy_send[0, 0, pl.ds(x, 1), :] = occ_v[x, 0:1, :]
        iy_send[1, 0, pl.ds(x, 1), :] = occ_v[x, Y - 1:Y, :]
        iy_send[0, 1, pl.ds(x, 1), :] = reg_v[x, 0:1, :]
        iy_send[1, 1, pl.ds(x, 1), :] = reg_v[x, Y - 1:Y, :]
        return 0

    looped(0, X, pack_ints, 0)

    def fold(a):
        return jnp.sum(a.reshape(Y // SUB, SUB, Z), axis=0)

    def zero_acc(n):
        return tuple(jnp.zeros((SUB, Z), f32) for _ in range(n))

    def add_rc(acc, reg, u):
        out = list(acc)
        for g in range(G):
            m = reg == g
            for c in range(3):
                out[g * 3 + c] = acc[g * 3 + c] + fold(jnp.where(m, u[c], 0.0))
        return tuple(out)

    base = (me * ncr) % LANES

    def make_row(p, acc, first):
        a = jnp.concatenate([jnp.sum(b, axis=0, keepdims=True) for b in acc], axis=0)
        col = jnp.sum(a, axis=1, keepdims=True)
        n = len(acc)
        k = lax.broadcasted_iota(jnp.int32, (n, LANES), 0)
        lane = lax.broadcasted_iota(jnp.int32, (n, LANES), 1)
        target = (base + first + k) & (LANES - 1)
        row = jnp.sum(jnp.where(lane == target, col, 0.0), axis=0, keepdims=True)
        row_send[p, 0:1, :] = row
        rows[p, pl.ds(me, 1), :] = row

    def gather_start(p):
        def send(i, _):
            pltpu.make_async_remote_copy(
                src_ref=row_send.at[p, pl.ds(0, 1)], dst_ref=rows.at[p, pl.ds(me, 1)],
                send_sem=ag_send.at[p], recv_sem=ag_recv.at[p],
                device_id=peer(i), device_id_type=MESH).start()
            return 0
        lax.fori_loop(1, ND, send, 0, unroll=ND <= 64)

    def gather_wait(p, sem):
        part = rows.at[p, pl.ds(0, ND - 1)]
        pltpu.make_async_copy(part, part, sem.at[p]).wait()

    def coarse_vector(p):
        tiles = []
        for t in range(NC // LANES):
            lo = (LANES * t) // ncr // SUB * SUB
            hi = min(ND, -(-(-(-(LANES * (t + 1)) // ncr)) // SUB) * SUB)
            d = lax.broadcasted_iota(jnp.int32, (hi - lo, LANES), 0) + lo
            j = lax.broadcasted_iota(jnp.int32, (hi - lo, LANES), 1) + LANES * t
            m = (j >= d * ncr) & (j < d * ncr + ncr)
            tiles.append(jnp.sum(jnp.where(m, rows[p, lo:hi, :], 0.0), axis=0, keepdims=True))
        return tiles

    def total(p, s):
        d = lax.broadcasted_iota(jnp.int32, (ND, LANES), 0)
        lane = lax.broadcasted_iota(jnp.int32, (ND, LANES), 1)
        m = lane == ((d * ncr + ncr + s) & (LANES - 1))
        v = jnp.sum(jnp.where(m, rows[p], 0.0), axis=0, keepdims=True)
        return jnp.sum(v, axis=1, keepdims=True)

    def answers(tiles, ref):
        s = ref[:, 0:LANES] * tiles[0]
        for t in range(1, len(tiles)):
            s = s + ref[:, t * LANES:(t + 1) * LANES] * tiles[t]
        q = jnp.sum(s, axis=1, keepdims=True)
        return [q[i:i + 1, :] for i in range(ncr)]

    def spread(reg, q):
        masks = [reg == g for g in range(G)]
        out = []
        for c in range(3):
            s = jnp.zeros(reg.shape, f32)
            for g in range(G):
                s = jnp.where(masks[g], q[g * 3 + c], s)
            out.append(s)
        return out

    def halo(slot, d, src, dst):
        return pltpu.make_async_remote_copy(
            src_ref=src, dst_ref=dst, send_sem=hs_send.at[slot, d],
            recv_sem=hs_recv.at[slot, d ^ 1], device_id=to[d], device_id_type=MESH)

    def copies(kind, d):
        e = d ^ 1
        if kind == 0:
            if d < 2:
                x = 0 if d == 0 else X - 1
                return [halo(0, d, occ_v.at[x], ix_in.at[e, 0]),
                        halo(1, d, reg_v.at[x], ix_in.at[e, 1])]
            return [halo(0, d, iy_send.at[d - 2, 0], iy_in.at[e - 2, 0]),
                    halo(1, d, iy_send.at[d - 2, 1], iy_in.at[e - 2, 1])]
        if kind == 1:
            return [halo(2, d, c_v, c_in.at[e])]
        p = kind - 2
        if d < 2:
            return [halo(3 + p, d, wx_send.at[p, d], wx_in.at[p, e])]
        return [halo(3 + p, d, wy_send.at[p, d - 2], wy_in.at[p, e - 2])]

    def halo_start(kind):
        for d in range(4):
            @pl.when(has[d])
            def _():
                for c in copies(kind, d):
                    c.start()

    def halo_wait(kind):
        for d in range(4):
            @pl.when(has[d])
            def _():
                for c in copies(kind, d ^ 1):
                    c.wait_recv()

    def halo_done(kind):
        for d in range(4):
            @pl.when(has[d])
            def _():
                for c in copies(kind, d):
                    c.wait_send()

    loads[2].wait()
    acc = looped(0, X, lambda x, a: add_rc(a, reg_v[x], [r_v[c, x] for c in range(3)]),
                        zero_acc(ncr))
    make_row(0, acc, 0)
    loads[3].wait()

    pl.semaphore_wait(barrier, ND - 1)
    halo_start(0)
    gather_start(0)
    halo_start(1)

    def stiff_of(o):
        return soft_stiff + (bone_stiff - soft_stiff) * o.astype(f32)

    def own_k(x, _):
        k_p[x + 1] = stiff_of(occ_v[x])
        return 0

    looped(0, X, own_k, 0)
    halo_wait(0)
    for d in range(2):
        @pl.when(has[d])
        def _():
            k_p[0 if d == 0 else X + 1] = stiff_of(ix_in[d, 0])

        @pl.when(jnp.logical_not(has[d]))
        def _():
            k_p[0 if d == 0 else X + 1] = jnp.zeros((Y, Z), f32)

    row_id = lax.broadcasted_iota(jnp.int32, (Y, Z), 0)
    lane_id = lax.broadcasted_iota(jnp.int32, (Y, Z), 1)
    side_lo = jnp.where(has[2], 1.0, 0.0).astype(f32)
    side_hi = jnp.where(has[3], 1.0, 0.0).astype(f32)

    def yshift(u, lo, hi):
        down = jnp.where(row_id == 0, lo, pltpu.roll(u, 1, 0))
        up = jnp.where(row_id == Y - 1, hi, pltpu.roll(u, Y - 1, 0))
        return down, up

    def save_faces(p, x, w):
        for c in range(3):
            wy_send[p, 0, c, pl.ds(x, 1), :] = w[c][0:1, :]
            wy_send[p, 1, c, pl.ds(x, 1), :] = w[c][Y - 1:Y, :]

    def coefficients(x, _):
        k = k_p[x + 1]
        lo = stiff_of(iy_in[0, 0, pl.ds(x, 1), :]) * side_lo
        hi = stiff_of(iy_in[1, 0, pl.ds(x, 1), :]) * side_hi
        down, up = yshift(k, lo, hi)
        back = jnp.where(lane_id == 0, 0.0, pltpu.roll(k, 1, 1))
        ahead = jnp.where(lane_id == Z - 1, 0.0, pltpu.roll(k, Z - 1, 1))
        xm = 0.5 * (k + k_p[x])
        xp = 0.5 * (k + k_p[x + 2])
        ym = 0.5 * (k + down)
        yp = 0.5 * (k + up)
        zm = 0.5 * (k + back)
        zp = 0.5 * (k + ahead)
        diag = xm + xp + ym + yp + zm + zp + 0.5 * k
        inv = 1.0 / diag
        kx[x] = xm
        kx[x + 1] = xp
        kym[x] = ym
        kyp[x] = yp
        kzm[x] = jnp.where(lane_id == 0, 0.0, zm)
        kzp[x] = jnp.where(lane_id == Z - 1, 0.0, zp)
        dg[x] = diag - 0.25 * k
        invd[x] = inv
        w = [r_v[c, x] * inv for c in range(3)]
        for c in range(3):
            z_p[c, x + 1] = w[c]
        save_faces(0, x, w)
        return 0

    looped(0, X, coefficients, 0)
    for c in range(3):
        wx_send[0, 0, c] = z_p[c, 1]
        wx_send[0, 1, c] = z_p[c, X]
    halo_start(2)

    def edges(p, qs, pad, side):
        for d in range(2):
            s = spread(ix_in[d, 1], qs[d])
            for c in range(3):
                pad[c, 0 if d == 0 else X + 1] = wx_in[p, d, c] + s[c]
        for d in range(2):
            s = spread(iy_in[d, 1], qs[2 + d])
            for c in range(3):
                side[d, c] = wy_in[p, d, c] + s[c]

    def operate(pad, side, x):
        k = k_p[x + 1]
        u = [pad[c, x + 1] for c in range(3)]
        k4 = 0.25 * k * (u[0] + u[1] + u[2])
        out = []
        for c in range(3):
            down, up = yshift(u[c], side[0, c, pl.ds(x, 1), :], side[1, c, pl.ds(x, 1), :])
            a = dg[x] * u[c] + k4
            a = a - (kx[x] * pad[c, x] + kx[x + 1] * pad[c, x + 2])
            a = a - (kym[x] * down + kyp[x] * up)
            a = a - (kzm[x] * pltpu.roll(u[c], 1, 1) + kzp[x] * pltpu.roll(u[c], Z - 1, 1))
            out.append(a)
        return u, out

    gather_wait(0, ag_recv)
    halo_wait(1)
    tiles = coarse_vector(0)
    q = answers(tiles, c_v)
    qs = [answers(tiles, c_in.at[d]) for d in range(4)]

    def add_spread(x, _):
        s = spread(reg_v[x], q)
        for c in range(3):
            z = z_p[c, x + 1] + s[c]
            z_p[c, x + 1] = z
            z0_v[c, x] = z
        return 0

    looped(0, X, add_spread, 0)
    halo_wait(2)
    edges(0, qs, z_p, zy)

    def dots(a, b):
        return fold(a[0] * b[0] + a[1] * b[1] + a[2] * b[2])

    def first(x, carry):
        u, a = operate(z_p, zy, x)
        r = [r_v[c, x] for c in range(3)]
        w = []
        for c in range(3):
            y_v[c, x] = a[c]
            w.append(a[c] * invd[x])
            v_p[c, x + 1] = w[c]
        save_faces(1, x, w)
        acc = add_rc(carry[:ncr], reg_v[x], a)
        return acc + (carry[ncr] + dots(r, u), carry[ncr + 1] + dots(a, u))

    acc = looped(0, X, first, zero_acc(ncr + 2))
    make_row(1, acc, 0)
    gather_start(1)
    for c in range(3):
        wx_send[1, 0, c] = v_p[c, 1]
        wx_send[1, 1, c] = v_p[c, X]
    halo_start(3)
    halo_wait(3)
    gather_wait(1, ag_recv)
    tiles = coarse_vector(1)
    q = answers(tiles, c_v)
    qs = [answers(tiles, c_in.at[d]) for d in range(4)]
    rz0 = total(1, 0)
    alpha0 = rz0 / total(1, 1)

    def add_spread_v(x, _):
        s = spread(reg_v[x], q)
        for c in range(3):
            v_p[c, x + 1] = v_p[c, x + 1] + s[c]
        return 0

    looped(0, X, add_spread_v, 0)
    edges(1, qs, v_p, vy)

    def second(x, carry):
        u, a = operate(v_p, vy, x)
        r, z, az = [], [], []
        for c in range(3):
            y = y_v[c, x]
            r.append(r_v[c, x] - alpha0 * y)
            z.append(z_p[c, x + 1] - alpha0 * u[c])
            az.append(y - alpha0 * a[c])
            r_v[c, x] = r[c]
            z1_v[c, x] = z[c]
            az_v[c, x] = az[c]
        return (carry[0] + dots(r, z), carry[1] + dots(az, z))

    acc = looped(0, X, second, zero_acc(2))
    make_row(2, acc, ncr)
    gather_start(2)
    gather_wait(2, ag_recv)
    rz1 = total(2, 0)
    beta = rz1 / rz0
    alpha1 = rz1 / (total(2, 1) - beta * rz1 / alpha0)
    along = alpha0 + alpha1 * beta
    a1b = alpha1 * beta

    sc_v[0:1, :] = jnp.broadcast_to(along, (1, LANES))
    sc_v[1:2, :] = jnp.broadcast_to(alpha1, (1, LANES))
    sc_v[2:3, :] = jnp.broadcast_to(a1b, (1, LANES))
    for kind in range(4):
        halo_done(kind)
    for p in range(3):
        gather_wait(p, ag_send)


def finish_wide(z0_v, z1_v, r_v, az_v, y_v, sc_v, x_out, res_out, xb, rb, sem):
    along = sc_v[0:1, 0:1]
    alpha1 = sc_v[1:2, 0:1]
    a1b = sc_v[2:3, 0:1]
    X = z0_v.shape[1]
    copies = []
    for c in range(3):
        for x in range(X):
            xb[c, x] = along * z0_v[c, x] + alpha1 * z1_v[c, x]
            rb[c, x] = r_v[c, x] - alpha1 * az_v[c, x] - a1b * y_v[c, x]
        for n, (src, dst) in enumerate(((xb, x_out), (rb, res_out))):
            copies.append(pltpu.make_async_copy(src.at[c], dst.at[c], sem.at[n, c]))
            copies[-1].start()
    for copy in copies:
        copy.wait()


def local_wide(nw, nn, right_side, occupancy, region, coarse_inverse):
    _, X, Y, Z = right_side.shape
    ncr, NC = coarse_inverse.shape
    ND = nw * nn
    f32, i32 = jnp.float32, jnp.int32
    V = pltpu.VMEM
    field, pad, scal = (3, X, Y, Z), (3, X + 2, Y, Z), (X, Y, Z)
    scratch = [
        V(scal, i32), V(scal, i32), V((ncr, NC), f32),
        V((X + 2, Y, Z), f32), V((X + 1, Y, Z), f32),
        V(scal, f32), V(scal, f32), V(scal, f32), V(scal, f32), V(scal, f32), V(scal, f32),
        V(pad, f32), V(pad, f32),
        V((2, 3, X, Z), f32), V((2, 3, X, Z), f32),
        V((2, 2, Y, Z), i32), V((2, 2, X, Z), i32), V((2, 2, X, Z), i32),
        V((4, ncr, NC), f32),
        V((2, 2, 3, Y, Z), f32), V((2, 2, 3, Y, Z), f32),
        V((2, 2, 3, X, Z), f32), V((2, 2, 3, X, Z), f32),
        V((3, SUB, LANES), f32), V((3, ND, LANES), f32),
        pltpu.SemaphoreType.DMA((4,)),
        pltpu.SemaphoreType.DMA((5, 4)), pltpu.SemaphoreType.DMA((5, 4)),
        pltpu.SemaphoreType.DMA((3,)), pltpu.SemaphoreType.DMA((3,)),
    ]
    parts = pl.pallas_call(
        functools.partial(kernel_wide, nw, nn),
        out_shape=(V(field, f32),) * 5 + (V((SUB, LANES), f32),),
        in_specs=[pl.BlockSpec(memory_space=pltpu.HBM)] * 4,
        out_specs=(pl.BlockSpec(memory_space=pltpu.VMEM),) * 6,
        scratch_shapes=scratch,
        compiler_params=pltpu.CompilerParams(collective_id=0, has_side_effects=True, vmem_limit_bytes=32 * 1024 * 1024),
    )(*[pltpu.with_memory_space_constraint(a, pltpu.HBM) for a in (right_side, occupancy, region, coarse_inverse)])
    return pl.pallas_call(
        finish_wide,
        out_shape=(jax.ShapeDtypeStruct(field, f32),) * 2,
        in_specs=[pl.BlockSpec(memory_space=pltpu.VMEM)] * 6,
        out_specs=(pl.BlockSpec(memory_space=pltpu.HBM),) * 2,
        scratch_shapes=[V(field, f32), V(field, f32), pltpu.SemaphoreType.DMA((2, 3))],
        compiler_params=pltpu.CompilerParams(vmem_limit_bytes=16 * 1024 * 1024),
    )(*parts)


REPLICATED_BYTES = 4 * 1024 * 1024
DEEP = 3
AROUND = ((-1, 0), (1, 0), (0, -1), (0, 1), (-1, -1), (-1, 1), (1, -1), (1, 1))
BACK = tuple(AROUND.index((-a, -b)) for a, b in AROUND)


def group_of(n):
    return max(d for d in range(1, n + 1) if n % d == 0 and d * d <= n)


def spread_over(reg, q, G):
    masks = [reg == g for g in range(G)]
    out = []
    for c in range(3):
        s = jnp.zeros(reg.shape, jnp.float32)
        for g in range(G):
            s = jnp.where(masks[g], q[g * 3 + c], s)
        out.append(s)
    return out


def stencil(u, prev, after, faces, x, rows):
    kx, kym, kyp, kzm, kzp = faces
    YE, Z = u.shape
    low, high = pltpu.roll(u, 1, 0)[0:rows], pltpu.roll(u, YE - 1, 0)[0:rows]
    v = u[0:rows]
    a = kx[x, 0:rows] * prev[0:rows] + kx[x + 1, 0:rows] * after[0:rows]
    a = a + (kym[x, 0:rows] * low + kyp[x, 0:rows] * high)
    return a + (kzm[x, 0:rows] * pltpu.roll(v, 1, 1) + kzp[x, 0:rows] * pltpu.roll(v, Z - 1, 1))


def kernel(nw, nn, r_hbm, occ_hbm, reg_hbm, ci_hbm,
           z_o, g_o, r_o, y_o, ag_o, reg_o, k4, dg, kx, kym, kyp, kzm, kzp, q_o, sc_o,
           occ_e, reg_e, r_e, k_e, invd, z_e, g_e,
           call, c_in, qpair, row_send, rows, ac_send, ac,
           load_sem, hs_send, hs_recv, hc_send, hc_recv, ag_send, ag_recv, cs_send, cs_recv, ready):
    E, YE, Z = occ_e.shape
    X, Y = E - 2 * DEEP, YE - SUB
    ncr, NC = c_in.shape[1:]
    G = ncr // 3
    ND = nw * nn
    NH = ND // 2
    wi = lax.axis_index("wide")
    ni = lax.axis_index("narrow")
    me = wi * nn + ni
    half, slot = lax.rem(wi, 2), (wi // 2) * nn + ni
    f32 = jnp.float32
    GP = group_of(nw) * nn
    NG = ND // GP
    grp, pos = me // GP, lax.rem(me, GP)
    own = pl.ds(DEEP, X)

    loads = [pltpu.make_async_copy(s, d, load_sem.at[i]) for i, (s, d) in enumerate((
        (reg_hbm, reg_e.at[own, pl.ds(0, Y)]), (r_hbm, r_e.at[:, own, pl.ds(0, Y)]),
        (occ_hbm, occ_e.at[own, pl.ds(0, Y)]), (ci_hbm, call.at[half, slot])))]
    for l in loads:
        l.start()

    barrier = pltpu.get_barrier_semaphore()

    def at(t):
        return (t // nn, lax.rem(t, nn))

    def wait_for(sem, count):
        @pl.when(count > 0)
        def _():
            pl.semaphore_wait(sem, count)

    def greet(t, _):
        pl.semaphore_signal(barrier, inc=1, device_id=at(t), device_id_type=MESH)
        return 0

    lax.fori_loop(me + 1, ND, greet, 0)

    def kind_of(low, high):
        apart = high // GP - low // GP
        k = jnp.where(lax.rem(high, GP) == lax.rem(low, GP), apart, NG + 1)
        aside = lax.rem(high, nn) - lax.rem(low, nn)
        touch = jnp.logical_and(high // nn - low // nn == 1, jnp.logical_and(aside >= -1, aside <= 1))
        k = jnp.where(touch, NG, k)
        return jnp.where(apart == 0, 0, k)

    def tell(i, _):
        t = me - 1 - i
        pl.semaphore_signal(ready.at[kind_of(t, me)], inc=1, device_id=at(t), device_id_type=MESH)
        return 0

    has = []
    for a, b in AROUND:
        h = jnp.logical_and(wi + a >= 0, wi + a < nw)
        has.append(jnp.logical_and(h, jnp.logical_and(ni + b >= 0, ni + b < nn)))

    def part(arr, d, into):
        a, b = AROUND[d]
        deep = {0: DEEP, 1: 2, 2: 2}[arr] if a == 0 or b == 0 else {0: 2, 1: 1, 2: 1}[arr]
        if into:
            xs = {-1: (DEEP - deep, deep), 0: (DEEP, X), 1: (DEEP + X, deep)}[a]
            ys = {-1: (YE - deep, deep), 0: (0, Y), 1: (Y, deep)}[b]
        else:
            xs = {-1: (DEEP, deep), 0: (DEEP, X), 1: (DEEP + X - deep, deep)}[a]
            ys = {-1: (0, deep), 0: (0, Y), 1: (Y - deep, deep)}[b]
        xs, ys = pl.ds(*xs), pl.ds(*ys)
        return (slice(None), xs, ys) if arr == 2 else (xs, ys)

    fields = (occ_e, reg_e, r_e)
    for d in range(8):
        @pl.when(jnp.logical_not(has[d]))
        def _():
            for n, ref in enumerate(fields):
                where = part(n, d, True)
                v = ref[where]
                ref[where] = jnp.full(v.shape, (-1, -1, 0)[n], v.dtype)
            c_in[d] = jnp.zeros((ncr, NC), f32)

    wait_for(barrier, me)
    lax.fori_loop(0, me, tell, 0)

    def fold(a):
        return jnp.sum(a.reshape(a.shape[0] // SUB, SUB, Z), axis=0)

    def zero_acc(n):
        return tuple(jnp.zeros((SUB, Z), f32) for _ in range(n))

    def add_rc(acc, reg, u):
        out = list(acc)
        for g in range(G):
            m = reg == g
            for c in range(3):
                out[g * 3 + c] = acc[g * 3 + c] + fold(jnp.where(m, u[c], 0.0))
        return out

    base = (me * ncr) % LANES

    def column(acc):
        a = jnp.concatenate([jnp.sum(b, axis=0, keepdims=True) for b in acc], axis=0)
        return jnp.sum(a, axis=1, keepdims=True)

    def make_row(p, acc):
        col = column(acc)
        n = len(acc)
        k = lax.broadcasted_iota(jnp.int32, (n, LANES), 0)
        lane = lax.broadcasted_iota(jnp.int32, (n, LANES), 1)
        target = (base + k) & (LANES - 1)
        row = jnp.sum(jnp.where(lane == target, col, 0.0), axis=0, keepdims=True)
        row_send[p, 0:1, :] = row
        rows[p, pl.ds(me, 1), :] = row

    def row_to(p, t, sem):
        pltpu.make_async_remote_copy(
            src_ref=row_send.at[p, pl.ds(0, 1)], dst_ref=rows.at[p, pl.ds(me, 1)],
            send_sem=ag_send.at[sem], recv_sem=ag_recv.at[sem],
            device_id=at(t), device_id_type=MESH).start()

    def rows_wait(p, count, sem):
        if count:
            some = rows.at[p, pl.ds(0, count)]
            pltpu.make_async_copy(some, some, sem).wait()

    def by_group(count, sem):
        for n in range(NG):
            @pl.when(grp == n)
            def _():
                rows_wait(0, count(n), sem)

    def each_peer(send):
        def body(i, _):
            send(lax.rem(me + i, ND))
            return 0
        lax.fori_loop(1, ND, body, 0, unroll=ND <= 64)

    loads[0].wait()
    loads[1].wait()
    acc = looped(0, X, lambda x, a: tuple(add_rc(
        a, reg_e[x + DEEP, 0:Y], [r_e[c, x + DEEP, 0:Y] for c in range(3)])), zero_acc(ncr))
    make_row(0, acc)

    wait_for(ready.at[0], GP - 1 - pos)

    def inside(i, _):
        row_to(0, grp * GP + lax.rem(pos + i, GP), 0)
        return 0

    def below(i, _):
        row_to(0, grp * GP - 1 - i, 2)
        return 0

    lax.fori_loop(1, GP, inside, 0, unroll=GP <= 64)
    lax.fori_loop(0, grp * GP, below, 0)

    def halo(n, d):
        a, b = AROUND[d]
        e = BACK[d]
        return pltpu.make_async_remote_copy(
            src_ref=fields[n].at[part(n, d, False)], dst_ref=fields[n].at[part(n, e, True)],
            send_sem=hs_send.at[n, d], recv_sem=hs_recv.at[n, e],
            device_id=(wi + a, ni + b), device_id_type=MESH)

    def halo_c(d):
        a, b = AROUND[d]
        return pltpu.make_async_remote_copy(
            src_ref=call.at[half, slot], dst_ref=c_in.at[BACK[d]],
            send_sem=hc_send.at[d], recv_sem=hc_recv.at[BACK[d]],
            device_id=(wi + a, ni + b), device_id_type=MESH)

    def arrived(n, d):
        where = part(n, d, True)
        pltpu.make_async_remote_copy(
            src_ref=fields[n].at[where], dst_ref=fields[n].at[where],
            send_sem=hs_send.at[n, d], recv_sem=hs_recv.at[n, d],
            device_id=(wi, ni), device_id_type=MESH).wait_recv()

    beside = jnp.where(kind_of(me, me + nn) == NG, 1, 0)
    touching = jnp.where(wi < nw - 1, beside * (
        1 + jnp.where(ni > 0, 1, 0) + jnp.where(ni < nn - 1, 1, 0)), 0)
    loads[2].wait()
    wait_for(ready.at[NG], touching)
    for n in range(3):
        for d in range(8):
            @pl.when(has[d])
            def _():
                halo(n, d).start()
    loads[3].wait()
    for d in range(8):
        @pl.when(has[d])
        def _():
            halo_c(d).start()

    rows_wait(0, GP - 1, ag_recv.at[0])
    mine = rows.at[0, pl.ds(pl.multiple_of(grp * GP, GP), GP)]
    for k in range(1, NG):
        @pl.when(grp + k < NG)
        def _():
            if k * GP != nn:
                pl.semaphore_wait(ready.at[k], 1)
            pltpu.make_async_remote_copy(
                src_ref=mine, dst_ref=mine, send_sem=ag_send.at[1], recv_sem=ag_recv.at[1],
                device_id=at(me + k * GP), device_id_type=MESH).start()

    rest = ND - 1 - me - (GP - 1 - pos) - touching
    if GP != nn:
        rest = rest - (NG - 1 - grp)
    wait_for(ready.at[NG + 1], rest)

    def send_c(i, _):
        t = lax.rem(slot + i, NH)
        pltpu.make_async_remote_copy(
            src_ref=call.at[half, slot], dst_ref=call.at[half, slot],
            send_sem=cs_send.at[0], recv_sem=cs_recv.at[0],
            device_id=((t // nn) * 2 + half, lax.rem(t, nn)), device_id_type=MESH).start()
        return 0

    lax.fori_loop(1, NH, send_c, 0)

    for n in range(3):
        for d in range(8):
            @pl.when(has[d])
            def _():
                arrived(n, d)

    lane_id = lax.broadcasted_iota(jnp.int32, (YE, Z), 1)

    def stiffness(x, _):
        o = occ_e[x]
        k_e[x] = jnp.where(o < 0, 0.0, soft_stiff + (bone_stiff - soft_stiff) * o.astype(f32))
        return 0

    lax.fori_loop(0, E, stiffness, 0, unroll=True)

    def pairs(acc, first, second, value):
        out = list(acc)
        for g in range(G):
            t = jnp.where(second == g, value, 0.0)
            for h in range(G):
                out[h * G + g] = acc[h * G + g] + fold(jnp.where(first == h, t, 0.0))
        return out

    row8 = lax.broadcasted_iota(jnp.int32, (SUB, Z), 0)

    def coefficients(x):
        k = k_e[x]
        low, high = pltpu.roll(k, 1, 0), pltpu.roll(k, YE - 1, 0)
        back = jnp.where(lane_id == 0, 0.0, pltpu.roll(k, 1, 1))
        ahead = jnp.where(lane_id == Z - 1, 0.0, pltpu.roll(k, Z - 1, 1))
        xm = 0.5 * (k + k_e[x - 1])
        xp = 0.5 * (k + k_e[x + 1])
        ym = 0.5 * (k + low)
        yp = 0.5 * (k + high)
        zm = 0.5 * (k + back)
        zp = 0.5 * (k + ahead)
        diag = xm + xp + ym + yp + zm + zp + 0.5 * k
        inv = jnp.where(k > 0.0, 1.0 / diag, 0.0)
        zp = jnp.where(lane_id == Z - 1, 0.0, zp)
        kx[x] = xm
        kx[x + 1] = xp
        kym[x] = ym
        kyp[x] = yp
        kzm[x] = jnp.where(lane_id == 0, 0.0, zm)
        kzp[x] = zp
        d = diag - 0.25 * k
        dg[x] = d
        k4[x] = 0.25 * k
        invd[x] = inv
        reg_o[x] = reg_e[x]
        for c in range(3):
            z_e[c, x] = r_e[c, x] * inv
        return xp, yp, zp, d, 0.25 * k

    def edge_plane(x):
        coefficients(x)

    for x in (1, 2, DEEP + X, DEEP + X + 1):
        edge_plane(x)

    n2 = G * G

    def inner(i, carry):
        x = i + DEEP
        xp, yp, zp, d, kq = coefficients(x)
        reg = reg_e[x]
        r16 = reg[0:Y]
        up = pltpu.roll(reg, YE - 1, 0)
        inside_x = jnp.where(i < X - 1, xp[0:Y], 0.0)
        to_x = xp[0:Y] - inside_x
        last = yp[Y - SUB:Y]
        inside_y = jnp.concatenate([yp[0:Y - SUB], jnp.where(row8 == SUB - 1, 0.0, last)], axis=0)
        to_y = jnp.where(row8 == SUB - 1, last, 0.0)
        ahead = pltpu.roll(r16, Z - 1, 1)
        after = reg_e[x + 1, 0:Y]
        own_acc, x_acc, y_acc = list(carry[:n2]), list(carry[n2:2 * n2]), list(carry[2 * n2:3 * n2])
        sums = list(carry[3 * n2:])
        for g in range(G):
            t = jnp.where(after == g, inside_x, 0.0) + jnp.where(up[0:Y] == g, inside_y, 0.0)
            t = t + jnp.where(ahead == g, zp[0:Y], 0.0)
            for h in range(G):
                own_acc[h * G + g] = own_acc[h * G + g] + fold(jnp.where(r16 == h, t, 0.0))
            m = r16 == g
            sums[g] = sums[g] + fold(jnp.where(m, d[0:Y], 0.0))
            sums[G + g] = sums[G + g] + fold(jnp.where(m, kq[0:Y], 0.0))
        y_acc = pairs(y_acc, r16[Y - SUB:Y], up[Y - SUB:Y], to_y)
        return tuple(own_acc) + tuple(x_acc) + tuple(y_acc) + tuple(sums)

    acc = lax.fori_loop(0, X, inner, zero_acc(3 * n2 + 2 * G), unroll=2)
    top = DEEP + X - 1
    x_acc = pairs(zero_acc(n2), reg_e[top, 0:Y], reg_e[top + 1, 0:Y], kx[top + 1, 0:Y])
    cols = [column(acc[:n2]), column(x_acc), column(acc[2 * n2:3 * n2]), column(acc[3 * n2:])]

    lane = lax.broadcasted_iota(jnp.int32, (n2, LANES), 1)
    pair = lax.broadcasted_iota(jnp.int32, (n2, LANES), 0)
    at_pair = jnp.logical_and(lane >= 3 * pair, lane < 3 * pair + 3)

    def lanes_of(col, mask):
        return jnp.sum(jnp.where(mask, col, 0.0), axis=0, keepdims=True)

    lane_g = lax.broadcasted_iota(jnp.int32, (2 * G, LANES), 1)
    row_g = lax.broadcasted_iota(jnp.int32, (2 * G, LANES), 0)
    start = jnp.where(row_g < G, 3 * (G + 1) * row_g, 3 * n2 + 9 * (row_g - G))
    at_sum = jnp.logical_and(lane_g >= start, lane_g < start + jnp.where(row_g < G, 3, 9))
    ac_rows = (lanes_of(cols[0], at_pair) * -2.0 + lanes_of(cols[3], at_sum),
               lanes_of(cols[1], at_pair) * -2.0, lanes_of(cols[2], at_pair) * -2.0)
    for n in range(3):
        ac_send[n, 0:1, :] = ac_rows[n]
        ac[n, pl.ds(me, 1), :] = ac_rows[n]

    def send_ac(t):
        pltpu.make_async_remote_copy(
            src_ref=ac_send.at[:, pl.ds(0, 1)], dst_ref=ac.at[:, pl.ds(me, 1)],
            send_sem=ag_send.at[4], recv_sem=ag_recv.at[4],
            device_id=at(t), device_id_type=MESH).start()

    each_peer(send_ac)

    def coarse_vector(block):
        tiles = []
        for t in range(NC // LANES):
            lo = (LANES * t) // ncr // SUB * SUB
            hi = min(ND, -(-(-(-(LANES * (t + 1)) // ncr)) // SUB) * SUB)
            d = lax.broadcasted_iota(jnp.int32, (hi - lo, LANES), 0) + lo
            j = lax.broadcasted_iota(jnp.int32, (hi - lo, LANES), 1) + LANES * t
            m = (j >= d * ncr) & (j < d * ncr + ncr)
            tiles.append(jnp.sum(jnp.where(m, block[lo:hi, :], 0.0), axis=0, keepdims=True))
        return tiles

    def total(block, s):
        d = lax.broadcasted_iota(jnp.int32, (ND, LANES), 0)
        lane = lax.broadcasted_iota(jnp.int32, (ND, LANES), 1)
        m = lane == ((d * ncr + ncr + s) & (LANES - 1))
        v = jnp.sum(jnp.where(m, block, 0.0), axis=0, keepdims=True)
        return jnp.sum(v, axis=1, keepdims=True)

    def solve(tiles, block):
        s = block[:, 0:LANES] * tiles[0]
        for t in range(1, len(tiles)):
            s = s + block[:, t * LANES:(t + 1) * LANES] * tiles[t]
        return jnp.sum(s, axis=1, keepdims=True)

    def as_list(q):
        return [q[i:i + 1, :] for i in range(ncr)]

    by_group(lambda n: (NG - 1 - n) * GP, ag_recv.at[2])
    by_group(lambda n: n * GP, ag_recv.at[1])
    for d in range(8):
        @pl.when(has[d])
        def _():
            pltpu.make_async_remote_copy(
                src_ref=c_in.at[d], dst_ref=c_in.at[d], send_sem=hc_send.at[d], recv_sem=hc_recv.at[d],
                device_id=(wi, ni), device_id_type=MESH).wait_recv()
    tiles = coarse_vector(rows[0])
    q = as_list(solve(tiles, call[half, slot]))
    qn = [as_list(solve(tiles, c_in[d])) for d in range(8)]

    def either(hi, lo):
        return [jnp.where(row8 < SUB // 2, a, b) for a, b in zip(hi, lo)]

    def add_spread(x, q_in, q_out):
        s = spread_over(reg_e[x, 0:Y], q_in, G)
        t = spread_over(reg_e[x, Y:YE], q_out, G)
        for c in range(3):
            z_e[c, x, 0:Y] = z_e[c, x, 0:Y] + s[c]
            z_e[c, x, Y:YE] = z_e[c, x, Y:YE] + t[c]

    q_side = either(qn[3], qn[2])

    def spread_own(i, _):
        add_spread(i + DEEP, q, q_side)
        return 0

    looped(0, X, spread_own, 0)
    q_low, q_high = either(qn[5], qn[4]), either(qn[7], qn[6])
    for x in (1, 2):
        add_spread(x, qn[0], q_low)
    for x in (DEEP + X, DEEP + X + 1):
        add_spread(x, qn[1], q_high)

    faces = (kx, kym, kyp, kzm, kzp)

    def apply(ref, x, rows_):
        u = [ref[c, x] for c in range(3)]
        kk = k4[x, 0:rows_] * (u[0] + u[1] + u[2])[0:rows_]
        return u, [dg[x, 0:rows_] * u[c][0:rows_] + kk
                   - stencil(u[c], ref[c, x - 1], ref[c, x + 1], faces, x, rows_) for c in range(3)]

    def dots(a, b):
        return fold(a[0] * b[0] + a[1] * b[1] + a[2] * b[2])

    for x in (DEEP - 1, DEEP + X):
        _, a = apply(z_e, x, YE)
        for c in range(3):
            g_e[c, x] = a[c] * invd[x]

    def first(i, carry):
        x = i + DEEP
        u, a = apply(z_e, x, YE)
        w = []
        for c in range(3):
            w.append(a[c] * invd[x])
            g_e[c, x] = w[c]
        y = [a[c][0:Y] for c in range(3)]
        u = [u[c][0:Y] for c in range(3)]
        w = [w[c][0:Y] for c in range(3)]
        r = [r_e[c, x, 0:Y] for c in range(3)]
        for c in range(3):
            y_o[c, i] = y[c]
            z_o[c, i] = u[c]
            g_o[c, i] = w[c]
            r_o[c, i] = r[c]
        acc = add_rc(carry[:ncr], reg_e[x, 0:Y], y)
        return tuple(acc) + (carry[ncr] + dots(r, u), carry[ncr + 1] + dots(y, u), carry[ncr + 2] + dots(y, w))

    acc1 = lax.fori_loop(0, X, first, zero_acc(ncr + 3), unroll=4)

    def second(i, carry):
        x = i + DEEP
        w, a = apply(g_e, x, Y)
        for c in range(3):
            ag_o[c, i] = a[c]
        acc = add_rc(carry[:ncr], reg_e[x, 0:Y], a)
        return tuple(acc) + (carry[ncr] + dots([v[0:Y] for v in w], a),)

    acc2 = lax.fori_loop(0, X, second, zero_acc(ncr + 1), unroll=4)
    make_row(1, tuple(acc1) + (acc2[ncr],) + tuple(acc2[:ncr]))
    each_peer(lambda t: row_to(1, t, 3))

    others = call.at[half, pl.ds(0, NH - 1)]
    pltpu.make_async_copy(others, others, cs_recv.at[0]).wait()
    swap = pltpu.make_async_remote_copy(
        src_ref=call.at[half], dst_ref=call.at[half], send_sem=cs_send.at[1], recv_sem=cs_recv.at[1],
        device_id=(wi + 1 - 2 * half, ni), device_id_type=MESH)
    swap.start()
    some = ac.at[:, pl.ds(0, ND - 1)]
    pltpu.make_async_copy(some, some, ag_recv.at[4]).wait()
    swap.wait_recv()
    rows_wait(1, ND - 1, ag_recv.at[3])

    block = rows[1]
    b1 = coarse_vector(block)
    h1 = coarse_vector(pltpu.roll(block, LANES - ncr - 4, 1))
    rr = lax.broadcasted_iota(jnp.int32, (ncr, LANES), 0)
    ll = lax.broadcasted_iota(jnp.int32, (ncr, LANES), 1)
    m0, m1 = rr < 0, rr < 0
    for h in range(G):
        for g in range(G):
            for c in range(3):
                k = (h * G + g) * 3 + c
                m0 = jnp.logical_or(m0, (ll == k) & (rr == h * 3 + c))
                m1 = jnp.logical_or(m1, (ll == k) & (rr == g * 3 + c))
        for c in range(3):
            for e in range(3):
                k = 3 * n2 + h * 9 + c * 3 + e
                m0 = jnp.logical_or(m0, (ll == k) & (rr == h * 3 + c))
                m1 = jnp.logical_or(m1, (ll == k) & (rr == h * 3 + e))
    lines = [jnp.zeros((1, LANES), f32) for _ in b1]
    for w in range(nw):
        for n in range(nn):
            d = w * nn + n
            q1 = solve(b1, call[w % 2, (w // 2) * nn + n])
            qpair[0, d:d + 1, :] = jnp.sum(jnp.where(m0, q1, 0.0), axis=0, keepdims=True)
            qpair[1, d:d + 1, :] = jnp.sum(jnp.where(m1, q1, 0.0), axis=0, keepdims=True)
            for t in range(d * ncr // LANES, (d * ncr + ncr - 1) // LANES + 1):
                lines[t] = lines[t] + jnp.sum(jnp.where(ll + LANES * t == rr + d * ncr, q1, 0.0), axis=0, keepdims=True)
    first_q, second_q = qpair[0], qpair[1]
    dev = lax.broadcasted_iota(jnp.int32, (ND, LANES), 0)
    next_x = jnp.where(dev < ND - nn, pltpu.roll(second_q, ND - nn, 0), 0.0)
    next_y = jnp.where(dev < ND - 1, pltpu.roll(second_q, ND - 1, 0), 0.0)
    energy = jnp.sum(first_q * (ac[0] * second_q + ac[1] * next_x + ac[2] * next_y), axis=0, keepdims=True)
    for t in range(len(b1)):
        energy = energy + 2.0 * h1[t] * lines[t]
    yv = b1[0] * lines[0]
    for t in range(1, len(b1)):
        yv = yv + b1[t] * lines[t]
    yv = total(block, 2) + jnp.sum(yv, axis=1, keepdims=True)
    vav = total(block, 3) + jnp.sum(energy, axis=1, keepdims=True)
    rz0, zy = total(block, 0), total(block, 1)
    alpha0 = rz0 / zy
    rz1 = alpha0 * alpha0 * yv - rz0
    zaz = zy - 2.0 * alpha0 * yv + alpha0 * alpha0 * vav
    beta = rz1 / rz0
    alpha1 = rz1 / (zaz - beta * rz1 / alpha0)
    a1b = alpha1 * beta
    for n, v in enumerate((alpha0 + a1b + alpha1, alpha1 * alpha0)):
        sc_o[n:n + 1, :] = jnp.broadcast_to(v, (1, LANES))
    q_o[0] = jnp.broadcast_to(solve(b1, call[half, slot]), (ncr, LANES))
    for d in range(4):
        q_o[d + 1] = jnp.broadcast_to(solve(b1, c_in[d]), (ncr, LANES))

    rows_wait(0, GP - 1, ag_send.at[0])
    by_group(lambda n: n * GP, ag_send.at[2])
    by_group(lambda n: (NG - 1 - n) * GP, ag_send.at[1])
    rows_wait(1, ND - 1, ag_send.at[3])
    pltpu.make_async_copy(some, some, ag_send.at[4]).wait()
    pltpu.make_async_copy(others, others, cs_send.at[0]).wait()
    swap.wait_send()
    for d in range(8):
        @pl.when(has[d])
        def _():
            for n in range(3):
                halo(n, d).wait_send()
            halo_c(d).wait_send()


def finish(z_v, g_v, r_v, y_v, ag_v, reg_v, k4, dg, kx, kym, kyp, kzm, kzp, q_v, sc_v, x_out, res_out, s_e, xb, rb, sem):
    a, b = sc_v[0:1, 0:1], sc_v[1:2, 0:1]
    E, YE, Z = reg_v.shape
    X, Y = E - 2 * DEEP, YE - SUB
    G = q_v.shape[1] // 3
    row8 = lax.broadcasted_iota(jnp.int32, (SUB, Z), 0)
    q = [[q_v[d, i:i + 1, :] for i in range(3 * G)] for d in range(5)]
    side = [jnp.where(row8 < SUB // 2, hi, lo) for hi, lo in zip(q[4], q[3])]

    def fill(x, q_in):
        s = spread_over(reg_v[x, 0:Y], q_in, G)
        t = spread_over(reg_v[x, Y:YE], side, G)
        for c in range(3):
            s_e[c, x, 0:Y] = s[c]
            s_e[c, x, Y:YE] = t[c]

    def fill_own(i, _):
        fill(i + DEEP, q[0])
        return 0

    fill(DEEP - 1, q[1])
    fill(DEEP + X, q[2])
    looped(0, X, fill_own, 0)
    faces = (kx, kym, kyp, kzm, kzp)
    copies = []
    parts = 4
    step = X // parts

    def plane(i, _):
        x = i + DEEP
        u = [s_e[c, x] for c in range(3)]
        kk = k4[x, 0:Y] * (u[0] + u[1] + u[2])[0:Y]
        for c in range(3):
            av = ag_v[c, i] + (dg[x, 0:Y] * u[c][0:Y] + kk
                               - stencil(u[c], s_e[c, x - 1], s_e[c, x + 1], faces, x, Y))
            xb[c, i] = a * z_v[c, i] - b * (g_v[c, i] + u[c][0:Y])
            rb[c, i] = r_v[c, i] - a * y_v[c, i] + b * av
        return 0

    for n in range(parts):
        lax.fori_loop(n * step, (n + 1) * step, plane, 0, unroll=True)
        for m, (src, dst) in enumerate(((xb, x_out), (rb, res_out))):
            where = (slice(None), pl.ds(n * step, step))
            copies.append(pltpu.make_async_copy(src.at[where], dst.at[where], sem.at[m, n]))
            copies[-1].start()
    for copy in copies:
        copy.wait()


def local_fast(nw, nn, right_side, occupancy, region, coarse_inverse):
    _, X, Y, Z = right_side.shape
    ncr, NC = coarse_inverse.shape
    ND = nw * nn
    f32, i32 = jnp.float32, jnp.int32
    V = pltpu.VMEM
    E, YE = X + 2 * DEEP, Y + SUB
    field, ext, scal = (3, X, Y, Z), (3, E, YE, Z), (E, YE, Z)
    ng = nw // group_of(nw)
    DMA = pltpu.SemaphoreType.DMA
    scratch = [
        V(scal, i32), V(scal, i32), V(ext, f32), V(scal, f32), V(scal, f32), V(ext, f32), V(ext, f32),
        V((2, ND // 2, ncr, NC), f32), V((8, ncr, NC), f32), V((2, ND, LANES), f32),
        V((2, SUB, LANES), f32), V((2, ND, LANES), f32), V((3, SUB, LANES), f32), V((3, ND, LANES), f32),
        DMA((4,)), DMA((3, 8)), DMA((3, 8)), DMA((8,)), DMA((8,)), DMA((5,)), DMA((5,)), DMA((2,)), DMA((2,)),
        pltpu.SemaphoreType.REGULAR((ng + 2,)),
    ]
    outs = (V(field, f32),) * 5 + (V(scal, i32),) + (V(scal, f32),) * 7 + (V((5, ncr, LANES), f32), V((SUB, LANES), f32))
    parts = pl.pallas_call(
        functools.partial(kernel, nw, nn),
        out_shape=outs,
        in_specs=[pl.BlockSpec(memory_space=pltpu.HBM)] * 4,
        out_specs=(pl.BlockSpec(memory_space=pltpu.VMEM),) * len(outs),
        scratch_shapes=scratch,
        compiler_params=pltpu.CompilerParams(collective_id=0, has_side_effects=True, vmem_limit_bytes=32 * 1024 * 1024),
    )(*[pltpu.with_memory_space_constraint(a, pltpu.HBM) for a in (right_side, occupancy, region, coarse_inverse)])
    return pl.pallas_call(
        finish,
        out_shape=(jax.ShapeDtypeStruct(field, f32),) * 2,
        in_specs=[pl.BlockSpec(memory_space=pltpu.VMEM)] * len(outs),
        out_specs=(pl.BlockSpec(memory_space=pltpu.HBM),) * 2,
        scratch_shapes=[V(ext, f32), V(field, f32), V(field, f32), DMA((2, 4))],
        compiler_params=pltpu.CompilerParams(vmem_limit_bytes=24 * 1024 * 1024),
    )(*parts)


def local(nw, nn, right_side, occupancy, region, coarse_inverse):
    nc = coarse_inverse.shape[1]
    run = local_fast if nw % 2 == 0 and nc * nc * 4 <= REPLICATED_BYTES else local_wide
    return run(nw, nn, right_side, occupancy, region, coarse_inverse)


def solution(mesh):
    return jax.shard_map(
        functools.partial(local, mesh.shape["wide"], mesh.shape["narrow"]),
        mesh=mesh,
        in_specs=(
            P(None, "wide", "narrow", None),
            P("wide", "narrow", None),
            P("wide", "narrow", None),
            P(("wide", "narrow"), None),
        ),
        out_specs=(P(None, "wide", "narrow", None), P(None, "wide", "narrow", None)),
        check_vma=False,
    )
```

```python
import functools

import jax
import jax.numpy as jnp
from jax import lax
from jax.experimental import pallas as pl
from jax.experimental.pallas import tpu as pltpu
from jax.sharding import PartitionSpec as P

LANES = 128
SUB = 8
UNROLL = 16
looped = functools.partial(lax.fori_loop, unroll=UNROLL)
MESH = pl.DeviceIdType.MESH
bone_stiff = 1.0
soft_stiff = 0.1


def kernel_wide(nw, nn, r_hbm, occ_hbm, reg_hbm, ci_hbm,
           z0_v, z1_v, r_v, az_v, y_v, sc_v,
            occ_v, reg_v, c_v, k_p, kx, kym, kyp, kzm, kzp, dg, invd,
           z_p, v_p, zy, vy,
           ix_in, iy_send, iy_in, c_in, wx_send, wx_in, wy_send, wy_in,
           row_send, rows, load_sem, hs_send, hs_recv, ag_send, ag_recv):
    X, Y, Z = occ_v.shape
    ncr, NC = c_v.shape
    G = ncr // 3
    ND = nw * nn
    wi = lax.axis_index("wide")
    ni = lax.axis_index("narrow")
    me = wi * nn + ni
    f32 = jnp.float32

    loads = [pltpu.make_async_copy(s, d, load_sem.at[i]) for i, (s, d) in enumerate(
        ((occ_hbm, occ_v), (reg_hbm, reg_v), (r_hbm, r_v), (ci_hbm, c_v)))]
    for l in loads:
        l.start()

    def peer(i):
        t = lax.rem(me + i, ND)
        return (t // nn, lax.rem(t, nn))

    barrier = pltpu.get_barrier_semaphore()

    def greet(i, _):
        pl.semaphore_signal(barrier, inc=1, device_id=peer(i), device_id_type=MESH)
        return 0

    lax.fori_loop(1, ND, greet, 0, unroll=ND <= 64)

    has = (wi > 0, wi < nw - 1, ni > 0, ni < nn - 1)
    to = ((wi - 1, ni), (wi + 1, ni), (wi, ni - 1), (wi, ni + 1))

    for d in range(4):
        @pl.when(jnp.logical_not(has[d]))
        def _():
            c_in[d] = jnp.zeros((ncr, NC), f32)
            for p in range(2):
                if d < 2:
                    wx_in[p, d] = jnp.zeros((3, Y, Z), f32)
                else:
                    wy_in[p, d - 2] = jnp.zeros((3, X, Z), f32)
            if d < 2:
                ix_in[d] = jnp.zeros((2, Y, Z), jnp.int32)
            else:
                iy_in[d - 2] = jnp.zeros((2, X, Z), jnp.int32)

    loads[0].wait()
    loads[1].wait()

    def pack_ints(x, _):
        iy_send[0, 0, pl.ds(x, 1), :] = occ_v[x, 0:1, :]
        iy_send[1, 0, pl.ds(x, 1), :] = occ_v[x, Y - 1:Y, :]
        iy_send[0, 1, pl.ds(x, 1), :] = reg_v[x, 0:1, :]
        iy_send[1, 1, pl.ds(x, 1), :] = reg_v[x, Y - 1:Y, :]
        return 0

    looped(0, X, pack_ints, 0)

    def fold(a):
        return jnp.sum(a.reshape(Y // SUB, SUB, Z), axis=0)

    def zero_acc(n):
        return tuple(jnp.zeros((SUB, Z), f32) for _ in range(n))

    def add_rc(acc, reg, u):
        out = list(acc)
        for g in range(G):
            m = reg == g
            for c in range(3):
                out[g * 3 + c] = acc[g * 3 + c] + fold(jnp.where(m, u[c], 0.0))
        return tuple(out)

    base = (me * ncr) % LANES

    def make_row(p, acc, first):
        a = jnp.concatenate([jnp.sum(b, axis=0, keepdims=True) for b in acc], axis=0)
        col = jnp.sum(a, axis=1, keepdims=True)
        n = len(acc)
        k = lax.broadcasted_iota(jnp.int32, (n, LANES), 0)
        lane = lax.broadcasted_iota(jnp.int32, (n, LANES), 1)
        target = (base + first + k) & (LANES - 1)
        row = jnp.sum(jnp.where(lane == target, col, 0.0), axis=0, keepdims=True)
        row_send[p, 0:1, :] = row
        rows[p, pl.ds(me, 1), :] = row

    def gather_start(p):
        def send(i, _):
            pltpu.make_async_remote_copy(
                src_ref=row_send.at[p, pl.ds(0, 1)], dst_ref=rows.at[p, pl.ds(me, 1)],
                send_sem=ag_send.at[p], recv_sem=ag_recv.at[p],
                device_id=peer(i), device_id_type=MESH).start()
            return 0
        lax.fori_loop(1, ND, send, 0, unroll=ND <= 64)

    def gather_wait(p, sem):
        part = rows.at[p, pl.ds(0, ND - 1)]
        pltpu.make_async_copy(part, part, sem.at[p]).wait()

    def coarse_vector(p):
        tiles = []
        for t in range(NC // LANES):
            lo = (LANES * t) // ncr // SUB * SUB
            hi = min(ND, -(-(-(-(LANES * (t + 1)) // ncr)) // SUB) * SUB)
            d = lax.broadcasted_iota(jnp.int32, (hi - lo, LANES), 0) + lo
            j = lax.broadcasted_iota(jnp.int32, (hi - lo, LANES), 1) + LANES * t
            m = (j >= d * ncr) & (j < d * ncr + ncr)
            tiles.append(jnp.sum(jnp.where(m, rows[p, lo:hi, :], 0.0), axis=0, keepdims=True))
        return tiles

    def total(p, s):
        d = lax.broadcasted_iota(jnp.int32, (ND, LANES), 0)
        lane = lax.broadcasted_iota(jnp.int32, (ND, LANES), 1)
        m = lane == ((d * ncr + ncr + s) & (LANES - 1))
        v = jnp.sum(jnp.where(m, rows[p], 0.0), axis=0, keepdims=True)
        return jnp.sum(v, axis=1, keepdims=True)

    def answers(tiles, ref):
        s = ref[:, 0:LANES] * tiles[0]
        for t in range(1, len(tiles)):
            s = s + ref[:, t * LANES:(t + 1) * LANES] * tiles[t]
        q = jnp.sum(s, axis=1, keepdims=True)
        return [q[i:i + 1, :] for i in range(ncr)]

    def spread(reg, q):
        masks = [reg == g for g in range(G)]
        out = []
        for c in range(3):
            s = jnp.zeros(reg.shape, f32)
            for g in range(G):
                s = jnp.where(masks[g], q[g * 3 + c], s)
            out.append(s)
        return out

    def halo(slot, d, src, dst):
        return pltpu.make_async_remote_copy(
            src_ref=src, dst_ref=dst, send_sem=hs_send.at[slot, d],
            recv_sem=hs_recv.at[slot, d ^ 1], device_id=to[d], device_id_type=MESH)

    def copies(kind, d):
        e = d ^ 1
        if kind == 0:
            if d < 2:
                x = 0 if d == 0 else X - 1
                return [halo(0, d, occ_v.at[x], ix_in.at[e, 0]),
                        halo(1, d, reg_v.at[x], ix_in.at[e, 1])]
            return [halo(0, d, iy_send.at[d - 2, 0], iy_in.at[e - 2, 0]),
                    halo(1, d, iy_send.at[d - 2, 1], iy_in.at[e - 2, 1])]
        if kind == 1:
            return [halo(2, d, c_v, c_in.at[e])]
        p = kind - 2
        if d < 2:
            return [halo(3 + p, d, wx_send.at[p, d], wx_in.at[p, e])]
        return [halo(3 + p, d, wy_send.at[p, d - 2], wy_in.at[p, e - 2])]

    def halo_start(kind):
        for d in range(4):
            @pl.when(has[d])
            def _():
                for c in copies(kind, d):
                    c.start()

    def halo_wait(kind):
        for d in range(4):
            @pl.when(has[d])
            def _():
                for c in copies(kind, d ^ 1):
                    c.wait_recv()

    def halo_done(kind):
        for d in range(4):
            @pl.when(has[d])
            def _():
                for c in copies(kind, d):
                    c.wait_send()

    loads[2].wait()
    acc = looped(0, X, lambda x, a: add_rc(a, reg_v[x], [r_v[c, x] for c in range(3)]),
                        zero_acc(ncr))
    make_row(0, acc, 0)
    loads[3].wait()

    pl.semaphore_wait(barrier, ND - 1)
    halo_start(0)
    gather_start(0)
    halo_start(1)

    def stiff_of(o):
        return soft_stiff + (bone_stiff - soft_stiff) * o.astype(f32)

    def own_k(x, _):
        k_p[x + 1] = stiff_of(occ_v[x])
        return 0

    looped(0, X, own_k, 0)
    halo_wait(0)
    for d in range(2):
        @pl.when(has[d])
        def _():
            k_p[0 if d == 0 else X + 1] = stiff_of(ix_in[d, 0])

        @pl.when(jnp.logical_not(has[d]))
        def _():
            k_p[0 if d == 0 else X + 1] = jnp.zeros((Y, Z), f32)

    row_id = lax.broadcasted_iota(jnp.int32, (Y, Z), 0)
    lane_id = lax.broadcasted_iota(jnp.int32, (Y, Z), 1)
    side_lo = jnp.where(has[2], 1.0, 0.0).astype(f32)
    side_hi = jnp.where(has[3], 1.0, 0.0).astype(f32)

    def yshift(u, lo, hi):
        down = jnp.where(row_id == 0, lo, pltpu.roll(u, 1, 0))
        up = jnp.where(row_id == Y - 1, hi, pltpu.roll(u, Y - 1, 0))
        return down, up

    def save_faces(p, x, w):
        for c in range(3):
            wy_send[p, 0, c, pl.ds(x, 1), :] = w[c][0:1, :]
            wy_send[p, 1, c, pl.ds(x, 1), :] = w[c][Y - 1:Y, :]

    def coefficients(x, _):
        k = k_p[x + 1]
        lo = stiff_of(iy_in[0, 0, pl.ds(x, 1), :]) * side_lo
        hi = stiff_of(iy_in[1, 0, pl.ds(x, 1), :]) * side_hi
        down, up = yshift(k, lo, hi)
        back = jnp.where(lane_id == 0, 0.0, pltpu.roll(k, 1, 1))
        ahead = jnp.where(lane_id == Z - 1, 0.0, pltpu.roll(k, Z - 1, 1))
        xm = 0.5 * (k + k_p[x])
        xp = 0.5 * (k + k_p[x + 2])
        ym = 0.5 * (k + down)
        yp = 0.5 * (k + up)
        zm = 0.5 * (k + back)
        zp = 0.5 * (k + ahead)
        diag = xm + xp + ym + yp + zm + zp + 0.5 * k
        inv = 1.0 / diag
        kx[x] = xm
        kx[x + 1] = xp
        kym[x] = ym
        kyp[x] = yp
        kzm[x] = jnp.where(lane_id == 0, 0.0, zm)
        kzp[x] = jnp.where(lane_id == Z - 1, 0.0, zp)
        dg[x] = diag - 0.25 * k
        invd[x] = inv
        w = [r_v[c, x] * inv for c in range(3)]
        for c in range(3):
            z_p[c, x + 1] = w[c]
        save_faces(0, x, w)
        return 0

    looped(0, X, coefficients, 0)
    for c in range(3):
        wx_send[0, 0, c] = z_p[c, 1]
        wx_send[0, 1, c] = z_p[c, X]
    halo_start(2)

    def edges(p, qs, pad, side):
        for d in range(2):
            s = spread(ix_in[d, 1], qs[d])
            for c in range(3):
                pad[c, 0 if d == 0 else X + 1] = wx_in[p, d, c] + s[c]
        for d in range(2):
            s = spread(iy_in[d, 1], qs[2 + d])
            for c in range(3):
                side[d, c] = wy_in[p, d, c] + s[c]

    def operate(pad, side, x):
        k = k_p[x + 1]
        u = [pad[c, x + 1] for c in range(3)]
        k4 = 0.25 * k * (u[0] + u[1] + u[2])
        out = []
        for c in range(3):
            down, up = yshift(u[c], side[0, c, pl.ds(x, 1), :], side[1, c, pl.ds(x, 1), :])
            a = dg[x] * u[c] + k4
            a = a - (kx[x] * pad[c, x] + kx[x + 1] * pad[c, x + 2])
            a = a - (kym[x] * down + kyp[x] * up)
            a = a - (kzm[x] * pltpu.roll(u[c], 1, 1) + kzp[x] * pltpu.roll(u[c], Z - 1, 1))
            out.append(a)
        return u, out

    gather_wait(0, ag_recv)
    halo_wait(1)
    tiles = coarse_vector(0)
    q = answers(tiles, c_v)
    qs = [answers(tiles, c_in.at[d]) for d in range(4)]

    def add_spread(x, _):
        s = spread(reg_v[x], q)
        for c in range(3):
            z = z_p[c, x + 1] + s[c]
            z_p[c, x + 1] = z
            z0_v[c, x] = z
        return 0

    looped(0, X, add_spread, 0)
    halo_wait(2)
    edges(0, qs, z_p, zy)

    def dots(a, b):
        return fold(a[0] * b[0] + a[1] * b[1] + a[2] * b[2])

    def first(x, carry):
        u, a = operate(z_p, zy, x)
        r = [r_v[c, x] for c in range(3)]
        w = []
        for c in range(3):
            y_v[c, x] = a[c]
            w.append(a[c] * invd[x])
            v_p[c, x + 1] = w[c]
        save_faces(1, x, w)
        acc = add_rc(carry[:ncr], reg_v[x], a)
        return acc + (carry[ncr] + dots(r, u), carry[ncr + 1] + dots(a, u))

    acc = looped(0, X, first, zero_acc(ncr + 2))
    make_row(1, acc, 0)
    gather_start(1)
    for c in range(3):
        wx_send[1, 0, c] = v_p[c, 1]
        wx_send[1, 1, c] = v_p[c, X]
    halo_start(3)
    halo_wait(3)
    gather_wait(1, ag_recv)
    tiles = coarse_vector(1)
    q = answers(tiles, c_v)
    qs = [answers(tiles, c_in.at[d]) for d in range(4)]
    rz0 = total(1, 0)
    alpha0 = rz0 / total(1, 1)

    def add_spread_v(x, _):
        s = spread(reg_v[x], q)
        for c in range(3):
            v_p[c, x + 1] = v_p[c, x + 1] + s[c]
        return 0

    looped(0, X, add_spread_v, 0)
    edges(1, qs, v_p, vy)

    def second(x, carry):
        u, a = operate(v_p, vy, x)
        r, z, az = [], [], []
        for c in range(3):
            y = y_v[c, x]
            r.append(r_v[c, x] - alpha0 * y)
            z.append(z_p[c, x + 1] - alpha0 * u[c])
            az.append(y - alpha0 * a[c])
            r_v[c, x] = r[c]
            z1_v[c, x] = z[c]
            az_v[c, x] = az[c]
        return (carry[0] + dots(r, z), carry[1] + dots(az, z))

    acc = looped(0, X, second, zero_acc(2))
    make_row(2, acc, ncr)
    gather_start(2)
    gather_wait(2, ag_recv)
    rz1 = total(2, 0)
    beta = rz1 / rz0
    alpha1 = rz1 / (total(2, 1) - beta * rz1 / alpha0)
    along = alpha0 + alpha1 * beta
    a1b = alpha1 * beta

    sc_v[0:1, :] = jnp.broadcast_to(along, (1, LANES))
    sc_v[1:2, :] = jnp.broadcast_to(alpha1, (1, LANES))
    sc_v[2:3, :] = jnp.broadcast_to(a1b, (1, LANES))
    for kind in range(4):
        halo_done(kind)
    for p in range(3):
        gather_wait(p, ag_send)


def finish_wide(z0_v, z1_v, r_v, az_v, y_v, sc_v, x_out, res_out, xb, rb, sem):
    along = sc_v[0:1, 0:1]
    alpha1 = sc_v[1:2, 0:1]
    a1b = sc_v[2:3, 0:1]
    X = z0_v.shape[1]
    copies = []
    for c in range(3):
        for x in range(X):
            xb[c, x] = along * z0_v[c, x] + alpha1 * z1_v[c, x]
            rb[c, x] = r_v[c, x] - alpha1 * az_v[c, x] - a1b * y_v[c, x]
        for n, (src, dst) in enumerate(((xb, x_out), (rb, res_out))):
            copies.append(pltpu.make_async_copy(src.at[c], dst.at[c], sem.at[n, c]))
            copies[-1].start()
    for copy in copies:
        copy.wait()


def local_wide(nw, nn, right_side, occupancy, region, coarse_inverse):
    _, X, Y, Z = right_side.shape
    ncr, NC = coarse_inverse.shape
    ND = nw * nn
    f32, i32 = jnp.float32, jnp.int32
    V = pltpu.VMEM
    field, pad, scal = (3, X, Y, Z), (3, X + 2, Y, Z), (X, Y, Z)
    scratch = [
        V(scal, i32), V(scal, i32), V((ncr, NC), f32),
        V((X + 2, Y, Z), f32), V((X + 1, Y, Z), f32),
        V(scal, f32), V(scal, f32), V(scal, f32), V(scal, f32), V(scal, f32), V(scal, f32),
        V(pad, f32), V(pad, f32),
        V((2, 3, X, Z), f32), V((2, 3, X, Z), f32),
        V((2, 2, Y, Z), i32), V((2, 2, X, Z), i32), V((2, 2, X, Z), i32),
        V((4, ncr, NC), f32),
        V((2, 2, 3, Y, Z), f32), V((2, 2, 3, Y, Z), f32),
        V((2, 2, 3, X, Z), f32), V((2, 2, 3, X, Z), f32),
        V((3, SUB, LANES), f32), V((3, ND, LANES), f32),
        pltpu.SemaphoreType.DMA((4,)),
        pltpu.SemaphoreType.DMA((5, 4)), pltpu.SemaphoreType.DMA((5, 4)),
        pltpu.SemaphoreType.DMA((3,)), pltpu.SemaphoreType.DMA((3,)),
    ]
    parts = pl.pallas_call(
        functools.partial(kernel_wide, nw, nn),
        out_shape=(V(field, f32),) * 5 + (V((SUB, LANES), f32),),
        in_specs=[pl.BlockSpec(memory_space=pltpu.HBM)] * 4,
        out_specs=(pl.BlockSpec(memory_space=pltpu.VMEM),) * 6,
        scratch_shapes=scratch,
        compiler_params=pltpu.CompilerParams(collective_id=0, has_side_effects=True, vmem_limit_bytes=32 * 1024 * 1024),
    )(*[pltpu.with_memory_space_constraint(a, pltpu.HBM) for a in (right_side, occupancy, region, coarse_inverse)])
    return pl.pallas_call(
        finish_wide,
        out_shape=(jax.ShapeDtypeStruct(field, f32),) * 2,
        in_specs=[pl.BlockSpec(memory_space=pltpu.VMEM)] * 6,
        out_specs=(pl.BlockSpec(memory_space=pltpu.HBM),) * 2,
        scratch_shapes=[V(field, f32), V(field, f32), pltpu.SemaphoreType.DMA((2, 3))],
        compiler_params=pltpu.CompilerParams(vmem_limit_bytes=16 * 1024 * 1024),
    )(*parts)


REPLICATED_BYTES = 4 * 1024 * 1024
DEEP = 3
AROUND = ((-1, 0), (1, 0), (0, -1), (0, 1), (-1, -1), (-1, 1), (1, -1), (1, 1))
BACK = tuple(AROUND.index((-a, -b)) for a, b in AROUND)


def group_of(n):
    return max(d for d in range(1, n + 1) if n % d == 0 and d * d <= n)


def spread_over(reg, q, G):
    masks = [reg == g for g in range(G)]
    out = []
    for c in range(3):
        s = jnp.zeros(reg.shape, jnp.float32)
        for g in range(G):
            s = jnp.where(masks[g], q[g * 3 + c], s)
        out.append(s)
    return out


def stencil(u, prev, after, faces, x, rows):
    kx, kym, kyp, kzm, kzp = faces
    YE, Z = u.shape
    low, high = pltpu.roll(u, 1, 0)[0:rows], pltpu.roll(u, YE - 1, 0)[0:rows]
    v = u[0:rows]
    a = kx[x, 0:rows] * prev[0:rows] + kx[x + 1, 0:rows] * after[0:rows]
    a = a + (kym[x, 0:rows] * low + kyp[x, 0:rows] * high)
    return a + (kzm[x, 0:rows] * pltpu.roll(v, 1, 1) + kzp[x, 0:rows] * pltpu.roll(v, Z - 1, 1))


def kernel(nw, nn, r_hbm, occ_hbm, reg_hbm, ci_hbm,
           z_o, g_o, r_o, y_o, ag_o, reg_o, k4, dg, kx, kym, kyp, kzm, kzp, q_o, sc_o,
           occ_e, reg_e, r_e, k_e, invd, z_e, g_e,
           call, c_in, y_face, y_label, qpair, row_send, rows, ac_send, ac,
           load_sem, hs_send, hs_recv, hc_send, hc_recv, ag_send, ag_recv, cs_send, cs_recv, ready):
    E, YE, Z = occ_e.shape
    X, Y = E - 2 * DEEP, YE - SUB
    ncr, NC = c_in.shape[1:]
    G = ncr // 3
    ND = nw * nn
    NH = ND // 2
    wi = lax.axis_index("wide")
    ni = lax.axis_index("narrow")
    me = wi * nn + ni
    f32 = jnp.float32
    GW = group_of(nw)
    GP = GW * nn
    NG = ND // GP
    grp, pos = me // GP, lax.rem(me, GP)
    half, place = lax.rem(wi, 2), (lax.rem(wi, GW) // 2) * nn + ni
    slot = place * NG + grp
    own = pl.ds(DEEP, X)

    loads = [pltpu.make_async_copy(s, d, load_sem.at[i]) for i, (s, d) in enumerate((
        (reg_hbm, reg_e.at[own, pl.ds(0, Y)]), (r_hbm, r_e.at[:, own, pl.ds(0, Y)]),
        (occ_hbm, occ_e.at[own, pl.ds(0, Y)]), (ci_hbm, call.at[half, slot])))]
    for l in loads:
        l.start()

    barrier = pltpu.get_barrier_semaphore()

    def at(t):
        return (t // nn, lax.rem(t, nn))

    def wait_for(sem, count):
        @pl.when(count > 0)
        def _():
            pl.semaphore_wait(sem, count)

    def column_of(group):
        return (wi + (group - grp) * GW, ni)

    at_low = jnp.logical_and(lax.rem(wi, GW) == 0, wi > 0)
    at_high = jnp.logical_and(lax.rem(wi, GW) == GW - 1, wi < nw - 1)
    aside = 1 + jnp.where(ni > 0, 1, 0) + jnp.where(ni < nn - 1, 1, 0)

    def touching(ahead, signal):
        @pl.when(at_high if ahead > 0 else at_low)
        def _():
            for b in (-1, 0, 1):
                @pl.when(jnp.logical_and(ni + b >= 0, ni + b < nn))
                def _():
                    signal((wi + ahead, ni + b))

    def say(sem):
        return lambda device: pl.semaphore_signal(sem, inc=1, device_id=device, device_id_type=MESH)

    for i in range(1, GP):
        @pl.when(pos + i < GP)
        def _():
            say(barrier)(at(me + i))
    touching(1, say(barrier))
    for k in range(1, NG):
        @pl.when(grp + k < NG)
        def _():
            say(barrier)(column_of(grp + k))

    def tell():
        for i in range(1, GP):
            @pl.when(pos >= i)
            def _():
                say(ready.at[0])(at(me - i))
        touching(-1, say(ready.at[NG]))
        for k in range(1, NG):
            @pl.when(grp >= k)
            def _():
                say(ready.at[k])(column_of(grp - k))

    has = []
    for a, b in AROUND:
        h = jnp.logical_and(wi + a >= 0, wi + a < nw)
        has.append(jnp.logical_and(h, jnp.logical_and(ni + b >= 0, ni + b < nn)))

    def part(arr, d, into):
        a, b = AROUND[d]
        deep = {0: DEEP, 1: 2, 2: 2}[arr] if a == 0 or b == 0 else {0: 2, 1: 1, 2: 1}[arr]
        if into:
            xs = {-1: (DEEP - deep, deep), 0: (DEEP, X), 1: (DEEP + X, deep)}[a]
            ys = {-1: (YE - deep, deep), 0: (0, Y), 1: (Y, deep)}[b]
        else:
            xs = {-1: (DEEP, deep), 0: (DEEP, X), 1: (DEEP + X - deep, deep)}[a]
            ys = {-1: (0, deep), 0: (0, Y), 1: (Y - deep, deep)}[b]
        xs, ys = pl.ds(*xs), pl.ds(*ys)
        return (slice(None), xs, ys) if arr == 2 else (xs, ys)

    fields = (occ_e, reg_e, r_e)
    for d in range(8):
        @pl.when(jnp.logical_not(has[d]))
        def _():
            for n, ref in enumerate(fields):
                where = part(n, d, True)
                v = ref[where]
                ref[where] = jnp.full(v.shape, (-1, -1, 0)[n], v.dtype)
            c_in[d] = jnp.zeros((ncr, NC), f32)

    wait_for(barrier, pos + grp + jnp.where(at_low, aside, 0))
    tell()

    def fold(a):
        return jnp.sum(a.reshape(a.shape[0] // SUB, SUB, Z), axis=0)

    def zero_acc(n):
        return tuple(jnp.zeros((SUB, Z), f32) for _ in range(n))

    def add_rc(acc, reg, u):
        out = list(acc)
        for g in range(G):
            m = reg == g
            for c in range(3):
                out[g * 3 + c] = acc[g * 3 + c] + fold(jnp.where(m, u[c], 0.0))
        return out

    base = (me * ncr) % LANES

    def column(acc):
        a = jnp.concatenate([jnp.sum(b, axis=0, keepdims=True) for b in acc], axis=0)
        return jnp.sum(a, axis=1, keepdims=True)

    def make_row(p, acc):
        col = column(acc)
        n = len(acc)
        k = lax.broadcasted_iota(jnp.int32, (n, LANES), 0)
        lane = lax.broadcasted_iota(jnp.int32, (n, LANES), 1)
        target = (base + k) & (LANES - 1)
        row = jnp.sum(jnp.where(lane == target, col, 0.0), axis=0, keepdims=True)
        row_send[p, 0:1, :] = row
        rows[p, pl.ds(me, 1), :] = row

    def row_to(p, t, sem):
        pltpu.make_async_remote_copy(
            src_ref=row_send.at[p, pl.ds(0, 1)], dst_ref=rows.at[p, pl.ds(me, 1)],
            send_sem=ag_send.at[sem], recv_sem=ag_recv.at[sem],
            device_id=at(t), device_id_type=MESH).start()

    def rows_wait(p, count, sem):
        if count:
            some = rows.at[p, pl.ds(0, count)]
            pltpu.make_async_copy(some, some, sem).wait()

    def each_peer(send):
        def body(i, _):
            send(lax.rem(me + i, ND))
            return 0
        lax.fori_loop(1, ND, body, 0, unroll=ND <= 64)

    loads[0].wait()
    loads[1].wait()
    acc = looped(0, X, lambda x, a: tuple(add_rc(
        a, reg_e[x + DEEP, 0:Y], [r_e[c, x + DEEP, 0:Y] for c in range(3)])), zero_acc(ncr))
    make_row(0, acc)

    wait_for(ready.at[0], GP - 1 - pos)

    def inside(i, _):
        row_to(0, grp * GP + lax.rem(pos + i, GP), 0)
        return 0

    lax.fori_loop(1, GP, inside, 0, unroll=GP <= 64)

    def halo(n, d):
        a, b = AROUND[d]
        e = BACK[d]
        return pltpu.make_async_remote_copy(
            src_ref=fields[n].at[part(n, d, False)], dst_ref=fields[n].at[part(n, e, True)],
            send_sem=hs_send.at[n, d], recv_sem=hs_recv.at[n, e],
            device_id=(wi + a, ni + b), device_id_type=MESH)

    def halo_c(d):
        a, b = AROUND[d]
        return pltpu.make_async_remote_copy(
            src_ref=call.at[half, slot], dst_ref=c_in.at[BACK[d]],
            send_sem=hc_send.at[d], recv_sem=hc_recv.at[BACK[d]],
            device_id=(wi + a, ni + b), device_id_type=MESH)

    def arrived(n, d):
        where = part(n, d, True)
        pltpu.make_async_remote_copy(
            src_ref=fields[n].at[where], dst_ref=fields[n].at[where],
            send_sem=hs_send.at[n, d], recv_sem=hs_recv.at[n, d],
            device_id=(wi, ni), device_id_type=MESH).wait_recv()

    loads[2].wait()
    wait_for(ready.at[NG], jnp.where(at_high, aside, 0))
    for n in range(3):
        for d in range(8):
            @pl.when(has[d])
            def _():
                halo(n, d).start()
    loads[3].wait()
    for d in range(8):
        @pl.when(has[d])
        def _():
            halo_c(d).start()

    def c_column(group):
        pltpu.make_async_remote_copy(
            src_ref=call.at[half, slot], dst_ref=call.at[half, slot],
            send_sem=cs_send.at[0], recv_sem=cs_recv.at[0],
            device_id=column_of(group), device_id_type=MESH).start()

    for k in range(1, NG):
        @pl.when(grp >= k)
        def _():
            c_column(grp - k)

    def stiff_of(o):
        return jnp.where(o < 0, 0.0, soft_stiff + (bone_stiff - soft_stiff) * o.astype(f32))

    n2 = G * G

    def pairs(acc, first, seconds):
        out = list(acc)
        for g in range(G):
            t = None
            for label, value in seconds:
                v = jnp.where(label == g, value, 0.0)
                t = v if t is None else t + v
            for h in range(G):
                out[h * G + g] = acc[h * G + g] + fold(jnp.where(first == h, t, 0.0))
        return out

    row16 = lax.broadcasted_iota(jnp.int32, (Y, Z), 0)
    lane16 = lax.broadcasted_iota(jnp.int32, (Y, Z), 1)

    def own_pairs(i, carry):
        x = i + DEEP
        k, reg = stiff_of(occ_e[x, 0:Y]), reg_e[x, 0:Y]
        later = jnp.minimum(i + 1, X - 1) + DEEP
        kx_in = jnp.where(i < X - 1, 0.5 * (k + stiff_of(occ_e[later, 0:Y])), 0.0)
        ky_in = jnp.where(row16 == Y - 1, 0.0, 0.5 * (k + pltpu.roll(k, Y - 1, 0)))
        kz_in = jnp.where(lane16 == Z - 1, 0.0, 0.5 * (k + pltpu.roll(k, Z - 1, 1)))
        acc = pairs(carry[:n2], reg, ((reg_e[later, 0:Y], kx_in), (pltpu.roll(reg, Y - 1, 0), ky_in),
                                      (pltpu.roll(reg, Z - 1, 1), kz_in)))
        sums = [carry[n2 + g] + fold(jnp.where(reg == g, 0.25 * k, 0.0)) for g in range(G)]
        return tuple(acc) + tuple(sums)

    own_acc = lax.fori_loop(0, X, own_pairs, zero_acc(n2 + G), unroll=2)
    own_col = column(own_acc)

    rows_wait(0, GP - 1, ag_recv.at[0])
    mine = rows.at[0, pl.ds(pl.multiple_of(grp * GP, GP), GP)]

    def across(group):
        pltpu.make_async_remote_copy(
            src_ref=mine, dst_ref=mine, send_sem=ag_send.at[1], recv_sem=ag_recv.at[1],
            device_id=column_of(group), device_id_type=MESH).start()

    for k in range(1, NG):
        @pl.when(grp >= k)
        def _():
            across(grp - k)

    for k in range(1, NG):
        @pl.when(grp + k < NG)
        def _():
            pl.semaphore_wait(ready.at[k], 1)
            across(grp + k)

    for k in range(1, NG):
        @pl.when(grp + k < NG)
        def _():
            c_column(grp + k)

    for d in range(8):
        @pl.when(has[d])
        def _():
            arrived(0, d)

    lane_id = lax.broadcasted_iota(jnp.int32, (YE, Z), 1)

    def stiffness(x, _):
        k_e[x] = stiff_of(occ_e[x])
        return 0

    lax.fori_loop(0, E, stiffness, 0, unroll=True)
    row8 = lax.broadcasted_iota(jnp.int32, (SUB, Z), 0)

    def coefficients(x):
        k = k_e[x]
        low, high = pltpu.roll(k, 1, 0), pltpu.roll(k, YE - 1, 0)
        back = jnp.where(lane_id == 0, 0.0, pltpu.roll(k, 1, 1))
        ahead = jnp.where(lane_id == Z - 1, 0.0, pltpu.roll(k, Z - 1, 1))
        xm = 0.5 * (k + k_e[x - 1])
        xp = 0.5 * (k + k_e[x + 1])
        ym = 0.5 * (k + low)
        yp = 0.5 * (k + high)
        zm = 0.5 * (k + back)
        zp = 0.5 * (k + ahead)
        diag = xm + xp + ym + yp + zm + zp + 0.5 * k
        inv = jnp.where(k > 0.0, 1.0 / diag, 0.0)
        zp = jnp.where(lane_id == Z - 1, 0.0, zp)
        kx[x] = xm
        kx[x + 1] = xp
        kym[x] = ym
        kyp[x] = yp
        kzm[x] = jnp.where(lane_id == 0, 0.0, zm)
        kzp[x] = zp
        d = diag - 0.25 * k
        dg[x] = d
        k4[x] = 0.25 * k
        invd[x] = inv
        return d

    for x in (1, 2, DEEP + X, DEEP + X + 1):
        coefficients(x)

    def inner(i, sums):
        d = coefficients(i + DEEP)[0:Y]
        reg = reg_e[i + DEEP, 0:Y]
        return tuple(sums[g] + fold(jnp.where(reg == g, d, 0.0)) for g in range(G))

    sum_acc = lax.fori_loop(0, X, inner, zero_acc(G), unroll=4)

    for n in (2, 1):
        for d in range(8):
            @pl.when(has[d])
            def _():
                arrived(n, d)

    def side_rows(i, _):
        x = i + DEEP
        y_face[pl.ds(i, 1), :] = kyp[x, Y - 1:Y, :]
        y_label[0, pl.ds(i, 1), :] = reg_e[x, Y - 1:Y, :]
        y_label[1, pl.ds(i, 1), :] = reg_e[x, Y:Y + 1, :]
        return 0

    looped(0, X, side_rows, 0)
    top = DEEP + X - 1
    x_acc = pairs(zero_acc(n2), reg_e[top, 0:Y], ((reg_e[top + 1, 0:Y], kx[top + 1, 0:Y]),))
    y_acc = pairs(zero_acc(n2), y_label[0], ((y_label[1], y_face[...]),))
    rim_col = column(tuple(x_acc) + tuple(y_acc) + tuple(sum_acc))

    lane = lax.broadcasted_iota(jnp.int32, (n2, LANES), 1)
    pair = lax.broadcasted_iota(jnp.int32, (n2, LANES), 0)
    at_pair = jnp.logical_and(lane >= 3 * pair, lane < 3 * pair + 3)

    def lanes_of(col, mask):
        return jnp.sum(jnp.where(mask, col, 0.0), axis=0, keepdims=True)

    lane_g = lax.broadcasted_iota(jnp.int32, (G, LANES), 1)
    row_g = lax.broadcasted_iota(jnp.int32, (G, LANES), 0)
    diag_at, sum_at = 3 * (G + 1) * row_g, 3 * n2 + 9 * row_g
    at_diag = jnp.logical_and(lane_g >= diag_at, lane_g < diag_at + 3)
    at_sum = jnp.logical_and(lane_g >= sum_at, lane_g < sum_at + 9)
    ac_rows = (lanes_of(own_col[0:n2], at_pair) * -2.0 + lanes_of(rim_col[2 * n2:], at_diag)
               + lanes_of(own_col[n2:], at_sum),
               lanes_of(rim_col[0:n2], at_pair) * -2.0, lanes_of(rim_col[n2:2 * n2], at_pair) * -2.0)
    for n in range(3):
        ac_send[n, 0:1, :] = ac_rows[n]
        ac[n, pl.ds(me, 1), :] = ac_rows[n]

    def send_ac(t):
        pltpu.make_async_remote_copy(
            src_ref=ac_send.at[:, pl.ds(0, 1)], dst_ref=ac.at[:, pl.ds(me, 1)],
            send_sem=ag_send.at[3], recv_sem=ag_recv.at[3],
            device_id=at(t), device_id_type=MESH).start()

    def coarse_vector(block):
        tiles = []
        for t in range(NC // LANES):
            lo = (LANES * t) // ncr // SUB * SUB
            hi = min(ND, -(-(-(-(LANES * (t + 1)) // ncr)) // SUB) * SUB)
            d = lax.broadcasted_iota(jnp.int32, (hi - lo, LANES), 0) + lo
            j = lax.broadcasted_iota(jnp.int32, (hi - lo, LANES), 1) + LANES * t
            m = (j >= d * ncr) & (j < d * ncr + ncr)
            tiles.append(jnp.sum(jnp.where(m, block[lo:hi, :], 0.0), axis=0, keepdims=True))
        return tiles

    def total(block, s):
        d = lax.broadcasted_iota(jnp.int32, (ND, LANES), 0)
        lane = lax.broadcasted_iota(jnp.int32, (ND, LANES), 1)
        m = lane == ((d * ncr + ncr + s) & (LANES - 1))
        v = jnp.sum(jnp.where(m, block, 0.0), axis=0, keepdims=True)
        return jnp.sum(v, axis=1, keepdims=True)

    def solve(tiles, block):
        s = block[:, 0:LANES] * tiles[0]
        for t in range(1, len(tiles)):
            s = s + block[:, t * LANES:(t + 1) * LANES] * tiles[t]
        return jnp.sum(s, axis=1, keepdims=True)

    def as_list(q):
        return [q[i:i + 1, :] for i in range(ncr)]

    rows_wait(0, ND - GP, ag_recv.at[1])
    for d in range(8):
        @pl.when(has[d])
        def _():
            pltpu.make_async_remote_copy(
                src_ref=c_in.at[d], dst_ref=c_in.at[d], send_sem=hc_send.at[d], recv_sem=hc_recv.at[d],
                device_id=(wi, ni), device_id_type=MESH).wait_recv()
    each_peer(send_ac)
    tiles = coarse_vector(rows[0])
    q = as_list(solve(tiles, call[half, slot]))
    qn = [as_list(solve(tiles, c_in[d])) for d in range(8)]

    def either(hi, lo):
        return [jnp.where(row8 < SUB // 2, a, b) for a, b in zip(hi, lo)]

    def add_spread(x, q_in, q_out):
        s = spread_over(reg_e[x, 0:Y], q_in, G)
        t = spread_over(reg_e[x, Y:YE], q_out, G)
        inv = invd[x]
        reg_o[x] = reg_e[x]
        for c in range(3):
            z_e[c, x, 0:Y] = r_e[c, x, 0:Y] * inv[0:Y] + s[c]
            z_e[c, x, Y:YE] = r_e[c, x, Y:YE] * inv[Y:YE] + t[c]

    column_c = call.at[half, pl.ds(0, NG - 1)]
    pltpu.make_async_copy(column_c, column_c, cs_recv.at[0]).wait()
    for i in range(1, GP // 2):
        p = lax.rem(place + i, GP // 2)
        block = call.at[half, pl.ds(place * NG, NG)]
        pltpu.make_async_remote_copy(
            src_ref=block, dst_ref=block, send_sem=cs_send.at[1], recv_sem=cs_recv.at[1],
            device_id=(grp * GW + (p // nn) * 2 + half, lax.rem(p, nn)), device_id_type=MESH).start()

    q_side = either(qn[3], qn[2])

    def spread_own(i, _):
        add_spread(i + DEEP, q, q_side)
        return 0

    looped(0, X, spread_own, 0)
    q_low, q_high = either(qn[5], qn[4]), either(qn[7], qn[6])
    for x in (1, 2):
        add_spread(x, qn[0], q_low)
    for x in (DEEP + X, DEEP + X + 1):
        add_spread(x, qn[1], q_high)

    faces = (kx, kym, kyp, kzm, kzp)

    def apply(ref, x, rows_):
        u = [ref[c, x] for c in range(3)]
        kk = k4[x, 0:rows_] * (u[0] + u[1] + u[2])[0:rows_]
        return u, [dg[x, 0:rows_] * u[c][0:rows_] + kk
                   - stencil(u[c], ref[c, x - 1], ref[c, x + 1], faces, x, rows_) for c in range(3)]

    def dots(a, b):
        return fold(a[0] * b[0] + a[1] * b[1] + a[2] * b[2])

    for x in (DEEP - 1, DEEP + X):
        _, a = apply(z_e, x, YE)
        for c in range(3):
            g_e[c, x] = a[c] * invd[x]

    def first(i, carry):
        x = i + DEEP
        u, a = apply(z_e, x, YE)
        w = []
        for c in range(3):
            w.append(a[c] * invd[x])
            g_e[c, x] = w[c]
        y = [a[c][0:Y] for c in range(3)]
        u = [u[c][0:Y] for c in range(3)]
        w = [w[c][0:Y] for c in range(3)]
        r = [r_e[c, x, 0:Y] for c in range(3)]
        for c in range(3):
            y_o[c, i] = y[c]
            z_o[c, i] = u[c]
            g_o[c, i] = w[c]
            r_o[c, i] = r[c]
        acc = add_rc(carry[:ncr], reg_e[x, 0:Y], y)
        return tuple(acc) + (carry[ncr] + dots(r, u), carry[ncr + 1] + dots(y, u), carry[ncr + 2] + dots(y, w))

    acc1 = lax.fori_loop(0, X, first, zero_acc(ncr + 3), unroll=4)

    def second(i, carry):
        x = i + DEEP
        w, a = apply(g_e, x, Y)
        for c in range(3):
            ag_o[c, i] = a[c]
        acc = add_rc(carry[:ncr], reg_e[x, 0:Y], a)
        return tuple(acc) + (carry[ncr] + dots([v[0:Y] for v in w], a),)

    acc2 = lax.fori_loop(0, X, second, zero_acc(ncr + 1), unroll=4)
    make_row(1, tuple(acc1) + (acc2[ncr],) + tuple(acc2[:ncr]))
    each_peer(lambda t: row_to(1, t, 2))

    others = call.at[half, pl.ds(0, NH - NG)]
    pltpu.make_async_copy(others, others, cs_recv.at[1]).wait()
    swap = pltpu.make_async_remote_copy(
        src_ref=call.at[half], dst_ref=call.at[half], send_sem=cs_send.at[2], recv_sem=cs_recv.at[2],
        device_id=(wi + 1 - 2 * half, ni), device_id_type=MESH)
    swap.start()
    some = ac.at[:, pl.ds(0, ND - 1)]
    pltpu.make_async_copy(some, some, ag_recv.at[3]).wait()
    swap.wait_recv()
    rows_wait(1, ND - 1, ag_recv.at[2])

    block = rows[1]
    b1 = coarse_vector(block)
    h1 = coarse_vector(pltpu.roll(block, LANES - ncr - 4, 1))
    rr = lax.broadcasted_iota(jnp.int32, (ncr, LANES), 0)
    ll = lax.broadcasted_iota(jnp.int32, (ncr, LANES), 1)
    m0, m1 = rr < 0, rr < 0
    for h in range(G):
        for g in range(G):
            for c in range(3):
                k = (h * G + g) * 3 + c
                m0 = jnp.logical_or(m0, (ll == k) & (rr == h * 3 + c))
                m1 = jnp.logical_or(m1, (ll == k) & (rr == g * 3 + c))
        for c in range(3):
            for e in range(3):
                k = 3 * n2 + h * 9 + c * 3 + e
                m0 = jnp.logical_or(m0, (ll == k) & (rr == h * 3 + c))
                m1 = jnp.logical_or(m1, (ll == k) & (rr == h * 3 + e))
    lines = [jnp.zeros((1, LANES), f32) for _ in b1]
    for w in range(nw):
        for n in range(nn):
            d = w * nn + n
            q1 = solve(b1, call[w % 2, ((w % GW) // 2 * nn + n) * NG + w // GW])
            qpair[0, d:d + 1, :] = jnp.sum(jnp.where(m0, q1, 0.0), axis=0, keepdims=True)
            qpair[1, d:d + 1, :] = jnp.sum(jnp.where(m1, q1, 0.0), axis=0, keepdims=True)
            for t in range(d * ncr // LANES, (d * ncr + ncr - 1) // LANES + 1):
                lines[t] = lines[t] + jnp.sum(jnp.where(ll + LANES * t == rr + d * ncr, q1, 0.0), axis=0, keepdims=True)
    first_q, second_q = qpair[0], qpair[1]
    dev = lax.broadcasted_iota(jnp.int32, (ND, LANES), 0)
    next_x = jnp.where(dev < ND - nn, pltpu.roll(second_q, ND - nn, 0), 0.0)
    next_y = jnp.where(dev < ND - 1, pltpu.roll(second_q, ND - 1, 0), 0.0)
    energy = jnp.sum(first_q * (ac[0] * second_q + ac[1] * next_x + ac[2] * next_y), axis=0, keepdims=True)
    for t in range(len(b1)):
        energy = energy + 2.0 * h1[t] * lines[t]
    yv = b1[0] * lines[0]
    for t in range(1, len(b1)):
        yv = yv + b1[t] * lines[t]
    yv = total(block, 2) + jnp.sum(yv, axis=1, keepdims=True)
    vav = total(block, 3) + jnp.sum(energy, axis=1, keepdims=True)
    rz0, zy = total(block, 0), total(block, 1)
    alpha0 = rz0 / zy
    rz1 = alpha0 * alpha0 * yv - rz0
    zaz = zy - 2.0 * alpha0 * yv + alpha0 * alpha0 * vav
    beta = rz1 / rz0
    alpha1 = rz1 / (zaz - beta * rz1 / alpha0)
    a1b = alpha1 * beta
    for n, v in enumerate((alpha0 + a1b + alpha1, alpha1 * alpha0)):
        sc_o[n:n + 1, :] = jnp.broadcast_to(v, (1, LANES))
    q_o[0] = jnp.broadcast_to(solve(b1, call[half, slot]), (ncr, LANES))
    for d in range(4):
        q_o[d + 1] = jnp.broadcast_to(solve(b1, c_in[d]), (ncr, LANES))

    rows_wait(0, GP - 1, ag_send.at[0])
    rows_wait(0, ND - GP, ag_send.at[1])
    rows_wait(1, ND - 1, ag_send.at[2])
    pltpu.make_async_copy(some, some, ag_send.at[3]).wait()
    pltpu.make_async_copy(column_c, column_c, cs_send.at[0]).wait()
    pltpu.make_async_copy(others, others, cs_send.at[1]).wait()
    swap.wait_send()
    for d in range(8):
        @pl.when(has[d])
        def _():
            for n in range(3):
                halo(n, d).wait_send()
            halo_c(d).wait_send()


def finish(z_v, g_v, r_v, y_v, ag_v, reg_v, k4, dg, kx, kym, kyp, kzm, kzp, q_v, sc_v, x_out, res_out, s_e, xb, rb, sem):
    a, b = sc_v[0:1, 0:1], sc_v[1:2, 0:1]
    E, YE, Z = reg_v.shape
    X, Y = E - 2 * DEEP, YE - SUB
    G = q_v.shape[1] // 3
    row8 = lax.broadcasted_iota(jnp.int32, (SUB, Z), 0)
    q = [[q_v[d, i:i + 1, :] for i in range(3 * G)] for d in range(5)]
    side = [jnp.where(row8 < SUB // 2, hi, lo) for hi, lo in zip(q[4], q[3])]

    def fill(x, q_in):
        s = spread_over(reg_v[x, 0:Y], q_in, G)
        t = spread_over(reg_v[x, Y:YE], side, G)
        for c in range(3):
            s_e[c, x, 0:Y] = s[c]
            s_e[c, x, Y:YE] = t[c]

    def fill_own(i, _):
        fill(i + DEEP, q[0])
        return 0

    fill(DEEP - 1, q[1])
    fill(DEEP + X, q[2])
    looped(0, X, fill_own, 0)
    faces = (kx, kym, kyp, kzm, kzp)
    copies = []
    parts = 4
    step = X // parts

    def plane(i, _):
        x = i + DEEP
        u = [s_e[c, x] for c in range(3)]
        kk = k4[x, 0:Y] * (u[0] + u[1] + u[2])[0:Y]
        for c in range(3):
            av = ag_v[c, i] + (dg[x, 0:Y] * u[c][0:Y] + kk
                               - stencil(u[c], s_e[c, x - 1], s_e[c, x + 1], faces, x, Y))
            xb[c, i] = a * z_v[c, i] - b * (g_v[c, i] + u[c][0:Y])
            rb[c, i] = r_v[c, i] - a * y_v[c, i] + b * av
        return 0

    for n in range(parts):
        lax.fori_loop(n * step, (n + 1) * step, plane, 0, unroll=True)
        for m, (src, dst) in enumerate(((xb, x_out), (rb, res_out))):
            where = (slice(None), pl.ds(n * step, step))
            copies.append(pltpu.make_async_copy(src.at[where], dst.at[where], sem.at[m, n]))
            copies[-1].start()
    for copy in copies:
        copy.wait()


def local_fast(nw, nn, right_side, occupancy, region, coarse_inverse):
    _, X, Y, Z = right_side.shape
    ncr, NC = coarse_inverse.shape
    ND = nw * nn
    f32, i32 = jnp.float32, jnp.int32
    V = pltpu.VMEM
    E, YE = X + 2 * DEEP, Y + SUB
    field, ext, scal = (3, X, Y, Z), (3, E, YE, Z), (E, YE, Z)
    ng = nw // group_of(nw)
    DMA = pltpu.SemaphoreType.DMA
    scratch = [
        V(scal, i32), V(scal, i32), V(ext, f32), V(scal, f32), V(scal, f32), V(ext, f32), V(ext, f32),
        V((2, ND // 2, ncr, NC), f32), V((8, ncr, NC), f32), V((X, Z), f32), V((2, X, Z), i32), V((2, ND, LANES), f32),
        V((2, SUB, LANES), f32), V((2, ND, LANES), f32), V((3, SUB, LANES), f32), V((3, ND, LANES), f32),
        DMA((4,)), DMA((3, 8)), DMA((3, 8)), DMA((8,)), DMA((8,)), DMA((4,)), DMA((4,)), DMA((3,)), DMA((3,)),
        pltpu.SemaphoreType.REGULAR((ng + 1,)),
    ]
    outs = (V(field, f32),) * 5 + (V(scal, i32),) + (V(scal, f32),) * 7 + (V((5, ncr, LANES), f32), V((SUB, LANES), f32))
    parts = pl.pallas_call(
        functools.partial(kernel, nw, nn),
        out_shape=outs,
        in_specs=[pl.BlockSpec(memory_space=pltpu.HBM)] * 4,
        out_specs=(pl.BlockSpec(memory_space=pltpu.VMEM),) * len(outs),
        scratch_shapes=scratch,
        compiler_params=pltpu.CompilerParams(collective_id=0, has_side_effects=True, vmem_limit_bytes=32 * 1024 * 1024),
    )(*[pltpu.with_memory_space_constraint(a, pltpu.HBM) for a in (right_side, occupancy, region, coarse_inverse)])
    return pl.pallas_call(
        finish,
        out_shape=(jax.ShapeDtypeStruct(field, f32),) * 2,
        in_specs=[pl.BlockSpec(memory_space=pltpu.VMEM)] * len(outs),
        out_specs=(pl.BlockSpec(memory_space=pltpu.HBM),) * 2,
        scratch_shapes=[V(ext, f32), V(field, f32), V(field, f32), DMA((2, 4))],
        compiler_params=pltpu.CompilerParams(vmem_limit_bytes=24 * 1024 * 1024),
    )(*parts)


def local(nw, nn, right_side, occupancy, region, coarse_inverse):
    nc = coarse_inverse.shape[1]
    run = local_fast if group_of(nw) % 2 == 0 and nc * nc * 4 <= REPLICATED_BYTES else local_wide
    return run(nw, nn, right_side, occupancy, region, coarse_inverse)


def solution(mesh):
    return jax.shard_map(
        functools.partial(local, mesh.shape["wide"], mesh.shape["narrow"]),
        mesh=mesh,
        in_specs=(
            P(None, "wide", "narrow", None),
            P("wide", "narrow", None),
            P("wide", "narrow", None),
            P(("wide", "narrow"), None),
        ),
        out_specs=(P(None, "wide", "narrow", None), P(None, "wide", "narrow", None)),
        check_vma=False,
    )
```

```python
import functools

import jax
import jax.numpy as jnp
from jax import lax
from jax.experimental import pallas as pl
from jax.experimental.pallas import tpu as pltpu
from jax.sharding import PartitionSpec as P

LANES = 128
SUB = 8
UNROLL = 16
looped = functools.partial(lax.fori_loop, unroll=UNROLL)
MESH = pl.DeviceIdType.MESH
bone_stiff = 1.0
soft_stiff = 0.1


def kernel_wide(nw, nn, r_hbm, occ_hbm, reg_hbm, ci_hbm,
           z0_v, z1_v, r_v, az_v, y_v, sc_v,
            occ_v, reg_v, c_v, k_p, kx, kym, kyp, kzm, kzp, dg, invd,
           z_p, v_p, zy, vy,
           ix_in, iy_send, iy_in, c_in, wx_send, wx_in, wy_send, wy_in,
           row_send, rows, load_sem, hs_send, hs_recv, ag_send, ag_recv):
    X, Y, Z = occ_v.shape
    ncr, NC = c_v.shape
    G = ncr // 3
    ND = nw * nn
    wi = lax.axis_index("wide")
    ni = lax.axis_index("narrow")
    me = wi * nn + ni
    f32 = jnp.float32

    loads = [pltpu.make_async_copy(s, d, load_sem.at[i]) for i, (s, d) in enumerate(
        ((occ_hbm, occ_v), (reg_hbm, reg_v), (r_hbm, r_v), (ci_hbm, c_v)))]
    for l in loads:
        l.start()

    def peer(i):
        t = lax.rem(me + i, ND)
        return (t // nn, lax.rem(t, nn))

    barrier = pltpu.get_barrier_semaphore()

    def greet(i, _):
        pl.semaphore_signal(barrier, inc=1, device_id=peer(i), device_id_type=MESH)
        return 0

    lax.fori_loop(1, ND, greet, 0, unroll=ND <= 64)

    has = (wi > 0, wi < nw - 1, ni > 0, ni < nn - 1)
    to = ((wi - 1, ni), (wi + 1, ni), (wi, ni - 1), (wi, ni + 1))

    for d in range(4):
        @pl.when(jnp.logical_not(has[d]))
        def _():
            c_in[d] = jnp.zeros((ncr, NC), f32)
            for p in range(2):
                if d < 2:
                    wx_in[p, d] = jnp.zeros((3, Y, Z), f32)
                else:
                    wy_in[p, d - 2] = jnp.zeros((3, X, Z), f32)
            if d < 2:
                ix_in[d] = jnp.zeros((2, Y, Z), jnp.int32)
            else:
                iy_in[d - 2] = jnp.zeros((2, X, Z), jnp.int32)

    loads[0].wait()
    loads[1].wait()

    def pack_ints(x, _):
        iy_send[0, 0, pl.ds(x, 1), :] = occ_v[x, 0:1, :]
        iy_send[1, 0, pl.ds(x, 1), :] = occ_v[x, Y - 1:Y, :]
        iy_send[0, 1, pl.ds(x, 1), :] = reg_v[x, 0:1, :]
        iy_send[1, 1, pl.ds(x, 1), :] = reg_v[x, Y - 1:Y, :]
        return 0

    looped(0, X, pack_ints, 0)

    def fold(a):
        return jnp.sum(a.reshape(Y // SUB, SUB, Z), axis=0)

    def zero_acc(n):
        return tuple(jnp.zeros((SUB, Z), f32) for _ in range(n))

    def add_rc(acc, reg, u):
        out = list(acc)
        for g in range(G):
            m = reg == g
            for c in range(3):
                out[g * 3 + c] = acc[g * 3 + c] + fold(jnp.where(m, u[c], 0.0))
        return tuple(out)

    base = (me * ncr) % LANES

    def make_row(p, acc, first):
        a = jnp.concatenate([jnp.sum(b, axis=0, keepdims=True) for b in acc], axis=0)
        col = jnp.sum(a, axis=1, keepdims=True)
        n = len(acc)
        k = lax.broadcasted_iota(jnp.int32, (n, LANES), 0)
        lane = lax.broadcasted_iota(jnp.int32, (n, LANES), 1)
        target = (base + first + k) & (LANES - 1)
        row = jnp.sum(jnp.where(lane == target, col, 0.0), axis=0, keepdims=True)
        row_send[p, 0:1, :] = row
        rows[p, pl.ds(me, 1), :] = row

    def gather_start(p):
        def send(i, _):
            pltpu.make_async_remote_copy(
                src_ref=row_send.at[p, pl.ds(0, 1)], dst_ref=rows.at[p, pl.ds(me, 1)],
                send_sem=ag_send.at[p], recv_sem=ag_recv.at[p],
                device_id=peer(i), device_id_type=MESH).start()
            return 0
        lax.fori_loop(1, ND, send, 0, unroll=ND <= 64)

    def gather_wait(p, sem):
        part = rows.at[p, pl.ds(0, ND - 1)]
        pltpu.make_async_copy(part, part, sem.at[p]).wait()

    def coarse_vector(p):
        tiles = []
        for t in range(NC // LANES):
            lo = (LANES * t) // ncr // SUB * SUB
            hi = min(ND, -(-(-(-(LANES * (t + 1)) // ncr)) // SUB) * SUB)
            d = lax.broadcasted_iota(jnp.int32, (hi - lo, LANES), 0) + lo
            j = lax.broadcasted_iota(jnp.int32, (hi - lo, LANES), 1) + LANES * t
            m = (j >= d * ncr) & (j < d * ncr + ncr)
            tiles.append(jnp.sum(jnp.where(m, rows[p, lo:hi, :], 0.0), axis=0, keepdims=True))
        return tiles

    def total(p, s):
        d = lax.broadcasted_iota(jnp.int32, (ND, LANES), 0)
        lane = lax.broadcasted_iota(jnp.int32, (ND, LANES), 1)
        m = lane == ((d * ncr + ncr + s) & (LANES - 1))
        v = jnp.sum(jnp.where(m, rows[p], 0.0), axis=0, keepdims=True)
        return jnp.sum(v, axis=1, keepdims=True)

    def answers(tiles, ref):
        s = ref[:, 0:LANES] * tiles[0]
        for t in range(1, len(tiles)):
            s = s + ref[:, t * LANES:(t + 1) * LANES] * tiles[t]
        q = jnp.sum(s, axis=1, keepdims=True)
        return [q[i:i + 1, :] for i in range(ncr)]

    def spread(reg, q):
        masks = [reg == g for g in range(G)]
        out = []
        for c in range(3):
            s = jnp.zeros(reg.shape, f32)
            for g in range(G):
                s = jnp.where(masks[g], q[g * 3 + c], s)
            out.append(s)
        return out

    def halo(slot, d, src, dst):
        return pltpu.make_async_remote_copy(
            src_ref=src, dst_ref=dst, send_sem=hs_send.at[slot, d],
            recv_sem=hs_recv.at[slot, d ^ 1], device_id=to[d], device_id_type=MESH)

    def copies(kind, d):
        e = d ^ 1
        if kind == 0:
            if d < 2:
                x = 0 if d == 0 else X - 1
                return [halo(0, d, occ_v.at[x], ix_in.at[e, 0]),
                        halo(1, d, reg_v.at[x], ix_in.at[e, 1])]
            return [halo(0, d, iy_send.at[d - 2, 0], iy_in.at[e - 2, 0]),
                    halo(1, d, iy_send.at[d - 2, 1], iy_in.at[e - 2, 1])]
        if kind == 1:
            return [halo(2, d, c_v, c_in.at[e])]
        p = kind - 2
        if d < 2:
            return [halo(3 + p, d, wx_send.at[p, d], wx_in.at[p, e])]
        return [halo(3 + p, d, wy_send.at[p, d - 2], wy_in.at[p, e - 2])]

    def halo_start(kind):
        for d in range(4):
            @pl.when(has[d])
            def _():
                for c in copies(kind, d):
                    c.start()

    def halo_wait(kind):
        for d in range(4):
            @pl.when(has[d])
            def _():
                for c in copies(kind, d ^ 1):
                    c.wait_recv()

    def halo_done(kind):
        for d in range(4):
            @pl.when(has[d])
            def _():
                for c in copies(kind, d):
                    c.wait_send()

    loads[2].wait()
    acc = looped(0, X, lambda x, a: add_rc(a, reg_v[x], [r_v[c, x] for c in range(3)]),
                        zero_acc(ncr))
    make_row(0, acc, 0)
    loads[3].wait()

    pl.semaphore_wait(barrier, ND - 1)
    halo_start(0)
    gather_start(0)
    halo_start(1)

    def stiff_of(o):
        return soft_stiff + (bone_stiff - soft_stiff) * o.astype(f32)

    def own_k(x, _):
        k_p[x + 1] = stiff_of(occ_v[x])
        return 0

    looped(0, X, own_k, 0)
    halo_wait(0)
    for d in range(2):
        @pl.when(has[d])
        def _():
            k_p[0 if d == 0 else X + 1] = stiff_of(ix_in[d, 0])

        @pl.when(jnp.logical_not(has[d]))
        def _():
            k_p[0 if d == 0 else X + 1] = jnp.zeros((Y, Z), f32)

    row_id = lax.broadcasted_iota(jnp.int32, (Y, Z), 0)
    lane_id = lax.broadcasted_iota(jnp.int32, (Y, Z), 1)
    side_lo = jnp.where(has[2], 1.0, 0.0).astype(f32)
    side_hi = jnp.where(has[3], 1.0, 0.0).astype(f32)

    def yshift(u, lo, hi):
        down = jnp.where(row_id == 0, lo, pltpu.roll(u, 1, 0))
        up = jnp.where(row_id == Y - 1, hi, pltpu.roll(u, Y - 1, 0))
        return down, up

    def save_faces(p, x, w):
        for c in range(3):
            wy_send[p, 0, c, pl.ds(x, 1), :] = w[c][0:1, :]
            wy_send[p, 1, c, pl.ds(x, 1), :] = w[c][Y - 1:Y, :]

    def coefficients(x, _):
        k = k_p[x + 1]
        lo = stiff_of(iy_in[0, 0, pl.ds(x, 1), :]) * side_lo
        hi = stiff_of(iy_in[1, 0, pl.ds(x, 1), :]) * side_hi
        down, up = yshift(k, lo, hi)
        back = jnp.where(lane_id == 0, 0.0, pltpu.roll(k, 1, 1))
        ahead = jnp.where(lane_id == Z - 1, 0.0, pltpu.roll(k, Z - 1, 1))
        xm = 0.5 * (k + k_p[x])
        xp = 0.5 * (k + k_p[x + 2])
        ym = 0.5 * (k + down)
        yp = 0.5 * (k + up)
        zm = 0.5 * (k + back)
        zp = 0.5 * (k + ahead)
        diag = xm + xp + ym + yp + zm + zp + 0.5 * k
        inv = 1.0 / diag
        kx[x] = xm
        kx[x + 1] = xp
        kym[x] = ym
        kyp[x] = yp
        kzm[x] = jnp.where(lane_id == 0, 0.0, zm)
        kzp[x] = jnp.where(lane_id == Z - 1, 0.0, zp)
        dg[x] = diag - 0.25 * k
        invd[x] = inv
        w = [r_v[c, x] * inv for c in range(3)]
        for c in range(3):
            z_p[c, x + 1] = w[c]
        save_faces(0, x, w)
        return 0

    looped(0, X, coefficients, 0)
    for c in range(3):
        wx_send[0, 0, c] = z_p[c, 1]
        wx_send[0, 1, c] = z_p[c, X]
    halo_start(2)

    def edges(p, qs, pad, side):
        for d in range(2):
            s = spread(ix_in[d, 1], qs[d])
            for c in range(3):
                pad[c, 0 if d == 0 else X + 1] = wx_in[p, d, c] + s[c]
        for d in range(2):
            s = spread(iy_in[d, 1], qs[2 + d])
            for c in range(3):
                side[d, c] = wy_in[p, d, c] + s[c]

    def operate(pad, side, x):
        k = k_p[x + 1]
        u = [pad[c, x + 1] for c in range(3)]
        k4 = 0.25 * k * (u[0] + u[1] + u[2])
        out = []
        for c in range(3):
            down, up = yshift(u[c], side[0, c, pl.ds(x, 1), :], side[1, c, pl.ds(x, 1), :])
            a = dg[x] * u[c] + k4
            a = a - (kx[x] * pad[c, x] + kx[x + 1] * pad[c, x + 2])
            a = a - (kym[x] * down + kyp[x] * up)
            a = a - (kzm[x] * pltpu.roll(u[c], 1, 1) + kzp[x] * pltpu.roll(u[c], Z - 1, 1))
            out.append(a)
        return u, out

    gather_wait(0, ag_recv)
    halo_wait(1)
    tiles = coarse_vector(0)
    q = answers(tiles, c_v)
    qs = [answers(tiles, c_in.at[d]) for d in range(4)]

    def add_spread(x, _):
        s = spread(reg_v[x], q)
        for c in range(3):
            z = z_p[c, x + 1] + s[c]
            z_p[c, x + 1] = z
            z0_v[c, x] = z
        return 0

    looped(0, X, add_spread, 0)
    halo_wait(2)
    edges(0, qs, z_p, zy)

    def dots(a, b):
        return fold(a[0] * b[0] + a[1] * b[1] + a[2] * b[2])

    def first(x, carry):
        u, a = operate(z_p, zy, x)
        r = [r_v[c, x] for c in range(3)]
        w = []
        for c in range(3):
            y_v[c, x] = a[c]
            w.append(a[c] * invd[x])
            v_p[c, x + 1] = w[c]
        save_faces(1, x, w)
        acc = add_rc(carry[:ncr], reg_v[x], a)
        return acc + (carry[ncr] + dots(r, u), carry[ncr + 1] + dots(a, u))

    acc = looped(0, X, first, zero_acc(ncr + 2))
    make_row(1, acc, 0)
    gather_start(1)
    for c in range(3):
        wx_send[1, 0, c] = v_p[c, 1]
        wx_send[1, 1, c] = v_p[c, X]
    halo_start(3)
    halo_wait(3)
    gather_wait(1, ag_recv)
    tiles = coarse_vector(1)
    q = answers(tiles, c_v)
    qs = [answers(tiles, c_in.at[d]) for d in range(4)]
    rz0 = total(1, 0)
    alpha0 = rz0 / total(1, 1)

    def add_spread_v(x, _):
        s = spread(reg_v[x], q)
        for c in range(3):
            v_p[c, x + 1] = v_p[c, x + 1] + s[c]
        return 0

    looped(0, X, add_spread_v, 0)
    edges(1, qs, v_p, vy)

    def second(x, carry):
        u, a = operate(v_p, vy, x)
        r, z, az = [], [], []
        for c in range(3):
            y = y_v[c, x]
            r.append(r_v[c, x] - alpha0 * y)
            z.append(z_p[c, x + 1] - alpha0 * u[c])
            az.append(y - alpha0 * a[c])
            r_v[c, x] = r[c]
            z1_v[c, x] = z[c]
            az_v[c, x] = az[c]
        return (carry[0] + dots(r, z), carry[1] + dots(az, z))

    acc = looped(0, X, second, zero_acc(2))
    make_row(2, acc, ncr)
    gather_start(2)
    gather_wait(2, ag_recv)
    rz1 = total(2, 0)
    beta = rz1 / rz0
    alpha1 = rz1 / (total(2, 1) - beta * rz1 / alpha0)
    along = alpha0 + alpha1 * beta
    a1b = alpha1 * beta

    sc_v[0:1, :] = jnp.broadcast_to(along, (1, LANES))
    sc_v[1:2, :] = jnp.broadcast_to(alpha1, (1, LANES))
    sc_v[2:3, :] = jnp.broadcast_to(a1b, (1, LANES))
    for kind in range(4):
        halo_done(kind)
    for p in range(3):
        gather_wait(p, ag_send)


def finish_wide(z0_v, z1_v, r_v, az_v, y_v, sc_v, x_out, res_out, xb, rb, sem):
    along = sc_v[0:1, 0:1]
    alpha1 = sc_v[1:2, 0:1]
    a1b = sc_v[2:3, 0:1]
    X = z0_v.shape[1]
    copies = []
    for c in range(3):
        for x in range(X):
            xb[c, x] = along * z0_v[c, x] + alpha1 * z1_v[c, x]
            rb[c, x] = r_v[c, x] - alpha1 * az_v[c, x] - a1b * y_v[c, x]
        for n, (src, dst) in enumerate(((xb, x_out), (rb, res_out))):
            copies.append(pltpu.make_async_copy(src.at[c], dst.at[c], sem.at[n, c]))
            copies[-1].start()
    for copy in copies:
        copy.wait()


def local_wide(nw, nn, right_side, occupancy, region, coarse_inverse):
    _, X, Y, Z = right_side.shape
    ncr, NC = coarse_inverse.shape
    ND = nw * nn
    f32, i32 = jnp.float32, jnp.int32
    V = pltpu.VMEM
    field, pad, scal = (3, X, Y, Z), (3, X + 2, Y, Z), (X, Y, Z)
    scratch = [
        V(scal, i32), V(scal, i32), V((ncr, NC), f32),
        V((X + 2, Y, Z), f32), V((X + 1, Y, Z), f32),
        V(scal, f32), V(scal, f32), V(scal, f32), V(scal, f32), V(scal, f32), V(scal, f32),
        V(pad, f32), V(pad, f32),
        V((2, 3, X, Z), f32), V((2, 3, X, Z), f32),
        V((2, 2, Y, Z), i32), V((2, 2, X, Z), i32), V((2, 2, X, Z), i32),
        V((4, ncr, NC), f32),
        V((2, 2, 3, Y, Z), f32), V((2, 2, 3, Y, Z), f32),
        V((2, 2, 3, X, Z), f32), V((2, 2, 3, X, Z), f32),
        V((3, SUB, LANES), f32), V((3, ND, LANES), f32),
        pltpu.SemaphoreType.DMA((4,)),
        pltpu.SemaphoreType.DMA((5, 4)), pltpu.SemaphoreType.DMA((5, 4)),
        pltpu.SemaphoreType.DMA((3,)), pltpu.SemaphoreType.DMA((3,)),
    ]
    parts = pl.pallas_call(
        functools.partial(kernel_wide, nw, nn),
        out_shape=(V(field, f32),) * 5 + (V((SUB, LANES), f32),),
        in_specs=[pl.BlockSpec(memory_space=pltpu.HBM)] * 4,
        out_specs=(pl.BlockSpec(memory_space=pltpu.VMEM),) * 6,
        scratch_shapes=scratch,
        compiler_params=pltpu.CompilerParams(collective_id=0, has_side_effects=True, vmem_limit_bytes=32 * 1024 * 1024),
    )(*[pltpu.with_memory_space_constraint(a, pltpu.HBM) for a in (right_side, occupancy, region, coarse_inverse)])
    return pl.pallas_call(
        finish_wide,
        out_shape=(jax.ShapeDtypeStruct(field, f32),) * 2,
        in_specs=[pl.BlockSpec(memory_space=pltpu.VMEM)] * 6,
        out_specs=(pl.BlockSpec(memory_space=pltpu.HBM),) * 2,
        scratch_shapes=[V(field, f32), V(field, f32), pltpu.SemaphoreType.DMA((2, 3))],
        compiler_params=pltpu.CompilerParams(vmem_limit_bytes=16 * 1024 * 1024),
    )(*parts)


REPLICATED_BYTES = 4 * 1024 * 1024
DEEP = 3
AROUND = ((-1, 0), (1, 0), (0, -1), (0, 1), (-1, -1), (-1, 1), (1, -1), (1, 1))
BACK = tuple(AROUND.index((-a, -b)) for a, b in AROUND)


def group_of(n):
    return max(d for d in range(1, n + 1) if n % d == 0 and d * d <= n)


def spread_over(reg, q, G):
    masks = [reg == g for g in range(G)]
    out = []
    for c in range(3):
        s = jnp.zeros(reg.shape, jnp.float32)
        for g in range(G):
            s = jnp.where(masks[g], q[g * 3 + c], s)
        out.append(s)
    return out


def stencil(u, prev, after, faces, x, rows):
    kx, kym, kyp, kzm, kzp = faces
    YE, Z = u.shape
    low, high = pltpu.roll(u, 1, 0)[0:rows], pltpu.roll(u, YE - 1, 0)[0:rows]
    v = u[0:rows]
    a = kx[x, 0:rows] * prev[0:rows] + kx[x + 1, 0:rows] * after[0:rows]
    a = a + (kym[x, 0:rows] * low + kyp[x, 0:rows] * high)
    return a + (kzm[x, 0:rows] * pltpu.roll(v, 1, 1) + kzp[x, 0:rows] * pltpu.roll(v, Z - 1, 1))


def kernel(nw, nn, r_hbm, occ_hbm, reg_hbm, ci_hbm,
           z_o, g_o, r_o, y_o, ag_o, reg_o, k4, dg, kx, kym, kyp, kzm, kzp, q_o, sc_o,
           occ_e, reg_e, r_e, k_e, invd, z_e, g_e,
           call, c_in, y_face, y_label, qpair, row_send, rows,
           load_sem, hs_send, hs_recv, hc_send, hc_recv, ag_send, ag_recv, cs_send, cs_recv, ready):
    E, YE, Z = occ_e.shape
    X, Y = E - 2 * DEEP, YE - SUB
    ncr, NC = c_in.shape[1:]
    G = ncr // 3
    ND = nw * nn
    NH = ND // 2
    wi = lax.axis_index("wide")
    ni = lax.axis_index("narrow")
    me = wi * nn + ni
    f32 = jnp.float32
    GW = group_of(nw)
    GP = GW * nn
    NG = ND // GP
    grp, pos = me // GP, lax.rem(me, GP)
    half, place = lax.rem(wi, 2), (lax.rem(wi, GW) // 2) * nn + ni
    slot = place * NG + grp
    own = pl.ds(DEEP, X)

    loads = [pltpu.make_async_copy(s, d, load_sem.at[i]) for i, (s, d) in enumerate((
        (reg_hbm, reg_e.at[own, pl.ds(0, Y)]), (r_hbm, r_e.at[:, own, pl.ds(0, Y)]),
        (occ_hbm, occ_e.at[own, pl.ds(0, Y)]), (ci_hbm, call.at[half, slot])))]
    for l in loads:
        l.start()

    barrier = pltpu.get_barrier_semaphore()

    def at(t):
        return (t // nn, lax.rem(t, nn))

    def wait_for(sem, count):
        @pl.when(count > 0)
        def _():
            pl.semaphore_wait(sem, count)

    def column_of(group):
        return (wi + (group - grp) * GW, ni)

    at_low = jnp.logical_and(lax.rem(wi, GW) == 0, wi > 0)
    at_high = jnp.logical_and(lax.rem(wi, GW) == GW - 1, wi < nw - 1)
    aside = 1 + jnp.where(ni > 0, 1, 0) + jnp.where(ni < nn - 1, 1, 0)

    def touching(ahead, signal):
        @pl.when(at_high if ahead > 0 else at_low)
        def _():
            for b in (-1, 0, 1):
                @pl.when(jnp.logical_and(ni + b >= 0, ni + b < nn))
                def _():
                    signal((wi + ahead, ni + b))

    def say(sem):
        return lambda device: pl.semaphore_signal(sem, inc=1, device_id=device, device_id_type=MESH)

    for i in range(1, GP):
        say(barrier)(at(grp * GP + lax.rem(pos + i, GP)))
    touching(1, say(barrier))
    for k in range(1, NG):
        @pl.when(grp + k < NG)
        def _():
            say(barrier)(column_of(grp + k))

    def tell():
        touching(-1, say(ready.at[0]))
        for k in range(1, NG):
            @pl.when(grp >= k)
            def _():
                say(ready.at[k])(column_of(grp - k))

    has = []
    for a, b in AROUND:
        h = jnp.logical_and(wi + a >= 0, wi + a < nw)
        has.append(jnp.logical_and(h, jnp.logical_and(ni + b >= 0, ni + b < nn)))

    def part(arr, d, into):
        a, b = AROUND[d]
        deep = {0: DEEP, 1: 2, 2: 2}[arr] if a == 0 or b == 0 else {0: 2, 1: 1, 2: 1}[arr]
        if into:
            xs = {-1: (DEEP - deep, deep), 0: (DEEP, X), 1: (DEEP + X, deep)}[a]
            ys = {-1: (YE - deep, deep), 0: (0, Y), 1: (Y, deep)}[b]
        else:
            xs = {-1: (DEEP, deep), 0: (DEEP, X), 1: (DEEP + X - deep, deep)}[a]
            ys = {-1: (0, deep), 0: (0, Y), 1: (Y - deep, deep)}[b]
        xs, ys = pl.ds(*xs), pl.ds(*ys)
        return (slice(None), xs, ys) if arr == 2 else (xs, ys)

    fields = (occ_e, reg_e, r_e)
    for d in range(8):
        @pl.when(jnp.logical_not(has[d]))
        def _():
            for n, ref in enumerate(fields):
                where = part(n, d, True)
                v = ref[where]
                ref[where] = jnp.full(v.shape, (-1, -1, 0)[n], v.dtype)
            c_in[d] = jnp.zeros((ncr, NC), f32)

    wait_for(barrier, GP - 1 + grp + jnp.where(at_low, aside, 0))
    tell()

    def fold(a):
        return jnp.sum(a.reshape(a.shape[0] // SUB, SUB, Z), axis=0)

    def zero_acc(n):
        return tuple(jnp.zeros((SUB, Z), f32) for _ in range(n))

    def add_rc(acc, reg, u):
        out = list(acc)
        for g in range(G):
            m = reg == g
            for c in range(3):
                out[g * 3 + c] = acc[g * 3 + c] + fold(jnp.where(m, u[c], 0.0))
        return out

    base = (me * ncr) % LANES

    def column(acc):
        a = jnp.concatenate([jnp.sum(b, axis=0, keepdims=True) for b in acc], axis=0)
        return jnp.sum(a, axis=1, keepdims=True)

    def make_row(p, acc):
        col = column(acc)
        n = len(acc)
        k = lax.broadcasted_iota(jnp.int32, (n, LANES), 0)
        lane = lax.broadcasted_iota(jnp.int32, (n, LANES), 1)
        target = (base + k) & (LANES - 1)
        row = jnp.sum(jnp.where(lane == target, col, 0.0), axis=0, keepdims=True)
        row_send[p, 0:1, :] = row
        rows[p, pl.ds(me, 1), :] = row

    def rows_to(p, count, t, sem):
        pltpu.make_async_remote_copy(
            src_ref=row_send.at[pl.ds(p, count), pl.ds(0, 1)], dst_ref=rows.at[pl.ds(p, count), pl.ds(me, 1)],
            send_sem=ag_send.at[sem], recv_sem=ag_recv.at[sem],
            device_id=at(t), device_id_type=MESH).start()

    def rows_wait(p, count, devices, sem):
        if devices:
            some = rows.at[pl.ds(p, count), pl.ds(0, devices)]
            pltpu.make_async_copy(some, some, sem).wait()

    def each_peer(send):
        def body(i, _):
            send(lax.rem(me + i, ND))
            return 0
        lax.fori_loop(1, ND, body, 0, unroll=ND <= 64)

    loads[0].wait()
    loads[1].wait()
    acc = looped(0, X, lambda x, a: tuple(add_rc(
        a, reg_e[x + DEEP, 0:Y], [r_e[c, x + DEEP, 0:Y] for c in range(3)])), zero_acc(ncr))
    make_row(0, acc)

    def inside(i, _):
        rows_to(0, 1, grp * GP + lax.rem(pos + i, GP), 0)
        return 0

    lax.fori_loop(1, GP, inside, 0, unroll=GP <= 64)

    def halo(n, d):
        a, b = AROUND[d]
        e = BACK[d]
        return pltpu.make_async_remote_copy(
            src_ref=fields[n].at[part(n, d, False)], dst_ref=fields[n].at[part(n, e, True)],
            send_sem=hs_send.at[n, d], recv_sem=hs_recv.at[n, e],
            device_id=(wi + a, ni + b), device_id_type=MESH)

    def halo_c(d):
        a, b = AROUND[d]
        return pltpu.make_async_remote_copy(
            src_ref=call.at[half, slot], dst_ref=c_in.at[BACK[d]],
            send_sem=hc_send.at[d], recv_sem=hc_recv.at[BACK[d]],
            device_id=(wi + a, ni + b), device_id_type=MESH)

    def arrived(n, d):
        where = part(n, d, True)
        pltpu.make_async_remote_copy(
            src_ref=fields[n].at[where], dst_ref=fields[n].at[where],
            send_sem=hs_send.at[n, d], recv_sem=hs_recv.at[n, d],
            device_id=(wi, ni), device_id_type=MESH).wait_recv()

    loads[2].wait()
    loads[3].wait()

    def halo_start(crossing):
        for n in range(4):
            for d, (a, b) in enumerate(AROUND):
                if a > 0 or not crossing:
                    now = at_high if crossing else jnp.logical_not(at_high)

                    @pl.when(jnp.logical_and(has[d], now) if a > 0 else has[d])
                    def _():
                        (halo_c(d) if n == 3 else halo(n, d)).start()

    halo_start(False)

    def c_column(group):
        pltpu.make_async_remote_copy(
            src_ref=call.at[half, slot], dst_ref=call.at[half, slot],
            send_sem=cs_send.at[0], recv_sem=cs_recv.at[0],
            device_id=column_of(group), device_id_type=MESH).start()

    for k in range(1, NG):
        @pl.when(grp >= k)
        def _():
            c_column(grp - k)

    def c_group(block, sem):
        for i in range(1, GP // 2):
            p = lax.rem(place + i, GP // 2)
            pltpu.make_async_remote_copy(
                src_ref=call.at[half, block], dst_ref=call.at[half, block],
                send_sem=cs_send.at[sem], recv_sem=cs_recv.at[sem],
                device_id=(grp * GW + (p // nn) * 2 + half, lax.rem(p, nn)), device_id_type=MESH).start()

    def c_wait(blocks, sem):
        some = call.at[half, pl.ds(0, blocks)]
        pltpu.make_async_copy(some, some, sem).wait()

    c_group(slot, 1)

    def stiff_of(o):
        return jnp.where(o < 0, 0.0, soft_stiff + (bone_stiff - soft_stiff) * o.astype(f32))

    n2 = G * G

    def pairs(acc, first, seconds):
        out = list(acc)
        for g in range(G):
            t = None
            for label, value in seconds:
                v = jnp.where(label == g, value, 0.0)
                t = v if t is None else t + v
            for h in range(G):
                out[h * G + g] = acc[h * G + g] + fold(jnp.where(first == h, t, 0.0))
        return out

    row16 = lax.broadcasted_iota(jnp.int32, (Y, Z), 0)
    lane16 = lax.broadcasted_iota(jnp.int32, (Y, Z), 1)

    def own_pairs(i, carry):
        x = i + DEEP
        k, reg = stiff_of(occ_e[x, 0:Y]), reg_e[x, 0:Y]
        later = jnp.minimum(i + 1, X - 1) + DEEP
        kx_in = jnp.where(i < X - 1, 0.5 * (k + stiff_of(occ_e[later, 0:Y])), 0.0)
        ky_in = jnp.where(row16 == Y - 1, 0.0, 0.5 * (k + pltpu.roll(k, Y - 1, 0)))
        kz_in = jnp.where(lane16 == Z - 1, 0.0, 0.5 * (k + pltpu.roll(k, Z - 1, 1)))
        acc = pairs(carry[:n2], reg, ((reg_e[later, 0:Y], kx_in), (pltpu.roll(reg, Y - 1, 0), ky_in),
                                      (pltpu.roll(reg, Z - 1, 1), kz_in)))
        sums = [carry[n2 + g] + fold(jnp.where(reg == g, 0.25 * k, 0.0)) for g in range(G)]
        return tuple(acc) + tuple(sums)

    own_acc = lax.fori_loop(0, X, own_pairs, zero_acc(n2 + G), unroll=2)
    own_col = column(own_acc)

    wait_for(ready.at[0], jnp.where(at_high, aside, 0))
    halo_start(True)
    for k in range(1, NG):
        @pl.when(grp + k < NG)
        def _():
            pl.semaphore_wait(ready.at[k], 1)
            c_column(grp + k)

    rows_wait(0, 1, GP - 1, ag_recv.at[0])
    mine = rows.at[0, pl.ds(pl.multiple_of(grp * GP, GP), GP)]

    def across(group):
        pltpu.make_async_remote_copy(
            src_ref=mine, dst_ref=mine, send_sem=ag_send.at[1], recv_sem=ag_recv.at[1],
            device_id=column_of(group), device_id_type=MESH).start()

    for k in range(1, NG):
        @pl.when(grp >= k)
        def _():
            across(grp - k)

    for k in range(1, NG):
        @pl.when(grp + k < NG)
        def _():
            across(grp + k)

    for d in range(8):
        @pl.when(has[d])
        def _():
            arrived(0, d)

    lane_id = lax.broadcasted_iota(jnp.int32, (YE, Z), 1)

    def stiffness(x, _):
        k_e[x] = stiff_of(occ_e[x])
        return 0

    lax.fori_loop(0, E, stiffness, 0, unroll=True)
    row8 = lax.broadcasted_iota(jnp.int32, (SUB, Z), 0)

    def coefficients(x):
        k = k_e[x]
        low, high = pltpu.roll(k, 1, 0), pltpu.roll(k, YE - 1, 0)
        back = jnp.where(lane_id == 0, 0.0, pltpu.roll(k, 1, 1))
        ahead = jnp.where(lane_id == Z - 1, 0.0, pltpu.roll(k, Z - 1, 1))
        xm = 0.5 * (k + k_e[x - 1])
        xp = 0.5 * (k + k_e[x + 1])
        ym = 0.5 * (k + low)
        yp = 0.5 * (k + high)
        zm = 0.5 * (k + back)
        zp = 0.5 * (k + ahead)
        diag = xm + xp + ym + yp + zm + zp + 0.5 * k
        inv = jnp.where(k > 0.0, 1.0 / diag, 0.0)
        zp = jnp.where(lane_id == Z - 1, 0.0, zp)
        kx[x] = xm
        kx[x + 1] = xp
        kym[x] = ym
        kyp[x] = yp
        kzm[x] = jnp.where(lane_id == 0, 0.0, zm)
        kzp[x] = zp
        d = diag - 0.25 * k
        dg[x] = d
        k4[x] = 0.25 * k
        invd[x] = inv
        return d

    for x in (1, 2, DEEP + X, DEEP + X + 1):
        coefficients(x)

    def inner(i, sums):
        d = coefficients(i + DEEP)[0:Y]
        reg = reg_e[i + DEEP, 0:Y]
        return tuple(sums[g] + fold(jnp.where(reg == g, d, 0.0)) for g in range(G))

    sum_acc = lax.fori_loop(0, X, inner, zero_acc(G), unroll=4)

    for n in (2, 1):
        for d in range(8):
            @pl.when(has[d])
            def _():
                arrived(n, d)

    def side_rows(i, _):
        x = i + DEEP
        y_face[pl.ds(i, 1), :] = kyp[x, Y - 1:Y, :]
        y_label[0, pl.ds(i, 1), :] = reg_e[x, Y - 1:Y, :]
        y_label[1, pl.ds(i, 1), :] = reg_e[x, Y:Y + 1, :]
        return 0

    looped(0, X, side_rows, 0)
    top = DEEP + X - 1
    x_acc = pairs(zero_acc(n2), reg_e[top, 0:Y], ((reg_e[top + 1, 0:Y], kx[top + 1, 0:Y]),))
    y_acc = pairs(zero_acc(n2), y_label[0], ((y_label[1], y_face[...]),))
    rim_col = column(tuple(x_acc) + tuple(y_acc) + tuple(sum_acc))

    lane = lax.broadcasted_iota(jnp.int32, (n2, LANES), 1)
    pair = lax.broadcasted_iota(jnp.int32, (n2, LANES), 0)
    at_pair = jnp.logical_and(lane >= 3 * pair, lane < 3 * pair + 3)

    def lanes_of(col, mask):
        return jnp.sum(jnp.where(mask, col, 0.0), axis=0, keepdims=True)

    lane_g = lax.broadcasted_iota(jnp.int32, (G, LANES), 1)
    row_g = lax.broadcasted_iota(jnp.int32, (G, LANES), 0)
    diag_at, sum_at = 3 * (G + 1) * row_g, 3 * n2 + 9 * row_g
    at_diag = jnp.logical_and(lane_g >= diag_at, lane_g < diag_at + 3)
    at_sum = jnp.logical_and(lane_g >= sum_at, lane_g < sum_at + 9)
    ac_rows = (lanes_of(own_col[0:n2], at_pair) * -2.0 + lanes_of(rim_col[2 * n2:], at_diag)
               + lanes_of(own_col[n2:], at_sum),
               lanes_of(rim_col[0:n2], at_pair) * -2.0, lanes_of(rim_col[n2:2 * n2], at_pair) * -2.0)
    for n in range(3):
        row_send[n + 2, 0:1, :] = ac_rows[n]
        rows[n + 2, pl.ds(me, 1), :] = ac_rows[n]

    def coarse_vector(block):
        tiles = []
        for t in range(NC // LANES):
            lo = (LANES * t) // ncr // SUB * SUB
            hi = min(ND, -(-(-(-(LANES * (t + 1)) // ncr)) // SUB) * SUB)
            d = lax.broadcasted_iota(jnp.int32, (hi - lo, LANES), 0) + lo
            j = lax.broadcasted_iota(jnp.int32, (hi - lo, LANES), 1) + LANES * t
            m = (j >= d * ncr) & (j < d * ncr + ncr)
            tiles.append(jnp.sum(jnp.where(m, block[lo:hi, :], 0.0), axis=0, keepdims=True))
        return tiles

    def total(block, s):
        d = lax.broadcasted_iota(jnp.int32, (ND, LANES), 0)
        lane = lax.broadcasted_iota(jnp.int32, (ND, LANES), 1)
        m = lane == ((d * ncr + ncr + s) & (LANES - 1))
        v = jnp.sum(jnp.where(m, block, 0.0), axis=0, keepdims=True)
        return jnp.sum(v, axis=1, keepdims=True)

    def solve(tiles, block):
        s = block[:, 0:LANES] * tiles[0]
        for t in range(1, len(tiles)):
            s = s + block[:, t * LANES:(t + 1) * LANES] * tiles[t]
        return jnp.sum(s, axis=1, keepdims=True)

    def as_list(q):
        return [q[i:i + 1, :] for i in range(ncr)]

    c_wait(NG - 1, cs_recv.at[0])
    for k in range(1, NG):
        c_group(place * NG + lax.rem(grp + k, NG), 2)

    rows_wait(0, 1, ND - GP, ag_recv.at[1])
    for d in range(8):
        @pl.when(has[d])
        def _():
            pltpu.make_async_remote_copy(
                src_ref=c_in.at[d], dst_ref=c_in.at[d], send_sem=hc_send.at[d], recv_sem=hc_recv.at[d],
                device_id=(wi, ni), device_id_type=MESH).wait_recv()
    tiles = coarse_vector(rows[0])
    q = as_list(solve(tiles, call[half, slot]))
    qn = [as_list(solve(tiles, c_in[d])) for d in range(8)]

    def either(hi, lo):
        return [jnp.where(row8 < SUB // 2, a, b) for a, b in zip(hi, lo)]

    def add_spread(x, q_in, q_out):
        s = spread_over(reg_e[x, 0:Y], q_in, G)
        t = spread_over(reg_e[x, Y:YE], q_out, G)
        inv = invd[x]
        reg_o[x] = reg_e[x]
        for c in range(3):
            z_e[c, x, 0:Y] = r_e[c, x, 0:Y] * inv[0:Y] + s[c]
            z_e[c, x, Y:YE] = r_e[c, x, Y:YE] * inv[Y:YE] + t[c]

    q_side = either(qn[3], qn[2])

    def spread_own(i, _):
        add_spread(i + DEEP, q, q_side)
        return 0

    looped(0, X, spread_own, 0)
    q_low, q_high = either(qn[5], qn[4]), either(qn[7], qn[6])
    for x in (1, 2):
        add_spread(x, qn[0], q_low)
    for x in (DEEP + X, DEEP + X + 1):
        add_spread(x, qn[1], q_high)

    faces = (kx, kym, kyp, kzm, kzp)

    def apply(ref, x, rows_):
        u = [ref[c, x] for c in range(3)]
        kk = k4[x, 0:rows_] * (u[0] + u[1] + u[2])[0:rows_]
        return u, [dg[x, 0:rows_] * u[c][0:rows_] + kk
                   - stencil(u[c], ref[c, x - 1], ref[c, x + 1], faces, x, rows_) for c in range(3)]

    def dots(a, b):
        return fold(a[0] * b[0] + a[1] * b[1] + a[2] * b[2])

    for x in (DEEP - 1, DEEP + X):
        _, a = apply(z_e, x, YE)
        for c in range(3):
            g_e[c, x] = a[c] * invd[x]

    def first(i, carry):
        x = i + DEEP
        u, a = apply(z_e, x, YE)
        w = []
        for c in range(3):
            w.append(a[c] * invd[x])
            g_e[c, x] = w[c]
        y = [a[c][0:Y] for c in range(3)]
        u = [u[c][0:Y] for c in range(3)]
        w = [w[c][0:Y] for c in range(3)]
        r = [r_e[c, x, 0:Y] for c in range(3)]
        for c in range(3):
            y_o[c, i] = y[c]
            z_o[c, i] = u[c]
            g_o[c, i] = w[c]
            r_o[c, i] = r[c]
        acc = add_rc(carry[:ncr], reg_e[x, 0:Y], y)
        return tuple(acc) + (carry[ncr] + dots(r, u), carry[ncr + 1] + dots(y, u), carry[ncr + 2] + dots(y, w))

    acc1 = lax.fori_loop(0, X, first, zero_acc(ncr + 3), unroll=4)

    def second(i, carry):
        x = i + DEEP
        w, a = apply(g_e, x, Y)
        for c in range(3):
            ag_o[c, i] = a[c]
        acc = add_rc(carry[:ncr], reg_e[x, 0:Y], a)
        return tuple(acc) + (carry[ncr] + dots([v[0:Y] for v in w], a),)

    acc2 = lax.fori_loop(0, X, second, zero_acc(ncr + 1), unroll=4)
    make_row(1, tuple(acc1) + (acc2[ncr],) + tuple(acc2[:ncr]))
    each_peer(lambda t: rows_to(1, 4, t, 2))

    c_wait(GP // 2 - 1, cs_recv.at[1])
    c_wait((GP // 2 - 1) * (NG - 1), cs_recv.at[2])
    swap = pltpu.make_async_remote_copy(
        src_ref=call.at[half], dst_ref=call.at[half], send_sem=cs_send.at[3], recv_sem=cs_recv.at[3],
        device_id=(wi + 1 - 2 * half, ni), device_id_type=MESH)
    swap.start()
    swap.wait_recv()
    rows_wait(1, 4, ND - 1, ag_recv.at[2])

    block = rows[1]
    b1 = coarse_vector(block)
    h1 = coarse_vector(pltpu.roll(block, LANES - ncr - 4, 1))
    rr = lax.broadcasted_iota(jnp.int32, (ncr, LANES), 0)
    ll = lax.broadcasted_iota(jnp.int32, (ncr, LANES), 1)
    m0, m1 = rr < 0, rr < 0
    for h in range(G):
        for g in range(G):
            for c in range(3):
                k = (h * G + g) * 3 + c
                m0 = jnp.logical_or(m0, (ll == k) & (rr == h * 3 + c))
                m1 = jnp.logical_or(m1, (ll == k) & (rr == g * 3 + c))
        for c in range(3):
            for e in range(3):
                k = 3 * n2 + h * 9 + c * 3 + e
                m0 = jnp.logical_or(m0, (ll == k) & (rr == h * 3 + c))
                m1 = jnp.logical_or(m1, (ll == k) & (rr == h * 3 + e))
    lines = [jnp.zeros((1, LANES), f32) for _ in b1]
    for w in range(nw):
        for n in range(nn):
            d = w * nn + n
            q1 = solve(b1, call[w % 2, ((w % GW) // 2 * nn + n) * NG + w // GW])
            qpair[0, d:d + 1, :] = jnp.sum(jnp.where(m0, q1, 0.0), axis=0, keepdims=True)
            qpair[1, d:d + 1, :] = jnp.sum(jnp.where(m1, q1, 0.0), axis=0, keepdims=True)
            for t in range(d * ncr // LANES, (d * ncr + ncr - 1) // LANES + 1):
                lines[t] = lines[t] + jnp.sum(jnp.where(ll + LANES * t == rr + d * ncr, q1, 0.0), axis=0, keepdims=True)
    first_q, second_q = qpair[0], qpair[1]
    dev = lax.broadcasted_iota(jnp.int32, (ND, LANES), 0)
    next_x = jnp.where(dev < ND - nn, pltpu.roll(second_q, ND - nn, 0), 0.0)
    next_y = jnp.where(dev < ND - 1, pltpu.roll(second_q, ND - 1, 0), 0.0)
    energy = jnp.sum(first_q * (rows[2] * second_q + rows[3] * next_x + rows[4] * next_y), axis=0, keepdims=True)
    for t in range(len(b1)):
        energy = energy + 2.0 * h1[t] * lines[t]
    yv = b1[0] * lines[0]
    for t in range(1, len(b1)):
        yv = yv + b1[t] * lines[t]
    yv = total(block, 2) + jnp.sum(yv, axis=1, keepdims=True)
    vav = total(block, 3) + jnp.sum(energy, axis=1, keepdims=True)
    rz0, zy = total(block, 0), total(block, 1)
    alpha0 = rz0 / zy
    rz1 = alpha0 * alpha0 * yv - rz0
    zaz = zy - 2.0 * alpha0 * yv + alpha0 * alpha0 * vav
    beta = rz1 / rz0
    alpha1 = rz1 / (zaz - beta * rz1 / alpha0)
    a1b = alpha1 * beta
    for n, v in enumerate((alpha0 + a1b + alpha1, alpha1 * alpha0)):
        sc_o[n:n + 1, :] = jnp.broadcast_to(v, (1, LANES))
    q_o[0] = jnp.broadcast_to(solve(b1, call[half, slot]), (ncr, LANES))
    for d in range(4):
        q_o[d + 1] = jnp.broadcast_to(solve(b1, c_in[d]), (ncr, LANES))

    rows_wait(0, 1, GP - 1, ag_send.at[0])
    rows_wait(0, 1, ND - GP, ag_send.at[1])
    rows_wait(1, 4, ND - 1, ag_send.at[2])
    c_wait(NG - 1, cs_send.at[0])
    c_wait(GP // 2 - 1, cs_send.at[1])
    c_wait((GP // 2 - 1) * (NG - 1), cs_send.at[2])
    swap.wait_send()
    for d in range(8):
        @pl.when(has[d])
        def _():
            for n in range(3):
                halo(n, d).wait_send()
            halo_c(d).wait_send()


def finish(z_v, g_v, r_v, y_v, ag_v, reg_v, k4, dg, kx, kym, kyp, kzm, kzp, q_v, sc_v, x_out, res_out, s_e, xb, rb, sem):
    a, b = sc_v[0:1, 0:1], sc_v[1:2, 0:1]
    E, YE, Z = reg_v.shape
    X, Y = E - 2 * DEEP, YE - SUB
    G = q_v.shape[1] // 3
    row8 = lax.broadcasted_iota(jnp.int32, (SUB, Z), 0)
    q = [[q_v[d, i:i + 1, :] for i in range(3 * G)] for d in range(5)]
    side = [jnp.where(row8 < SUB // 2, hi, lo) for hi, lo in zip(q[4], q[3])]

    def fill(x, q_in):
        s = spread_over(reg_v[x, 0:Y], q_in, G)
        t = spread_over(reg_v[x, Y:YE], side, G)
        for c in range(3):
            s_e[c, x, 0:Y] = s[c]
            s_e[c, x, Y:YE] = t[c]

    def fill_own(i, _):
        fill(i + DEEP, q[0])
        return 0

    fill(DEEP - 1, q[1])
    fill(DEEP + X, q[2])
    looped(0, X, fill_own, 0)
    faces = (kx, kym, kyp, kzm, kzp)
    copies = []
    parts = 4
    step = X // parts

    def plane(i, _):
        x = i + DEEP
        u = [s_e[c, x] for c in range(3)]
        kk = k4[x, 0:Y] * (u[0] + u[1] + u[2])[0:Y]
        for c in range(3):
            av = ag_v[c, i] + (dg[x, 0:Y] * u[c][0:Y] + kk
                               - stencil(u[c], s_e[c, x - 1], s_e[c, x + 1], faces, x, Y))
            xb[c, i] = a * z_v[c, i] - b * (g_v[c, i] + u[c][0:Y])
            rb[c, i] = r_v[c, i] - a * y_v[c, i] + b * av
        return 0

    for n in range(parts):
        lax.fori_loop(n * step, (n + 1) * step, plane, 0, unroll=True)
        for m, (src, dst) in enumerate(((xb, x_out), (rb, res_out))):
            where = (slice(None), pl.ds(n * step, step))
            copies.append(pltpu.make_async_copy(src.at[where], dst.at[where], sem.at[m, n]))
            copies[-1].start()
    for copy in copies:
        copy.wait()


def local_fast(nw, nn, right_side, occupancy, region, coarse_inverse):
    _, X, Y, Z = right_side.shape
    ncr, NC = coarse_inverse.shape
    ND = nw * nn
    f32, i32 = jnp.float32, jnp.int32
    V = pltpu.VMEM
    E, YE = X + 2 * DEEP, Y + SUB
    field, ext, scal = (3, X, Y, Z), (3, E, YE, Z), (E, YE, Z)
    ng = nw // group_of(nw)
    DMA = pltpu.SemaphoreType.DMA
    scratch = [
        V(scal, i32), V(scal, i32), V(ext, f32), V(scal, f32), V(scal, f32), V(ext, f32), V(ext, f32),
        V((2, ND // 2, ncr, NC), f32), V((8, ncr, NC), f32), V((X, Z), f32), V((2, X, Z), i32), V((2, ND, LANES), f32),
        V((5, SUB, LANES), f32), V((5, ND, LANES), f32),
        DMA((4,)), DMA((3, 8)), DMA((3, 8)), DMA((8,)), DMA((8,)), DMA((3,)), DMA((3,)), DMA((4,)), DMA((4,)),
        pltpu.SemaphoreType.REGULAR((ng,)),
    ]
    outs = (V(field, f32),) * 5 + (V(scal, i32),) + (V(scal, f32),) * 7 + (V((5, ncr, LANES), f32), V((SUB, LANES), f32))
    parts = pl.pallas_call(
        functools.partial(kernel, nw, nn),
        out_shape=outs,
        in_specs=[pl.BlockSpec(memory_space=pltpu.HBM)] * 4,
        out_specs=(pl.BlockSpec(memory_space=pltpu.VMEM),) * len(outs),
        scratch_shapes=scratch,
        compiler_params=pltpu.CompilerParams(collective_id=0, has_side_effects=True, vmem_limit_bytes=32 * 1024 * 1024),
    )(*[pltpu.with_memory_space_constraint(a, pltpu.HBM) for a in (right_side, occupancy, region, coarse_inverse)])
    return pl.pallas_call(
        finish,
        out_shape=(jax.ShapeDtypeStruct(field, f32),) * 2,
        in_specs=[pl.BlockSpec(memory_space=pltpu.VMEM)] * len(outs),
        out_specs=(pl.BlockSpec(memory_space=pltpu.HBM),) * 2,
        scratch_shapes=[V(ext, f32), V(field, f32), V(field, f32), DMA((2, 4))],
        compiler_params=pltpu.CompilerParams(vmem_limit_bytes=24 * 1024 * 1024),
    )(*parts)


def local(nw, nn, right_side, occupancy, region, coarse_inverse):
    nc = coarse_inverse.shape[1]
    run = local_fast if group_of(nw) % 2 == 0 and nc * nc * 4 <= REPLICATED_BYTES else local_wide
    return run(nw, nn, right_side, occupancy, region, coarse_inverse)


def solution(mesh):
    return jax.shard_map(
        functools.partial(local, mesh.shape["wide"], mesh.shape["narrow"]),
        mesh=mesh,
        in_specs=(
            P(None, "wide", "narrow", None),
            P("wide", "narrow", None),
            P("wide", "narrow", None),
            P(("wide", "narrow"), None),
        ),
        out_specs=(P(None, "wide", "narrow", None), P(None, "wide", "narrow", None)),
        check_vma=False,
    )
```

```python
import functools

import jax
import jax.numpy as jnp
from jax import lax
from jax.experimental import pallas as pl
from jax.experimental.pallas import tpu as pltpu
from jax.sharding import PartitionSpec as P

LANES = 128
SUB = 8
UNROLL = 16
looped = functools.partial(lax.fori_loop, unroll=UNROLL)
MESH = pl.DeviceIdType.MESH
bone_stiff = 1.0
soft_stiff = 0.1


def kernel_wide(nw, nn, r_hbm, occ_hbm, reg_hbm, ci_hbm,
           z0_v, z1_v, r_v, az_v, y_v, sc_v,
            occ_v, reg_v, c_v, k_p, kx, kym, kyp, kzm, kzp, dg, invd,
           z_p, v_p, zy, vy,
           ix_in, iy_send, iy_in, c_in, wx_send, wx_in, wy_send, wy_in,
           row_send, rows, load_sem, hs_send, hs_recv, ag_send, ag_recv):
    X, Y, Z = occ_v.shape
    ncr, NC = c_v.shape
    G = ncr // 3
    ND = nw * nn
    wi = lax.axis_index("wide")
    ni = lax.axis_index("narrow")
    me = wi * nn + ni
    f32 = jnp.float32

    loads = [pltpu.make_async_copy(s, d, load_sem.at[i]) for i, (s, d) in enumerate(
        ((occ_hbm, occ_v), (reg_hbm, reg_v), (r_hbm, r_v), (ci_hbm, c_v)))]
    for l in loads:
        l.start()

    def peer(i):
        t = lax.rem(me + i, ND)
        return (t // nn, lax.rem(t, nn))

    barrier = pltpu.get_barrier_semaphore()

    def greet(i, _):
        pl.semaphore_signal(barrier, inc=1, device_id=peer(i), device_id_type=MESH)
        return 0

    lax.fori_loop(1, ND, greet, 0, unroll=ND <= 64)

    has = (wi > 0, wi < nw - 1, ni > 0, ni < nn - 1)
    to = ((wi - 1, ni), (wi + 1, ni), (wi, ni - 1), (wi, ni + 1))

    for d in range(4):
        @pl.when(jnp.logical_not(has[d]))
        def _():
            c_in[d] = jnp.zeros((ncr, NC), f32)
            for p in range(2):
                if d < 2:
                    wx_in[p, d] = jnp.zeros((3, Y, Z), f32)
                else:
                    wy_in[p, d - 2] = jnp.zeros((3, X, Z), f32)
            if d < 2:
                ix_in[d] = jnp.zeros((2, Y, Z), jnp.int32)
            else:
                iy_in[d - 2] = jnp.zeros((2, X, Z), jnp.int32)

    loads[0].wait()
    loads[1].wait()

    def pack_ints(x, _):
        iy_send[0, 0, pl.ds(x, 1), :] = occ_v[x, 0:1, :]
        iy_send[1, 0, pl.ds(x, 1), :] = occ_v[x, Y - 1:Y, :]
        iy_send[0, 1, pl.ds(x, 1), :] = reg_v[x, 0:1, :]
        iy_send[1, 1, pl.ds(x, 1), :] = reg_v[x, Y - 1:Y, :]
        return 0

    looped(0, X, pack_ints, 0)

    def fold(a):
        return jnp.sum(a.reshape(Y // SUB, SUB, Z), axis=0)

    def zero_acc(n):
        return tuple(jnp.zeros((SUB, Z), f32) for _ in range(n))

    def add_rc(acc, reg, u):
        out = list(acc)
        for g in range(G):
            m = reg == g
            for c in range(3):
                out[g * 3 + c] = acc[g * 3 + c] + fold(jnp.where(m, u[c], 0.0))
        return tuple(out)

    base = (me * ncr) % LANES

    def make_row(p, acc, first):
        a = jnp.concatenate([jnp.sum(b, axis=0, keepdims=True) for b in acc], axis=0)
        col = jnp.sum(a, axis=1, keepdims=True)
        n = len(acc)
        k = lax.broadcasted_iota(jnp.int32, (n, LANES), 0)
        lane = lax.broadcasted_iota(jnp.int32, (n, LANES), 1)
        target = (base + first + k) & (LANES - 1)
        row = jnp.sum(jnp.where(lane == target, col, 0.0), axis=0, keepdims=True)
        row_send[p, 0:1, :] = row
        rows[p, pl.ds(me, 1), :] = row

    def gather_start(p):
        def send(i, _):
            pltpu.make_async_remote_copy(
                src_ref=row_send.at[p, pl.ds(0, 1)], dst_ref=rows.at[p, pl.ds(me, 1)],
                send_sem=ag_send.at[p], recv_sem=ag_recv.at[p],
                device_id=peer(i), device_id_type=MESH).start()
            return 0
        lax.fori_loop(1, ND, send, 0, unroll=ND <= 64)

    def gather_wait(p, sem):
        part = rows.at[p, pl.ds(0, ND - 1)]
        pltpu.make_async_copy(part, part, sem.at[p]).wait()

    def coarse_vector(p):
        tiles = []
        for t in range(NC // LANES):
            lo = (LANES * t) // ncr // SUB * SUB
            hi = min(ND, -(-(-(-(LANES * (t + 1)) // ncr)) // SUB) * SUB)
            d = lax.broadcasted_iota(jnp.int32, (hi - lo, LANES), 0) + lo
            j = lax.broadcasted_iota(jnp.int32, (hi - lo, LANES), 1) + LANES * t
            m = (j >= d * ncr) & (j < d * ncr + ncr)
            tiles.append(jnp.sum(jnp.where(m, rows[p, lo:hi, :], 0.0), axis=0, keepdims=True))
        return tiles

    def total(p, s):
        d = lax.broadcasted_iota(jnp.int32, (ND, LANES), 0)
        lane = lax.broadcasted_iota(jnp.int32, (ND, LANES), 1)
        m = lane == ((d * ncr + ncr + s) & (LANES - 1))
        v = jnp.sum(jnp.where(m, rows[p], 0.0), axis=0, keepdims=True)
        return jnp.sum(v, axis=1, keepdims=True)

    def answers(tiles, ref):
        s = ref[:, 0:LANES] * tiles[0]
        for t in range(1, len(tiles)):
            s = s + ref[:, t * LANES:(t + 1) * LANES] * tiles[t]
        q = jnp.sum(s, axis=1, keepdims=True)
        return [q[i:i + 1, :] for i in range(ncr)]

    def spread(reg, q):
        masks = [reg == g for g in range(G)]
        out = []
        for c in range(3):
            s = jnp.zeros(reg.shape, f32)
            for g in range(G):
                s = jnp.where(masks[g], q[g * 3 + c], s)
            out.append(s)
        return out

    def halo(slot, d, src, dst):
        return pltpu.make_async_remote_copy(
            src_ref=src, dst_ref=dst, send_sem=hs_send.at[slot, d],
            recv_sem=hs_recv.at[slot, d ^ 1], device_id=to[d], device_id_type=MESH)

    def copies(kind, d):
        e = d ^ 1
        if kind == 0:
            if d < 2:
                x = 0 if d == 0 else X - 1
                return [halo(0, d, occ_v.at[x], ix_in.at[e, 0]),
                        halo(1, d, reg_v.at[x], ix_in.at[e, 1])]
            return [halo(0, d, iy_send.at[d - 2, 0], iy_in.at[e - 2, 0]),
                    halo(1, d, iy_send.at[d - 2, 1], iy_in.at[e - 2, 1])]
        if kind == 1:
            return [halo(2, d, c_v, c_in.at[e])]
        p = kind - 2
        if d < 2:
            return [halo(3 + p, d, wx_send.at[p, d], wx_in.at[p, e])]
        return [halo(3 + p, d, wy_send.at[p, d - 2], wy_in.at[p, e - 2])]

    def halo_start(kind):
        for d in range(4):
            @pl.when(has[d])
            def _():
                for c in copies(kind, d):
                    c.start()

    def halo_wait(kind):
        for d in range(4):
            @pl.when(has[d])
            def _():
                for c in copies(kind, d ^ 1):
                    c.wait_recv()

    def halo_done(kind):
        for d in range(4):
            @pl.when(has[d])
            def _():
                for c in copies(kind, d):
                    c.wait_send()

    loads[2].wait()
    acc = looped(0, X, lambda x, a: add_rc(a, reg_v[x], [r_v[c, x] for c in range(3)]),
                        zero_acc(ncr))
    make_row(0, acc, 0)
    loads[3].wait()

    pl.semaphore_wait(barrier, ND - 1)
    halo_start(0)
    gather_start(0)
    halo_start(1)

    def stiff_of(o):
        return soft_stiff + (bone_stiff - soft_stiff) * o.astype(f32)

    def own_k(x, _):
        k_p[x + 1] = stiff_of(occ_v[x])
        return 0

    looped(0, X, own_k, 0)
    halo_wait(0)
    for d in range(2):
        @pl.when(has[d])
        def _():
            k_p[0 if d == 0 else X + 1] = stiff_of(ix_in[d, 0])

        @pl.when(jnp.logical_not(has[d]))
        def _():
            k_p[0 if d == 0 else X + 1] = jnp.zeros((Y, Z), f32)

    row_id = lax.broadcasted_iota(jnp.int32, (Y, Z), 0)
    lane_id = lax.broadcasted_iota(jnp.int32, (Y, Z), 1)
    side_lo = jnp.where(has[2], 1.0, 0.0).astype(f32)
    side_hi = jnp.where(has[3], 1.0, 0.0).astype(f32)

    def yshift(u, lo, hi):
        down = jnp.where(row_id == 0, lo, pltpu.roll(u, 1, 0))
        up = jnp.where(row_id == Y - 1, hi, pltpu.roll(u, Y - 1, 0))
        return down, up

    def save_faces(p, x, w):
        for c in range(3):
            wy_send[p, 0, c, pl.ds(x, 1), :] = w[c][0:1, :]
            wy_send[p, 1, c, pl.ds(x, 1), :] = w[c][Y - 1:Y, :]

    def coefficients(x, _):
        k = k_p[x + 1]
        lo = stiff_of(iy_in[0, 0, pl.ds(x, 1), :]) * side_lo
        hi = stiff_of(iy_in[1, 0, pl.ds(x, 1), :]) * side_hi
        down, up = yshift(k, lo, hi)
        back = jnp.where(lane_id == 0, 0.0, pltpu.roll(k, 1, 1))
        ahead = jnp.where(lane_id == Z - 1, 0.0, pltpu.roll(k, Z - 1, 1))
        xm = 0.5 * (k + k_p[x])
        xp = 0.5 * (k + k_p[x + 2])
        ym = 0.5 * (k + down)
        yp = 0.5 * (k + up)
        zm = 0.5 * (k + back)
        zp = 0.5 * (k + ahead)
        diag = xm + xp + ym + yp + zm + zp + 0.5 * k
        inv = 1.0 / diag
        kx[x] = xm
        kx[x + 1] = xp
        kym[x] = ym
        kyp[x] = yp
        kzm[x] = jnp.where(lane_id == 0, 0.0, zm)
        kzp[x] = jnp.where(lane_id == Z - 1, 0.0, zp)
        dg[x] = diag - 0.25 * k
        invd[x] = inv
        w = [r_v[c, x] * inv for c in range(3)]
        for c in range(3):
            z_p[c, x + 1] = w[c]
        save_faces(0, x, w)
        return 0

    looped(0, X, coefficients, 0)
    for c in range(3):
        wx_send[0, 0, c] = z_p[c, 1]
        wx_send[0, 1, c] = z_p[c, X]
    halo_start(2)

    def edges(p, qs, pad, side):
        for d in range(2):
            s = spread(ix_in[d, 1], qs[d])
            for c in range(3):
                pad[c, 0 if d == 0 else X + 1] = wx_in[p, d, c] + s[c]
        for d in range(2):
            s = spread(iy_in[d, 1], qs[2 + d])
            for c in range(3):
                side[d, c] = wy_in[p, d, c] + s[c]

    def operate(pad, side, x):
        k = k_p[x + 1]
        u = [pad[c, x + 1] for c in range(3)]
        k4 = 0.25 * k * (u[0] + u[1] + u[2])
        out = []
        for c in range(3):
            down, up = yshift(u[c], side[0, c, pl.ds(x, 1), :], side[1, c, pl.ds(x, 1), :])
            a = dg[x] * u[c] + k4
            a = a - (kx[x] * pad[c, x] + kx[x + 1] * pad[c, x + 2])
            a = a - (kym[x] * down + kyp[x] * up)
            a = a - (kzm[x] * pltpu.roll(u[c], 1, 1) + kzp[x] * pltpu.roll(u[c], Z - 1, 1))
            out.append(a)
        return u, out

    gather_wait(0, ag_recv)
    halo_wait(1)
    tiles = coarse_vector(0)
    q = answers(tiles, c_v)
    qs = [answers(tiles, c_in.at[d]) for d in range(4)]

    def add_spread(x, _):
        s = spread(reg_v[x], q)
        for c in range(3):
            z = z_p[c, x + 1] + s[c]
            z_p[c, x + 1] = z
            z0_v[c, x] = z
        return 0

    looped(0, X, add_spread, 0)
    halo_wait(2)
    edges(0, qs, z_p, zy)

    def dots(a, b):
        return fold(a[0] * b[0] + a[1] * b[1] + a[2] * b[2])

    def first(x, carry):
        u, a = operate(z_p, zy, x)
        r = [r_v[c, x] for c in range(3)]
        w = []
        for c in range(3):
            y_v[c, x] = a[c]
            w.append(a[c] * invd[x])
            v_p[c, x + 1] = w[c]
        save_faces(1, x, w)
        acc = add_rc(carry[:ncr], reg_v[x], a)
        return acc + (carry[ncr] + dots(r, u), carry[ncr + 1] + dots(a, u))

    acc = looped(0, X, first, zero_acc(ncr + 2))
    make_row(1, acc, 0)
    gather_start(1)
    for c in range(3):
        wx_send[1, 0, c] = v_p[c, 1]
        wx_send[1, 1, c] = v_p[c, X]
    halo_start(3)
    halo_wait(3)
    gather_wait(1, ag_recv)
    tiles = coarse_vector(1)
    q = answers(tiles, c_v)
    qs = [answers(tiles, c_in.at[d]) for d in range(4)]
    rz0 = total(1, 0)
    alpha0 = rz0 / total(1, 1)

    def add_spread_v(x, _):
        s = spread(reg_v[x], q)
        for c in range(3):
            v_p[c, x + 1] = v_p[c, x + 1] + s[c]
        return 0

    looped(0, X, add_spread_v, 0)
    edges(1, qs, v_p, vy)

    def second(x, carry):
        u, a = operate(v_p, vy, x)
        r, z, az = [], [], []
        for c in range(3):
            y = y_v[c, x]
            r.append(r_v[c, x] - alpha0 * y)
            z.append(z_p[c, x + 1] - alpha0 * u[c])
            az.append(y - alpha0 * a[c])
            r_v[c, x] = r[c]
            z1_v[c, x] = z[c]
            az_v[c, x] = az[c]
        return (carry[0] + dots(r, z), carry[1] + dots(az, z))

    acc = looped(0, X, second, zero_acc(2))
    make_row(2, acc, ncr)
    gather_start(2)
    gather_wait(2, ag_recv)
    rz1 = total(2, 0)
    beta = rz1 / rz0
    alpha1 = rz1 / (total(2, 1) - beta * rz1 / alpha0)
    along = alpha0 + alpha1 * beta
    a1b = alpha1 * beta

    sc_v[0:1, :] = jnp.broadcast_to(along, (1, LANES))
    sc_v[1:2, :] = jnp.broadcast_to(alpha1, (1, LANES))
    sc_v[2:3, :] = jnp.broadcast_to(a1b, (1, LANES))
    for kind in range(4):
        halo_done(kind)
    for p in range(3):
        gather_wait(p, ag_send)


def finish_wide(z0_v, z1_v, r_v, az_v, y_v, sc_v, x_out, res_out, xb, rb, sem):
    along = sc_v[0:1, 0:1]
    alpha1 = sc_v[1:2, 0:1]
    a1b = sc_v[2:3, 0:1]
    X = z0_v.shape[1]
    copies = []
    for c in range(3):
        for x in range(X):
            xb[c, x] = along * z0_v[c, x] + alpha1 * z1_v[c, x]
            rb[c, x] = r_v[c, x] - alpha1 * az_v[c, x] - a1b * y_v[c, x]
        for n, (src, dst) in enumerate(((xb, x_out), (rb, res_out))):
            copies.append(pltpu.make_async_copy(src.at[c], dst.at[c], sem.at[n, c]))
            copies[-1].start()
    for copy in copies:
        copy.wait()


def local_wide(nw, nn, right_side, occupancy, region, coarse_inverse):
    _, X, Y, Z = right_side.shape
    ncr, NC = coarse_inverse.shape
    ND = nw * nn
    f32, i32 = jnp.float32, jnp.int32
    V = pltpu.VMEM
    field, pad, scal = (3, X, Y, Z), (3, X + 2, Y, Z), (X, Y, Z)
    scratch = [
        V(scal, i32), V(scal, i32), V((ncr, NC), f32),
        V((X + 2, Y, Z), f32), V((X + 1, Y, Z), f32),
        V(scal, f32), V(scal, f32), V(scal, f32), V(scal, f32), V(scal, f32), V(scal, f32),
        V(pad, f32), V(pad, f32),
        V((2, 3, X, Z), f32), V((2, 3, X, Z), f32),
        V((2, 2, Y, Z), i32), V((2, 2, X, Z), i32), V((2, 2, X, Z), i32),
        V((4, ncr, NC), f32),
        V((2, 2, 3, Y, Z), f32), V((2, 2, 3, Y, Z), f32),
        V((2, 2, 3, X, Z), f32), V((2, 2, 3, X, Z), f32),
        V((3, SUB, LANES), f32), V((3, ND, LANES), f32),
        pltpu.SemaphoreType.DMA((4,)),
        pltpu.SemaphoreType.DMA((5, 4)), pltpu.SemaphoreType.DMA((5, 4)),
        pltpu.SemaphoreType.DMA((3,)), pltpu.SemaphoreType.DMA((3,)),
    ]
    parts = pl.pallas_call(
        functools.partial(kernel_wide, nw, nn),
        out_shape=(V(field, f32),) * 5 + (V((SUB, LANES), f32),),
        in_specs=[pl.BlockSpec(memory_space=pltpu.HBM)] * 4,
        out_specs=(pl.BlockSpec(memory_space=pltpu.VMEM),) * 6,
        scratch_shapes=scratch,
        compiler_params=pltpu.CompilerParams(collective_id=0, has_side_effects=True, vmem_limit_bytes=32 * 1024 * 1024),
    )(*[pltpu.with_memory_space_constraint(a, pltpu.HBM) for a in (right_side, occupancy, region, coarse_inverse)])
    return pl.pallas_call(
        finish_wide,
        out_shape=(jax.ShapeDtypeStruct(field, f32),) * 2,
        in_specs=[pl.BlockSpec(memory_space=pltpu.VMEM)] * 6,
        out_specs=(pl.BlockSpec(memory_space=pltpu.HBM),) * 2,
        scratch_shapes=[V(field, f32), V(field, f32), pltpu.SemaphoreType.DMA((2, 3))],
        compiler_params=pltpu.CompilerParams(vmem_limit_bytes=16 * 1024 * 1024),
    )(*parts)


REPLICATED_BYTES = 4 * 1024 * 1024
DEEP = 3
AROUND = ((-1, 0), (1, 0), (0, -1), (0, 1), (-1, -1), (-1, 1), (1, -1), (1, 1))
BACK = tuple(AROUND.index((-a, -b)) for a, b in AROUND)


def group_of(n):
    return max(d for d in range(1, n + 1) if n % d == 0 and d * d <= n)


def spread_over(reg, q, G):
    masks = [reg == g for g in range(G)]
    out = []
    for c in range(3):
        s = jnp.zeros(reg.shape, jnp.float32)
        for g in range(G):
            s = jnp.where(masks[g], q[g * 3 + c], s)
        out.append(s)
    return out


def stencil(u, prev, after, faces, x, rows):
    kx, kym, kyp, kzm, kzp = faces
    YE, Z = u.shape
    low, high = pltpu.roll(u, 1, 0)[0:rows], pltpu.roll(u, YE - 1, 0)[0:rows]
    v = u[0:rows]
    a = kx[x, 0:rows] * prev[0:rows] + kx[x + 1, 0:rows] * after[0:rows]
    a = a + (kym[x, 0:rows] * low + kyp[x, 0:rows] * high)
    return a + (kzm[x, 0:rows] * pltpu.roll(v, 1, 1) + kzp[x, 0:rows] * pltpu.roll(v, Z - 1, 1))


def kernel(nw, nn, r_hbm, occ_hbm, reg_hbm, ci_hbm,
           z_o, g_o, r_o, y_o, ag_o, reg_o, k4, dg, kx, kym, kyp, kzm, kzp, q_o, sc_o,
           occ_e, reg_e, r_e, k_e, invd, z_e, g_e,
           call, c_in, y_face, y_label, qpair, row_send, rows,
           load_sem, hs_send, hs_recv, hc_send, hc_recv, ag_send, ag_recv, cs_send, cs_recv, ready):
    E, YE, Z = occ_e.shape
    X, Y = E - 2 * DEEP, YE - SUB
    ncr, NC = c_in.shape[1:]
    G = ncr // 3
    ND = nw * nn
    NH = ND // 2
    wi = lax.axis_index("wide")
    ni = lax.axis_index("narrow")
    me = wi * nn + ni
    f32 = jnp.float32
    GW = group_of(nw)
    GP = GW * nn
    NG = ND // GP
    grp, pos = me // GP, lax.rem(me, GP)
    half, place = lax.rem(wi, 2), (lax.rem(wi, GW) // 2) * nn + ni
    slot = place * NG + grp
    own = pl.ds(DEEP, X)

    loads = [pltpu.make_async_copy(s, d, load_sem.at[i]) for i, (s, d) in enumerate((
        (reg_hbm, reg_e.at[own, pl.ds(0, Y)]), (r_hbm, r_e.at[:, own, pl.ds(0, Y)]),
        (occ_hbm, occ_e.at[own, pl.ds(0, Y)]), (ci_hbm, call.at[half, slot])))]
    for l in loads:
        l.start()

    barrier = pltpu.get_barrier_semaphore()

    def at(t):
        return (t // nn, lax.rem(t, nn))

    def wait_for(sem, count):
        @pl.when(count > 0)
        def _():
            pl.semaphore_wait(sem, count)

    def column_of(group):
        return (wi + (group - grp) * GW, ni)

    at_low = jnp.logical_and(lax.rem(wi, GW) == 0, wi > 0)
    at_high = jnp.logical_and(lax.rem(wi, GW) == GW - 1, wi < nw - 1)
    aside = 1 + jnp.where(ni > 0, 1, 0) + jnp.where(ni < nn - 1, 1, 0)

    def touching(ahead, signal):
        @pl.when(at_high if ahead > 0 else at_low)
        def _():
            for b in (-1, 0, 1):
                @pl.when(jnp.logical_and(ni + b >= 0, ni + b < nn))
                def _():
                    signal((wi + ahead, ni + b))

    def say(sem):
        return lambda device: pl.semaphore_signal(sem, inc=1, device_id=device, device_id_type=MESH)

    for i in range(1, GP):
        say(barrier)(at(grp * GP + lax.rem(pos + i, GP)))
    touching(1, say(barrier))
    touching(-1, say(barrier))
    for k in range(1, NG):
        @pl.when(grp + k < NG)
        def _():
            say(barrier)(column_of(grp + k))

    def tell():
        for k in range(1, NG):
            @pl.when(grp >= k)
            def _():
                say(ready.at[k])(column_of(grp - k))

    has = []
    for a, b in AROUND:
        h = jnp.logical_and(wi + a >= 0, wi + a < nw)
        has.append(jnp.logical_and(h, jnp.logical_and(ni + b >= 0, ni + b < nn)))

    def part(arr, d, into):
        a, b = AROUND[d]
        deep = {0: DEEP, 1: 2, 2: 2}[arr] if a == 0 or b == 0 else {0: 2, 1: 1, 2: 1}[arr]
        if into:
            xs = {-1: (DEEP - deep, deep), 0: (DEEP, X), 1: (DEEP + X, deep)}[a]
            ys = {-1: (YE - deep, deep), 0: (0, Y), 1: (Y, deep)}[b]
        else:
            xs = {-1: (DEEP, deep), 0: (DEEP, X), 1: (DEEP + X - deep, deep)}[a]
            ys = {-1: (0, deep), 0: (0, Y), 1: (Y - deep, deep)}[b]
        xs, ys = pl.ds(*xs), pl.ds(*ys)
        return (slice(None), xs, ys) if arr == 2 else (xs, ys)

    fields = (occ_e, reg_e, r_e)
    for d in range(8):
        @pl.when(jnp.logical_not(has[d]))
        def _():
            for n, ref in enumerate(fields):
                where = part(n, d, True)
                v = ref[where]
                ref[where] = jnp.full(v.shape, (-1, -1, 0)[n], v.dtype)
            c_in[d] = jnp.zeros((ncr, NC), f32)

    wait_for(barrier, GP - 1 + grp + jnp.where(at_low, aside, 0) + jnp.where(at_high, aside, 0))
    tell()

    def fold(a):
        return jnp.sum(a.reshape(a.shape[0] // SUB, SUB, Z), axis=0)

    def zero_acc(n):
        return tuple(jnp.zeros((SUB, Z), f32) for _ in range(n))

    def add_rc(acc, reg, u):
        out = list(acc)
        for g in range(G):
            m = reg == g
            for c in range(3):
                out[g * 3 + c] = acc[g * 3 + c] + fold(jnp.where(m, u[c], 0.0))
        return out

    base = (me * ncr) % LANES

    def column(acc):
        a = jnp.concatenate([jnp.sum(b, axis=0, keepdims=True) for b in acc], axis=0)
        return jnp.sum(a, axis=1, keepdims=True)

    def make_row(p, acc):
        col = column(acc)
        n = len(acc)
        k = lax.broadcasted_iota(jnp.int32, (n, LANES), 0)
        lane = lax.broadcasted_iota(jnp.int32, (n, LANES), 1)
        target = (base + k) & (LANES - 1)
        row = jnp.sum(jnp.where(lane == target, col, 0.0), axis=0, keepdims=True)
        row_send[p, 0:1, :] = row
        rows[p, pl.ds(me, 1), :] = row

    def rows_to(p, count, t, sem):
        pltpu.make_async_remote_copy(
            src_ref=row_send.at[pl.ds(p, count), pl.ds(0, 1)], dst_ref=rows.at[pl.ds(p, count), pl.ds(me, 1)],
            send_sem=ag_send.at[sem], recv_sem=ag_recv.at[sem],
            device_id=at(t), device_id_type=MESH).start()

    def rows_wait(p, count, devices, sem):
        if devices:
            some = rows.at[pl.ds(p, count), pl.ds(0, devices)]
            pltpu.make_async_copy(some, some, sem).wait()

    def each_peer(send):
        def body(i, _):
            send(lax.rem(me + i, ND))
            return 0
        lax.fori_loop(1, ND, body, 0, unroll=ND <= 64)

    loads[0].wait()
    loads[1].wait()
    acc = looped(0, X, lambda x, a: tuple(add_rc(
        a, reg_e[x + DEEP, 0:Y], [r_e[c, x + DEEP, 0:Y] for c in range(3)])), zero_acc(ncr))
    make_row(0, acc)

    def inside(i, _):
        rows_to(0, 1, grp * GP + lax.rem(pos + i, GP), 0)
        return 0

    lax.fori_loop(1, GP, inside, 0, unroll=GP <= 64)

    def halo(n, d):
        a, b = AROUND[d]
        e = BACK[d]
        return pltpu.make_async_remote_copy(
            src_ref=fields[n].at[part(n, d, False)], dst_ref=fields[n].at[part(n, e, True)],
            send_sem=hs_send.at[n, d], recv_sem=hs_recv.at[n, e],
            device_id=(wi + a, ni + b), device_id_type=MESH)

    def halo_c(d):
        a, b = AROUND[d]
        return pltpu.make_async_remote_copy(
            src_ref=call.at[half, slot], dst_ref=c_in.at[BACK[d]],
            send_sem=hc_send.at[d], recv_sem=hc_recv.at[BACK[d]],
            device_id=(wi + a, ni + b), device_id_type=MESH)

    def arrived(n, d):
        where = part(n, d, True)
        pltpu.make_async_remote_copy(
            src_ref=fields[n].at[where], dst_ref=fields[n].at[where],
            send_sem=hs_send.at[n, d], recv_sem=hs_recv.at[n, d],
            device_id=(wi, ni), device_id_type=MESH).wait_recv()

    loads[2].wait()
    loads[3].wait()

    for n in range(4):
        for d in range(8):
            @pl.when(has[d])
            def _():
                (halo_c(d) if n == 3 else halo(n, d)).start()

    def c_column(group):
        pltpu.make_async_remote_copy(
            src_ref=call.at[half, slot], dst_ref=call.at[half, slot],
            send_sem=cs_send.at[0], recv_sem=cs_recv.at[0],
            device_id=column_of(group), device_id_type=MESH).start()

    for k in range(1, NG):
        @pl.when(grp >= k)
        def _():
            c_column(grp - k)

    def c_group(block, sem):
        for i in range(1, GP // 2):
            p = lax.rem(place + i, GP // 2)
            pltpu.make_async_remote_copy(
                src_ref=call.at[half, block], dst_ref=call.at[half, block],
                send_sem=cs_send.at[sem], recv_sem=cs_recv.at[sem],
                device_id=(grp * GW + (p // nn) * 2 + half, lax.rem(p, nn)), device_id_type=MESH).start()

    def c_wait(blocks, sem):
        some = call.at[half, pl.ds(0, blocks)]
        pltpu.make_async_copy(some, some, sem).wait()

    c_group(slot, 1)

    def stiff_of(o):
        return jnp.where(o < 0, 0.0, soft_stiff + (bone_stiff - soft_stiff) * o.astype(f32))

    n2 = G * G

    def pairs(acc, first, seconds):
        out = list(acc)
        for g in range(G):
            t = None
            for label, value in seconds:
                v = jnp.where(label == g, value, 0.0)
                t = v if t is None else t + v
            for h in range(G):
                out[h * G + g] = acc[h * G + g] + fold(jnp.where(first == h, t, 0.0))
        return out

    row16 = lax.broadcasted_iota(jnp.int32, (Y, Z), 0)
    lane16 = lax.broadcasted_iota(jnp.int32, (Y, Z), 1)

    def own_pairs(i, carry):
        x = i + DEEP
        k, reg = stiff_of(occ_e[x, 0:Y]), reg_e[x, 0:Y]
        later = jnp.minimum(i + 1, X - 1) + DEEP
        kx_in = jnp.where(i < X - 1, 0.5 * (k + stiff_of(occ_e[later, 0:Y])), 0.0)
        ky_in = jnp.where(row16 == Y - 1, 0.0, 0.5 * (k + pltpu.roll(k, Y - 1, 0)))
        kz_in = jnp.where(lane16 == Z - 1, 0.0, 0.5 * (k + pltpu.roll(k, Z - 1, 1)))
        acc = pairs(carry[:n2], reg, ((reg_e[later, 0:Y], kx_in), (pltpu.roll(reg, Y - 1, 0), ky_in),
                                      (pltpu.roll(reg, Z - 1, 1), kz_in)))
        sums = [carry[n2 + g] + fold(jnp.where(reg == g, 0.25 * k, 0.0)) for g in range(G)]
        return tuple(acc) + tuple(sums)

    own_acc = lax.fori_loop(0, X, own_pairs, zero_acc(n2 + G), unroll=2)
    own_col = column(own_acc)

    def c_up(k):
        @pl.when(grp + k < NG)
        def _():
            pl.semaphore_wait(ready.at[k], 1)
            c_column(grp + k)

    for k in range(1, NG):
        c_up(k)

    rows_wait(0, 1, GP - 1, ag_recv.at[0])
    mine = rows.at[0, pl.ds(pl.multiple_of(grp * GP, GP), GP)]

    def across(group):
        pltpu.make_async_remote_copy(
            src_ref=mine, dst_ref=mine, send_sem=ag_send.at[1], recv_sem=ag_recv.at[1],
            device_id=column_of(group), device_id_type=MESH).start()

    for k in range(1, NG):
        @pl.when(grp >= k)
        def _():
            across(grp - k)

    for k in range(1, NG):
        @pl.when(grp + k < NG)
        def _():
            across(grp + k)

    for d in range(8):
        @pl.when(has[d])
        def _():
            arrived(0, d)

    lane_id = lax.broadcasted_iota(jnp.int32, (YE, Z), 1)

    def stiffness(x, _):
        k_e[x] = stiff_of(occ_e[x])
        return 0

    lax.fori_loop(0, E, stiffness, 0, unroll=True)
    row8 = lax.broadcasted_iota(jnp.int32, (SUB, Z), 0)

    def coefficients(x):
        k = k_e[x]
        low, high = pltpu.roll(k, 1, 0), pltpu.roll(k, YE - 1, 0)
        back = jnp.where(lane_id == 0, 0.0, pltpu.roll(k, 1, 1))
        ahead = jnp.where(lane_id == Z - 1, 0.0, pltpu.roll(k, Z - 1, 1))
        xm = 0.5 * (k + k_e[x - 1])
        xp = 0.5 * (k + k_e[x + 1])
        ym = 0.5 * (k + low)
        yp = 0.5 * (k + high)
        zm = 0.5 * (k + back)
        zp = 0.5 * (k + ahead)
        diag = xm + xp + ym + yp + zm + zp + 0.5 * k
        inv = jnp.where(k > 0.0, 1.0 / diag, 0.0)
        zp = jnp.where(lane_id == Z - 1, 0.0, zp)
        kx[x] = xm
        kx[x + 1] = xp
        kym[x] = ym
        kyp[x] = yp
        kzm[x] = jnp.where(lane_id == 0, 0.0, zm)
        kzp[x] = zp
        d = diag - 0.25 * k
        dg[x] = d
        k4[x] = 0.25 * k
        invd[x] = inv
        return d

    for x in (1, 2, DEEP + X, DEEP + X + 1):
        coefficients(x)

    def inner(i, sums):
        d = coefficients(i + DEEP)[0:Y]
        reg = reg_e[i + DEEP, 0:Y]
        return tuple(sums[g] + fold(jnp.where(reg == g, d, 0.0)) for g in range(G))

    sum_acc = lax.fori_loop(0, X, inner, zero_acc(G), unroll=4)

    for n in (2, 1):
        for d in range(8):
            @pl.when(has[d])
            def _():
                arrived(n, d)

    def side_rows(i, _):
        x = i + DEEP
        y_face[pl.ds(i, 1), :] = kyp[x, Y - 1:Y, :]
        y_label[0, pl.ds(i, 1), :] = reg_e[x, Y - 1:Y, :]
        y_label[1, pl.ds(i, 1), :] = reg_e[x, Y:Y + 1, :]
        return 0

    looped(0, X, side_rows, 0)
    top = DEEP + X - 1
    x_acc = pairs(zero_acc(n2), reg_e[top, 0:Y], ((reg_e[top + 1, 0:Y], kx[top + 1, 0:Y]),))
    y_acc = pairs(zero_acc(n2), y_label[0], ((y_label[1], y_face[...]),))
    rim_col = column(tuple(x_acc) + tuple(y_acc) + tuple(sum_acc))

    lane = lax.broadcasted_iota(jnp.int32, (n2, LANES), 1)
    pair = lax.broadcasted_iota(jnp.int32, (n2, LANES), 0)
    at_pair = jnp.logical_and(lane >= 3 * pair, lane < 3 * pair + 3)

    def lanes_of(col, mask):
        return jnp.sum(jnp.where(mask, col, 0.0), axis=0, keepdims=True)

    lane_g = lax.broadcasted_iota(jnp.int32, (G, LANES), 1)
    row_g = lax.broadcasted_iota(jnp.int32, (G, LANES), 0)
    diag_at, sum_at = 3 * (G + 1) * row_g, 3 * n2 + 9 * row_g
    at_diag = jnp.logical_and(lane_g >= diag_at, lane_g < diag_at + 3)
    at_sum = jnp.logical_and(lane_g >= sum_at, lane_g < sum_at + 9)
    ac_rows = (lanes_of(own_col[0:n2], at_pair) * -2.0 + lanes_of(rim_col[2 * n2:], at_diag)
               + lanes_of(own_col[n2:], at_sum),
               lanes_of(rim_col[0:n2], at_pair) * -2.0, lanes_of(rim_col[n2:2 * n2], at_pair) * -2.0)
    for n in range(3):
        row_send[n + 2, 0:1, :] = ac_rows[n]
        rows[n + 2, pl.ds(me, 1), :] = ac_rows[n]

    def coarse_vector(block):
        tiles = []
        for t in range(NC // LANES):
            lo = (LANES * t) // ncr // SUB * SUB
            hi = min(ND, -(-(-(-(LANES * (t + 1)) // ncr)) // SUB) * SUB)
            d = lax.broadcasted_iota(jnp.int32, (hi - lo, LANES), 0) + lo
            j = lax.broadcasted_iota(jnp.int32, (hi - lo, LANES), 1) + LANES * t
            m = (j >= d * ncr) & (j < d * ncr + ncr)
            tiles.append(jnp.sum(jnp.where(m, block[lo:hi, :], 0.0), axis=0, keepdims=True))
        return tiles

    def total(block, s):
        d = lax.broadcasted_iota(jnp.int32, (ND, LANES), 0)
        lane = lax.broadcasted_iota(jnp.int32, (ND, LANES), 1)
        m = lane == ((d * ncr + ncr + s) & (LANES - 1))
        v = jnp.sum(jnp.where(m, block, 0.0), axis=0, keepdims=True)
        return jnp.sum(v, axis=1, keepdims=True)

    def solve(tiles, block):
        s = block[:, 0:LANES] * tiles[0]
        for t in range(1, len(tiles)):
            s = s + block[:, t * LANES:(t + 1) * LANES] * tiles[t]
        return jnp.sum(s, axis=1, keepdims=True)

    def as_list(q):
        return [q[i:i + 1, :] for i in range(ncr)]

    c_wait(NG - 1, cs_recv.at[0])
    for k in range(1, NG):
        c_group(place * NG + lax.rem(grp + k, NG), 2)

    rows_wait(0, 1, ND - GP, ag_recv.at[1])
    for d in range(8):
        @pl.when(has[d])
        def _():
            pltpu.make_async_remote_copy(
                src_ref=c_in.at[d], dst_ref=c_in.at[d], send_sem=hc_send.at[d], recv_sem=hc_recv.at[d],
                device_id=(wi, ni), device_id_type=MESH).wait_recv()
    tiles = coarse_vector(rows[0])
    q = as_list(solve(tiles, call[half, slot]))
    qn = [as_list(solve(tiles, c_in[d])) for d in range(8)]

    def either(hi, lo):
        return [jnp.where(row8 < SUB // 2, a, b) for a, b in zip(hi, lo)]

    def add_spread(x, q_in, q_out):
        s = spread_over(reg_e[x, 0:Y], q_in, G)
        t = spread_over(reg_e[x, Y:YE], q_out, G)
        inv = invd[x]
        reg_o[x] = reg_e[x]
        for c in range(3):
            z_e[c, x, 0:Y] = r_e[c, x, 0:Y] * inv[0:Y] + s[c]
            z_e[c, x, Y:YE] = r_e[c, x, Y:YE] * inv[Y:YE] + t[c]

    q_side = either(qn[3], qn[2])

    def spread_own(i, _):
        add_spread(i + DEEP, q, q_side)
        return 0

    looped(0, X, spread_own, 0)
    q_low, q_high = either(qn[5], qn[4]), either(qn[7], qn[6])
    for x in (1, 2):
        add_spread(x, qn[0], q_low)
    for x in (DEEP + X, DEEP + X + 1):
        add_spread(x, qn[1], q_high)

    faces = (kx, kym, kyp, kzm, kzp)

    def apply(ref, x, rows_):
        u = [ref[c, x] for c in range(3)]
        kk = k4[x, 0:rows_] * (u[0] + u[1] + u[2])[0:rows_]
        return u, [dg[x, 0:rows_] * u[c][0:rows_] + kk
                   - stencil(u[c], ref[c, x - 1], ref[c, x + 1], faces, x, rows_) for c in range(3)]

    def dots(a, b):
        return fold(a[0] * b[0] + a[1] * b[1] + a[2] * b[2])

    for x in (DEEP - 1, DEEP + X):
        _, a = apply(z_e, x, YE)
        for c in range(3):
            g_e[c, x] = a[c] * invd[x]

    def first(i, carry):
        x = i + DEEP
        u, a = apply(z_e, x, YE)
        w = []
        for c in range(3):
            w.append(a[c] * invd[x])
            g_e[c, x] = w[c]
        y = [a[c][0:Y] for c in range(3)]
        u = [u[c][0:Y] for c in range(3)]
        w = [w[c][0:Y] for c in range(3)]
        r = [r_e[c, x, 0:Y] for c in range(3)]
        for c in range(3):
            y_o[c, i] = y[c]
            z_o[c, i] = u[c]
            g_o[c, i] = w[c]
            r_o[c, i] = r[c]
        acc = add_rc(carry[:ncr], reg_e[x, 0:Y], y)
        return tuple(acc) + (carry[ncr] + dots(r, u), carry[ncr + 1] + dots(y, u), carry[ncr + 2] + dots(y, w))

    acc1 = lax.fori_loop(0, X, first, zero_acc(ncr + 3), unroll=4)

    def second(i, carry):
        x = i + DEEP
        w, a = apply(g_e, x, Y)
        for c in range(3):
            ag_o[c, i] = a[c]
        acc = add_rc(carry[:ncr], reg_e[x, 0:Y], a)
        return tuple(acc) + (carry[ncr] + dots([v[0:Y] for v in w], a),)

    acc2 = lax.fori_loop(0, X, second, zero_acc(ncr + 1), unroll=4)
    make_row(1, tuple(acc1) + (acc2[ncr],) + tuple(acc2[:ncr]))
    each_peer(lambda t: rows_to(1, 4, t, 2))

    c_wait(GP // 2 - 1, cs_recv.at[1])
    c_wait((GP // 2 - 1) * (NG - 1), cs_recv.at[2])
    swap = pltpu.make_async_remote_copy(
        src_ref=call.at[half], dst_ref=call.at[half], send_sem=cs_send.at[3], recv_sem=cs_recv.at[3],
        device_id=(wi + 1 - 2 * half, ni), device_id_type=MESH)
    swap.start()
    rows_wait(0, 1, GP - 1, ag_send.at[0])
    rows_wait(0, 1, ND - GP, ag_send.at[1])
    c_wait(NG - 1, cs_send.at[0])
    c_wait(GP // 2 - 1, cs_send.at[1])
    c_wait((GP // 2 - 1) * (NG - 1), cs_send.at[2])
    for d in range(8):
        @pl.when(has[d])
        def _():
            for n in range(3):
                halo(n, d).wait_send()
            halo_c(d).wait_send()
    swap.wait_recv()
    rows_wait(1, 4, ND - 1, ag_recv.at[2])

    block = rows[1]
    b1 = coarse_vector(block)
    h1 = coarse_vector(pltpu.roll(block, LANES - ncr - 4, 1))
    rr = lax.broadcasted_iota(jnp.int32, (ncr, LANES), 0)
    ll = lax.broadcasted_iota(jnp.int32, (ncr, LANES), 1)
    m0, m1 = rr < 0, rr < 0
    for h in range(G):
        for g in range(G):
            for c in range(3):
                k = (h * G + g) * 3 + c
                m0 = jnp.logical_or(m0, (ll == k) & (rr == h * 3 + c))
                m1 = jnp.logical_or(m1, (ll == k) & (rr == g * 3 + c))
        for c in range(3):
            for e in range(3):
                k = 3 * n2 + h * 9 + c * 3 + e
                m0 = jnp.logical_or(m0, (ll == k) & (rr == h * 3 + c))
                m1 = jnp.logical_or(m1, (ll == k) & (rr == h * 3 + e))
    lines = [jnp.zeros((1, LANES), f32) for _ in b1]
    for w in range(nw):
        for n in range(nn):
            d = w * nn + n
            q1 = solve(b1, call[w % 2, ((w % GW) // 2 * nn + n) * NG + w // GW])
            qpair[0, d:d + 1, :] = jnp.sum(jnp.where(m0, q1, 0.0), axis=0, keepdims=True)
            qpair[1, d:d + 1, :] = jnp.sum(jnp.where(m1, q1, 0.0), axis=0, keepdims=True)
            for t in range(d * ncr // LANES, (d * ncr + ncr - 1) // LANES + 1):
                lines[t] = lines[t] + jnp.sum(jnp.where(ll + LANES * t == rr + d * ncr, q1, 0.0), axis=0, keepdims=True)
    first_q, second_q = qpair[0], qpair[1]
    dev = lax.broadcasted_iota(jnp.int32, (ND, LANES), 0)
    next_x = jnp.where(dev < ND - nn, pltpu.roll(second_q, ND - nn, 0), 0.0)
    next_y = jnp.where(dev < ND - 1, pltpu.roll(second_q, ND - 1, 0), 0.0)
    energy = jnp.sum(first_q * (rows[2] * second_q + rows[3] * next_x + rows[4] * next_y), axis=0, keepdims=True)
    for t in range(len(b1)):
        energy = energy + 2.0 * h1[t] * lines[t]
    yv = b1[0] * lines[0]
    for t in range(1, len(b1)):
        yv = yv + b1[t] * lines[t]
    yv = total(block, 2) + jnp.sum(yv, axis=1, keepdims=True)
    vav = total(block, 3) + jnp.sum(energy, axis=1, keepdims=True)
    rz0, zy = total(block, 0), total(block, 1)
    alpha0 = rz0 / zy
    rz1 = alpha0 * alpha0 * yv - rz0
    zaz = zy - 2.0 * alpha0 * yv + alpha0 * alpha0 * vav
    beta = rz1 / rz0
    alpha1 = rz1 / (zaz - beta * rz1 / alpha0)
    a1b = alpha1 * beta
    for n, v in enumerate((alpha0 + a1b + alpha1, alpha1 * alpha0)):
        sc_o[n:n + 1, :] = jnp.broadcast_to(v, (1, LANES))
    q_o[0] = jnp.broadcast_to(solve(b1, call[half, slot]), (ncr, LANES))
    for d in range(4):
        q_o[d + 1] = jnp.broadcast_to(solve(b1, c_in[d]), (ncr, LANES))

    rows_wait(1, 4, ND - 1, ag_send.at[2])
    swap.wait_send()


def finish(z_v, g_v, r_v, y_v, ag_v, reg_v, k4, dg, kx, kym, kyp, kzm, kzp, q_v, sc_v, x_out, res_out, s_e, xb, rb, sem):
    a, b = sc_v[0:1, 0:1], sc_v[1:2, 0:1]
    E, YE, Z = reg_v.shape
    X, Y = E - 2 * DEEP, YE - SUB
    G = q_v.shape[1] // 3
    row8 = lax.broadcasted_iota(jnp.int32, (SUB, Z), 0)
    q = [[q_v[d, i:i + 1, :] for i in range(3 * G)] for d in range(5)]
    side = [jnp.where(row8 < SUB // 2, hi, lo) for hi, lo in zip(q[4], q[3])]

    def fill(x, q_in):
        s = spread_over(reg_v[x, 0:Y], q_in, G)
        t = spread_over(reg_v[x, Y:YE], side, G)
        for c in range(3):
            s_e[c, x, 0:Y] = s[c]
            s_e[c, x, Y:YE] = t[c]

    def fill_own(i, _):
        fill(i + DEEP, q[0])
        return 0

    fill(DEEP - 1, q[1])
    fill(DEEP + X, q[2])
    looped(0, X, fill_own, 0)
    faces = (kx, kym, kyp, kzm, kzp)
    copies = []
    parts = 4
    step = X // parts

    def plane(i, _):
        x = i + DEEP
        u = [s_e[c, x] for c in range(3)]
        kk = k4[x, 0:Y] * (u[0] + u[1] + u[2])[0:Y]
        for c in range(3):
            av = ag_v[c, i] + (dg[x, 0:Y] * u[c][0:Y] + kk
                               - stencil(u[c], s_e[c, x - 1], s_e[c, x + 1], faces, x, Y))
            xb[c, i] = a * z_v[c, i] - b * (g_v[c, i] + u[c][0:Y])
            rb[c, i] = r_v[c, i] - a * y_v[c, i] + b * av
        return 0

    for n in range(parts):
        lax.fori_loop(n * step, (n + 1) * step, plane, 0, unroll=True)
        for m, (src, dst) in enumerate(((xb, x_out), (rb, res_out))):
            where = (slice(None), pl.ds(n * step, step))
            copies.append(pltpu.make_async_copy(src.at[where], dst.at[where], sem.at[m, n]))
            copies[-1].start()
    for copy in copies:
        copy.wait()


def local_fast(nw, nn, right_side, occupancy, region, coarse_inverse):
    _, X, Y, Z = right_side.shape
    ncr, NC = coarse_inverse.shape
    ND = nw * nn
    f32, i32 = jnp.float32, jnp.int32
    V = pltpu.VMEM
    E, YE = X + 2 * DEEP, Y + SUB
    field, ext, scal = (3, X, Y, Z), (3, E, YE, Z), (E, YE, Z)
    ng = nw // group_of(nw)
    DMA = pltpu.SemaphoreType.DMA
    scratch = [
        V(scal, i32), V(scal, i32), V(ext, f32), V(scal, f32), V(scal, f32), V(ext, f32), V(ext, f32),
        V((2, ND // 2, ncr, NC), f32), V((8, ncr, NC), f32), V((X, Z), f32), V((2, X, Z), i32), V((2, ND, LANES), f32),
        V((5, SUB, LANES), f32), V((5, ND, LANES), f32),
        DMA((4,)), DMA((3, 8)), DMA((3, 8)), DMA((8,)), DMA((8,)), DMA((3,)), DMA((3,)), DMA((4,)), DMA((4,)),
        pltpu.SemaphoreType.REGULAR((ng,)),
    ]
    outs = (V(field, f32),) * 5 + (V(scal, i32),) + (V(scal, f32),) * 7 + (V((5, ncr, LANES), f32), V((SUB, LANES), f32))
    parts = pl.pallas_call(
        functools.partial(kernel, nw, nn),
        out_shape=outs,
        in_specs=[pl.BlockSpec(memory_space=pltpu.HBM)] * 4,
        out_specs=(pl.BlockSpec(memory_space=pltpu.VMEM),) * len(outs),
        scratch_shapes=scratch,
        compiler_params=pltpu.CompilerParams(collective_id=0, has_side_effects=True, vmem_limit_bytes=32 * 1024 * 1024),
    )(*[pltpu.with_memory_space_constraint(a, pltpu.HBM) for a in (right_side, occupancy, region, coarse_inverse)])
    return pl.pallas_call(
        finish,
        out_shape=(jax.ShapeDtypeStruct(field, f32),) * 2,
        in_specs=[pl.BlockSpec(memory_space=pltpu.VMEM)] * len(outs),
        out_specs=(pl.BlockSpec(memory_space=pltpu.HBM),) * 2,
        scratch_shapes=[V(ext, f32), V(field, f32), V(field, f32), DMA((2, 4))],
        compiler_params=pltpu.CompilerParams(vmem_limit_bytes=24 * 1024 * 1024),
    )(*parts)


def local(nw, nn, right_side, occupancy, region, coarse_inverse):
    nc = coarse_inverse.shape[1]
    run = local_fast if group_of(nw) % 2 == 0 and nc * nc * 4 <= REPLICATED_BYTES else local_wide
    return run(nw, nn, right_side, occupancy, region, coarse_inverse)


def solution(mesh):
    return jax.shard_map(
        functools.partial(local, mesh.shape["wide"], mesh.shape["narrow"]),
        mesh=mesh,
        in_specs=(
            P(None, "wide", "narrow", None),
            P("wide", "narrow", None),
            P("wide", "narrow", None),
            P(("wide", "narrow"), None),
        ),
        out_specs=(P(None, "wide", "narrow", None), P(None, "wide", "narrow", None)),
        check_vma=False,
    )
```

```python
import functools

import jax
import jax.numpy as jnp
from jax import lax
from jax.experimental import pallas as pl
from jax.experimental.pallas import tpu as pltpu
from jax.sharding import PartitionSpec as P

LANES = 128
SUB = 8
UNROLL = 16
looped = functools.partial(lax.fori_loop, unroll=UNROLL)
MESH = pl.DeviceIdType.MESH
bone_stiff = 1.0
soft_stiff = 0.1


def kernel_wide(nw, nn, r_hbm, occ_hbm, reg_hbm, ci_hbm,
           z0_v, z1_v, r_v, az_v, y_v, sc_v,
            occ_v, reg_v, c_v, k_p, kx, kym, kyp, kzm, kzp, dg, invd,
           z_p, v_p, zy, vy,
           ix_in, iy_send, iy_in, c_in, wx_send, wx_in, wy_send, wy_in,
           row_send, rows, load_sem, hs_send, hs_recv, ag_send, ag_recv):
    X, Y, Z = occ_v.shape
    ncr, NC = c_v.shape
    G = ncr // 3
    ND = nw * nn
    wi = lax.axis_index("wide")
    ni = lax.axis_index("narrow")
    me = wi * nn + ni
    f32 = jnp.float32

    loads = [pltpu.make_async_copy(s, d, load_sem.at[i]) for i, (s, d) in enumerate(
        ((occ_hbm, occ_v), (reg_hbm, reg_v), (r_hbm, r_v), (ci_hbm, c_v)))]
    for l in loads:
        l.start()

    def peer(i):
        t = lax.rem(me + i, ND)
        return (t // nn, lax.rem(t, nn))

    barrier = pltpu.get_barrier_semaphore()

    def greet(i, _):
        pl.semaphore_signal(barrier, inc=1, device_id=peer(i), device_id_type=MESH)
        return 0

    lax.fori_loop(1, ND, greet, 0, unroll=ND <= 64)

    has = (wi > 0, wi < nw - 1, ni > 0, ni < nn - 1)
    to = ((wi - 1, ni), (wi + 1, ni), (wi, ni - 1), (wi, ni + 1))

    for d in range(4):
        @pl.when(jnp.logical_not(has[d]))
        def _():
            c_in[d] = jnp.zeros((ncr, NC), f32)
            for p in range(2):
                if d < 2:
                    wx_in[p, d] = jnp.zeros((3, Y, Z), f32)
                else:
                    wy_in[p, d - 2] = jnp.zeros((3, X, Z), f32)
            if d < 2:
                ix_in[d] = jnp.zeros((2, Y, Z), jnp.int32)
            else:
                iy_in[d - 2] = jnp.zeros((2, X, Z), jnp.int32)

    loads[0].wait()
    loads[1].wait()

    def pack_ints(x, _):
        iy_send[0, 0, pl.ds(x, 1), :] = occ_v[x, 0:1, :]
        iy_send[1, 0, pl.ds(x, 1), :] = occ_v[x, Y - 1:Y, :]
        iy_send[0, 1, pl.ds(x, 1), :] = reg_v[x, 0:1, :]
        iy_send[1, 1, pl.ds(x, 1), :] = reg_v[x, Y - 1:Y, :]
        return 0

    looped(0, X, pack_ints, 0)

    def fold(a):
        return jnp.sum(a.reshape(Y // SUB, SUB, Z), axis=0)

    def zero_acc(n):
        return tuple(jnp.zeros((SUB, Z), f32) for _ in range(n))

    def add_rc(acc, reg, u):
        out = list(acc)
        for g in range(G):
            m = reg == g
            for c in range(3):
                out[g * 3 + c] = acc[g * 3 + c] + fold(jnp.where(m, u[c], 0.0))
        return tuple(out)

    base = (me * ncr) % LANES

    def make_row(p, acc, first):
        a = jnp.concatenate([jnp.sum(b, axis=0, keepdims=True) for b in acc], axis=0)
        col = jnp.sum(a, axis=1, keepdims=True)
        n = len(acc)
        k = lax.broadcasted_iota(jnp.int32, (n, LANES), 0)
        lane = lax.broadcasted_iota(jnp.int32, (n, LANES), 1)
        target = (base + first + k) & (LANES - 1)
        row = jnp.sum(jnp.where(lane == target, col, 0.0), axis=0, keepdims=True)
        row_send[p, 0:1, :] = row
        rows[p, pl.ds(me, 1), :] = row

    def gather_start(p):
        def send(i, _):
            pltpu.make_async_remote_copy(
                src_ref=row_send.at[p, pl.ds(0, 1)], dst_ref=rows.at[p, pl.ds(me, 1)],
                send_sem=ag_send.at[p], recv_sem=ag_recv.at[p],
                device_id=peer(i), device_id_type=MESH).start()
            return 0
        lax.fori_loop(1, ND, send, 0, unroll=ND <= 64)

    def gather_wait(p, sem):
        part = rows.at[p, pl.ds(0, ND - 1)]
        pltpu.make_async_copy(part, part, sem.at[p]).wait()

    def coarse_vector(p):
        tiles = []
        for t in range(NC // LANES):
            lo = (LANES * t) // ncr // SUB * SUB
            hi = min(ND, -(-(-(-(LANES * (t + 1)) // ncr)) // SUB) * SUB)
            d = lax.broadcasted_iota(jnp.int32, (hi - lo, LANES), 0) + lo
            j = lax.broadcasted_iota(jnp.int32, (hi - lo, LANES), 1) + LANES * t
            m = (j >= d * ncr) & (j < d * ncr + ncr)
            tiles.append(jnp.sum(jnp.where(m, rows[p, lo:hi, :], 0.0), axis=0, keepdims=True))
        return tiles

    def total(p, s):
        d = lax.broadcasted_iota(jnp.int32, (ND, LANES), 0)
        lane = lax.broadcasted_iota(jnp.int32, (ND, LANES), 1)
        m = lane == ((d * ncr + ncr + s) & (LANES - 1))
        v = jnp.sum(jnp.where(m, rows[p], 0.0), axis=0, keepdims=True)
        return jnp.sum(v, axis=1, keepdims=True)

    def answers(tiles, ref):
        s = ref[:, 0:LANES] * tiles[0]
        for t in range(1, len(tiles)):
            s = s + ref[:, t * LANES:(t + 1) * LANES] * tiles[t]
        q = jnp.sum(s, axis=1, keepdims=True)
        return [q[i:i + 1, :] for i in range(ncr)]

    def spread(reg, q):
        masks = [reg == g for g in range(G)]
        out = []
        for c in range(3):
            s = jnp.zeros(reg.shape, f32)
            for g in range(G):
                s = jnp.where(masks[g], q[g * 3 + c], s)
            out.append(s)
        return out

    def halo(slot, d, src, dst):
        return pltpu.make_async_remote_copy(
            src_ref=src, dst_ref=dst, send_sem=hs_send.at[slot, d],
            recv_sem=hs_recv.at[slot, d ^ 1], device_id=to[d], device_id_type=MESH)

    def copies(kind, d):
        e = d ^ 1
        if kind == 0:
            if d < 2:
                x = 0 if d == 0 else X - 1
                return [halo(0, d, occ_v.at[x], ix_in.at[e, 0]),
                        halo(1, d, reg_v.at[x], ix_in.at[e, 1])]
            return [halo(0, d, iy_send.at[d - 2, 0], iy_in.at[e - 2, 0]),
                    halo(1, d, iy_send.at[d - 2, 1], iy_in.at[e - 2, 1])]
        if kind == 1:
            return [halo(2, d, c_v, c_in.at[e])]
        p = kind - 2
        if d < 2:
            return [halo(3 + p, d, wx_send.at[p, d], wx_in.at[p, e])]
        return [halo(3 + p, d, wy_send.at[p, d - 2], wy_in.at[p, e - 2])]

    def halo_start(kind):
        for d in range(4):
            @pl.when(has[d])
            def _():
                for c in copies(kind, d):
                    c.start()

    def halo_wait(kind):
        for d in range(4):
            @pl.when(has[d])
            def _():
                for c in copies(kind, d ^ 1):
                    c.wait_recv()

    def halo_done(kind):
        for d in range(4):
            @pl.when(has[d])
            def _():
                for c in copies(kind, d):
                    c.wait_send()

    loads[2].wait()
    acc = looped(0, X, lambda x, a: add_rc(a, reg_v[x], [r_v[c, x] for c in range(3)]),
                        zero_acc(ncr))
    make_row(0, acc, 0)
    loads[3].wait()

    pl.semaphore_wait(barrier, ND - 1)
    halo_start(0)
    gather_start(0)
    halo_start(1)

    def stiff_of(o):
        return soft_stiff + (bone_stiff - soft_stiff) * o.astype(f32)

    def own_k(x, _):
        k_p[x + 1] = stiff_of(occ_v[x])
        return 0

    looped(0, X, own_k, 0)
    halo_wait(0)
    for d in range(2):
        @pl.when(has[d])
        def _():
            k_p[0 if d == 0 else X + 1] = stiff_of(ix_in[d, 0])

        @pl.when(jnp.logical_not(has[d]))
        def _():
            k_p[0 if d == 0 else X + 1] = jnp.zeros((Y, Z), f32)

    row_id = lax.broadcasted_iota(jnp.int32, (Y, Z), 0)
    lane_id = lax.broadcasted_iota(jnp.int32, (Y, Z), 1)
    side_lo = jnp.where(has[2], 1.0, 0.0).astype(f32)
    side_hi = jnp.where(has[3], 1.0, 0.0).astype(f32)

    def yshift(u, lo, hi):
        down = jnp.where(row_id == 0, lo, pltpu.roll(u, 1, 0))
        up = jnp.where(row_id == Y - 1, hi, pltpu.roll(u, Y - 1, 0))
        return down, up

    def save_faces(p, x, w):
        for c in range(3):
            wy_send[p, 0, c, pl.ds(x, 1), :] = w[c][0:1, :]
            wy_send[p, 1, c, pl.ds(x, 1), :] = w[c][Y - 1:Y, :]

    def coefficients(x, _):
        k = k_p[x + 1]
        lo = stiff_of(iy_in[0, 0, pl.ds(x, 1), :]) * side_lo
        hi = stiff_of(iy_in[1, 0, pl.ds(x, 1), :]) * side_hi
        down, up = yshift(k, lo, hi)
        back = jnp.where(lane_id == 0, 0.0, pltpu.roll(k, 1, 1))
        ahead = jnp.where(lane_id == Z - 1, 0.0, pltpu.roll(k, Z - 1, 1))
        xm = 0.5 * (k + k_p[x])
        xp = 0.5 * (k + k_p[x + 2])
        ym = 0.5 * (k + down)
        yp = 0.5 * (k + up)
        zm = 0.5 * (k + back)
        zp = 0.5 * (k + ahead)
        diag = xm + xp + ym + yp + zm + zp + 0.5 * k
        inv = 1.0 / diag
        kx[x] = xm
        kx[x + 1] = xp
        kym[x] = ym
        kyp[x] = yp
        kzm[x] = jnp.where(lane_id == 0, 0.0, zm)
        kzp[x] = jnp.where(lane_id == Z - 1, 0.0, zp)
        dg[x] = diag - 0.25 * k
        invd[x] = inv
        w = [r_v[c, x] * inv for c in range(3)]
        for c in range(3):
            z_p[c, x + 1] = w[c]
        save_faces(0, x, w)
        return 0

    looped(0, X, coefficients, 0)
    for c in range(3):
        wx_send[0, 0, c] = z_p[c, 1]
        wx_send[0, 1, c] = z_p[c, X]
    halo_start(2)

    def edges(p, qs, pad, side):
        for d in range(2):
            s = spread(ix_in[d, 1], qs[d])
            for c in range(3):
                pad[c, 0 if d == 0 else X + 1] = wx_in[p, d, c] + s[c]
        for d in range(2):
            s = spread(iy_in[d, 1], qs[2 + d])
            for c in range(3):
                side[d, c] = wy_in[p, d, c] + s[c]

    def operate(pad, side, x):
        k = k_p[x + 1]
        u = [pad[c, x + 1] for c in range(3)]
        k4 = 0.25 * k * (u[0] + u[1] + u[2])
        out = []
        for c in range(3):
            down, up = yshift(u[c], side[0, c, pl.ds(x, 1), :], side[1, c, pl.ds(x, 1), :])
            a = dg[x] * u[c] + k4
            a = a - (kx[x] * pad[c, x] + kx[x + 1] * pad[c, x + 2])
            a = a - (kym[x] * down + kyp[x] * up)
            a = a - (kzm[x] * pltpu.roll(u[c], 1, 1) + kzp[x] * pltpu.roll(u[c], Z - 1, 1))
            out.append(a)
        return u, out

    gather_wait(0, ag_recv)
    halo_wait(1)
    tiles = coarse_vector(0)
    q = answers(tiles, c_v)
    qs = [answers(tiles, c_in.at[d]) for d in range(4)]

    def add_spread(x, _):
        s = spread(reg_v[x], q)
        for c in range(3):
            z = z_p[c, x + 1] + s[c]
            z_p[c, x + 1] = z
            z0_v[c, x] = z
        return 0

    looped(0, X, add_spread, 0)
    halo_wait(2)
    edges(0, qs, z_p, zy)

    def dots(a, b):
        return fold(a[0] * b[0] + a[1] * b[1] + a[2] * b[2])

    def first(x, carry):
        u, a = operate(z_p, zy, x)
        r = [r_v[c, x] for c in range(3)]
        w = []
        for c in range(3):
            y_v[c, x] = a[c]
            w.append(a[c] * invd[x])
            v_p[c, x + 1] = w[c]
        save_faces(1, x, w)
        acc = add_rc(carry[:ncr], reg_v[x], a)
        return acc + (carry[ncr] + dots(r, u), carry[ncr + 1] + dots(a, u))

    acc = looped(0, X, first, zero_acc(ncr + 2))
    make_row(1, acc, 0)
    gather_start(1)
    for c in range(3):
        wx_send[1, 0, c] = v_p[c, 1]
        wx_send[1, 1, c] = v_p[c, X]
    halo_start(3)
    halo_wait(3)
    gather_wait(1, ag_recv)
    tiles = coarse_vector(1)
    q = answers(tiles, c_v)
    qs = [answers(tiles, c_in.at[d]) for d in range(4)]
    rz0 = total(1, 0)
    alpha0 = rz0 / total(1, 1)

    def add_spread_v(x, _):
        s = spread(reg_v[x], q)
        for c in range(3):
            v_p[c, x + 1] = v_p[c, x + 1] + s[c]
        return 0

    looped(0, X, add_spread_v, 0)
    edges(1, qs, v_p, vy)

    def second(x, carry):
        u, a = operate(v_p, vy, x)
        r, z, az = [], [], []
        for c in range(3):
            y = y_v[c, x]
            r.append(r_v[c, x] - alpha0 * y)
            z.append(z_p[c, x + 1] - alpha0 * u[c])
            az.append(y - alpha0 * a[c])
            r_v[c, x] = r[c]
            z1_v[c, x] = z[c]
            az_v[c, x] = az[c]
        return (carry[0] + dots(r, z), carry[1] + dots(az, z))

    acc = looped(0, X, second, zero_acc(2))
    make_row(2, acc, ncr)
    gather_start(2)
    gather_wait(2, ag_recv)
    rz1 = total(2, 0)
    beta = rz1 / rz0
    alpha1 = rz1 / (total(2, 1) - beta * rz1 / alpha0)
    along = alpha0 + alpha1 * beta
    a1b = alpha1 * beta

    sc_v[0:1, :] = jnp.broadcast_to(along, (1, LANES))
    sc_v[1:2, :] = jnp.broadcast_to(alpha1, (1, LANES))
    sc_v[2:3, :] = jnp.broadcast_to(a1b, (1, LANES))
    for kind in range(4):
        halo_done(kind)
    for p in range(3):
        gather_wait(p, ag_send)


def finish_wide(z0_v, z1_v, r_v, az_v, y_v, sc_v, x_out, res_out, xb, rb, sem):
    along = sc_v[0:1, 0:1]
    alpha1 = sc_v[1:2, 0:1]
    a1b = sc_v[2:3, 0:1]
    X = z0_v.shape[1]
    copies = []
    for c in range(3):
        for x in range(X):
            xb[c, x] = along * z0_v[c, x] + alpha1 * z1_v[c, x]
            rb[c, x] = r_v[c, x] - alpha1 * az_v[c, x] - a1b * y_v[c, x]
        for n, (src, dst) in enumerate(((xb, x_out), (rb, res_out))):
            copies.append(pltpu.make_async_copy(src.at[c], dst.at[c], sem.at[n, c]))
            copies[-1].start()
    for copy in copies:
        copy.wait()


def local_wide(nw, nn, right_side, occupancy, region, coarse_inverse):
    _, X, Y, Z = right_side.shape
    ncr, NC = coarse_inverse.shape
    ND = nw * nn
    f32, i32 = jnp.float32, jnp.int32
    V = pltpu.VMEM
    field, pad, scal = (3, X, Y, Z), (3, X + 2, Y, Z), (X, Y, Z)
    scratch = [
        V(scal, i32), V(scal, i32), V((ncr, NC), f32),
        V((X + 2, Y, Z), f32), V((X + 1, Y, Z), f32),
        V(scal, f32), V(scal, f32), V(scal, f32), V(scal, f32), V(scal, f32), V(scal, f32),
        V(pad, f32), V(pad, f32),
        V((2, 3, X, Z), f32), V((2, 3, X, Z), f32),
        V((2, 2, Y, Z), i32), V((2, 2, X, Z), i32), V((2, 2, X, Z), i32),
        V((4, ncr, NC), f32),
        V((2, 2, 3, Y, Z), f32), V((2, 2, 3, Y, Z), f32),
        V((2, 2, 3, X, Z), f32), V((2, 2, 3, X, Z), f32),
        V((3, SUB, LANES), f32), V((3, ND, LANES), f32),
        pltpu.SemaphoreType.DMA((4,)),
        pltpu.SemaphoreType.DMA((5, 4)), pltpu.SemaphoreType.DMA((5, 4)),
        pltpu.SemaphoreType.DMA((3,)), pltpu.SemaphoreType.DMA((3,)),
    ]
    parts = pl.pallas_call(
        functools.partial(kernel_wide, nw, nn),
        out_shape=(V(field, f32),) * 5 + (V((SUB, LANES), f32),),
        in_specs=[pl.BlockSpec(memory_space=pltpu.HBM)] * 4,
        out_specs=(pl.BlockSpec(memory_space=pltpu.VMEM),) * 6,
        scratch_shapes=scratch,
        compiler_params=pltpu.CompilerParams(collective_id=0, has_side_effects=True, vmem_limit_bytes=32 * 1024 * 1024),
    )(*[pltpu.with_memory_space_constraint(a, pltpu.HBM) for a in (right_side, occupancy, region, coarse_inverse)])
    return pl.pallas_call(
        finish_wide,
        out_shape=(jax.ShapeDtypeStruct(field, f32),) * 2,
        in_specs=[pl.BlockSpec(memory_space=pltpu.VMEM)] * 6,
        out_specs=(pl.BlockSpec(memory_space=pltpu.HBM),) * 2,
        scratch_shapes=[V(field, f32), V(field, f32), pltpu.SemaphoreType.DMA((2, 3))],
        compiler_params=pltpu.CompilerParams(vmem_limit_bytes=16 * 1024 * 1024),
    )(*parts)


REPLICATED_BYTES = 4 * 1024 * 1024
DEEP = 3
AROUND = ((-1, 0), (1, 0), (0, -1), (0, 1), (-1, -1), (-1, 1), (1, -1), (1, 1))
BACK = tuple(AROUND.index((-a, -b)) for a, b in AROUND)


def group_of(n):
    return max(d for d in range(1, n + 1) if n % d == 0 and d * d <= n)


def spread_over(reg, q, G):
    masks = [reg == g for g in range(G)]
    out = []
    for c in range(3):
        s = jnp.zeros(reg.shape, jnp.float32)
        for g in range(G):
            s = jnp.where(masks[g], q[g * 3 + c], s)
        out.append(s)
    return out


def stencil(u, prev, after, faces, x, rows):
    kx, kym, kyp, kzm, kzp = faces
    YE, Z = u.shape
    low, high = pltpu.roll(u, 1, 0)[0:rows], pltpu.roll(u, YE - 1, 0)[0:rows]
    v = u[0:rows]
    a = kx[x, 0:rows] * prev[0:rows] + kx[x + 1, 0:rows] * after[0:rows]
    a = a + (kym[x, 0:rows] * low + kyp[x, 0:rows] * high)
    return a + (kzm[x, 0:rows] * pltpu.roll(v, 1, 1) + kzp[x, 0:rows] * pltpu.roll(v, Z - 1, 1))


def kernel(nw, nn, r_hbm, occ_hbm, reg_hbm, ci_hbm,
           z_o, g_o, r_o, y_o, ag_o, reg_o, k4, dg, kx, kym, kyp, kzm, kzp, q_o, sc_o,
           occ_e, reg_e, r_e, k_e, invd, z_e, g_e,
           call, c_in, y_face, y_label, qpair, row_send, rows, sizes,
           load_sem, send, recv, ready):
    E, YE, Z = occ_e.shape
    X, Y = E - 2 * DEEP, YE - SUB
    ncr, NC = c_in.shape[1:]
    G = ncr // 3
    ND = nw * nn
    NH = ND // 2
    wi = lax.axis_index("wide")
    ni = lax.axis_index("narrow")
    me = wi * nn + ni
    f32 = jnp.float32
    GW = group_of(nw)
    GP = GW * nn
    NG = ND // GP
    grp, pos = me // GP, lax.rem(me, GP)
    half, place = lax.rem(wi, 2), (lax.rem(wi, GW) // 2) * nn + ni
    here = half * NH + place * NG + grp
    own = pl.ds(DEEP, X)

    loads = [pltpu.make_async_copy(s, d, load_sem.at[i]) for s, d, i in (
        (reg_hbm, reg_e.at[own, pl.ds(0, Y)], 0), (r_hbm, r_e.at[:, own, pl.ds(0, Y)], 0),
        (occ_hbm, occ_e.at[own, pl.ds(0, Y)], 1), (ci_hbm, call.at[here], 2))]
    for l in loads:
        l.start()

    barrier = pltpu.get_barrier_semaphore()

    def at(t):
        return (t // nn, lax.rem(t, nn))

    def wait_for(sem, count):
        @pl.when(count > 0)
        def _():
            pl.semaphore_wait(sem, count)

    def column_of(group):
        return (wi + (group - grp) * GW, ni)

    at_low = jnp.logical_and(lax.rem(wi, GW) == 0, wi > 0)
    at_high = jnp.logical_and(lax.rem(wi, GW) == GW - 1, wi < nw - 1)
    aside = 1 + jnp.where(ni > 0, 1, 0) + jnp.where(ni < nn - 1, 1, 0)

    def touching(ahead, signal):
        @pl.when(at_high if ahead > 0 else at_low)
        def _():
            for b in (-1, 0, 1):
                @pl.when(jnp.logical_and(ni + b >= 0, ni + b < nn))
                def _():
                    signal((wi + ahead, ni + b))

    def say(sem):
        return lambda device: pl.semaphore_signal(sem, inc=1, device_id=device, device_id_type=MESH)

    for i in range(1, GP):
        say(barrier)(at(grp * GP + lax.rem(pos + i, GP)))
    touching(1, say(barrier))
    touching(-1, say(barrier))
    for k in range(1, NG):
        @pl.when(grp + k < NG)
        def _():
            say(barrier)(column_of(grp + k))

    def tell():
        for k in range(1, NG):
            @pl.when(grp >= k)
            def _():
                say(ready.at[k - 1])(column_of(grp - k))

    def take(rows_of, sem):
        some = sizes.at[pl.ds(0, rows_of)]
        pltpu.make_async_copy(some, some, sem).wait()

    def take_c(blocks, sem):
        some = call.at[pl.ds(0, blocks)]
        pltpu.make_async_copy(some, some, sem).wait()

    def by_neighbours(wait):
        nx = jnp.where(wi > 0, 1, 0) + jnp.where(wi < nw - 1, 1, 0)
        ny = jnp.where(ni > 0, 1, 0) + jnp.where(ni < nn - 1, 1, 0)
        for a in ((1,) if nw == 2 else (1, 2)):
            for b in (range(min(nn, 2)) if nn == 1 else (1,) if nn == 2 else (1, 2)):
                @pl.when(jnp.logical_and(nx == a, ny == b))
                def _():
                    wait(a, b)

    def halo_rows(n, a, b):
        deep, corner, count = ((DEEP, 2, 1), (2, 1, 1), (2, 1, 3))[n]
        return count * (a * deep * Y + b * deep * X + a * b * corner * corner)

    has = []
    for a, b in AROUND:
        h = jnp.logical_and(wi + a >= 0, wi + a < nw)
        has.append(jnp.logical_and(h, jnp.logical_and(ni + b >= 0, ni + b < nn)))

    def part(arr, d, into):
        a, b = AROUND[d]
        deep = {0: DEEP, 1: 2, 2: 2}[arr] if a == 0 or b == 0 else {0: 2, 1: 1, 2: 1}[arr]
        if into:
            xs = {-1: (DEEP - deep, deep), 0: (DEEP, X), 1: (DEEP + X, deep)}[a]
            ys = {-1: (YE - deep, deep), 0: (0, Y), 1: (Y, deep)}[b]
        else:
            xs = {-1: (DEEP, deep), 0: (DEEP, X), 1: (DEEP + X - deep, deep)}[a]
            ys = {-1: (0, deep), 0: (0, Y), 1: (Y - deep, deep)}[b]
        xs, ys = pl.ds(*xs), pl.ds(*ys)
        return (slice(None), xs, ys) if arr == 2 else (xs, ys)

    fields = (occ_e, reg_e, r_e)
    for d in range(8):
        @pl.when(jnp.logical_not(has[d]))
        def _():
            for n, ref in enumerate(fields):
                where = part(n, d, True)
                v = ref[where]
                ref[where] = jnp.full(v.shape, (-1, -1, 0)[n], v.dtype)
            c_in[d] = jnp.zeros((ncr, NC), f32)

    wait_for(barrier, GP - 1 + grp + jnp.where(at_low, aside, 0) + jnp.where(at_high, aside, 0))
    tell()

    def fold(a):
        return jnp.sum(a.reshape(a.shape[0] // SUB, SUB, Z), axis=0)

    def zero_acc(n):
        return tuple(jnp.zeros((SUB, Z), f32) for _ in range(n))

    def add_rc(acc, reg, u):
        out = list(acc)
        for g in range(G):
            m = reg == g
            for c in range(3):
                out[g * 3 + c] = acc[g * 3 + c] + fold(jnp.where(m, u[c], 0.0))
        return out

    base = (me * ncr) % LANES

    def column(acc):
        a = jnp.concatenate([jnp.sum(b, axis=0, keepdims=True) for b in acc], axis=0)
        return jnp.sum(a, axis=1, keepdims=True)

    def make_row(p, acc):
        col = column(acc)
        n = len(acc)
        k = lax.broadcasted_iota(jnp.int32, (n, LANES), 0)
        lane = lax.broadcasted_iota(jnp.int32, (n, LANES), 1)
        target = (base + k) & (LANES - 1)
        row = jnp.sum(jnp.where(lane == target, col, 0.0), axis=0, keepdims=True)
        row_send[p, 0:1, :] = row
        rows[p, pl.ds(me, 1), :] = row

    def rows_to(p, count, t, out, sem):
        pltpu.make_async_remote_copy(
            src_ref=row_send.at[pl.ds(p, count), pl.ds(0, 1)], dst_ref=rows.at[pl.ds(p, count), pl.ds(me, 1)],
            send_sem=send.at[out], recv_sem=recv.at[sem],
            device_id=at(t), device_id_type=MESH).start()

    def each_peer(send):
        def body(i, _):
            send(lax.rem(me + i, ND))
            return 0
        lax.fori_loop(1, ND, body, 0, unroll=ND <= 64)

    take(4 * X * Y, load_sem.at[0])
    acc = looped(0, X, lambda x, a: tuple(add_rc(
        a, reg_e[x + DEEP, 0:Y], [r_e[c, x + DEEP, 0:Y] for c in range(3)])), zero_acc(ncr))
    make_row(0, acc)

    def inside(i, _):
        rows_to(0, 1, grp * GP + lax.rem(pos + i, GP), 0, 3)
        return 0

    lax.fori_loop(1, GP, inside, 0, unroll=GP <= 64)

    def halo(n, d):
        a, b = AROUND[d]
        e = BACK[d]
        return pltpu.make_async_remote_copy(
            src_ref=fields[n].at[part(n, d, False)], dst_ref=fields[n].at[part(n, e, True)],
            send_sem=send.at[0], recv_sem=recv.at[min(n, 1)],
            device_id=(wi + a, ni + b), device_id_type=MESH)

    def halo_c(d):
        a, b = AROUND[d]
        return pltpu.make_async_remote_copy(
            src_ref=call.at[here], dst_ref=c_in.at[BACK[d]],
            send_sem=send.at[1], recv_sem=recv.at[2],
            device_id=(wi + a, ni + b), device_id_type=MESH)

    loads[2].wait()
    loads[3].wait()

    for n in range(4):
        for d in range(8):
            @pl.when(has[d])
            def _():
                (halo_c(d) if n == 3 else halo(n, d)).start()

    def c_column(group):
        pltpu.make_async_remote_copy(
            src_ref=call.at[here], dst_ref=call.at[here],
            send_sem=send.at[2], recv_sem=recv.at[5],
            device_id=column_of(group), device_id_type=MESH).start()

    for k in range(1, NG):
        @pl.when(grp >= k)
        def _():
            c_column(grp - k)

    def c_group(block):
        for i in range(1, GP // 2):
            p = lax.rem(place + i, GP // 2)
            pltpu.make_async_remote_copy(
                src_ref=call.at[block], dst_ref=call.at[block],
                send_sem=send.at[2], recv_sem=recv.at[6],
                device_id=(grp * GW + (p // nn) * 2 + half, lax.rem(p, nn)), device_id_type=MESH).start()

    c_group(here)

    def stiff_of(o):
        return jnp.where(o < 0, 0.0, soft_stiff + (bone_stiff - soft_stiff) * o.astype(f32))

    n2 = G * G

    def pairs(acc, first, seconds):
        out = list(acc)
        for g in range(G):
            t = None
            for label, value in seconds:
                v = jnp.where(label == g, value, 0.0)
                t = v if t is None else t + v
            for h in range(G):
                out[h * G + g] = acc[h * G + g] + fold(jnp.where(first == h, t, 0.0))
        return out

    row16 = lax.broadcasted_iota(jnp.int32, (Y, Z), 0)
    lane16 = lax.broadcasted_iota(jnp.int32, (Y, Z), 1)

    def own_pairs(i, carry):
        x = i + DEEP
        k, reg = stiff_of(occ_e[x, 0:Y]), reg_e[x, 0:Y]
        later = jnp.minimum(i + 1, X - 1) + DEEP
        kx_in = jnp.where(i < X - 1, 0.5 * (k + stiff_of(occ_e[later, 0:Y])), 0.0)
        ky_in = jnp.where(row16 == Y - 1, 0.0, 0.5 * (k + pltpu.roll(k, Y - 1, 0)))
        kz_in = jnp.where(lane16 == Z - 1, 0.0, 0.5 * (k + pltpu.roll(k, Z - 1, 1)))
        acc = pairs(carry[:n2], reg, ((reg_e[later, 0:Y], kx_in), (pltpu.roll(reg, Y - 1, 0), ky_in),
                                      (pltpu.roll(reg, Z - 1, 1), kz_in)))
        sums = [carry[n2 + g] + fold(jnp.where(reg == g, 0.25 * k, 0.0)) for g in range(G)]
        return tuple(acc) + tuple(sums)

    own_acc = lax.fori_loop(0, X, own_pairs, zero_acc(n2 + G), unroll=2)
    own_col = column(own_acc)

    def c_up(k):
        @pl.when(grp + k < NG)
        def _():
            pl.semaphore_wait(ready.at[k - 1], 1)
            c_column(grp + k)

    for k in range(1, NG):
        c_up(k)

    take(GP - 1, recv.at[3])
    mine = rows.at[0, pl.ds(pl.multiple_of(grp * GP, GP), GP)]

    def across(group):
        pltpu.make_async_remote_copy(
            src_ref=mine, dst_ref=mine, send_sem=send.at[0], recv_sem=recv.at[4],
            device_id=column_of(group), device_id_type=MESH).start()

    for k in range(1, NG):
        @pl.when(grp >= k)
        def _():
            across(grp - k)

    for k in range(1, NG):
        @pl.when(grp + k < NG)
        def _():
            across(grp + k)

    by_neighbours(lambda a, b: take(halo_rows(0, a, b), recv.at[0]))

    lane_id = lax.broadcasted_iota(jnp.int32, (YE, Z), 1)

    def stiffness(x, _):
        k_e[x] = stiff_of(occ_e[x])
        return 0

    lax.fori_loop(0, E, stiffness, 0, unroll=True)
    row8 = lax.broadcasted_iota(jnp.int32, (SUB, Z), 0)

    def coefficients(x):
        k = k_e[x]
        low, high = pltpu.roll(k, 1, 0), pltpu.roll(k, YE - 1, 0)
        back = jnp.where(lane_id == 0, 0.0, pltpu.roll(k, 1, 1))
        ahead = jnp.where(lane_id == Z - 1, 0.0, pltpu.roll(k, Z - 1, 1))
        xm = 0.5 * (k + k_e[x - 1])
        xp = 0.5 * (k + k_e[x + 1])
        ym = 0.5 * (k + low)
        yp = 0.5 * (k + high)
        zm = 0.5 * (k + back)
        zp = 0.5 * (k + ahead)
        diag = xm + xp + ym + yp + zm + zp + 0.5 * k
        inv = jnp.where(k > 0.0, 1.0 / diag, 0.0)
        zp = jnp.where(lane_id == Z - 1, 0.0, zp)
        kx[x] = xm
        kx[x + 1] = xp
        kym[x] = ym
        kyp[x] = yp
        kzm[x] = jnp.where(lane_id == 0, 0.0, zm)
        kzp[x] = zp
        d = diag - 0.25 * k
        dg[x] = d
        k4[x] = 0.25 * k
        invd[x] = inv
        return d

    for x in (1, 2, DEEP + X, DEEP + X + 1):
        coefficients(x)

    def inner(i, sums):
        d = coefficients(i + DEEP)[0:Y]
        reg = reg_e[i + DEEP, 0:Y]
        return tuple(sums[g] + fold(jnp.where(reg == g, d, 0.0)) for g in range(G))

    sum_acc = lax.fori_loop(0, X, inner, zero_acc(G), unroll=4)

    by_neighbours(lambda a, b: take(halo_rows(1, a, b) + halo_rows(2, a, b), recv.at[1]))

    def side_rows(i, _):
        x = i + DEEP
        y_face[pl.ds(i, 1), :] = kyp[x, Y - 1:Y, :]
        y_label[0, pl.ds(i, 1), :] = reg_e[x, Y - 1:Y, :]
        y_label[1, pl.ds(i, 1), :] = reg_e[x, Y:Y + 1, :]
        return 0

    looped(0, X, side_rows, 0)
    top = DEEP + X - 1
    x_acc = pairs(zero_acc(n2), reg_e[top, 0:Y], ((reg_e[top + 1, 0:Y], kx[top + 1, 0:Y]),))
    y_acc = pairs(zero_acc(n2), y_label[0], ((y_label[1], y_face[...]),))
    rim_col = column(tuple(x_acc) + tuple(y_acc) + tuple(sum_acc))

    lane = lax.broadcasted_iota(jnp.int32, (n2, LANES), 1)
    pair = lax.broadcasted_iota(jnp.int32, (n2, LANES), 0)
    at_pair = jnp.logical_and(lane >= 3 * pair, lane < 3 * pair + 3)

    def lanes_of(col, mask):
        return jnp.sum(jnp.where(mask, col, 0.0), axis=0, keepdims=True)

    lane_g = lax.broadcasted_iota(jnp.int32, (G, LANES), 1)
    row_g = lax.broadcasted_iota(jnp.int32, (G, LANES), 0)
    diag_at, sum_at = 3 * (G + 1) * row_g, 3 * n2 + 9 * row_g
    at_diag = jnp.logical_and(lane_g >= diag_at, lane_g < diag_at + 3)
    at_sum = jnp.logical_and(lane_g >= sum_at, lane_g < sum_at + 9)
    ac_rows = (lanes_of(own_col[0:n2], at_pair) * -2.0 + lanes_of(rim_col[2 * n2:], at_diag)
               + lanes_of(own_col[n2:], at_sum),
               lanes_of(rim_col[0:n2], at_pair) * -2.0, lanes_of(rim_col[n2:2 * n2], at_pair) * -2.0)
    for n in range(3):
        row_send[n + 2, 0:1, :] = ac_rows[n]
        rows[n + 2, pl.ds(me, 1), :] = ac_rows[n]

    def coarse_vector(block):
        tiles = []
        for t in range(NC // LANES):
            lo = (LANES * t) // ncr // SUB * SUB
            hi = min(ND, -(-(-(-(LANES * (t + 1)) // ncr)) // SUB) * SUB)
            d = lax.broadcasted_iota(jnp.int32, (hi - lo, LANES), 0) + lo
            j = lax.broadcasted_iota(jnp.int32, (hi - lo, LANES), 1) + LANES * t
            m = (j >= d * ncr) & (j < d * ncr + ncr)
            tiles.append(jnp.sum(jnp.where(m, block[lo:hi, :], 0.0), axis=0, keepdims=True))
        return tiles

    def total(block, s):
        d = lax.broadcasted_iota(jnp.int32, (ND, LANES), 0)
        lane = lax.broadcasted_iota(jnp.int32, (ND, LANES), 1)
        m = lane == ((d * ncr + ncr + s) & (LANES - 1))
        v = jnp.sum(jnp.where(m, block, 0.0), axis=0, keepdims=True)
        return jnp.sum(v, axis=1, keepdims=True)

    def solve(tiles, block):
        s = block[:, 0:LANES] * tiles[0]
        for t in range(1, len(tiles)):
            s = s + block[:, t * LANES:(t + 1) * LANES] * tiles[t]
        return jnp.sum(s, axis=1, keepdims=True)

    def as_list(q):
        return [q[i:i + 1, :] for i in range(ncr)]

    take_c(NG - 1, recv.at[5])
    for k in range(1, NG):
        c_group(half * NH + place * NG + lax.rem(grp + k, NG))

    take(ND - GP, recv.at[4])
    by_neighbours(lambda a, b: take_c(a + b + a * b, recv.at[2]))
    tiles = coarse_vector(rows[0])
    q = as_list(solve(tiles, call[here]))
    qn = [as_list(solve(tiles, c_in[d])) for d in range(8)]

    def either(hi, lo):
        return [jnp.where(row8 < SUB // 2, a, b) for a, b in zip(hi, lo)]

    def add_spread(x, q_in, q_out):
        s = spread_over(reg_e[x, 0:Y], q_in, G)
        t = spread_over(reg_e[x, Y:YE], q_out, G)
        inv = invd[x]
        reg_o[x] = reg_e[x]
        for c in range(3):
            z_e[c, x, 0:Y] = r_e[c, x, 0:Y] * inv[0:Y] + s[c]
            z_e[c, x, Y:YE] = r_e[c, x, Y:YE] * inv[Y:YE] + t[c]

    q_side = either(qn[3], qn[2])

    def spread_own(i, _):
        add_spread(i + DEEP, q, q_side)
        return 0

    looped(0, X, spread_own, 0)
    q_low, q_high = either(qn[5], qn[4]), either(qn[7], qn[6])
    for x in (1, 2):
        add_spread(x, qn[0], q_low)
    for x in (DEEP + X, DEEP + X + 1):
        add_spread(x, qn[1], q_high)

    faces = (kx, kym, kyp, kzm, kzp)

    def apply(ref, x, rows_):
        u = [ref[c, x] for c in range(3)]
        kk = k4[x, 0:rows_] * (u[0] + u[1] + u[2])[0:rows_]
        return u, [dg[x, 0:rows_] * u[c][0:rows_] + kk
                   - stencil(u[c], ref[c, x - 1], ref[c, x + 1], faces, x, rows_) for c in range(3)]

    def dots(a, b):
        return fold(a[0] * b[0] + a[1] * b[1] + a[2] * b[2])

    for x in (DEEP - 1, DEEP + X):
        _, a = apply(z_e, x, YE)
        for c in range(3):
            g_e[c, x] = a[c] * invd[x]

    def first(i, carry):
        x = i + DEEP
        u, a = apply(z_e, x, YE)
        w = []
        for c in range(3):
            w.append(a[c] * invd[x])
            g_e[c, x] = w[c]
        y = [a[c][0:Y] for c in range(3)]
        u = [u[c][0:Y] for c in range(3)]
        w = [w[c][0:Y] for c in range(3)]
        r = [r_e[c, x, 0:Y] for c in range(3)]
        for c in range(3):
            y_o[c, i] = y[c]
            z_o[c, i] = u[c]
            g_o[c, i] = w[c]
            r_o[c, i] = r[c]
        acc = add_rc(carry[:ncr], reg_e[x, 0:Y], y)
        return tuple(acc) + (carry[ncr] + dots(r, u), carry[ncr + 1] + dots(y, u), carry[ncr + 2] + dots(y, w))

    acc1 = lax.fori_loop(0, X, first, zero_acc(ncr + 3), unroll=4)

    def second(i, carry):
        x = i + DEEP
        w, a = apply(g_e, x, Y)
        for c in range(3):
            ag_o[c, i] = a[c]
        acc = add_rc(carry[:ncr], reg_e[x, 0:Y], a)
        return tuple(acc) + (carry[ncr] + dots([v[0:Y] for v in w], a),)

    acc2 = lax.fori_loop(0, X, second, zero_acc(ncr + 1), unroll=4)
    make_row(1, tuple(acc1) + (acc2[ncr],) + tuple(acc2[:ncr]))
    each_peer(lambda t: rows_to(1, 4, t, 3, 7))

    take_c((GP // 2 - 1) * NG, recv.at[6])
    swap_half = call.at[pl.ds(half * NH, NH)]
    swap = pltpu.make_async_remote_copy(
        src_ref=swap_half, dst_ref=swap_half, send_sem=send.at[2], recv_sem=recv.at[8],
        device_id=(wi + 1 - 2 * half, ni), device_id_type=MESH)
    swap.start()
    by_neighbours(lambda a, b: take(
        sum(halo_rows(n, a, b) for n in range(3)) + GP - 1 + (NG - 1) * GP, send.at[0]))
    by_neighbours(lambda a, b: take_c(a + b + a * b, send.at[1]))
    swap.wait_recv()
    take(4 * (ND - 1), recv.at[7])

    block = rows[1]
    b1 = coarse_vector(block)
    h1 = coarse_vector(pltpu.roll(block, LANES - ncr - 4, 1))
    rr = lax.broadcasted_iota(jnp.int32, (ncr, LANES), 0)
    ll = lax.broadcasted_iota(jnp.int32, (ncr, LANES), 1)
    m0, m1 = rr < 0, rr < 0
    for h in range(G):
        for g in range(G):
            for c in range(3):
                k = (h * G + g) * 3 + c
                m0 = jnp.logical_or(m0, (ll == k) & (rr == h * 3 + c))
                m1 = jnp.logical_or(m1, (ll == k) & (rr == g * 3 + c))
        for c in range(3):
            for e in range(3):
                k = 3 * n2 + h * 9 + c * 3 + e
                m0 = jnp.logical_or(m0, (ll == k) & (rr == h * 3 + c))
                m1 = jnp.logical_or(m1, (ll == k) & (rr == h * 3 + e))
    lines = [jnp.zeros((1, LANES), f32) for _ in b1]
    for w in range(nw):
        for n in range(nn):
            d = w * nn + n
            q1 = solve(b1, call[w % 2 * NH + ((w % GW) // 2 * nn + n) * NG + w // GW])
            qpair[0, d:d + 1, :] = jnp.sum(jnp.where(m0, q1, 0.0), axis=0, keepdims=True)
            qpair[1, d:d + 1, :] = jnp.sum(jnp.where(m1, q1, 0.0), axis=0, keepdims=True)
            for t in range(d * ncr // LANES, (d * ncr + ncr - 1) // LANES + 1):
                lines[t] = lines[t] + jnp.sum(jnp.where(ll + LANES * t == rr + d * ncr, q1, 0.0), axis=0, keepdims=True)
    first_q, second_q = qpair[0], qpair[1]
    dev = lax.broadcasted_iota(jnp.int32, (ND, LANES), 0)
    next_x = jnp.where(dev < ND - nn, pltpu.roll(second_q, ND - nn, 0), 0.0)
    next_y = jnp.where(dev < ND - 1, pltpu.roll(second_q, ND - 1, 0), 0.0)
    energy = jnp.sum(first_q * (rows[2] * second_q + rows[3] * next_x + rows[4] * next_y), axis=0, keepdims=True)
    for t in range(len(b1)):
        energy = energy + 2.0 * h1[t] * lines[t]
    yv = b1[0] * lines[0]
    for t in range(1, len(b1)):
        yv = yv + b1[t] * lines[t]
    yv = total(block, 2) + jnp.sum(yv, axis=1, keepdims=True)
    vav = total(block, 3) + jnp.sum(energy, axis=1, keepdims=True)
    rz0, zy = total(block, 0), total(block, 1)
    alpha0 = rz0 / zy
    rz1 = alpha0 * alpha0 * yv - rz0
    zaz = zy - 2.0 * alpha0 * yv + alpha0 * alpha0 * vav
    beta = rz1 / rz0
    alpha1 = rz1 / (zaz - beta * rz1 / alpha0)
    a1b = alpha1 * beta
    for n, v in enumerate((alpha0 + a1b + alpha1, alpha1 * alpha0)):
        sc_o[n:n + 1, :] = jnp.broadcast_to(v, (1, LANES))
    q_o[0] = jnp.broadcast_to(solve(b1, call[here]), (ncr, LANES))
    for d in range(4):
        q_o[d + 1] = jnp.broadcast_to(solve(b1, c_in[d]), (ncr, LANES))

    take(4 * (ND - 1), send.at[3])
    take_c(NG - 1 + (GP // 2 - 1) * NG + NH, send.at[2])


def finish(z_v, g_v, r_v, y_v, ag_v, reg_v, k4, dg, kx, kym, kyp, kzm, kzp, q_v, sc_v, x_out, res_out, s_e, xb, rb, sem):
    a, b = sc_v[0:1, 0:1], sc_v[1:2, 0:1]
    E, YE, Z = reg_v.shape
    X, Y = E - 2 * DEEP, YE - SUB
    G = q_v.shape[1] // 3
    row8 = lax.broadcasted_iota(jnp.int32, (SUB, Z), 0)
    q = [[q_v[d, i:i + 1, :] for i in range(3 * G)] for d in range(5)]
    side = [jnp.where(row8 < SUB // 2, hi, lo) for hi, lo in zip(q[4], q[3])]

    def fill(x, q_in):
        s = spread_over(reg_v[x, 0:Y], q_in, G)
        t = spread_over(reg_v[x, Y:YE], side, G)
        for c in range(3):
            s_e[c, x, 0:Y] = s[c]
            s_e[c, x, Y:YE] = t[c]

    def fill_own(i, _):
        fill(i + DEEP, q[0])
        return 0

    fill(DEEP - 1, q[1])
    fill(DEEP + X, q[2])
    looped(0, X, fill_own, 0)
    faces = (kx, kym, kyp, kzm, kzp)
    copies = []
    parts = 4
    step = X // parts

    def plane(i, _):
        x = i + DEEP
        u = [s_e[c, x] for c in range(3)]
        kk = k4[x, 0:Y] * (u[0] + u[1] + u[2])[0:Y]
        for c in range(3):
            av = ag_v[c, i] + (dg[x, 0:Y] * u[c][0:Y] + kk
                               - stencil(u[c], s_e[c, x - 1], s_e[c, x + 1], faces, x, Y))
            xb[c, i] = a * z_v[c, i] - b * (g_v[c, i] + u[c][0:Y])
            rb[c, i] = r_v[c, i] - a * y_v[c, i] + b * av
        return 0

    for n in range(parts):
        lax.fori_loop(n * step, (n + 1) * step, plane, 0, unroll=True)
        for m, (src, dst) in enumerate(((xb, x_out), (rb, res_out))):
            where = (slice(None), pl.ds(n * step, step))
            copies.append(pltpu.make_async_copy(src.at[where], dst.at[where], sem.at[m, n]))
            copies[-1].start()
    for copy in copies:
        copy.wait()


def local_fast(nw, nn, right_side, occupancy, region, coarse_inverse):
    _, X, Y, Z = right_side.shape
    ncr, NC = coarse_inverse.shape
    ND = nw * nn
    f32, i32 = jnp.float32, jnp.int32
    V = pltpu.VMEM
    E, YE = X + 2 * DEEP, Y + SUB
    field, ext, scal = (3, X, Y, Z), (3, E, YE, Z), (E, YE, Z)
    ng = nw // group_of(nw)
    DMA = pltpu.SemaphoreType.DMA
    scratch = [
        V(scal, i32), V(scal, i32), V(ext, f32), V(scal, f32), V(scal, f32), V(ext, f32), V(ext, f32),
        V((ND, ncr, NC), f32), V((8, ncr, NC), f32), V((X, Z), f32), V((2, X, Z), i32), V((2, ND, LANES), f32),
        V((5, SUB, LANES), f32), V((5, ND, LANES), f32), V((4 * X * Y, LANES), f32),
        DMA((3,)), DMA((4,)), DMA((9,)),
        pltpu.SemaphoreType.REGULAR((ng - 1,)),
    ]
    outs = (V(field, f32),) * 5 + (V(scal, i32),) + (V(scal, f32),) * 7 + (V((5, ncr, LANES), f32), V((SUB, LANES), f32))
    parts = pl.pallas_call(
        functools.partial(kernel, nw, nn),
        out_shape=outs,
        in_specs=[pl.BlockSpec(memory_space=pltpu.HBM)] * 4,
        out_specs=(pl.BlockSpec(memory_space=pltpu.VMEM),) * len(outs),
        scratch_shapes=scratch,
        compiler_params=pltpu.CompilerParams(collective_id=0, has_side_effects=True, vmem_limit_bytes=32 * 1024 * 1024),
    )(*[pltpu.with_memory_space_constraint(a, pltpu.HBM) for a in (right_side, occupancy, region, coarse_inverse)])
    return pl.pallas_call(
        finish,
        out_shape=(jax.ShapeDtypeStruct(field, f32),) * 2,
        in_specs=[pl.BlockSpec(memory_space=pltpu.VMEM)] * len(outs),
        out_specs=(pl.BlockSpec(memory_space=pltpu.HBM),) * 2,
        scratch_shapes=[V(ext, f32), V(field, f32), V(field, f32), DMA((2, 4))],
        compiler_params=pltpu.CompilerParams(vmem_limit_bytes=24 * 1024 * 1024),
    )(*parts)


def local(nw, nn, right_side, occupancy, region, coarse_inverse):
    nc = coarse_inverse.shape[1]
    run = local_fast if group_of(nw) % 2 == 0 and nc * nc * 4 <= REPLICATED_BYTES else local_wide
    return run(nw, nn, right_side, occupancy, region, coarse_inverse)


def solution(mesh):
    return jax.shard_map(
        functools.partial(local, mesh.shape["wide"], mesh.shape["narrow"]),
        mesh=mesh,
        in_specs=(
            P(None, "wide", "narrow", None),
            P("wide", "narrow", None),
            P("wide", "narrow", None),
            P(("wide", "narrow"), None),
        ),
        out_specs=(P(None, "wide", "narrow", None), P(None, "wide", "narrow", None)),
        check_vma=False,
    )
```

```python
import functools

import jax
import jax.numpy as jnp
from jax import lax
from jax.experimental import pallas as pl
from jax.experimental.pallas import tpu as pltpu
from jax.sharding import PartitionSpec as P

LANES = 128
SUB = 8
UNROLL = 16
looped = functools.partial(lax.fori_loop, unroll=UNROLL)
MESH = pl.DeviceIdType.MESH
bone_stiff = 1.0
soft_stiff = 0.1


def kernel_wide(nw, nn, r_hbm, occ_hbm, reg_hbm, ci_hbm,
           z0_v, z1_v, r_v, az_v, y_v, sc_v,
            occ_v, reg_v, c_v, k_p, kx, kym, kyp, kzm, kzp, dg, invd,
           z_p, v_p, zy, vy,
           ix_in, iy_send, iy_in, c_in, wx_send, wx_in, wy_send, wy_in,
           row_send, rows, load_sem, hs_send, hs_recv, ag_send, ag_recv):
    X, Y, Z = occ_v.shape
    ncr, NC = c_v.shape
    G = ncr // 3
    ND = nw * nn
    wi = lax.axis_index("wide")
    ni = lax.axis_index("narrow")
    me = wi * nn + ni
    f32 = jnp.float32

    loads = [pltpu.make_async_copy(s, d, load_sem.at[i]) for i, (s, d) in enumerate(
        ((occ_hbm, occ_v), (reg_hbm, reg_v), (r_hbm, r_v), (ci_hbm, c_v)))]
    for l in loads:
        l.start()

    def peer(i):
        t = lax.rem(me + i, ND)
        return (t // nn, lax.rem(t, nn))

    barrier = pltpu.get_barrier_semaphore()

    def greet(i, _):
        pl.semaphore_signal(barrier, inc=1, device_id=peer(i), device_id_type=MESH)
        return 0

    lax.fori_loop(1, ND, greet, 0, unroll=ND <= 64)

    has = (wi > 0, wi < nw - 1, ni > 0, ni < nn - 1)
    to = ((wi - 1, ni), (wi + 1, ni), (wi, ni - 1), (wi, ni + 1))

    for d in range(4):
        @pl.when(jnp.logical_not(has[d]))
        def _():
            c_in[d] = jnp.zeros((ncr, NC), f32)
            for p in range(2):
                if d < 2:
                    wx_in[p, d] = jnp.zeros((3, Y, Z), f32)
                else:
                    wy_in[p, d - 2] = jnp.zeros((3, X, Z), f32)
            if d < 2:
                ix_in[d] = jnp.zeros((2, Y, Z), jnp.int32)
            else:
                iy_in[d - 2] = jnp.zeros((2, X, Z), jnp.int32)

    loads[0].wait()
    loads[1].wait()

    def pack_ints(x, _):
        iy_send[0, 0, pl.ds(x, 1), :] = occ_v[x, 0:1, :]
        iy_send[1, 0, pl.ds(x, 1), :] = occ_v[x, Y - 1:Y, :]
        iy_send[0, 1, pl.ds(x, 1), :] = reg_v[x, 0:1, :]
        iy_send[1, 1, pl.ds(x, 1), :] = reg_v[x, Y - 1:Y, :]
        return 0

    looped(0, X, pack_ints, 0)

    def fold(a):
        return jnp.sum(a.reshape(Y // SUB, SUB, Z), axis=0)

    def zero_acc(n):
        return tuple(jnp.zeros((SUB, Z), f32) for _ in range(n))

    def add_rc(acc, reg, u):
        out = list(acc)
        for g in range(G):
            m = reg == g
            for c in range(3):
                out[g * 3 + c] = acc[g * 3 + c] + fold(jnp.where(m, u[c], 0.0))
        return tuple(out)

    base = (me * ncr) % LANES

    def make_row(p, acc, first):
        a = jnp.concatenate([jnp.sum(b, axis=0, keepdims=True) for b in acc], axis=0)
        col = jnp.sum(a, axis=1, keepdims=True)
        n = len(acc)
        k = lax.broadcasted_iota(jnp.int32, (n, LANES), 0)
        lane = lax.broadcasted_iota(jnp.int32, (n, LANES), 1)
        target = (base + first + k) & (LANES - 1)
        row = jnp.sum(jnp.where(lane == target, col, 0.0), axis=0, keepdims=True)
        row_send[p, 0:1, :] = row
        rows[p, pl.ds(me, 1), :] = row

    def gather_start(p):
        def send(i, _):
            pltpu.make_async_remote_copy(
                src_ref=row_send.at[p, pl.ds(0, 1)], dst_ref=rows.at[p, pl.ds(me, 1)],
                send_sem=ag_send.at[p], recv_sem=ag_recv.at[p],
                device_id=peer(i), device_id_type=MESH).start()
            return 0
        lax.fori_loop(1, ND, send, 0, unroll=ND <= 64)

    def gather_wait(p, sem):
        part = rows.at[p, pl.ds(0, ND - 1)]
        pltpu.make_async_copy(part, part, sem.at[p]).wait()

    def coarse_vector(p):
        tiles = []
        for t in range(NC // LANES):
            lo = (LANES * t) // ncr // SUB * SUB
            hi = min(ND, -(-(-(-(LANES * (t + 1)) // ncr)) // SUB) * SUB)
            d = lax.broadcasted_iota(jnp.int32, (hi - lo, LANES), 0) + lo
            j = lax.broadcasted_iota(jnp.int32, (hi - lo, LANES), 1) + LANES * t
            m = (j >= d * ncr) & (j < d * ncr + ncr)
            tiles.append(jnp.sum(jnp.where(m, rows[p, lo:hi, :], 0.0), axis=0, keepdims=True))
        return tiles

    def total(p, s):
        d = lax.broadcasted_iota(jnp.int32, (ND, LANES), 0)
        lane = lax.broadcasted_iota(jnp.int32, (ND, LANES), 1)
        m = lane == ((d * ncr + ncr + s) & (LANES - 1))
        v = jnp.sum(jnp.where(m, rows[p], 0.0), axis=0, keepdims=True)
        return jnp.sum(v, axis=1, keepdims=True)

    def answers(tiles, ref):
        s = ref[:, 0:LANES] * tiles[0]
        for t in range(1, len(tiles)):
            s = s + ref[:, t * LANES:(t + 1) * LANES] * tiles[t]
        q = jnp.sum(s, axis=1, keepdims=True)
        return [q[i:i + 1, :] for i in range(ncr)]

    def spread(reg, q):
        masks = [reg == g for g in range(G)]
        out = []
        for c in range(3):
            s = jnp.zeros(reg.shape, f32)
            for g in range(G):
                s = jnp.where(masks[g], q[g * 3 + c], s)
            out.append(s)
        return out

    def halo(slot, d, src, dst):
        return pltpu.make_async_remote_copy(
            src_ref=src, dst_ref=dst, send_sem=hs_send.at[slot, d],
            recv_sem=hs_recv.at[slot, d ^ 1], device_id=to[d], device_id_type=MESH)

    def copies(kind, d):
        e = d ^ 1
        if kind == 0:
            if d < 2:
                x = 0 if d == 0 else X - 1
                return [halo(0, d, occ_v.at[x], ix_in.at[e, 0]),
                        halo(1, d, reg_v.at[x], ix_in.at[e, 1])]
            return [halo(0, d, iy_send.at[d - 2, 0], iy_in.at[e - 2, 0]),
                    halo(1, d, iy_send.at[d - 2, 1], iy_in.at[e - 2, 1])]
        if kind == 1:
            return [halo(2, d, c_v, c_in.at[e])]
        p = kind - 2
        if d < 2:
            return [halo(3 + p, d, wx_send.at[p, d], wx_in.at[p, e])]
        return [halo(3 + p, d, wy_send.at[p, d - 2], wy_in.at[p, e - 2])]

    def halo_start(kind):
        for d in range(4):
            @pl.when(has[d])
            def _():
                for c in copies(kind, d):
                    c.start()

    def halo_wait(kind):
        for d in range(4):
            @pl.when(has[d])
            def _():
                for c in copies(kind, d ^ 1):
                    c.wait_recv()

    def halo_done(kind):
        for d in range(4):
            @pl.when(has[d])
            def _():
                for c in copies(kind, d):
                    c.wait_send()

    loads[2].wait()
    acc = looped(0, X, lambda x, a: add_rc(a, reg_v[x], [r_v[c, x] for c in range(3)]),
                        zero_acc(ncr))
    make_row(0, acc, 0)
    loads[3].wait()

    pl.semaphore_wait(barrier, ND - 1)
    halo_start(0)
    gather_start(0)
    halo_start(1)

    def stiff_of(o):
        return soft_stiff + (bone_stiff - soft_stiff) * o.astype(f32)

    def own_k(x, _):
        k_p[x + 1] = stiff_of(occ_v[x])
        return 0

    looped(0, X, own_k, 0)
    halo_wait(0)
    for d in range(2):
        @pl.when(has[d])
        def _():
            k_p[0 if d == 0 else X + 1] = stiff_of(ix_in[d, 0])

        @pl.when(jnp.logical_not(has[d]))
        def _():
            k_p[0 if d == 0 else X + 1] = jnp.zeros((Y, Z), f32)

    row_id = lax.broadcasted_iota(jnp.int32, (Y, Z), 0)
    lane_id = lax.broadcasted_iota(jnp.int32, (Y, Z), 1)
    side_lo = jnp.where(has[2], 1.0, 0.0).astype(f32)
    side_hi = jnp.where(has[3], 1.0, 0.0).astype(f32)

    def yshift(u, lo, hi):
        down = jnp.where(row_id == 0, lo, pltpu.roll(u, 1, 0))
        up = jnp.where(row_id == Y - 1, hi, pltpu.roll(u, Y - 1, 0))
        return down, up

    def save_faces(p, x, w):
        for c in range(3):
            wy_send[p, 0, c, pl.ds(x, 1), :] = w[c][0:1, :]
            wy_send[p, 1, c, pl.ds(x, 1), :] = w[c][Y - 1:Y, :]

    def coefficients(x, _):
        k = k_p[x + 1]
        lo = stiff_of(iy_in[0, 0, pl.ds(x, 1), :]) * side_lo
        hi = stiff_of(iy_in[1, 0, pl.ds(x, 1), :]) * side_hi
        down, up = yshift(k, lo, hi)
        back = jnp.where(lane_id == 0, 0.0, pltpu.roll(k, 1, 1))
        ahead = jnp.where(lane_id == Z - 1, 0.0, pltpu.roll(k, Z - 1, 1))
        xm = 0.5 * (k + k_p[x])
        xp = 0.5 * (k + k_p[x + 2])
        ym = 0.5 * (k + down)
        yp = 0.5 * (k + up)
        zm = 0.5 * (k + back)
        zp = 0.5 * (k + ahead)
        diag = xm + xp + ym + yp + zm + zp + 0.5 * k
        inv = 1.0 / diag
        kx[x] = xm
        kx[x + 1] = xp
        kym[x] = ym
        kyp[x] = yp
        kzm[x] = jnp.where(lane_id == 0, 0.0, zm)
        kzp[x] = jnp.where(lane_id == Z - 1, 0.0, zp)
        dg[x] = diag - 0.25 * k
        invd[x] = inv
        w = [r_v[c, x] * inv for c in range(3)]
        for c in range(3):
            z_p[c, x + 1] = w[c]
        save_faces(0, x, w)
        return 0

    looped(0, X, coefficients, 0)
    for c in range(3):
        wx_send[0, 0, c] = z_p[c, 1]
        wx_send[0, 1, c] = z_p[c, X]
    halo_start(2)

    def edges(p, qs, pad, side):
        for d in range(2):
            s = spread(ix_in[d, 1], qs[d])
            for c in range(3):
                pad[c, 0 if d == 0 else X + 1] = wx_in[p, d, c] + s[c]
        for d in range(2):
            s = spread(iy_in[d, 1], qs[2 + d])
            for c in range(3):
                side[d, c] = wy_in[p, d, c] + s[c]

    def operate(pad, side, x):
        k = k_p[x + 1]
        u = [pad[c, x + 1] for c in range(3)]
        k4 = 0.25 * k * (u[0] + u[1] + u[2])
        out = []
        for c in range(3):
            down, up = yshift(u[c], side[0, c, pl.ds(x, 1), :], side[1, c, pl.ds(x, 1), :])
            a = dg[x] * u[c] + k4
            a = a - (kx[x] * pad[c, x] + kx[x + 1] * pad[c, x + 2])
            a = a - (kym[x] * down + kyp[x] * up)
            a = a - (kzm[x] * pltpu.roll(u[c], 1, 1) + kzp[x] * pltpu.roll(u[c], Z - 1, 1))
            out.append(a)
        return u, out

    gather_wait(0, ag_recv)
    halo_wait(1)
    tiles = coarse_vector(0)
    q = answers(tiles, c_v)
    qs = [answers(tiles, c_in.at[d]) for d in range(4)]

    def add_spread(x, _):
        s = spread(reg_v[x], q)
        for c in range(3):
            z = z_p[c, x + 1] + s[c]
            z_p[c, x + 1] = z
            z0_v[c, x] = z
        return 0

    looped(0, X, add_spread, 0)
    halo_wait(2)
    edges(0, qs, z_p, zy)

    def dots(a, b):
        return fold(a[0] * b[0] + a[1] * b[1] + a[2] * b[2])

    def first(x, carry):
        u, a = operate(z_p, zy, x)
        r = [r_v[c, x] for c in range(3)]
        w = []
        for c in range(3):
            y_v[c, x] = a[c]
            w.append(a[c] * invd[x])
            v_p[c, x + 1] = w[c]
        save_faces(1, x, w)
        acc = add_rc(carry[:ncr], reg_v[x], a)
        return acc + (carry[ncr] + dots(r, u), carry[ncr + 1] + dots(a, u))

    acc = looped(0, X, first, zero_acc(ncr + 2))
    make_row(1, acc, 0)
    gather_start(1)
    for c in range(3):
        wx_send[1, 0, c] = v_p[c, 1]
        wx_send[1, 1, c] = v_p[c, X]
    halo_start(3)
    halo_wait(3)
    gather_wait(1, ag_recv)
    tiles = coarse_vector(1)
    q = answers(tiles, c_v)
    qs = [answers(tiles, c_in.at[d]) for d in range(4)]
    rz0 = total(1, 0)
    alpha0 = rz0 / total(1, 1)

    def add_spread_v(x, _):
        s = spread(reg_v[x], q)
        for c in range(3):
            v_p[c, x + 1] = v_p[c, x + 1] + s[c]
        return 0

    looped(0, X, add_spread_v, 0)
    edges(1, qs, v_p, vy)

    def second(x, carry):
        u, a = operate(v_p, vy, x)
        r, z, az = [], [], []
        for c in range(3):
            y = y_v[c, x]
            r.append(r_v[c, x] - alpha0 * y)
            z.append(z_p[c, x + 1] - alpha0 * u[c])
            az.append(y - alpha0 * a[c])
            r_v[c, x] = r[c]
            z1_v[c, x] = z[c]
            az_v[c, x] = az[c]
        return (carry[0] + dots(r, z), carry[1] + dots(az, z))

    acc = looped(0, X, second, zero_acc(2))
    make_row(2, acc, ncr)
    gather_start(2)
    gather_wait(2, ag_recv)
    rz1 = total(2, 0)
    beta = rz1 / rz0
    alpha1 = rz1 / (total(2, 1) - beta * rz1 / alpha0)
    along = alpha0 + alpha1 * beta
    a1b = alpha1 * beta

    sc_v[0:1, :] = jnp.broadcast_to(along, (1, LANES))
    sc_v[1:2, :] = jnp.broadcast_to(alpha1, (1, LANES))
    sc_v[2:3, :] = jnp.broadcast_to(a1b, (1, LANES))
    for kind in range(4):
        halo_done(kind)
    for p in range(3):
        gather_wait(p, ag_send)


def finish_wide(z0_v, z1_v, r_v, az_v, y_v, sc_v, x_out, res_out, xb, rb, sem):
    along = sc_v[0:1, 0:1]
    alpha1 = sc_v[1:2, 0:1]
    a1b = sc_v[2:3, 0:1]
    X = z0_v.shape[1]
    copies = []
    for c in range(3):
        for x in range(X):
            xb[c, x] = along * z0_v[c, x] + alpha1 * z1_v[c, x]
            rb[c, x] = r_v[c, x] - alpha1 * az_v[c, x] - a1b * y_v[c, x]
        for n, (src, dst) in enumerate(((xb, x_out), (rb, res_out))):
            copies.append(pltpu.make_async_copy(src.at[c], dst.at[c], sem.at[n, c]))
            copies[-1].start()
    for copy in copies:
        copy.wait()


def local_wide(nw, nn, right_side, occupancy, region, coarse_inverse):
    _, X, Y, Z = right_side.shape
    ncr, NC = coarse_inverse.shape
    ND = nw * nn
    f32, i32 = jnp.float32, jnp.int32
    V = pltpu.VMEM
    field, pad, scal = (3, X, Y, Z), (3, X + 2, Y, Z), (X, Y, Z)
    scratch = [
        V(scal, i32), V(scal, i32), V((ncr, NC), f32),
        V((X + 2, Y, Z), f32), V((X + 1, Y, Z), f32),
        V(scal, f32), V(scal, f32), V(scal, f32), V(scal, f32), V(scal, f32), V(scal, f32),
        V(pad, f32), V(pad, f32),
        V((2, 3, X, Z), f32), V((2, 3, X, Z), f32),
        V((2, 2, Y, Z), i32), V((2, 2, X, Z), i32), V((2, 2, X, Z), i32),
        V((4, ncr, NC), f32),
        V((2, 2, 3, Y, Z), f32), V((2, 2, 3, Y, Z), f32),
        V((2, 2, 3, X, Z), f32), V((2, 2, 3, X, Z), f32),
        V((3, SUB, LANES), f32), V((3, ND, LANES), f32),
        pltpu.SemaphoreType.DMA((4,)),
        pltpu.SemaphoreType.DMA((5, 4)), pltpu.SemaphoreType.DMA((5, 4)),
        pltpu.SemaphoreType.DMA((3,)), pltpu.SemaphoreType.DMA((3,)),
    ]
    parts = pl.pallas_call(
        functools.partial(kernel_wide, nw, nn),
        out_shape=(V(field, f32),) * 5 + (V((SUB, LANES), f32),),
        in_specs=[pl.BlockSpec(memory_space=pltpu.HBM)] * 4,
        out_specs=(pl.BlockSpec(memory_space=pltpu.VMEM),) * 6,
        scratch_shapes=scratch,
        compiler_params=pltpu.CompilerParams(collective_id=0, has_side_effects=True, vmem_limit_bytes=32 * 1024 * 1024),
    )(*[pltpu.with_memory_space_constraint(a, pltpu.HBM) for a in (right_side, occupancy, region, coarse_inverse)])
    return pl.pallas_call(
        finish_wide,
        out_shape=(jax.ShapeDtypeStruct(field, f32),) * 2,
        in_specs=[pl.BlockSpec(memory_space=pltpu.VMEM)] * 6,
        out_specs=(pl.BlockSpec(memory_space=pltpu.HBM),) * 2,
        scratch_shapes=[V(field, f32), V(field, f32), pltpu.SemaphoreType.DMA((2, 3))],
        compiler_params=pltpu.CompilerParams(vmem_limit_bytes=16 * 1024 * 1024),
    )(*parts)


REPLICATED_BYTES = 4 * 1024 * 1024
DEEP = 3
AROUND = ((-1, 0), (1, 0), (0, -1), (0, 1), (-1, -1), (-1, 1), (1, -1), (1, 1))
BACK = tuple(AROUND.index((-a, -b)) for a, b in AROUND)


def group_of(n):
    return max(d for d in range(1, n + 1) if n % d == 0 and d * d <= n)


def spread_over(reg, q, G, inside=False):
    masks = [reg == g for g in range(G)]
    out = []
    for c in range(3):
        s = q[(G - 1) * 3 + c] if inside else jnp.where(masks[G - 1], q[(G - 1) * 3 + c], 0.0)
        for g in range(G - 1):
            s = jnp.where(masks[g], q[g * 3 + c], s)
        out.append(s)
    return out


def rows_from(low, count):
    return pl.ds(SUB + low, count)


def both_sides(ref, Y, *at):
    row = lax.broadcasted_iota(jnp.int32, (SUB, LANES), 0)
    return jnp.where(row < SUB // 2, ref[(*at, pl.ds(SUB + Y, SUB))], ref[(*at, pl.ds(0, SUB))])


def apply(ref, coefficients, x, low, count):
    kx, kyp, kzm, kzp, dg, k4 = coefficients
    here, down, up = rows_from(low, count), rows_from(low - 1, count), rows_from(low + 1, count)
    u = [ref[c, x, here] for c in range(3)]
    kk = k4[x, here] * (u[0] + u[1] + u[2])
    out = []
    for c in range(3):
        a = kx[x, here] * ref[c, x - 1, here] + kx[x + 1, here] * ref[c, x + 1, here]
        a = a + (kyp[x, down] * ref[c, x, down] + kyp[x, here] * ref[c, x, up])
        a = a + (kzm[x, here] * pltpu.roll(u[c], 1, 1) + kzp[x, here] * pltpu.roll(u[c], LANES - 1, 1))
        out.append(dg[x, here] * u[c] + kk - a)
    return u, out


def kernel(nw, nn, r_hbm, occ_hbm, reg_hbm, ci_hbm,
           z_e, g_e, y_e, r_o, ag_o, reg_o, k4, dg, kx, kyp, kzm, kzp, q_o, sc_o,
           occ_e, reg_e, r_e, k_e, invd,
           call, c_in, y_face, y_label, qpair, row_send, rows, sizes,
           load_sem, send, recv, ready):
    E, YE, Z = occ_e.shape
    X, Y = E - 2 * DEEP, YE - 2 * SUB
    ncr, NC = c_in.shape[1:]
    G = ncr // 3
    ND = nw * nn
    NH = ND // 2
    wi = lax.axis_index("wide")
    ni = lax.axis_index("narrow")
    me = wi * nn + ni
    f32 = jnp.float32
    GW = group_of(nw)
    GP = GW * nn
    NG = ND // GP
    grp, pos = me // GP, lax.rem(me, GP)
    half, place = lax.rem(wi, 2), (lax.rem(wi, GW) // 2) * nn + ni
    here = half * NH + place * NG + grp
    own, inner_rows = pl.ds(DEEP, X), pl.ds(SUB, Y)

    loads = [pltpu.make_async_copy(s, d, load_sem.at[i]) for s, d, i in (
        (reg_hbm, reg_e.at[own, inner_rows], 0), (r_hbm, r_e.at[:, own, inner_rows], 0),
        (occ_hbm, occ_e.at[own, inner_rows], 1), (ci_hbm, call.at[here], 2))]
    for l in loads:
        l.start()

    barrier = pltpu.get_barrier_semaphore()

    def at(t):
        return (t // nn, lax.rem(t, nn))

    def wait_for(sem, count):
        @pl.when(count > 0)
        def _():
            pl.semaphore_wait(sem, count)

    def column_of(group):
        return (wi + (group - grp) * GW, ni)

    at_low = jnp.logical_and(lax.rem(wi, GW) == 0, wi > 0)
    at_high = jnp.logical_and(lax.rem(wi, GW) == GW - 1, wi < nw - 1)
    aside = 1 + jnp.where(ni > 0, 1, 0) + jnp.where(ni < nn - 1, 1, 0)

    def touching(ahead, signal):
        @pl.when(at_high if ahead > 0 else at_low)
        def _():
            for b in (-1, 0, 1):
                @pl.when(jnp.logical_and(ni + b >= 0, ni + b < nn))
                def _():
                    signal((wi + ahead, ni + b))

    def say(sem):
        return lambda device: pl.semaphore_signal(sem, inc=1, device_id=device, device_id_type=MESH)

    for i in range(1, GP):
        say(barrier)(at(grp * GP + lax.rem(pos + i, GP)))
    touching(1, say(barrier))
    touching(-1, say(barrier))
    for k in range(1, NG):
        @pl.when(grp + k < NG)
        def _():
            say(barrier)(column_of(grp + k))

    def tell():
        for k in range(1, NG):
            @pl.when(grp >= k)
            def _():
                say(ready.at[k - 1])(column_of(grp - k))

    def take(rows_of, sem):
        some = sizes.at[pl.ds(0, rows_of)]
        pltpu.make_async_copy(some, some, sem).wait()

    def take_c(blocks, sem):
        some = call.at[pl.ds(0, blocks)]
        pltpu.make_async_copy(some, some, sem).wait()

    def by_neighbours(wait):
        nx = jnp.where(wi > 0, 1, 0) + jnp.where(wi < nw - 1, 1, 0)
        ny = jnp.where(ni > 0, 1, 0) + jnp.where(ni < nn - 1, 1, 0)
        for a in ((1,) if nw == 2 else (1, 2)):
            for b in (range(min(nn, 2)) if nn == 1 else (1,) if nn == 2 else (1, 2)):
                @pl.when(jnp.logical_and(nx == a, ny == b))
                def _():
                    wait(a, b)

    def halo_rows(n, a, b):
        deep, corner, count = ((DEEP, 2, 1), (2, 1, 1), (2, 1, 3))[n]
        return count * (a * deep * Y + b * deep * X + a * b * corner * corner)

    has = []
    for a, b in AROUND:
        h = jnp.logical_and(wi + a >= 0, wi + a < nw)
        has.append(jnp.logical_and(h, jnp.logical_and(ni + b >= 0, ni + b < nn)))

    def part(arr, d, into):
        a, b = AROUND[d]
        deep = {0: DEEP, 1: 2, 2: 2}[arr] if a == 0 or b == 0 else {0: 2, 1: 1, 2: 1}[arr]
        if into:
            xs = {-1: (DEEP - deep, deep), 0: (DEEP, X), 1: (DEEP + X, deep)}[a]
            ys = {-1: (SUB - deep, deep), 0: (SUB, Y), 1: (SUB + Y, deep)}[b]
        else:
            xs = {-1: (DEEP, deep), 0: (DEEP, X), 1: (DEEP + X - deep, deep)}[a]
            ys = {-1: (SUB, deep), 0: (SUB, Y), 1: (SUB + Y - deep, deep)}[b]
        xs, ys = pl.ds(*xs), pl.ds(*ys)
        return (slice(None), xs, ys) if arr == 2 else (xs, ys)

    fields = (occ_e, reg_e, r_e)
    for d in range(8):
        @pl.when(jnp.logical_not(has[d]))
        def _():
            for n, ref in enumerate(fields):
                where = part(n, d, True)
                v = ref[where]
                ref[where] = jnp.full(v.shape, (-1, -1, 0)[n], v.dtype)
            c_in[d] = jnp.zeros((ncr, NC), f32)

    wait_for(barrier, GP - 1 + grp + jnp.where(at_low, aside, 0) + jnp.where(at_high, aside, 0))
    tell()

    def fold(a):
        return jnp.sum(a.reshape(a.shape[0] // SUB, SUB, Z), axis=0)

    def zero_acc(n):
        return tuple(jnp.zeros((SUB, Z), f32) for _ in range(n))

    def add_rc(acc, reg, u):
        out = list(acc)
        for g in range(G):
            m = reg == g
            for c in range(3):
                out[g * 3 + c] = acc[g * 3 + c] + fold(jnp.where(m, u[c], 0.0))
        return out

    base = (me * ncr) % LANES

    def column(acc):
        a = jnp.concatenate([jnp.sum(b, axis=0, keepdims=True) for b in acc], axis=0)
        return jnp.sum(a, axis=1, keepdims=True)

    def make_row(p, acc):
        col = column(acc)
        n = len(acc)
        k = lax.broadcasted_iota(jnp.int32, (n, LANES), 0)
        lane = lax.broadcasted_iota(jnp.int32, (n, LANES), 1)
        target = (base + k) & (LANES - 1)
        row = jnp.sum(jnp.where(lane == target, col, 0.0), axis=0, keepdims=True)
        row_send[p, 0:1, :] = row
        rows[p, pl.ds(me, 1), :] = row

    def rows_to(p, count, t, out, sem):
        pltpu.make_async_remote_copy(
            src_ref=row_send.at[pl.ds(p, count), pl.ds(0, 1)], dst_ref=rows.at[pl.ds(p, count), pl.ds(me, 1)],
            send_sem=send.at[out], recv_sem=recv.at[sem],
            device_id=at(t), device_id_type=MESH).start()

    def each_peer(send):
        def body(i, _):
            send(i + jnp.where(i < me, 0, 1))
            return 0
        lax.fori_loop(0, ND - 1, body, 0, unroll=ND <= 64)

    take(4 * X * Y, load_sem.at[0])
    acc = looped(0, X, lambda x, a: tuple(add_rc(
        a, reg_e[x + DEEP, inner_rows], [r_e[c, x + DEEP, inner_rows] for c in range(3)])), zero_acc(ncr))
    make_row(0, acc)

    def inside(i, _):
        rows_to(0, 1, grp * GP + lax.rem(pos + i, GP), 0, 3)
        return 0

    lax.fori_loop(1, GP, inside, 0, unroll=GP <= 64)

    def halo(n, d):
        a, b = AROUND[d]
        e = BACK[d]
        return pltpu.make_async_remote_copy(
            src_ref=fields[n].at[part(n, d, False)], dst_ref=fields[n].at[part(n, e, True)],
            send_sem=send.at[0], recv_sem=recv.at[min(n, 1)],
            device_id=(wi + a, ni + b), device_id_type=MESH)

    def halo_c(d):
        a, b = AROUND[d]
        return pltpu.make_async_remote_copy(
            src_ref=call.at[here], dst_ref=c_in.at[BACK[d]],
            send_sem=send.at[1], recv_sem=recv.at[2],
            device_id=(wi + a, ni + b), device_id_type=MESH)

    loads[2].wait()
    loads[3].wait()

    for n in range(4):
        for d in range(8):
            @pl.when(has[d])
            def _():
                (halo_c(d) if n == 3 else halo(n, d)).start()

    def c_column(group):
        pltpu.make_async_remote_copy(
            src_ref=call.at[here], dst_ref=call.at[here],
            send_sem=send.at[2], recv_sem=recv.at[5],
            device_id=column_of(group), device_id_type=MESH).start()

    for k in range(1, NG):
        @pl.when(grp >= k)
        def _():
            c_column(grp - k)

    def c_group(block):
        for i in range(1, GP // 2):
            p = lax.rem(place + i, GP // 2)
            pltpu.make_async_remote_copy(
                src_ref=call.at[block], dst_ref=call.at[block],
                send_sem=send.at[2], recv_sem=recv.at[6],
                device_id=(grp * GW + (p // nn) * 2 + half, lax.rem(p, nn)), device_id_type=MESH).start()

    c_group(here)

    def stiff_of(o):
        return jnp.where(o < 0, 0.0, soft_stiff + (bone_stiff - soft_stiff) * o.astype(f32))

    n2 = G * G

    def pairs(acc, first, seconds):
        out = list(acc)
        for g in range(G):
            t = None
            for label, value in seconds:
                v = jnp.where(label == g, value, 0.0)
                t = v if t is None else t + v
            for h in range(G):
                out[h * G + g] = acc[h * G + g] + fold(jnp.where(first == h, t, 0.0))
        return out

    row16 = lax.broadcasted_iota(jnp.int32, (Y, Z), 0)
    lane16 = lax.broadcasted_iota(jnp.int32, (Y, Z), 1)

    def own_pairs(i, carry):
        x = i + DEEP
        k, reg = stiff_of(occ_e[x, inner_rows]), reg_e[x, inner_rows]
        later = jnp.minimum(i + 1, X - 1) + DEEP
        kx_in = jnp.where(i < X - 1, 0.5 * (k + stiff_of(occ_e[later, inner_rows])), 0.0)
        ky_in = jnp.where(row16 == Y - 1, 0.0, 0.5 * (k + pltpu.roll(k, Y - 1, 0)))
        kz_in = jnp.where(lane16 == Z - 1, 0.0, 0.5 * (k + pltpu.roll(k, Z - 1, 1)))
        acc = pairs(carry[:n2], reg, ((reg_e[later, inner_rows], kx_in), (pltpu.roll(reg, Y - 1, 0), ky_in),
                                      (pltpu.roll(reg, Z - 1, 1), kz_in)))
        sums = [carry[n2 + g] + fold(jnp.where(reg == g, 0.25 * k, 0.0)) for g in range(G)]
        return tuple(acc) + tuple(sums)

    own_acc = lax.fori_loop(0, X, own_pairs, zero_acc(n2 + G), unroll=2)
    own_col = column(own_acc)

    def c_up(k):
        @pl.when(grp + k < NG)
        def _():
            pl.semaphore_wait(ready.at[k - 1], 1)
            c_column(grp + k)

    for k in range(1, NG):
        c_up(k)

    take(GP - 1, recv.at[3])
    mine = rows.at[0, pl.ds(pl.multiple_of(grp * GP, GP), GP)]

    def across(group):
        pltpu.make_async_remote_copy(
            src_ref=mine, dst_ref=mine, send_sem=send.at[0], recv_sem=recv.at[4],
            device_id=column_of(group), device_id_type=MESH).start()

    for k in range(1, NG):
        @pl.when(grp >= k)
        def _():
            across(grp - k)

    for k in range(1, NG):
        @pl.when(grp + k < NG)
        def _():
            across(grp + k)

    by_neighbours(lambda a, b: take(halo_rows(0, a, b), recv.at[0]))

    lane_id = lax.broadcasted_iota(jnp.int32, (Y + SUB, Z), 1)

    def stiffness(x, _):
        k_e[x] = stiff_of(occ_e[x])
        return 0

    lax.fori_loop(0, E, stiffness, 0, unroll=True)
    row8 = lax.broadcasted_iota(jnp.int32, (SUB, Z), 0)

    def coefficients(x):
        here = rows_from(-2, Y + SUB)
        k = k_e[x, here]
        low, high = k_e[x, rows_from(-3, Y + SUB)], k_e[x, rows_from(-1, Y + SUB)]
        back = jnp.where(lane_id == 0, 0.0, pltpu.roll(k, 1, 1))
        ahead = jnp.where(lane_id == Z - 1, 0.0, pltpu.roll(k, Z - 1, 1))
        xm = 0.5 * (k + k_e[x - 1, here])
        xp = 0.5 * (k + k_e[x + 1, here])
        ym = 0.5 * (k + low)
        yp = 0.5 * (k + high)
        zm = 0.5 * (k + back)
        zp = 0.5 * (k + ahead)
        diag = xm + xp + ym + yp + zm + zp + 0.5 * k
        kx[x, here] = xm
        kx[x + 1, here] = xp
        kyp[x, here] = yp
        kzm[x, here] = jnp.where(lane_id == 0, 0.0, zm)
        kzp[x, here] = jnp.where(lane_id == Z - 1, 0.0, zp)
        dg[x, here] = diag - 0.25 * k
        k4[x, here] = 0.25 * k
        invd[x, here] = jnp.where(k > 0.0, 1.0 / diag, 0.0)

    for x in (1, 2, DEEP + X, DEEP + X + 1):
        coefficients(x)

    def inner(i, sums):
        coefficients(i + DEEP)
        d, reg = dg[i + DEEP, inner_rows], reg_e[i + DEEP, inner_rows]
        return tuple(sums[g] + fold(jnp.where(reg == g, d, 0.0)) for g in range(G))

    sum_acc = lax.fori_loop(0, X, inner, zero_acc(G), unroll=4)

    by_neighbours(lambda a, b: take(halo_rows(1, a, b) + halo_rows(2, a, b), recv.at[1]))

    def side_rows(i, _):
        x = i + DEEP
        y_face[pl.ds(i, 1), :] = kyp[x, rows_from(Y - 1, 1), :]
        y_label[0, pl.ds(i, 1), :] = reg_e[x, rows_from(Y - 1, 1), :]
        y_label[1, pl.ds(i, 1), :] = reg_e[x, rows_from(Y, 1), :]
        return 0

    looped(0, X, side_rows, 0)
    top = DEEP + X - 1
    x_acc = pairs(zero_acc(n2), reg_e[top, inner_rows], ((reg_e[top + 1, inner_rows], kx[top + 1, inner_rows]),))
    y_acc = pairs(zero_acc(n2), y_label[0], ((y_label[1], y_face[...]),))
    rim_col = column(tuple(x_acc) + tuple(y_acc) + tuple(sum_acc))

    lane = lax.broadcasted_iota(jnp.int32, (n2, LANES), 1)
    pair = lax.broadcasted_iota(jnp.int32, (n2, LANES), 0)
    at_pair = jnp.logical_and(lane >= 3 * pair, lane < 3 * pair + 3)

    def lanes_of(col, mask):
        return jnp.sum(jnp.where(mask, col, 0.0), axis=0, keepdims=True)

    lane_g = lax.broadcasted_iota(jnp.int32, (G, LANES), 1)
    row_g = lax.broadcasted_iota(jnp.int32, (G, LANES), 0)
    diag_at, sum_at = 3 * (G + 1) * row_g, 3 * n2 + 9 * row_g
    at_diag = jnp.logical_and(lane_g >= diag_at, lane_g < diag_at + 3)
    at_sum = jnp.logical_and(lane_g >= sum_at, lane_g < sum_at + 9)
    ac_rows = (lanes_of(own_col[0:n2], at_pair) * -2.0 + lanes_of(rim_col[2 * n2:], at_diag)
               + lanes_of(own_col[n2:], at_sum),
               lanes_of(rim_col[0:n2], at_pair) * -2.0, lanes_of(rim_col[n2:2 * n2], at_pair) * -2.0)
    for n in range(3):
        row_send[n + 2, 0:1, :] = ac_rows[n]
        rows[n + 2, pl.ds(me, 1), :] = ac_rows[n]

    def coarse_vector(block):
        tiles = []
        for t in range(NC // LANES):
            lo = (LANES * t) // ncr // SUB * SUB
            hi = min(ND, -(-(-(-(LANES * (t + 1)) // ncr)) // SUB) * SUB)
            d = lax.broadcasted_iota(jnp.int32, (hi - lo, LANES), 0) + lo
            j = lax.broadcasted_iota(jnp.int32, (hi - lo, LANES), 1) + LANES * t
            m = (j >= d * ncr) & (j < d * ncr + ncr)
            tiles.append(jnp.sum(jnp.where(m, block[lo:hi, :], 0.0), axis=0, keepdims=True))
        return tiles

    def total(block, s):
        d = lax.broadcasted_iota(jnp.int32, (ND, LANES), 0)
        lane = lax.broadcasted_iota(jnp.int32, (ND, LANES), 1)
        m = lane == ((d * ncr + ncr + s) & (LANES - 1))
        v = jnp.sum(jnp.where(m, block, 0.0), axis=0, keepdims=True)
        return jnp.sum(v, axis=1, keepdims=True)

    def solve(tiles, block):
        s = block[:, 0:LANES] * tiles[0]
        for t in range(1, len(tiles)):
            s = s + block[:, t * LANES:(t + 1) * LANES] * tiles[t]
        return jnp.sum(s, axis=1, keepdims=True)

    def as_list(q):
        return [q[i:i + 1, :] for i in range(ncr)]

    take_c(NG - 1, recv.at[5])
    for k in range(1, NG):
        c_group(half * NH + place * NG + lax.rem(grp + k, NG))

    take(ND - GP, recv.at[4])
    by_neighbours(lambda a, b: take_c(a + b + a * b, recv.at[2]))
    tiles = coarse_vector(rows[0])
    q = as_list(solve(tiles, call[here]))
    qn = [as_list(solve(tiles, c_in[d])) for d in range(8)]

    def either(hi, lo):
        return [jnp.where(row8 < SUB // 2, a, b) for a, b in zip(hi, lo)]

    def add_spread(x, q_in, q_out, inside):
        reg, inv = reg_e[x, inner_rows], invd[x, inner_rows]
        s = spread_over(reg, q_in, G, inside)
        reg_o[x, inner_rows] = reg
        for c in range(3):
            z_e[c, x, inner_rows] = r_e[c, x, inner_rows] * inv + s[c]
        reg, inv = both_sides(reg_e, Y, x), both_sides(invd, Y, x)
        s = spread_over(reg, q_out, G)
        some = SUB // 2
        reg_o[x, rows_from(Y, some)] = reg[0:some]
        reg_o[x, rows_from(-some, some)] = reg[some:SUB]
        for c in range(3):
            z = both_sides(r_e, Y, c, x) * inv + s[c]
            z_e[c, x, rows_from(Y, some)] = z[0:some]
            z_e[c, x, rows_from(-some, some)] = z[some:SUB]

    q_side = either(qn[3], qn[2])

    def spread_own(i, _):
        add_spread(i + DEEP, q, q_side, True)
        return 0

    looped(0, X, spread_own, 0)
    q_low, q_high = either(qn[5], qn[4]), either(qn[7], qn[6])
    for x in (1, 2):
        add_spread(x, qn[0], q_low, False)
    for x in (DEEP + X, DEEP + X + 1):
        add_spread(x, qn[1], q_high, False)

    faces = (kx, kyp, kzm, kzp, dg, k4)

    def dots(a, b):
        return fold(a[0] * b[0] + a[1] * b[1] + a[2] * b[2])

    def first(i, _):
        x, some = i + DEEP - 1, rows_from(-1, Y + SUB)
        _, a = apply(z_e, faces, x, -1, Y + SUB)
        for c in range(3):
            y_e[c, x, some] = a[c]
            g_e[c, x, some] = a[c] * invd[x, some]
        return 0

    lax.fori_loop(0, X + 2, first, 0, unroll=(X + 2) // 2)

    def own_of(ref, x):
        return [ref[c, x, inner_rows] for c in range(3)]

    def second(i, carry):
        x = i + DEEP
        w, a = apply(g_e, faces, x, 0, Y)
        for c in range(3):
            ag_o[c, i] = a[c]
        acc = add_rc(carry[:ncr], reg_e[x, inner_rows], a)
        return tuple(acc) + (carry[ncr] + dots(w, a),)

    acc2 = lax.fori_loop(0, X, second, zero_acc(ncr + 1), unroll=8)

    def third(i, carry):
        x = i + DEEP
        r, z, y, w = own_of(r_e, x), own_of(z_e, x), own_of(y_e, x), own_of(g_e, x)
        for c in range(3):
            r_o[c, i] = r[c]
        acc = add_rc(carry[:ncr], reg_e[x, inner_rows], y)
        return tuple(acc) + (carry[ncr] + dots(r, z), carry[ncr + 1] + dots(y, z), carry[ncr + 2] + dots(y, w))

    acc1 = lax.fori_loop(0, X, third, zero_acc(ncr + 3), unroll=8)
    make_row(1, tuple(acc1) + (acc2[ncr],) + tuple(acc2[:ncr]))
    each_peer(lambda t: rows_to(1, 4, t, 3, 7))

    take_c((GP // 2 - 1) * NG, recv.at[6])
    swap_half = call.at[pl.ds(half * NH, NH)]
    swap = pltpu.make_async_remote_copy(
        src_ref=swap_half, dst_ref=swap_half, send_sem=send.at[2], recv_sem=recv.at[8],
        device_id=(wi + 1 - 2 * half, ni), device_id_type=MESH)
    swap.start()
    by_neighbours(lambda a, b: take(
        sum(halo_rows(n, a, b) for n in range(3)) + GP - 1 + (NG - 1) * GP, send.at[0]))
    by_neighbours(lambda a, b: take_c(a + b + a * b, send.at[1]))
    swap.wait_recv()
    take(4 * (ND - 1), recv.at[7])

    block = rows[1]
    b1 = coarse_vector(block)
    h1 = coarse_vector(pltpu.roll(block, LANES - ncr - 4, 1))
    rr = lax.broadcasted_iota(jnp.int32, (ncr, LANES), 0)
    ll = lax.broadcasted_iota(jnp.int32, (ncr, LANES), 1)
    m0, m1 = rr < 0, rr < 0
    for h in range(G):
        for g in range(G):
            for c in range(3):
                k = (h * G + g) * 3 + c
                m0 = jnp.logical_or(m0, (ll == k) & (rr == h * 3 + c))
                m1 = jnp.logical_or(m1, (ll == k) & (rr == g * 3 + c))
        for c in range(3):
            for e in range(3):
                k = 3 * n2 + h * 9 + c * 3 + e
                m0 = jnp.logical_or(m0, (ll == k) & (rr == h * 3 + c))
                m1 = jnp.logical_or(m1, (ll == k) & (rr == h * 3 + e))
    lines = [jnp.zeros((ncr, LANES), f32) for _ in b1]
    for w in range(nw):
        for n in range(nn):
            d = w * nn + n
            q1 = solve(b1, call[w % 2 * NH + ((w % GW) // 2 * nn + n) * NG + w // GW])
            qpair[0, d:d + 1, :] = jnp.sum(jnp.where(m0, q1, 0.0), axis=0, keepdims=True)
            qpair[1, d:d + 1, :] = jnp.sum(jnp.where(m1, q1, 0.0), axis=0, keepdims=True)
            for t in range(d * ncr // LANES, (d * ncr + ncr - 1) // LANES + 1):
                lines[t] = jnp.where(ll + LANES * t == rr + d * ncr, q1, lines[t])
    lines = [jnp.sum(v, axis=0, keepdims=True) for v in lines]
    first_q, second_q = qpair[0], qpair[1]
    dev = lax.broadcasted_iota(jnp.int32, (ND, LANES), 0)
    next_x = jnp.where(dev < ND - nn, pltpu.roll(second_q, ND - nn, 0), 0.0)
    next_y = jnp.where(dev < ND - 1, pltpu.roll(second_q, ND - 1, 0), 0.0)
    energy = jnp.sum(first_q * (rows[2] * second_q + rows[3] * next_x + rows[4] * next_y), axis=0, keepdims=True)
    for t in range(len(b1)):
        energy = energy + 2.0 * h1[t] * lines[t]
    yv = b1[0] * lines[0]
    for t in range(1, len(b1)):
        yv = yv + b1[t] * lines[t]
    yv = total(block, 2) + jnp.sum(yv, axis=1, keepdims=True)
    vav = total(block, 3) + jnp.sum(energy, axis=1, keepdims=True)
    rz0, zy = total(block, 0), total(block, 1)
    alpha0 = rz0 / zy
    rz1 = alpha0 * alpha0 * yv - rz0
    zaz = zy - 2.0 * alpha0 * yv + alpha0 * alpha0 * vav
    beta = rz1 / rz0
    alpha1 = rz1 / (zaz - beta * rz1 / alpha0)
    a1b = alpha1 * beta
    for n, v in enumerate((alpha0 + a1b + alpha1, alpha1 * alpha0)):
        sc_o[n:n + 1, :] = jnp.broadcast_to(v, (1, LANES))
    q_o[0] = jnp.broadcast_to(solve(b1, call[here]), (ncr, LANES))
    for d in range(4):
        q_o[d + 1] = jnp.broadcast_to(solve(b1, c_in[d]), (ncr, LANES))

    take(4 * (ND - 1), send.at[3])
    take_c(NG - 1 + (GP // 2 - 1) * NG + NH, send.at[2])


def finish(z_v, g_v, y_v, r_v, ag_v, reg_v, k4, dg, kx, kyp, kzm, kzp, q_v, sc_v, x_out, res_out, s_e, xb, rb, sem):
    a, b = sc_v[0:1, 0:1], sc_v[1:2, 0:1]
    E, YE, Z = reg_v.shape
    X, Y = E - 2 * DEEP, YE - 2 * SUB
    G = q_v.shape[1] // 3
    own = pl.ds(SUB, Y)
    row8 = lax.broadcasted_iota(jnp.int32, (SUB, Z), 0)
    q = [[q_v[d, i:i + 1, :] for i in range(3 * G)] for d in range(5)]
    side = [jnp.where(row8 < SUB // 2, hi, lo) for hi, lo in zip(q[4], q[3])]

    def fill(x, q_in, inside):
        s = spread_over(reg_v[x, own], q_in, G, inside)
        for c in range(3):
            s_e[c, x, own] = s[c]

    def fill_sides(x):
        s = spread_over(both_sides(reg_v, Y, x), side, G)
        some = SUB // 2
        for c in range(3):
            s_e[c, x, rows_from(Y, some)] = s[c][0:some]
            s_e[c, x, rows_from(-some, some)] = s[c][some:SUB]

    def fill_own(i, _):
        fill(i + DEEP, q[0], True)
        fill_sides(i + DEEP)
        return 0

    fill(DEEP - 1, q[1], False)
    fill(DEEP + X, q[2], False)
    looped(0, X, fill_own, 0)
    faces = (kx, kyp, kzm, kzp, dg, k4)
    parts = 4
    step = X // parts

    def plane(i, _):
        x = i + DEEP
        u, w = apply(s_e, faces, x, 0, Y)
        for c in range(3):
            xb[c, i] = a * z_v[c, x, own] - b * (g_v[c, x, own] + u[c])
            rb[c, i] = r_v[c, i] - a * y_v[c, x, own] + b * (ag_v[c, i] + w[c])
        return 0

    for n in range(parts):
        lax.fori_loop(n * step, (n + 1) * step, plane, 0, unroll=True)
        for m, (src, dst) in enumerate(((xb, x_out), (rb, res_out))):
            where = (slice(None), pl.ds(n * step, step))
            pltpu.make_async_copy(src.at[where], dst.at[where], sem.at[m]).start()
    pltpu.make_async_copy(xb, x_out, sem.at[0]).wait()
    pltpu.make_async_copy(rb, res_out, sem.at[1]).wait()


def local_fast(nw, nn, right_side, occupancy, region, coarse_inverse):
    _, X, Y, Z = right_side.shape
    ncr, NC = coarse_inverse.shape
    ND = nw * nn
    f32, i32 = jnp.float32, jnp.int32
    V = pltpu.VMEM
    E, YE = X + 2 * DEEP, Y + 2 * SUB
    field, ext, scal = (3, X, Y, Z), (3, E, YE, Z), (E, YE, Z)
    ng = nw // group_of(nw)
    DMA = pltpu.SemaphoreType.DMA
    scratch = [
        V(scal, i32), V(scal, i32), V(ext, f32), V(scal, f32), V(scal, f32),
        V((ND, ncr, NC), f32), V((8, ncr, NC), f32), V((X, Z), f32), V((2, X, Z), i32), V((2, ND, LANES), f32),
        V((5, SUB, LANES), f32), V((5, ND, LANES), f32), V((4 * X * Y, LANES), f32),
        DMA((3,)), DMA((4,)), DMA((9,)),
        pltpu.SemaphoreType.REGULAR((ng - 1,)),
    ]
    outs = (V(ext, f32),) * 3 + (V(field, f32),) * 2 + (V(scal, i32),) + (V(scal, f32),) * 6 + (V((5, ncr, LANES), f32), V((SUB, LANES), f32))
    parts = pl.pallas_call(
        functools.partial(kernel, nw, nn),
        out_shape=outs,
        in_specs=[pl.BlockSpec(memory_space=pltpu.HBM)] * 4,
        out_specs=(pl.BlockSpec(memory_space=pltpu.VMEM),) * len(outs),
        scratch_shapes=scratch,
        compiler_params=pltpu.CompilerParams(collective_id=0, has_side_effects=True, vmem_limit_bytes=32 * 1024 * 1024),
    )(*[pltpu.with_memory_space_constraint(a, pltpu.HBM) for a in (right_side, occupancy, region, coarse_inverse)])
    return pl.pallas_call(
        finish,
        out_shape=(jax.ShapeDtypeStruct(field, f32),) * 2,
        in_specs=[pl.BlockSpec(memory_space=pltpu.VMEM)] * len(outs),
        out_specs=(pl.BlockSpec(memory_space=pltpu.HBM),) * 2,
        scratch_shapes=[V(ext, f32), V(field, f32), V(field, f32), DMA((2,))],
        compiler_params=pltpu.CompilerParams(vmem_limit_bytes=24 * 1024 * 1024),
    )(*parts)


def local(nw, nn, right_side, occupancy, region, coarse_inverse):
    nc = coarse_inverse.shape[1]
    run = local_fast if group_of(nw) % 2 == 0 and nc * nc * 4 <= REPLICATED_BYTES else local_wide
    return run(nw, nn, right_side, occupancy, region, coarse_inverse)


def solution(mesh):
    return jax.shard_map(
        functools.partial(local, mesh.shape["wide"], mesh.shape["narrow"]),
        mesh=mesh,
        in_specs=(
            P(None, "wide", "narrow", None),
            P("wide", "narrow", None),
            P("wide", "narrow", None),
            P(("wide", "narrow"), None),
        ),
        out_specs=(P(None, "wide", "narrow", None), P(None, "wide", "narrow", None)),
        check_vma=False,
    )
```

```python
import functools

import jax
import jax.numpy as jnp
from jax import lax
from jax.experimental import pallas as pl
from jax.experimental.pallas import tpu as pltpu
from jax.sharding import PartitionSpec as P

LANES = 128
SUB = 8
UNROLL = 16
looped = functools.partial(lax.fori_loop, unroll=UNROLL)
MESH = pl.DeviceIdType.MESH
bone_stiff = 1.0
soft_stiff = 0.1


def kernel_wide(nw, nn, r_hbm, occ_hbm, reg_hbm, ci_hbm,
           z0_v, z1_v, r_v, az_v, y_v, sc_v,
            occ_v, reg_v, c_v, k_p, kx, kym, kyp, kzm, kzp, dg, invd,
           z_p, v_p, zy, vy,
           ix_in, iy_send, iy_in, c_in, wx_send, wx_in, wy_send, wy_in,
           row_send, rows, load_sem, hs_send, hs_recv, ag_send, ag_recv):
    X, Y, Z = occ_v.shape
    ncr, NC = c_v.shape
    G = ncr // 3
    ND = nw * nn
    wi = lax.axis_index("wide")
    ni = lax.axis_index("narrow")
    me = wi * nn + ni
    f32 = jnp.float32

    loads = [pltpu.make_async_copy(s, d, load_sem.at[i]) for i, (s, d) in enumerate(
        ((occ_hbm, occ_v), (reg_hbm, reg_v), (r_hbm, r_v), (ci_hbm, c_v)))]
    for l in loads:
        l.start()

    def peer(i):
        t = lax.rem(me + i, ND)
        return (t // nn, lax.rem(t, nn))

    barrier = pltpu.get_barrier_semaphore()

    def greet(i, _):
        pl.semaphore_signal(barrier, inc=1, device_id=peer(i), device_id_type=MESH)
        return 0

    lax.fori_loop(1, ND, greet, 0, unroll=ND <= 64)

    has = (wi > 0, wi < nw - 1, ni > 0, ni < nn - 1)
    to = ((wi - 1, ni), (wi + 1, ni), (wi, ni - 1), (wi, ni + 1))

    for d in range(4):
        @pl.when(jnp.logical_not(has[d]))
        def _():
            c_in[d] = jnp.zeros((ncr, NC), f32)
            for p in range(2):
                if d < 2:
                    wx_in[p, d] = jnp.zeros((3, Y, Z), f32)
                else:
                    wy_in[p, d - 2] = jnp.zeros((3, X, Z), f32)
            if d < 2:
                ix_in[d] = jnp.zeros((2, Y, Z), jnp.int32)
            else:
                iy_in[d - 2] = jnp.zeros((2, X, Z), jnp.int32)

    loads[0].wait()
    loads[1].wait()

    def pack_ints(x, _):
        iy_send[0, 0, pl.ds(x, 1), :] = occ_v[x, 0:1, :]
        iy_send[1, 0, pl.ds(x, 1), :] = occ_v[x, Y - 1:Y, :]
        iy_send[0, 1, pl.ds(x, 1), :] = reg_v[x, 0:1, :]
        iy_send[1, 1, pl.ds(x, 1), :] = reg_v[x, Y - 1:Y, :]
        return 0

    looped(0, X, pack_ints, 0)

    def fold(a):
        return jnp.sum(a.reshape(Y // SUB, SUB, Z), axis=0)

    def zero_acc(n):
        return tuple(jnp.zeros((SUB, Z), f32) for _ in range(n))

    def add_rc(acc, reg, u):
        out = list(acc)
        for g in range(G):
            m = reg == g
            for c in range(3):
                out[g * 3 + c] = acc[g * 3 + c] + fold(jnp.where(m, u[c], 0.0))
        return tuple(out)

    base = (me * ncr) % LANES

    def make_row(p, acc, first):
        a = jnp.concatenate([jnp.sum(b, axis=0, keepdims=True) for b in acc], axis=0)
        col = jnp.sum(a, axis=1, keepdims=True)
        n = len(acc)
        k = lax.broadcasted_iota(jnp.int32, (n, LANES), 0)
        lane = lax.broadcasted_iota(jnp.int32, (n, LANES), 1)
        target = (base + first + k) & (LANES - 1)
        row = jnp.sum(jnp.where(lane == target, col, 0.0), axis=0, keepdims=True)
        row_send[p, 0:1, :] = row
        rows[p, pl.ds(me, 1), :] = row

    def gather_start(p):
        def send(i, _):
            pltpu.make_async_remote_copy(
                src_ref=row_send.at[p, pl.ds(0, 1)], dst_ref=rows.at[p, pl.ds(me, 1)],
                send_sem=ag_send.at[p], recv_sem=ag_recv.at[p],
                device_id=peer(i), device_id_type=MESH).start()
            return 0
        lax.fori_loop(1, ND, send, 0, unroll=ND <= 64)

    def gather_wait(p, sem):
        part = rows.at[p, pl.ds(0, ND - 1)]
        pltpu.make_async_copy(part, part, sem.at[p]).wait()

    def coarse_vector(p):
        tiles = []
        for t in range(NC // LANES):
            lo = (LANES * t) // ncr // SUB * SUB
            hi = min(ND, -(-(-(-(LANES * (t + 1)) // ncr)) // SUB) * SUB)
            d = lax.broadcasted_iota(jnp.int32, (hi - lo, LANES), 0) + lo
            j = lax.broadcasted_iota(jnp.int32, (hi - lo, LANES), 1) + LANES * t
            m = (j >= d * ncr) & (j < d * ncr + ncr)
            tiles.append(jnp.sum(jnp.where(m, rows[p, lo:hi, :], 0.0), axis=0, keepdims=True))
        return tiles

    def total(p, s):
        d = lax.broadcasted_iota(jnp.int32, (ND, LANES), 0)
        lane = lax.broadcasted_iota(jnp.int32, (ND, LANES), 1)
        m = lane == ((d * ncr + ncr + s) & (LANES - 1))
        v = jnp.sum(jnp.where(m, rows[p], 0.0), axis=0, keepdims=True)
        return jnp.sum(v, axis=1, keepdims=True)

    def answers(tiles, ref):
        s = ref[:, 0:LANES] * tiles[0]
        for t in range(1, len(tiles)):
            s = s + ref[:, t * LANES:(t + 1) * LANES] * tiles[t]
        q = jnp.sum(s, axis=1, keepdims=True)
        return [q[i:i + 1, :] for i in range(ncr)]

    def spread(reg, q):
        masks = [reg == g for g in range(G)]
        out = []
        for c in range(3):
            s = jnp.zeros(reg.shape, f32)
            for g in range(G):
                s = jnp.where(masks[g], q[g * 3 + c], s)
            out.append(s)
        return out

    def halo(slot, d, src, dst):
        return pltpu.make_async_remote_copy(
            src_ref=src, dst_ref=dst, send_sem=hs_send.at[slot, d],
            recv_sem=hs_recv.at[slot, d ^ 1], device_id=to[d], device_id_type=MESH)

    def copies(kind, d):
        e = d ^ 1
        if kind == 0:
            if d < 2:
                x = 0 if d == 0 else X - 1
                return [halo(0, d, occ_v.at[x], ix_in.at[e, 0]),
                        halo(1, d, reg_v.at[x], ix_in.at[e, 1])]
            return [halo(0, d, iy_send.at[d - 2, 0], iy_in.at[e - 2, 0]),
                    halo(1, d, iy_send.at[d - 2, 1], iy_in.at[e - 2, 1])]
        if kind == 1:
            return [halo(2, d, c_v, c_in.at[e])]
        p = kind - 2
        if d < 2:
            return [halo(3 + p, d, wx_send.at[p, d], wx_in.at[p, e])]
        return [halo(3 + p, d, wy_send.at[p, d - 2], wy_in.at[p, e - 2])]

    def halo_start(kind):
        for d in range(4):
            @pl.when(has[d])
            def _():
                for c in copies(kind, d):
                    c.start()

    def halo_wait(kind):
        for d in range(4):
            @pl.when(has[d])
            def _():
                for c in copies(kind, d ^ 1):
                    c.wait_recv()

    def halo_done(kind):
        for d in range(4):
            @pl.when(has[d])
            def _():
                for c in copies(kind, d):
                    c.wait_send()

    loads[2].wait()
    acc = looped(0, X, lambda x, a: add_rc(a, reg_v[x], [r_v[c, x] for c in range(3)]),
                        zero_acc(ncr))
    make_row(0, acc, 0)
    loads[3].wait()

    pl.semaphore_wait(barrier, ND - 1)
    halo_start(0)
    gather_start(0)
    halo_start(1)

    def stiff_of(o):
        return soft_stiff + (bone_stiff - soft_stiff) * o.astype(f32)

    def own_k(x, _):
        k_p[x + 1] = stiff_of(occ_v[x])
        return 0

    looped(0, X, own_k, 0)
    halo_wait(0)
    for d in range(2):
        @pl.when(has[d])
        def _():
            k_p[0 if d == 0 else X + 1] = stiff_of(ix_in[d, 0])

        @pl.when(jnp.logical_not(has[d]))
        def _():
            k_p[0 if d == 0 else X + 1] = jnp.zeros((Y, Z), f32)

    row_id = lax.broadcasted_iota(jnp.int32, (Y, Z), 0)
    lane_id = lax.broadcasted_iota(jnp.int32, (Y, Z), 1)
    side_lo = jnp.where(has[2], 1.0, 0.0).astype(f32)
    side_hi = jnp.where(has[3], 1.0, 0.0).astype(f32)

    def yshift(u, lo, hi):
        down = jnp.where(row_id == 0, lo, pltpu.roll(u, 1, 0))
        up = jnp.where(row_id == Y - 1, hi, pltpu.roll(u, Y - 1, 0))
        return down, up

    def save_faces(p, x, w):
        for c in range(3):
            wy_send[p, 0, c, pl.ds(x, 1), :] = w[c][0:1, :]
            wy_send[p, 1, c, pl.ds(x, 1), :] = w[c][Y - 1:Y, :]

    def coefficients(x, _):
        k = k_p[x + 1]
        lo = stiff_of(iy_in[0, 0, pl.ds(x, 1), :]) * side_lo
        hi = stiff_of(iy_in[1, 0, pl.ds(x, 1), :]) * side_hi
        down, up = yshift(k, lo, hi)
        back = jnp.where(lane_id == 0, 0.0, pltpu.roll(k, 1, 1))
        ahead = jnp.where(lane_id == Z - 1, 0.0, pltpu.roll(k, Z - 1, 1))
        xm = 0.5 * (k + k_p[x])
        xp = 0.5 * (k + k_p[x + 2])
        ym = 0.5 * (k + down)
        yp = 0.5 * (k + up)
        zm = 0.5 * (k + back)
        zp = 0.5 * (k + ahead)
        diag = xm + xp + ym + yp + zm + zp + 0.5 * k
        inv = 1.0 / diag
        kx[x] = xm
        kx[x + 1] = xp
        kym[x] = ym
        kyp[x] = yp
        kzm[x] = jnp.where(lane_id == 0, 0.0, zm)
        kzp[x] = jnp.where(lane_id == Z - 1, 0.0, zp)
        dg[x] = diag - 0.25 * k
        invd[x] = inv
        w = [r_v[c, x] * inv for c in range(3)]
        for c in range(3):
            z_p[c, x + 1] = w[c]
        save_faces(0, x, w)
        return 0

    looped(0, X, coefficients, 0)
    for c in range(3):
        wx_send[0, 0, c] = z_p[c, 1]
        wx_send[0, 1, c] = z_p[c, X]
    halo_start(2)

    def edges(p, qs, pad, side):
        for d in range(2):
            s = spread(ix_in[d, 1], qs[d])
            for c in range(3):
                pad[c, 0 if d == 0 else X + 1] = wx_in[p, d, c] + s[c]
        for d in range(2):
            s = spread(iy_in[d, 1], qs[2 + d])
            for c in range(3):
                side[d, c] = wy_in[p, d, c] + s[c]

    def operate(pad, side, x):
        k = k_p[x + 1]
        u = [pad[c, x + 1] for c in range(3)]
        k4 = 0.25 * k * (u[0] + u[1] + u[2])
        out = []
        for c in range(3):
            down, up = yshift(u[c], side[0, c, pl.ds(x, 1), :], side[1, c, pl.ds(x, 1), :])
            a = dg[x] * u[c] + k4
            a = a - (kx[x] * pad[c, x] + kx[x + 1] * pad[c, x + 2])
            a = a - (kym[x] * down + kyp[x] * up)
            a = a - (kzm[x] * pltpu.roll(u[c], 1, 1) + kzp[x] * pltpu.roll(u[c], Z - 1, 1))
            out.append(a)
        return u, out

    gather_wait(0, ag_recv)
    halo_wait(1)
    tiles = coarse_vector(0)
    q = answers(tiles, c_v)
    qs = [answers(tiles, c_in.at[d]) for d in range(4)]

    def add_spread(x, _):
        s = spread(reg_v[x], q)
        for c in range(3):
            z = z_p[c, x + 1] + s[c]
            z_p[c, x + 1] = z
            z0_v[c, x] = z
        return 0

    looped(0, X, add_spread, 0)
    halo_wait(2)
    edges(0, qs, z_p, zy)

    def dots(a, b):
        return fold(a[0] * b[0] + a[1] * b[1] + a[2] * b[2])

    def first(x, carry):
        u, a = operate(z_p, zy, x)
        r = [r_v[c, x] for c in range(3)]
        w = []
        for c in range(3):
            y_v[c, x] = a[c]
            w.append(a[c] * invd[x])
            v_p[c, x + 1] = w[c]
        save_faces(1, x, w)
        acc = add_rc(carry[:ncr], reg_v[x], a)
        return acc + (carry[ncr] + dots(r, u), carry[ncr + 1] + dots(a, u))

    acc = looped(0, X, first, zero_acc(ncr + 2))
    make_row(1, acc, 0)
    gather_start(1)
    for c in range(3):
        wx_send[1, 0, c] = v_p[c, 1]
        wx_send[1, 1, c] = v_p[c, X]
    halo_start(3)
    halo_wait(3)
    gather_wait(1, ag_recv)
    tiles = coarse_vector(1)
    q = answers(tiles, c_v)
    qs = [answers(tiles, c_in.at[d]) for d in range(4)]
    rz0 = total(1, 0)
    alpha0 = rz0 / total(1, 1)

    def add_spread_v(x, _):
        s = spread(reg_v[x], q)
        for c in range(3):
            v_p[c, x + 1] = v_p[c, x + 1] + s[c]
        return 0

    looped(0, X, add_spread_v, 0)
    edges(1, qs, v_p, vy)

    def second(x, carry):
        u, a = operate(v_p, vy, x)
        r, z, az = [], [], []
        for c in range(3):
            y = y_v[c, x]
            r.append(r_v[c, x] - alpha0 * y)
            z.append(z_p[c, x + 1] - alpha0 * u[c])
            az.append(y - alpha0 * a[c])
            r_v[c, x] = r[c]
            z1_v[c, x] = z[c]
            az_v[c, x] = az[c]
        return (carry[0] + dots(r, z), carry[1] + dots(az, z))

    acc = looped(0, X, second, zero_acc(2))
    make_row(2, acc, ncr)
    gather_start(2)
    gather_wait(2, ag_recv)
    rz1 = total(2, 0)
    beta = rz1 / rz0
    alpha1 = rz1 / (total(2, 1) - beta * rz1 / alpha0)
    along = alpha0 + alpha1 * beta
    a1b = alpha1 * beta

    sc_v[0:1, :] = jnp.broadcast_to(along, (1, LANES))
    sc_v[1:2, :] = jnp.broadcast_to(alpha1, (1, LANES))
    sc_v[2:3, :] = jnp.broadcast_to(a1b, (1, LANES))
    for kind in range(4):
        halo_done(kind)
    for p in range(3):
        gather_wait(p, ag_send)


def finish_wide(z0_v, z1_v, r_v, az_v, y_v, sc_v, x_out, res_out, xb, rb, sem):
    along = sc_v[0:1, 0:1]
    alpha1 = sc_v[1:2, 0:1]
    a1b = sc_v[2:3, 0:1]
    X = z0_v.shape[1]
    copies = []
    for c in range(3):
        for x in range(X):
            xb[c, x] = along * z0_v[c, x] + alpha1 * z1_v[c, x]
            rb[c, x] = r_v[c, x] - alpha1 * az_v[c, x] - a1b * y_v[c, x]
        for n, (src, dst) in enumerate(((xb, x_out), (rb, res_out))):
            copies.append(pltpu.make_async_copy(src.at[c], dst.at[c], sem.at[n, c]))
            copies[-1].start()
    for copy in copies:
        copy.wait()


def local_wide(nw, nn, right_side, occupancy, region, coarse_inverse):
    _, X, Y, Z = right_side.shape
    ncr, NC = coarse_inverse.shape
    ND = nw * nn
    f32, i32 = jnp.float32, jnp.int32
    V = pltpu.VMEM
    field, pad, scal = (3, X, Y, Z), (3, X + 2, Y, Z), (X, Y, Z)
    scratch = [
        V(scal, i32), V(scal, i32), V((ncr, NC), f32),
        V((X + 2, Y, Z), f32), V((X + 1, Y, Z), f32),
        V(scal, f32), V(scal, f32), V(scal, f32), V(scal, f32), V(scal, f32), V(scal, f32),
        V(pad, f32), V(pad, f32),
        V((2, 3, X, Z), f32), V((2, 3, X, Z), f32),
        V((2, 2, Y, Z), i32), V((2, 2, X, Z), i32), V((2, 2, X, Z), i32),
        V((4, ncr, NC), f32),
        V((2, 2, 3, Y, Z), f32), V((2, 2, 3, Y, Z), f32),
        V((2, 2, 3, X, Z), f32), V((2, 2, 3, X, Z), f32),
        V((3, SUB, LANES), f32), V((3, ND, LANES), f32),
        pltpu.SemaphoreType.DMA((4,)),
        pltpu.SemaphoreType.DMA((5, 4)), pltpu.SemaphoreType.DMA((5, 4)),
        pltpu.SemaphoreType.DMA((3,)), pltpu.SemaphoreType.DMA((3,)),
    ]
    parts = pl.pallas_call(
        functools.partial(kernel_wide, nw, nn),
        out_shape=(V(field, f32),) * 5 + (V((SUB, LANES), f32),),
        in_specs=[pl.BlockSpec(memory_space=pltpu.HBM)] * 4,
        out_specs=(pl.BlockSpec(memory_space=pltpu.VMEM),) * 6,
        scratch_shapes=scratch,
        compiler_params=pltpu.CompilerParams(collective_id=0, has_side_effects=True, vmem_limit_bytes=32 * 1024 * 1024),
    )(*[pltpu.with_memory_space_constraint(a, pltpu.HBM) for a in (right_side, occupancy, region, coarse_inverse)])
    return pl.pallas_call(
        finish_wide,
        out_shape=(jax.ShapeDtypeStruct(field, f32),) * 2,
        in_specs=[pl.BlockSpec(memory_space=pltpu.VMEM)] * 6,
        out_specs=(pl.BlockSpec(memory_space=pltpu.HBM),) * 2,
        scratch_shapes=[V(field, f32), V(field, f32), pltpu.SemaphoreType.DMA((2, 3))],
        compiler_params=pltpu.CompilerParams(vmem_limit_bytes=16 * 1024 * 1024),
    )(*parts)


REPLICATED_BYTES = 4 * 1024 * 1024
DEEP = 3
AROUND = ((-1, 0), (1, 0), (0, -1), (0, 1), (-1, -1), (-1, 1), (1, -1), (1, 1))
BACK = tuple(AROUND.index((-a, -b)) for a, b in AROUND)


def group_of(n):
    return max(d for d in range(1, n + 1) if n % d == 0 and d * d <= n)


def spread_over(reg, q, G, inside=False):
    masks = [reg == g for g in range(G)]
    out = []
    for c in range(3):
        s = q[(G - 1) * 3 + c] if inside else jnp.where(masks[G - 1], q[(G - 1) * 3 + c], 0.0)
        for g in range(G - 1):
            s = jnp.where(masks[g], q[g * 3 + c], s)
        out.append(s)
    return out


def rows_from(low, count):
    return pl.ds(SUB + low, count)


def both_sides(ref, Y, *at):
    row = lax.broadcasted_iota(jnp.int32, (SUB, LANES), 0)
    return jnp.where(row < SUB // 2, ref[(*at, pl.ds(SUB + Y, SUB))], ref[(*at, pl.ds(0, SUB))])


def apply(ref, coefficients, x, low, count):
    kx, kyp, kzm, kzp, dg, k4 = coefficients
    here, down, up = rows_from(low, count), rows_from(low - 1, count), rows_from(low + 1, count)
    u = [ref[c, x, here] for c in range(3)]
    kk = k4[x, here] * (u[0] + u[1] + u[2])
    out = []
    for c in range(3):
        a = kx[x, here] * ref[c, x - 1, here] + kx[x + 1, here] * ref[c, x + 1, here]
        a = a + (kyp[x, down] * ref[c, x, down] + kyp[x, here] * ref[c, x, up])
        a = a + (kzm[x, here] * pltpu.roll(u[c], 1, 1) + kzp[x, here] * pltpu.roll(u[c], LANES - 1, 1))
        out.append(dg[x, here] * u[c] + kk - a)
    return u, out


def kernel(nw, nn, r_hbm, occ_hbm, reg_hbm, ci_hbm,
           z_e, g_e, y_e, r_o, ag_o, reg_o, k4, dg, kx, kyp, kzm, kzp, q_o, sc_o,
           occ_e, reg_e, r_e, k_e, invd,
           call, c_in, y_face, y_label, qpair, row_send, rows, sizes,
           load_sem, send, recv, ready):
    E, YE, Z = occ_e.shape
    X, Y = E - 2 * DEEP, YE - 2 * SUB
    ncr, NC = c_in.shape[1:]
    G = ncr // 3
    ND = nw * nn
    NH = ND // 2
    wi = lax.axis_index("wide")
    ni = lax.axis_index("narrow")
    me = wi * nn + ni
    f32 = jnp.float32
    GW = group_of(nw)
    GP = GW * nn
    NG = ND // GP
    grp, pos = me // GP, lax.rem(me, GP)
    half, place = lax.rem(wi, 2), (lax.rem(wi, GW) // 2) * nn + ni
    here = half * NH + place * NG + grp
    own, inner_rows = pl.ds(DEEP, X), pl.ds(SUB, Y)

    loads = [pltpu.make_async_copy(s, d, load_sem.at[i]) for s, d, i in (
        (reg_hbm, reg_e.at[own, inner_rows], 0), (r_hbm, r_e.at[:, own, inner_rows], 0),
        (occ_hbm, occ_e.at[own, inner_rows], 1), (ci_hbm, call.at[here], 2))]
    for l in loads:
        l.start()

    barrier = pltpu.get_barrier_semaphore()

    def at(t):
        return (t // nn, lax.rem(t, nn))

    def wait_for(sem, count):
        @pl.when(count > 0)
        def _():
            pl.semaphore_wait(sem, count)

    def column_of(group):
        return (wi + (group - grp) * GW, ni)

    at_low = jnp.logical_and(lax.rem(wi, GW) == 0, wi > 0)
    at_high = jnp.logical_and(lax.rem(wi, GW) == GW - 1, wi < nw - 1)
    aside = 1 + jnp.where(ni > 0, 1, 0) + jnp.where(ni < nn - 1, 1, 0)

    def touching(ahead, signal):
        @pl.when(at_high if ahead > 0 else at_low)
        def _():
            for b in (-1, 0, 1):
                @pl.when(jnp.logical_and(ni + b >= 0, ni + b < nn))
                def _():
                    signal((wi + ahead, ni + b))

    def say(sem):
        return lambda device: pl.semaphore_signal(sem, inc=1, device_id=device, device_id_type=MESH)

    for i in range(1, GP):
        say(barrier)(at(grp * GP + lax.rem(pos + i, GP)))
    touching(1, say(barrier))
    touching(-1, say(barrier))
    for k in range(1, NG):
        @pl.when(grp + k < NG)
        def _():
            say(barrier)(column_of(grp + k))

    def tell():
        for k in range(1, NG):
            @pl.when(grp >= k)
            def _():
                say(ready.at[k - 1])(column_of(grp - k))

    def take(rows_of, sem):
        some = sizes.at[pl.ds(0, rows_of)]
        pltpu.make_async_copy(some, some, sem).wait()

    def take_c(blocks, sem):
        some = call.at[pl.ds(0, blocks)]
        pltpu.make_async_copy(some, some, sem).wait()

    def by_neighbours(wait):
        nx = jnp.where(wi > 0, 1, 0) + jnp.where(wi < nw - 1, 1, 0)
        ny = jnp.where(ni > 0, 1, 0) + jnp.where(ni < nn - 1, 1, 0)
        for a in ((1,) if nw == 2 else (1, 2)):
            for b in (range(min(nn, 2)) if nn == 1 else (1,) if nn == 2 else (1, 2)):
                @pl.when(jnp.logical_and(nx == a, ny == b))
                def _():
                    wait(a, b)

    def halo_rows(n, a, b):
        deep, corner, count = ((DEEP, 2, 1), (2, 1, 1), (2, 1, 3))[n]
        return count * (a * deep * Y + b * deep * X + a * b * corner * corner)

    has = []
    for a, b in AROUND:
        h = jnp.logical_and(wi + a >= 0, wi + a < nw)
        has.append(jnp.logical_and(h, jnp.logical_and(ni + b >= 0, ni + b < nn)))

    def part(arr, d, into):
        a, b = AROUND[d]
        deep = {0: DEEP, 1: 2, 2: 2}[arr] if a == 0 or b == 0 else {0: 2, 1: 1, 2: 1}[arr]
        if into:
            xs = {-1: (DEEP - deep, deep), 0: (DEEP, X), 1: (DEEP + X, deep)}[a]
            ys = {-1: (SUB - deep, deep), 0: (SUB, Y), 1: (SUB + Y, deep)}[b]
        else:
            xs = {-1: (DEEP, deep), 0: (DEEP, X), 1: (DEEP + X - deep, deep)}[a]
            ys = {-1: (SUB, deep), 0: (SUB, Y), 1: (SUB + Y - deep, deep)}[b]
        xs, ys = pl.ds(*xs), pl.ds(*ys)
        return (slice(None), xs, ys) if arr == 2 else (xs, ys)

    fields = (occ_e, reg_e, r_e)
    for d in range(8):
        @pl.when(jnp.logical_not(has[d]))
        def _():
            for n, ref in enumerate(fields):
                where = part(n, d, True)
                v = ref[where]
                ref[where] = jnp.full(v.shape, (-1, -1, 0)[n], v.dtype)
            c_in[d] = jnp.zeros((ncr, NC), f32)

    wait_for(barrier, GP - 1 + grp + jnp.where(at_low, aside, 0) + jnp.where(at_high, aside, 0))
    tell()

    def fold(a):
        return jnp.sum(a.reshape(a.shape[0] // SUB, SUB, Z), axis=0)

    def zero_acc(n):
        return tuple(jnp.zeros((SUB, Z), f32) for _ in range(n))

    def add_rc(acc, reg, u):
        out = list(acc)
        for g in range(G):
            m = reg == g
            for c in range(3):
                out[g * 3 + c] = acc[g * 3 + c] + fold(jnp.where(m, u[c], 0.0))
        return out

    base = (me * ncr) % LANES

    def column(acc):
        a = jnp.concatenate([jnp.sum(b, axis=0, keepdims=True) for b in acc], axis=0)
        return jnp.sum(a, axis=1, keepdims=True)

    def make_row(p, acc):
        col = column(acc)
        n = len(acc)
        k = lax.broadcasted_iota(jnp.int32, (n, LANES), 0)
        lane = lax.broadcasted_iota(jnp.int32, (n, LANES), 1)
        target = (base + k) & (LANES - 1)
        row = jnp.sum(jnp.where(lane == target, col, 0.0), axis=0, keepdims=True)
        row_send[p, 0:1, :] = row
        rows[p, pl.ds(me, 1), :] = row

    def rows_to(p, count, t, out, sem):
        pltpu.make_async_remote_copy(
            src_ref=row_send.at[pl.ds(p, count), pl.ds(0, 1)], dst_ref=rows.at[pl.ds(p, count), pl.ds(me, 1)],
            send_sem=send.at[out], recv_sem=recv.at[sem],
            device_id=at(t), device_id_type=MESH).start()

    def each_peer(send):
        def body(i, _):
            send(i + jnp.where(i < me, 0, 1))
            return 0
        lax.fori_loop(0, ND - 1, body, 0, unroll=ND <= 64)

    take(4 * X * Y, load_sem.at[0])
    acc = looped(0, X, lambda x, a: tuple(add_rc(
        a, reg_e[x + DEEP, inner_rows], [r_e[c, x + DEEP, inner_rows] for c in range(3)])), zero_acc(ncr))
    make_row(0, acc)

    def inside(i, _):
        rows_to(0, 1, grp * GP + lax.rem(pos + i, GP), 0, 3)
        return 0

    lax.fori_loop(1, GP, inside, 0, unroll=GP <= 64)

    def halo(n, d):
        a, b = AROUND[d]
        e = BACK[d]
        return pltpu.make_async_remote_copy(
            src_ref=fields[n].at[part(n, d, False)], dst_ref=fields[n].at[part(n, e, True)],
            send_sem=send.at[0], recv_sem=recv.at[min(n, 1)],
            device_id=(wi + a, ni + b), device_id_type=MESH)

    def halo_c(d):
        a, b = AROUND[d]
        return pltpu.make_async_remote_copy(
            src_ref=call.at[here], dst_ref=c_in.at[BACK[d]],
            send_sem=send.at[1], recv_sem=recv.at[2],
            device_id=(wi + a, ni + b), device_id_type=MESH)

    loads[2].wait()
    loads[3].wait()

    for n in range(3):
        for d in range(8):
            @pl.when(has[d])
            def _():
                halo(n, d).start()

    def c_group(block, sem):
        for i in range(1, GP // 2):
            p = lax.rem(place + i, GP // 2)
            pltpu.make_async_remote_copy(
                src_ref=call.at[block], dst_ref=call.at[block],
                send_sem=send.at[2], recv_sem=recv.at[sem],
                device_id=(grp * GW + (p // nn) * 2 + half, lax.rem(p, nn)), device_id_type=MESH).start()

    c_group(here, 9)
    for d in range(8):
        if AROUND[d][0]:
            @pl.when(has[d])
            def _():
                halo_c(d).start()

    def c_column(group):
        pltpu.make_async_remote_copy(
            src_ref=call.at[here], dst_ref=call.at[here],
            send_sem=send.at[2], recv_sem=recv.at[5],
            device_id=column_of(group), device_id_type=MESH).start()

    for k in range(1, NG):
        @pl.when(grp >= k)
        def _():
            c_column(grp - k)

    def stiff_of(o):
        return jnp.where(o < 0, 0.0, soft_stiff + (bone_stiff - soft_stiff) * o.astype(f32))

    n2 = G * G

    def pairs(acc, first, seconds):
        out = list(acc)
        for g in range(G):
            t = None
            for label, value in seconds:
                v = jnp.where(label == g, value, 0.0)
                t = v if t is None else t + v
            for h in range(G):
                out[h * G + g] = acc[h * G + g] + fold(jnp.where(first == h, t, 0.0))
        return out

    row16 = lax.broadcasted_iota(jnp.int32, (Y, Z), 0)
    lane16 = lax.broadcasted_iota(jnp.int32, (Y, Z), 1)

    def own_pairs(i, carry):
        x = i + DEEP
        k, reg = stiff_of(occ_e[x, inner_rows]), reg_e[x, inner_rows]
        later = jnp.minimum(i + 1, X - 1) + DEEP
        kx_in = jnp.where(i < X - 1, 0.5 * (k + stiff_of(occ_e[later, inner_rows])), 0.0)
        ky_in = jnp.where(row16 == Y - 1, 0.0, 0.5 * (k + pltpu.roll(k, Y - 1, 0)))
        kz_in = jnp.where(lane16 == Z - 1, 0.0, 0.5 * (k + pltpu.roll(k, Z - 1, 1)))
        acc = pairs(carry[:n2], reg, ((reg_e[later, inner_rows], kx_in), (pltpu.roll(reg, Y - 1, 0), ky_in),
                                      (pltpu.roll(reg, Z - 1, 1), kz_in)))
        sums = [carry[n2 + g] + fold(jnp.where(reg == g, 0.25 * k, 0.0)) for g in range(G)]
        return tuple(acc) + tuple(sums)

    own_acc = lax.fori_loop(0, X, own_pairs, zero_acc(n2 + G), unroll=2)
    own_col = column(own_acc)

    def c_up(k):
        @pl.when(grp + k < NG)
        def _():
            pl.semaphore_wait(ready.at[k - 1], 1)
            c_column(grp + k)

    for k in range(1, NG):
        c_up(k)

    take(GP - 1, recv.at[3])
    mine = rows.at[0, pl.ds(pl.multiple_of(grp * GP, GP), GP)]

    def across(group):
        pltpu.make_async_remote_copy(
            src_ref=mine, dst_ref=mine, send_sem=send.at[0], recv_sem=recv.at[4],
            device_id=column_of(group), device_id_type=MESH).start()

    for k in range(1, NG):
        @pl.when(grp >= k)
        def _():
            across(grp - k)

    for k in range(1, NG):
        @pl.when(grp + k < NG)
        def _():
            across(grp + k)

    by_neighbours(lambda a, b: take(halo_rows(0, a, b), recv.at[0]))

    lane_id = lax.broadcasted_iota(jnp.int32, (Y + SUB, Z), 1)

    def stiffness(x, _):
        k_e[x] = stiff_of(occ_e[x])
        return 0

    lax.fori_loop(0, E, stiffness, 0, unroll=True)
    row8 = lax.broadcasted_iota(jnp.int32, (SUB, Z), 0)

    def coefficients(x):
        here = rows_from(-2, Y + SUB)
        k = k_e[x, here]
        low, high = k_e[x, rows_from(-3, Y + SUB)], k_e[x, rows_from(-1, Y + SUB)]
        back = jnp.where(lane_id == 0, 0.0, pltpu.roll(k, 1, 1))
        ahead = jnp.where(lane_id == Z - 1, 0.0, pltpu.roll(k, Z - 1, 1))
        xm = 0.5 * (k + k_e[x - 1, here])
        xp = 0.5 * (k + k_e[x + 1, here])
        ym = 0.5 * (k + low)
        yp = 0.5 * (k + high)
        zm = 0.5 * (k + back)
        zp = 0.5 * (k + ahead)
        diag = xm + xp + ym + yp + zm + zp + 0.5 * k
        kx[x, here] = xm
        kx[x + 1, here] = xp
        kyp[x, here] = yp
        kzm[x, here] = jnp.where(lane_id == 0, 0.0, zm)
        kzp[x, here] = jnp.where(lane_id == Z - 1, 0.0, zp)
        dg[x, here] = diag - 0.25 * k
        k4[x, here] = 0.25 * k
        invd[x, here] = jnp.where(k > 0.0, 1.0 / diag, 0.0)

    for x in (1, 2, DEEP + X, DEEP + X + 1):
        coefficients(x)

    def inner(i, sums):
        coefficients(i + DEEP)
        d, reg = dg[i + DEEP, inner_rows], reg_e[i + DEEP, inner_rows]
        return tuple(sums[g] + fold(jnp.where(reg == g, d, 0.0)) for g in range(G))

    sum_acc = lax.fori_loop(0, X, inner, zero_acc(G), unroll=4)

    by_neighbours(lambda a, b: take(halo_rows(1, a, b) + halo_rows(2, a, b), recv.at[1]))

    def side_rows(i, _):
        x = i + DEEP
        y_face[pl.ds(i, 1), :] = kyp[x, rows_from(Y - 1, 1), :]
        y_label[0, pl.ds(i, 1), :] = reg_e[x, rows_from(Y - 1, 1), :]
        y_label[1, pl.ds(i, 1), :] = reg_e[x, rows_from(Y, 1), :]
        return 0

    looped(0, X, side_rows, 0)
    top = DEEP + X - 1
    x_acc = pairs(zero_acc(n2), reg_e[top, inner_rows], ((reg_e[top + 1, inner_rows], kx[top + 1, inner_rows]),))
    y_acc = pairs(zero_acc(n2), y_label[0], ((y_label[1], y_face[...]),))
    rim_col = column(tuple(x_acc) + tuple(y_acc) + tuple(sum_acc))

    lane = lax.broadcasted_iota(jnp.int32, (n2, LANES), 1)
    pair = lax.broadcasted_iota(jnp.int32, (n2, LANES), 0)
    at_pair = jnp.logical_and(lane >= 3 * pair, lane < 3 * pair + 3)

    def lanes_of(col, mask):
        return jnp.sum(jnp.where(mask, col, 0.0), axis=0, keepdims=True)

    lane_g = lax.broadcasted_iota(jnp.int32, (G, LANES), 1)
    row_g = lax.broadcasted_iota(jnp.int32, (G, LANES), 0)
    diag_at, sum_at = 3 * (G + 1) * row_g, 3 * n2 + 9 * row_g
    at_diag = jnp.logical_and(lane_g >= diag_at, lane_g < diag_at + 3)
    at_sum = jnp.logical_and(lane_g >= sum_at, lane_g < sum_at + 9)
    ac_rows = (lanes_of(own_col[0:n2], at_pair) * -2.0 + lanes_of(rim_col[2 * n2:], at_diag)
               + lanes_of(own_col[n2:], at_sum),
               lanes_of(rim_col[0:n2], at_pair) * -2.0, lanes_of(rim_col[n2:2 * n2], at_pair) * -2.0)
    for n in range(3):
        row_send[n + 2, 0:1, :] = ac_rows[n]
        rows[n + 2, pl.ds(me, 1), :] = ac_rows[n]

    def coarse_vector(block):
        tiles = []
        for t in range(NC // LANES):
            lo = (LANES * t) // ncr // SUB * SUB
            hi = min(ND, -(-(-(-(LANES * (t + 1)) // ncr)) // SUB) * SUB)
            d = lax.broadcasted_iota(jnp.int32, (hi - lo, LANES), 0) + lo
            j = lax.broadcasted_iota(jnp.int32, (hi - lo, LANES), 1) + LANES * t
            m = (j >= d * ncr) & (j < d * ncr + ncr)
            tiles.append(jnp.sum(jnp.where(m, block[lo:hi, :], 0.0), axis=0, keepdims=True))
        return tiles

    def total(block, s):
        d = lax.broadcasted_iota(jnp.int32, (ND, LANES), 0)
        lane = lax.broadcasted_iota(jnp.int32, (ND, LANES), 1)
        m = lane == ((d * ncr + ncr + s) & (LANES - 1))
        v = jnp.sum(jnp.where(m, block, 0.0), axis=0, keepdims=True)
        return jnp.sum(v, axis=1, keepdims=True)

    def solve(tiles, block):
        s = block[:, 0:LANES] * tiles[0]
        for t in range(1, len(tiles)):
            s = s + block[:, t * LANES:(t + 1) * LANES] * tiles[t]
        return jnp.sum(s, axis=1, keepdims=True)

    def rows_of(d):
        a, b = AROUND[d]
        return c_in[d] if a else call[here + jnp.where(has[d], b * NG, 0)]

    def as_list(q):
        return [q[i:i + 1, :] for i in range(ncr)]

    take_c(NG - 1, recv.at[5])
    for k in range(1, NG):
        c_group(half * NH + place * NG + lax.rem(grp + k, NG), 6)

    take(ND - GP, recv.at[4])
    by_neighbours(lambda a, b: take_c(a + a * b, recv.at[2]))
    take_c(GP // 2 - 1, recv.at[9])
    tiles = coarse_vector(rows[0])
    q = as_list(solve(tiles, call[here]))
    qn = [as_list(solve(tiles, rows_of(d))) for d in range(8)]

    def either(hi, lo):
        return [jnp.where(row8 < SUB // 2, a, b) for a, b in zip(hi, lo)]

    def add_spread(x, q_in, q_out, inside):
        reg, inv = reg_e[x, inner_rows], invd[x, inner_rows]
        s = spread_over(reg, q_in, G, inside)
        reg_o[x, inner_rows] = reg
        for c in range(3):
            z_e[c, x, inner_rows] = r_e[c, x, inner_rows] * inv + s[c]
        reg, inv = both_sides(reg_e, Y, x), both_sides(invd, Y, x)
        s = spread_over(reg, q_out, G)
        some = SUB // 2
        reg_o[x, rows_from(Y, some)] = reg[0:some]
        reg_o[x, rows_from(-some, some)] = reg[some:SUB]
        for c in range(3):
            z = both_sides(r_e, Y, c, x) * inv + s[c]
            z_e[c, x, rows_from(Y, some)] = z[0:some]
            z_e[c, x, rows_from(-some, some)] = z[some:SUB]

    q_side = either(qn[3], qn[2])

    def spread_own(i, _):
        add_spread(i + DEEP, q, q_side, True)
        return 0

    looped(0, X, spread_own, 0)
    q_low, q_high = either(qn[5], qn[4]), either(qn[7], qn[6])
    for x in (1, 2):
        add_spread(x, qn[0], q_low, False)
    for x in (DEEP + X, DEEP + X + 1):
        add_spread(x, qn[1], q_high, False)

    faces = (kx, kyp, kzm, kzp, dg, k4)

    def dots(a, b):
        return fold(a[0] * b[0] + a[1] * b[1] + a[2] * b[2])

    def first(i, _):
        x, some = i + DEEP - 1, rows_from(-1, Y + SUB)
        _, a = apply(z_e, faces, x, -1, Y + SUB)
        for c in range(3):
            y_e[c, x, some] = a[c]
            g_e[c, x, some] = a[c] * invd[x, some]
        return 0

    lax.fori_loop(0, X + 2, first, 0, unroll=(X + 2) // 2)

    def own_of(ref, x):
        return [ref[c, x, inner_rows] for c in range(3)]

    def second(i, carry):
        x = i + DEEP
        w, a = apply(g_e, faces, x, 0, Y)
        for c in range(3):
            ag_o[c, i] = a[c]
        acc = add_rc(carry[:ncr], reg_e[x, inner_rows], a)
        return tuple(acc) + (carry[ncr] + dots(w, a),)

    acc2 = lax.fori_loop(0, X, second, zero_acc(ncr + 1), unroll=8)

    def third(i, carry):
        x = i + DEEP
        r, z, y, w = own_of(r_e, x), own_of(z_e, x), own_of(y_e, x), own_of(g_e, x)
        for c in range(3):
            r_o[c, i] = r[c]
        acc = add_rc(carry[:ncr], reg_e[x, inner_rows], y)
        return tuple(acc) + (carry[ncr] + dots(r, z), carry[ncr + 1] + dots(y, z), carry[ncr + 2] + dots(y, w))

    acc1 = lax.fori_loop(0, X, third, zero_acc(ncr + 3), unroll=8)
    make_row(1, tuple(acc1) + (acc2[ncr],) + tuple(acc2[:ncr]))
    each_peer(lambda t: rows_to(1, 4, t, 3, 7))

    take_c((GP // 2 - 1) * (NG - 1), recv.at[6])
    swap_half = call.at[pl.ds(half * NH, NH)]
    swap = pltpu.make_async_remote_copy(
        src_ref=swap_half, dst_ref=swap_half, send_sem=send.at[2], recv_sem=recv.at[8],
        device_id=(wi + 1 - 2 * half, ni), device_id_type=MESH)
    swap.start()
    by_neighbours(lambda a, b: take(
        sum(halo_rows(n, a, b) for n in range(3)) + GP - 1 + (NG - 1) * GP, send.at[0]))
    by_neighbours(lambda a, b: take_c(a + a * b, send.at[1]))
    swap.wait_recv()
    take(4 * (ND - 1), recv.at[7])

    block = rows[1]
    b1 = coarse_vector(block)
    h1 = coarse_vector(pltpu.roll(block, LANES - ncr - 4, 1))
    rr = lax.broadcasted_iota(jnp.int32, (ncr, LANES), 0)
    ll = lax.broadcasted_iota(jnp.int32, (ncr, LANES), 1)
    m0, m1 = rr < 0, rr < 0
    for h in range(G):
        for g in range(G):
            for c in range(3):
                k = (h * G + g) * 3 + c
                m0 = jnp.logical_or(m0, (ll == k) & (rr == h * 3 + c))
                m1 = jnp.logical_or(m1, (ll == k) & (rr == g * 3 + c))
        for c in range(3):
            for e in range(3):
                k = 3 * n2 + h * 9 + c * 3 + e
                m0 = jnp.logical_or(m0, (ll == k) & (rr == h * 3 + c))
                m1 = jnp.logical_or(m1, (ll == k) & (rr == h * 3 + e))
    lines = [jnp.zeros((ncr, LANES), f32) for _ in b1]
    for w in range(nw):
        for n in range(nn):
            d = w * nn + n
            q1 = solve(b1, call[w % 2 * NH + ((w % GW) // 2 * nn + n) * NG + w // GW])
            qpair[0, d:d + 1, :] = jnp.sum(jnp.where(m0, q1, 0.0), axis=0, keepdims=True)
            qpair[1, d:d + 1, :] = jnp.sum(jnp.where(m1, q1, 0.0), axis=0, keepdims=True)
            for t in range(d * ncr // LANES, (d * ncr + ncr - 1) // LANES + 1):
                lines[t] = jnp.where(ll + LANES * t == rr + d * ncr, q1, lines[t])
    lines = [jnp.sum(v, axis=0, keepdims=True) for v in lines]
    first_q, second_q = qpair[0], qpair[1]
    dev = lax.broadcasted_iota(jnp.int32, (ND, LANES), 0)
    next_x = jnp.where(dev < ND - nn, pltpu.roll(second_q, ND - nn, 0), 0.0)
    next_y = jnp.where(dev < ND - 1, pltpu.roll(second_q, ND - 1, 0), 0.0)
    energy = jnp.sum(first_q * (rows[2] * second_q + rows[3] * next_x + rows[4] * next_y), axis=0, keepdims=True)
    for t in range(len(b1)):
        energy = energy + 2.0 * h1[t] * lines[t]
    yv = b1[0] * lines[0]
    for t in range(1, len(b1)):
        yv = yv + b1[t] * lines[t]
    yv = total(block, 2) + jnp.sum(yv, axis=1, keepdims=True)
    vav = total(block, 3) + jnp.sum(energy, axis=1, keepdims=True)
    rz0, zy = total(block, 0), total(block, 1)
    alpha0 = rz0 / zy
    rz1 = alpha0 * alpha0 * yv - rz0
    zaz = zy - 2.0 * alpha0 * yv + alpha0 * alpha0 * vav
    beta = rz1 / rz0
    alpha1 = rz1 / (zaz - beta * rz1 / alpha0)
    a1b = alpha1 * beta
    for n, v in enumerate((alpha0 + a1b + alpha1, alpha1 * alpha0)):
        sc_o[n:n + 1, :] = jnp.broadcast_to(v, (1, LANES))
    q_o[0] = jnp.broadcast_to(solve(b1, call[here]), (ncr, LANES))
    for d in range(4):
        q_o[d + 1] = jnp.broadcast_to(solve(b1, rows_of(d)), (ncr, LANES))

    take(4 * (ND - 1), send.at[3])
    take_c(NG - 1 + (GP // 2 - 1) * NG + NH, send.at[2])


def finish(z_v, g_v, y_v, r_v, ag_v, reg_v, k4, dg, kx, kyp, kzm, kzp, q_v, sc_v, x_out, res_out, s_e, xb, rb, sem):
    a, b = sc_v[0:1, 0:1], sc_v[1:2, 0:1]
    E, YE, Z = reg_v.shape
    X, Y = E - 2 * DEEP, YE - 2 * SUB
    G = q_v.shape[1] // 3
    own = pl.ds(SUB, Y)
    row8 = lax.broadcasted_iota(jnp.int32, (SUB, Z), 0)
    q = [[q_v[d, i:i + 1, :] for i in range(3 * G)] for d in range(5)]
    side = [jnp.where(row8 < SUB // 2, hi, lo) for hi, lo in zip(q[4], q[3])]

    def fill(x, q_in, inside):
        s = spread_over(reg_v[x, own], q_in, G, inside)
        for c in range(3):
            s_e[c, x, own] = s[c]

    def fill_sides(x):
        s = spread_over(both_sides(reg_v, Y, x), side, G)
        some = SUB // 2
        for c in range(3):
            s_e[c, x, rows_from(Y, some)] = s[c][0:some]
            s_e[c, x, rows_from(-some, some)] = s[c][some:SUB]

    def fill_own(i, _):
        fill(i + DEEP, q[0], True)
        fill_sides(i + DEEP)
        return 0

    fill(DEEP - 1, q[1], False)
    fill(DEEP + X, q[2], False)
    looped(0, X, fill_own, 0)
    faces = (kx, kyp, kzm, kzp, dg, k4)
    parts = 4
    step = X // parts

    def plane(i, _):
        x = i + DEEP
        u, w = apply(s_e, faces, x, 0, Y)
        for c in range(3):
            xb[c, i] = a * z_v[c, x, own] - b * (g_v[c, x, own] + u[c])
            rb[c, i] = r_v[c, i] - a * y_v[c, x, own] + b * (ag_v[c, i] + w[c])
        return 0

    for n in range(parts):
        lax.fori_loop(n * step, (n + 1) * step, plane, 0, unroll=True)
        for m, (src, dst) in enumerate(((xb, x_out), (rb, res_out))):
            where = (slice(None), pl.ds(n * step, step))
            pltpu.make_async_copy(src.at[where], dst.at[where], sem.at[m]).start()
    pltpu.make_async_copy(xb, x_out, sem.at[0]).wait()
    pltpu.make_async_copy(rb, res_out, sem.at[1]).wait()


def local_fast(nw, nn, right_side, occupancy, region, coarse_inverse):
    _, X, Y, Z = right_side.shape
    ncr, NC = coarse_inverse.shape
    ND = nw * nn
    f32, i32 = jnp.float32, jnp.int32
    V = pltpu.VMEM
    E, YE = X + 2 * DEEP, Y + 2 * SUB
    field, ext, scal = (3, X, Y, Z), (3, E, YE, Z), (E, YE, Z)
    ng = nw // group_of(nw)
    DMA = pltpu.SemaphoreType.DMA
    scratch = [
        V(scal, i32), V(scal, i32), V(ext, f32), V(scal, f32), V(scal, f32),
        V((ND, ncr, NC), f32), V((8, ncr, NC), f32), V((X, Z), f32), V((2, X, Z), i32), V((2, ND, LANES), f32),
        V((5, SUB, LANES), f32), V((5, ND, LANES), f32), V((4 * X * Y, LANES), f32),
        DMA((3,)), DMA((4,)), DMA((10,)),
        pltpu.SemaphoreType.REGULAR((ng - 1,)),
    ]
    outs = (V(ext, f32),) * 3 + (V(field, f32),) * 2 + (V(scal, i32),) + (V(scal, f32),) * 6 + (V((5, ncr, LANES), f32), V((SUB, LANES), f32))
    parts = pl.pallas_call(
        functools.partial(kernel, nw, nn),
        out_shape=outs,
        in_specs=[pl.BlockSpec(memory_space=pltpu.HBM)] * 4,
        out_specs=(pl.BlockSpec(memory_space=pltpu.VMEM),) * len(outs),
        scratch_shapes=scratch,
        compiler_params=pltpu.CompilerParams(collective_id=0, has_side_effects=True, vmem_limit_bytes=32 * 1024 * 1024),
    )(*[pltpu.with_memory_space_constraint(a, pltpu.HBM) for a in (right_side, occupancy, region, coarse_inverse)])
    return pl.pallas_call(
        finish,
        out_shape=(jax.ShapeDtypeStruct(field, f32),) * 2,
        in_specs=[pl.BlockSpec(memory_space=pltpu.VMEM)] * len(outs),
        out_specs=(pl.BlockSpec(memory_space=pltpu.HBM),) * 2,
        scratch_shapes=[V(ext, f32), V(field, f32), V(field, f32), DMA((2,))],
        compiler_params=pltpu.CompilerParams(vmem_limit_bytes=24 * 1024 * 1024),
    )(*parts)


def local(nw, nn, right_side, occupancy, region, coarse_inverse):
    nc = coarse_inverse.shape[1]
    run = local_fast if group_of(nw) % 2 == 0 and nc * nc * 4 <= REPLICATED_BYTES else local_wide
    return run(nw, nn, right_side, occupancy, region, coarse_inverse)


def solution(mesh):
    return jax.shard_map(
        functools.partial(local, mesh.shape["wide"], mesh.shape["narrow"]),
        mesh=mesh,
        in_specs=(
            P(None, "wide", "narrow", None),
            P("wide", "narrow", None),
            P("wide", "narrow", None),
            P(("wide", "narrow"), None),
        ),
        out_specs=(P(None, "wide", "narrow", None), P(None, "wide", "narrow", None)),
        check_vma=False,
    )
```

```python
import functools

import jax
import jax.numpy as jnp
from jax import lax
from jax.experimental import pallas as pl
from jax.experimental.pallas import tpu as pltpu
from jax.sharding import PartitionSpec as P

LANES = 128
SUB = 8
UNROLL = 16
looped = functools.partial(lax.fori_loop, unroll=UNROLL)
MESH = pl.DeviceIdType.MESH
bone_stiff = 1.0
soft_stiff = 0.1


def kernel_wide(nw, nn, r_hbm, occ_hbm, reg_hbm, ci_hbm,
           z0_v, z1_v, r_v, az_v, y_v, sc_v,
            occ_v, reg_v, c_v, k_p, kx, kym, kyp, kzm, kzp, dg, invd,
           z_p, v_p, zy, vy,
           ix_in, iy_send, iy_in, c_in, wx_send, wx_in, wy_send, wy_in,
           row_send, rows, load_sem, hs_send, hs_recv, ag_send, ag_recv):
    X, Y, Z = occ_v.shape
    ncr, NC = c_v.shape
    G = ncr // 3
    ND = nw * nn
    wi = lax.axis_index("wide")
    ni = lax.axis_index("narrow")
    me = wi * nn + ni
    f32 = jnp.float32

    loads = [pltpu.make_async_copy(s, d, load_sem.at[i]) for i, (s, d) in enumerate(
        ((occ_hbm, occ_v), (reg_hbm, reg_v), (r_hbm, r_v), (ci_hbm, c_v)))]
    for l in loads:
        l.start()

    def peer(i):
        t = lax.rem(me + i, ND)
        return (t // nn, lax.rem(t, nn))

    barrier = pltpu.get_barrier_semaphore()

    def greet(i, _):
        pl.semaphore_signal(barrier, inc=1, device_id=peer(i), device_id_type=MESH)
        return 0

    lax.fori_loop(1, ND, greet, 0, unroll=ND <= 64)

    has = (wi > 0, wi < nw - 1, ni > 0, ni < nn - 1)
    to = ((wi - 1, ni), (wi + 1, ni), (wi, ni - 1), (wi, ni + 1))

    for d in range(4):
        @pl.when(jnp.logical_not(has[d]))
        def _():
            c_in[d] = jnp.zeros((ncr, NC), f32)
            for p in range(2):
                if d < 2:
                    wx_in[p, d] = jnp.zeros((3, Y, Z), f32)
                else:
                    wy_in[p, d - 2] = jnp.zeros((3, X, Z), f32)
            if d < 2:
                ix_in[d] = jnp.zeros((2, Y, Z), jnp.int32)
            else:
                iy_in[d - 2] = jnp.zeros((2, X, Z), jnp.int32)

    loads[0].wait()
    loads[1].wait()

    def pack_ints(x, _):
        iy_send[0, 0, pl.ds(x, 1), :] = occ_v[x, 0:1, :]
        iy_send[1, 0, pl.ds(x, 1), :] = occ_v[x, Y - 1:Y, :]
        iy_send[0, 1, pl.ds(x, 1), :] = reg_v[x, 0:1, :]
        iy_send[1, 1, pl.ds(x, 1), :] = reg_v[x, Y - 1:Y, :]
        return 0

    looped(0, X, pack_ints, 0)

    def fold(a):
        return jnp.sum(a.reshape(Y // SUB, SUB, Z), axis=0)

    def zero_acc(n):
        return tuple(jnp.zeros((SUB, Z), f32) for _ in range(n))

    def add_rc(acc, reg, u):
        out = list(acc)
        for g in range(G):
            m = reg == g
            for c in range(3):
                out[g * 3 + c] = acc[g * 3 + c] + fold(jnp.where(m, u[c], 0.0))
        return tuple(out)

    base = (me * ncr) % LANES

    def make_row(p, acc, first):
        a = jnp.concatenate([jnp.sum(b, axis=0, keepdims=True) for b in acc], axis=0)
        col = jnp.sum(a, axis=1, keepdims=True)
        n = len(acc)
        k = lax.broadcasted_iota(jnp.int32, (n, LANES), 0)
        lane = lax.broadcasted_iota(jnp.int32, (n, LANES), 1)
        target = (base + first + k) & (LANES - 1)
        row = jnp.sum(jnp.where(lane == target, col, 0.0), axis=0, keepdims=True)
        row_send[p, 0:1, :] = row
        rows[p, pl.ds(me, 1), :] = row

    def gather_start(p):
        def send(i, _):
            pltpu.make_async_remote_copy(
                src_ref=row_send.at[p, pl.ds(0, 1)], dst_ref=rows.at[p, pl.ds(me, 1)],
                send_sem=ag_send.at[p], recv_sem=ag_recv.at[p],
                device_id=peer(i), device_id_type=MESH).start()
            return 0
        lax.fori_loop(1, ND, send, 0, unroll=ND <= 64)

    def gather_wait(p, sem):
        part = rows.at[p, pl.ds(0, ND - 1)]
        pltpu.make_async_copy(part, part, sem.at[p]).wait()

    def coarse_vector(p):
        tiles = []
        for t in range(NC // LANES):
            lo = (LANES * t) // ncr // SUB * SUB
            hi = min(ND, -(-(-(-(LANES * (t + 1)) // ncr)) // SUB) * SUB)
            d = lax.broadcasted_iota(jnp.int32, (hi - lo, LANES), 0) + lo
            j = lax.broadcasted_iota(jnp.int32, (hi - lo, LANES), 1) + LANES * t
            m = (j >= d * ncr) & (j < d * ncr + ncr)
            tiles.append(jnp.sum(jnp.where(m, rows[p, lo:hi, :], 0.0), axis=0, keepdims=True))
        return tiles

    def total(p, s):
        d = lax.broadcasted_iota(jnp.int32, (ND, LANES), 0)
        lane = lax.broadcasted_iota(jnp.int32, (ND, LANES), 1)
        m = lane == ((d * ncr + ncr + s) & (LANES - 1))
        v = jnp.sum(jnp.where(m, rows[p], 0.0), axis=0, keepdims=True)
        return jnp.sum(v, axis=1, keepdims=True)

    def answers(tiles, ref):
        s = ref[:, 0:LANES] * tiles[0]
        for t in range(1, len(tiles)):
            s = s + ref[:, t * LANES:(t + 1) * LANES] * tiles[t]
        q = jnp.sum(s, axis=1, keepdims=True)
        return [q[i:i + 1, :] for i in range(ncr)]

    def spread(reg, q):
        masks = [reg == g for g in range(G)]
        out = []
        for c in range(3):
            s = jnp.zeros(reg.shape, f32)
            for g in range(G):
                s = jnp.where(masks[g], q[g * 3 + c], s)
            out.append(s)
        return out

    def halo(slot, d, src, dst):
        return pltpu.make_async_remote_copy(
            src_ref=src, dst_ref=dst, send_sem=hs_send.at[slot, d],
            recv_sem=hs_recv.at[slot, d ^ 1], device_id=to[d], device_id_type=MESH)

    def copies(kind, d):
        e = d ^ 1
        if kind == 0:
            if d < 2:
                x = 0 if d == 0 else X - 1
                return [halo(0, d, occ_v.at[x], ix_in.at[e, 0]),
                        halo(1, d, reg_v.at[x], ix_in.at[e, 1])]
            return [halo(0, d, iy_send.at[d - 2, 0], iy_in.at[e - 2, 0]),
                    halo(1, d, iy_send.at[d - 2, 1], iy_in.at[e - 2, 1])]
        if kind == 1:
            return [halo(2, d, c_v, c_in.at[e])]
        p = kind - 2
        if d < 2:
            return [halo(3 + p, d, wx_send.at[p, d], wx_in.at[p, e])]
        return [halo(3 + p, d, wy_send.at[p, d - 2], wy_in.at[p, e - 2])]

    def halo_start(kind):
        for d in range(4):
            @pl.when(has[d])
            def _():
                for c in copies(kind, d):
                    c.start()

    def halo_wait(kind):
        for d in range(4):
            @pl.when(has[d])
            def _():
                for c in copies(kind, d ^ 1):
                    c.wait_recv()

    def halo_done(kind):
        for d in range(4):
            @pl.when(has[d])
            def _():
                for c in copies(kind, d):
                    c.wait_send()

    loads[2].wait()
    acc = looped(0, X, lambda x, a: add_rc(a, reg_v[x], [r_v[c, x] for c in range(3)]),
                        zero_acc(ncr))
    make_row(0, acc, 0)
    loads[3].wait()

    pl.semaphore_wait(barrier, ND - 1)
    halo_start(0)
    gather_start(0)
    halo_start(1)

    def stiff_of(o):
        return soft_stiff + (bone_stiff - soft_stiff) * o.astype(f32)

    def own_k(x, _):
        k_p[x + 1] = stiff_of(occ_v[x])
        return 0

    looped(0, X, own_k, 0)
    halo_wait(0)
    for d in range(2):
        @pl.when(has[d])
        def _():
            k_p[0 if d == 0 else X + 1] = stiff_of(ix_in[d, 0])

        @pl.when(jnp.logical_not(has[d]))
        def _():
            k_p[0 if d == 0 else X + 1] = jnp.zeros((Y, Z), f32)

    row_id = lax.broadcasted_iota(jnp.int32, (Y, Z), 0)
    lane_id = lax.broadcasted_iota(jnp.int32, (Y, Z), 1)
    side_lo = jnp.where(has[2], 1.0, 0.0).astype(f32)
    side_hi = jnp.where(has[3], 1.0, 0.0).astype(f32)

    def yshift(u, lo, hi):
        down = jnp.where(row_id == 0, lo, pltpu.roll(u, 1, 0))
        up = jnp.where(row_id == Y - 1, hi, pltpu.roll(u, Y - 1, 0))
        return down, up

    def save_faces(p, x, w):
        for c in range(3):
            wy_send[p, 0, c, pl.ds(x, 1), :] = w[c][0:1, :]
            wy_send[p, 1, c, pl.ds(x, 1), :] = w[c][Y - 1:Y, :]

    def coefficients(x, _):
        k = k_p[x + 1]
        lo = stiff_of(iy_in[0, 0, pl.ds(x, 1), :]) * side_lo
        hi = stiff_of(iy_in[1, 0, pl.ds(x, 1), :]) * side_hi
        down, up = yshift(k, lo, hi)
        back = jnp.where(lane_id == 0, 0.0, pltpu.roll(k, 1, 1))
        ahead = jnp.where(lane_id == Z - 1, 0.0, pltpu.roll(k, Z - 1, 1))
        xm = 0.5 * (k + k_p[x])
        xp = 0.5 * (k + k_p[x + 2])
        ym = 0.5 * (k + down)
        yp = 0.5 * (k + up)
        zm = 0.5 * (k + back)
        zp = 0.5 * (k + ahead)
        diag = xm + xp + ym + yp + zm + zp + 0.5 * k
        inv = 1.0 / diag
        kx[x] = xm
        kx[x + 1] = xp
        kym[x] = ym
        kyp[x] = yp
        kzm[x] = jnp.where(lane_id == 0, 0.0, zm)
        kzp[x] = jnp.where(lane_id == Z - 1, 0.0, zp)
        dg[x] = diag - 0.25 * k
        invd[x] = inv
        w = [r_v[c, x] * inv for c in range(3)]
        for c in range(3):
            z_p[c, x + 1] = w[c]
        save_faces(0, x, w)
        return 0

    looped(0, X, coefficients, 0)
    for c in range(3):
        wx_send[0, 0, c] = z_p[c, 1]
        wx_send[0, 1, c] = z_p[c, X]
    halo_start(2)

    def edges(p, qs, pad, side):
        for d in range(2):
            s = spread(ix_in[d, 1], qs[d])
            for c in range(3):
                pad[c, 0 if d == 0 else X + 1] = wx_in[p, d, c] + s[c]
        for d in range(2):
            s = spread(iy_in[d, 1], qs[2 + d])
            for c in range(3):
                side[d, c] = wy_in[p, d, c] + s[c]

    def operate(pad, side, x):
        k = k_p[x + 1]
        u = [pad[c, x + 1] for c in range(3)]
        k4 = 0.25 * k * (u[0] + u[1] + u[2])
        out = []
        for c in range(3):
            down, up = yshift(u[c], side[0, c, pl.ds(x, 1), :], side[1, c, pl.ds(x, 1), :])
            a = dg[x] * u[c] + k4
            a = a - (kx[x] * pad[c, x] + kx[x + 1] * pad[c, x + 2])
            a = a - (kym[x] * down + kyp[x] * up)
            a = a - (kzm[x] * pltpu.roll(u[c], 1, 1) + kzp[x] * pltpu.roll(u[c], Z - 1, 1))
            out.append(a)
        return u, out

    gather_wait(0, ag_recv)
    halo_wait(1)
    tiles = coarse_vector(0)
    q = answers(tiles, c_v)
    qs = [answers(tiles, c_in.at[d]) for d in range(4)]

    def add_spread(x, _):
        s = spread(reg_v[x], q)
        for c in range(3):
            z = z_p[c, x + 1] + s[c]
            z_p[c, x + 1] = z
            z0_v[c, x] = z
        return 0

    looped(0, X, add_spread, 0)
    halo_wait(2)
    edges(0, qs, z_p, zy)

    def dots(a, b):
        return fold(a[0] * b[0] + a[1] * b[1] + a[2] * b[2])

    def first(x, carry):
        u, a = operate(z_p, zy, x)
        r = [r_v[c, x] for c in range(3)]
        w = []
        for c in range(3):
            y_v[c, x] = a[c]
            w.append(a[c] * invd[x])
            v_p[c, x + 1] = w[c]
        save_faces(1, x, w)
        acc = add_rc(carry[:ncr], reg_v[x], a)
        return acc + (carry[ncr] + dots(r, u), carry[ncr + 1] + dots(a, u))

    acc = looped(0, X, first, zero_acc(ncr + 2))
    make_row(1, acc, 0)
    gather_start(1)
    for c in range(3):
        wx_send[1, 0, c] = v_p[c, 1]
        wx_send[1, 1, c] = v_p[c, X]
    halo_start(3)
    halo_wait(3)
    gather_wait(1, ag_recv)
    tiles = coarse_vector(1)
    q = answers(tiles, c_v)
    qs = [answers(tiles, c_in.at[d]) for d in range(4)]
    rz0 = total(1, 0)
    alpha0 = rz0 / total(1, 1)

    def add_spread_v(x, _):
        s = spread(reg_v[x], q)
        for c in range(3):
            v_p[c, x + 1] = v_p[c, x + 1] + s[c]
        return 0

    looped(0, X, add_spread_v, 0)
    edges(1, qs, v_p, vy)

    def second(x, carry):
        u, a = operate(v_p, vy, x)
        r, z, az = [], [], []
        for c in range(3):
            y = y_v[c, x]
            r.append(r_v[c, x] - alpha0 * y)
            z.append(z_p[c, x + 1] - alpha0 * u[c])
            az.append(y - alpha0 * a[c])
            r_v[c, x] = r[c]
            z1_v[c, x] = z[c]
            az_v[c, x] = az[c]
        return (carry[0] + dots(r, z), carry[1] + dots(az, z))

    acc = looped(0, X, second, zero_acc(2))
    make_row(2, acc, ncr)
    gather_start(2)
    gather_wait(2, ag_recv)
    rz1 = total(2, 0)
    beta = rz1 / rz0
    alpha1 = rz1 / (total(2, 1) - beta * rz1 / alpha0)
    along = alpha0 + alpha1 * beta
    a1b = alpha1 * beta

    sc_v[0:1, :] = jnp.broadcast_to(along, (1, LANES))
    sc_v[1:2, :] = jnp.broadcast_to(alpha1, (1, LANES))
    sc_v[2:3, :] = jnp.broadcast_to(a1b, (1, LANES))
    for kind in range(4):
        halo_done(kind)
    for p in range(3):
        gather_wait(p, ag_send)


def finish_wide(z0_v, z1_v, r_v, az_v, y_v, sc_v, x_out, res_out, xb, rb, sem):
    along = sc_v[0:1, 0:1]
    alpha1 = sc_v[1:2, 0:1]
    a1b = sc_v[2:3, 0:1]
    X = z0_v.shape[1]
    copies = []
    for c in range(3):
        for x in range(X):
            xb[c, x] = along * z0_v[c, x] + alpha1 * z1_v[c, x]
            rb[c, x] = r_v[c, x] - alpha1 * az_v[c, x] - a1b * y_v[c, x]
        for n, (src, dst) in enumerate(((xb, x_out), (rb, res_out))):
            copies.append(pltpu.make_async_copy(src.at[c], dst.at[c], sem.at[n, c]))
            copies[-1].start()
    for copy in copies:
        copy.wait()


def local_wide(nw, nn, right_side, occupancy, region, coarse_inverse):
    _, X, Y, Z = right_side.shape
    ncr, NC = coarse_inverse.shape
    ND = nw * nn
    f32, i32 = jnp.float32, jnp.int32
    V = pltpu.VMEM
    field, pad, scal = (3, X, Y, Z), (3, X + 2, Y, Z), (X, Y, Z)
    scratch = [
        V(scal, i32), V(scal, i32), V((ncr, NC), f32),
        V((X + 2, Y, Z), f32), V((X + 1, Y, Z), f32),
        V(scal, f32), V(scal, f32), V(scal, f32), V(scal, f32), V(scal, f32), V(scal, f32),
        V(pad, f32), V(pad, f32),
        V((2, 3, X, Z), f32), V((2, 3, X, Z), f32),
        V((2, 2, Y, Z), i32), V((2, 2, X, Z), i32), V((2, 2, X, Z), i32),
        V((4, ncr, NC), f32),
        V((2, 2, 3, Y, Z), f32), V((2, 2, 3, Y, Z), f32),
        V((2, 2, 3, X, Z), f32), V((2, 2, 3, X, Z), f32),
        V((3, SUB, LANES), f32), V((3, ND, LANES), f32),
        pltpu.SemaphoreType.DMA((4,)),
        pltpu.SemaphoreType.DMA((5, 4)), pltpu.SemaphoreType.DMA((5, 4)),
        pltpu.SemaphoreType.DMA((3,)), pltpu.SemaphoreType.DMA((3,)),
    ]
    parts = pl.pallas_call(
        functools.partial(kernel_wide, nw, nn),
        out_shape=(V(field, f32),) * 5 + (V((SUB, LANES), f32),),
        in_specs=[pl.BlockSpec(memory_space=pltpu.HBM)] * 4,
        out_specs=(pl.BlockSpec(memory_space=pltpu.VMEM),) * 6,
        scratch_shapes=scratch,
        compiler_params=pltpu.CompilerParams(collective_id=0, has_side_effects=True, vmem_limit_bytes=32 * 1024 * 1024),
    )(*[pltpu.with_memory_space_constraint(a, pltpu.HBM) for a in (right_side, occupancy, region, coarse_inverse)])
    return pl.pallas_call(
        finish_wide,
        out_shape=(jax.ShapeDtypeStruct(field, f32),) * 2,
        in_specs=[pl.BlockSpec(memory_space=pltpu.VMEM)] * 6,
        out_specs=(pl.BlockSpec(memory_space=pltpu.HBM),) * 2,
        scratch_shapes=[V(field, f32), V(field, f32), pltpu.SemaphoreType.DMA((2, 3))],
        compiler_params=pltpu.CompilerParams(vmem_limit_bytes=16 * 1024 * 1024),
    )(*parts)


REPLICATED_BYTES = 4 * 1024 * 1024
DEEP = 3
AROUND = ((-1, 0), (1, 0), (0, -1), (0, 1), (-1, -1), (-1, 1), (1, -1), (1, 1))
BACK = tuple(AROUND.index((-a, -b)) for a, b in AROUND)


def group_of(n):
    return max(d for d in range(1, n + 1) if n % d == 0 and d * d <= n)


def spread_over(reg, q, G, inside=False):
    masks = [reg == g for g in range(G)]
    out = []
    for c in range(3):
        s = q[(G - 1) * 3 + c] if inside else jnp.where(masks[G - 1], q[(G - 1) * 3 + c], 0.0)
        for g in range(G - 1):
            s = jnp.where(masks[g], q[g * 3 + c], s)
        out.append(s)
    return out


def rows_from(low, count):
    return pl.ds(SUB + low, count)


def both_sides(ref, Y, *at):
    row = lax.broadcasted_iota(jnp.int32, (SUB, LANES), 0)
    return jnp.where(row < SUB // 2, ref[(*at, pl.ds(SUB + Y, SUB))], ref[(*at, pl.ds(0, SUB))])


def apply(ref, coefficients, x, low, count):
    kx, kyp, kzm, kzp, dg, k4 = coefficients
    here, down, up = rows_from(low, count), rows_from(low - 1, count), rows_from(low + 1, count)
    u = [ref[c, x, here] for c in range(3)]
    kk = k4[x, here] * (u[0] + u[1] + u[2])
    out = []
    for c in range(3):
        a = kx[x, here] * ref[c, x - 1, here] + kx[x + 1, here] * ref[c, x + 1, here]
        a = a + (kyp[x, down] * ref[c, x, down] + kyp[x, here] * ref[c, x, up])
        a = a + (kzm[x, here] * pltpu.roll(u[c], 1, 1) + kzp[x, here] * pltpu.roll(u[c], LANES - 1, 1))
        out.append(dg[x, here] * u[c] + kk - a)
    return u, out


def kernel(nw, nn, r_hbm, occ_hbm, reg_hbm, ci_hbm,
           z_e, g_e, y_e, r_o, ag_o, reg_o, k4, dg, kx, kyp, kzm, kzp, q_o, sc_o,
           occ_e, reg_e, r_e, k_e, invd,
           call, c_in, y_face, y_label, qpair, place_of, row_send, rows, sizes,
           load_sem, send, recv, ready):
    E, YE, Z = occ_e.shape
    X, Y = E - 2 * DEEP, YE - 2 * SUB
    ncr, NC = c_in.shape[1:]
    G = ncr // 3
    ND = nw * nn
    NH = ND // 2
    wi = lax.axis_index("wide")
    ni = lax.axis_index("narrow")
    me = wi * nn + ni
    f32 = jnp.float32
    GW = group_of(nw)
    GP = GW * nn
    NG = ND // GP
    grp, pos = me // GP, lax.rem(me, GP)
    half, place = lax.rem(wi, 2), (lax.rem(wi, GW) // 2) * nn + ni
    here = half * NH + place * NG + grp
    own, inner_rows = pl.ds(DEEP, X), pl.ds(SUB, Y)

    loads = [pltpu.make_async_copy(s, d, load_sem.at[i]) for s, d, i in (
        (reg_hbm, reg_e.at[own, inner_rows], 0), (r_hbm, r_e.at[:, own, inner_rows], 0),
        (occ_hbm, occ_e.at[own, inner_rows], 1), (ci_hbm, call.at[here], 2))]
    for l in loads:
        l.start()

    barrier = pltpu.get_barrier_semaphore()

    def at(t):
        return (t // nn, lax.rem(t, nn))

    def wait_for(sem, count):
        @pl.when(count > 0)
        def _():
            pl.semaphore_wait(sem, count)

    def column_of(group):
        return (wi + (group - grp) * GW, ni)

    at_low = jnp.logical_and(lax.rem(wi, GW) == 0, wi > 0)
    at_high = jnp.logical_and(lax.rem(wi, GW) == GW - 1, wi < nw - 1)
    aside = 1 + jnp.where(ni > 0, 1, 0) + jnp.where(ni < nn - 1, 1, 0)

    def touching(ahead, signal):
        @pl.when(at_high if ahead > 0 else at_low)
        def _():
            for b in (-1, 0, 1):
                @pl.when(jnp.logical_and(ni + b >= 0, ni + b < nn))
                def _():
                    signal((wi + ahead, ni + b))

    def say(sem):
        return lambda device: pl.semaphore_signal(sem, inc=1, device_id=device, device_id_type=MESH)

    for i in range(1, GP):
        say(barrier)(at(grp * GP + lax.rem(pos + i, GP)))
    touching(1, say(barrier))
    touching(-1, say(barrier))
    for k in range(1, NG):
        @pl.when(grp + k < NG)
        def _():
            say(barrier)(column_of(grp + k))

    def tell():
        for k in range(1, NG):
            @pl.when(grp >= k)
            def _():
                say(ready.at[k - 1])(column_of(grp - k))

    def take(rows_of, sem):
        some = sizes.at[pl.ds(0, rows_of)]
        pltpu.make_async_copy(some, some, sem).wait()

    def take_c(blocks, sem):
        some = call.at[pl.ds(0, blocks)]
        pltpu.make_async_copy(some, some, sem).wait()

    def by_neighbours(wait):
        nx = jnp.where(wi > 0, 1, 0) + jnp.where(wi < nw - 1, 1, 0)
        ny = jnp.where(ni > 0, 1, 0) + jnp.where(ni < nn - 1, 1, 0)
        for a in ((1,) if nw == 2 else (1, 2)):
            for b in (range(min(nn, 2)) if nn == 1 else (1,) if nn == 2 else (1, 2)):
                @pl.when(jnp.logical_and(nx == a, ny == b))
                def _():
                    wait(a, b)

    def halo_rows(n, a, b):
        deep, corner, count = ((DEEP, 2, 1), (2, 1, 1), (2, 1, 3))[n]
        return count * (a * deep * Y + b * deep * X + a * b * corner * corner)

    has = []
    for a, b in AROUND:
        h = jnp.logical_and(wi + a >= 0, wi + a < nw)
        has.append(jnp.logical_and(h, jnp.logical_and(ni + b >= 0, ni + b < nn)))

    def part(arr, d, into):
        a, b = AROUND[d]
        deep = {0: DEEP, 1: 2, 2: 2}[arr] if a == 0 or b == 0 else {0: 2, 1: 1, 2: 1}[arr]
        if into:
            xs = {-1: (DEEP - deep, deep), 0: (DEEP, X), 1: (DEEP + X, deep)}[a]
            ys = {-1: (SUB - deep, deep), 0: (SUB, Y), 1: (SUB + Y, deep)}[b]
        else:
            xs = {-1: (DEEP, deep), 0: (DEEP, X), 1: (DEEP + X - deep, deep)}[a]
            ys = {-1: (SUB, deep), 0: (SUB, Y), 1: (SUB + Y - deep, deep)}[b]
        xs, ys = pl.ds(*xs), pl.ds(*ys)
        return (slice(None), xs, ys) if arr == 2 else (xs, ys)

    fields = (occ_e, reg_e, r_e)
    for d in range(8):
        @pl.when(jnp.logical_not(has[d]))
        def _():
            for n, ref in enumerate(fields):
                where = part(n, d, True)
                v = ref[where]
                ref[where] = jnp.full(v.shape, (-1, -1, 0)[n], v.dtype)
            c_in[d] = jnp.zeros((ncr, NC), f32)

    wait_for(barrier, GP - 1 + grp + jnp.where(at_low, aside, 0) + jnp.where(at_high, aside, 0))
    tell()

    def fold(a):
        return jnp.sum(a.reshape(a.shape[0] // SUB, SUB, Z), axis=0)

    def zero_acc(n):
        return tuple(jnp.zeros((SUB, Z), f32) for _ in range(n))

    def add_rc(acc, reg, u):
        out = list(acc)
        for g in range(G):
            m = reg == g
            for c in range(3):
                out[g * 3 + c] = acc[g * 3 + c] + fold(jnp.where(m, u[c], 0.0))
        return out

    base = (me * ncr) % LANES

    def column(acc):
        a = jnp.concatenate([jnp.sum(b, axis=0, keepdims=True) for b in acc], axis=0)
        return jnp.sum(a, axis=1, keepdims=True)

    def make_row(p, acc):
        col = column(acc)
        n = len(acc)
        k = lax.broadcasted_iota(jnp.int32, (n, LANES), 0)
        lane = lax.broadcasted_iota(jnp.int32, (n, LANES), 1)
        target = (base + k) & (LANES - 1)
        row = jnp.sum(jnp.where(lane == target, col, 0.0), axis=0, keepdims=True)
        row_send[p, 0:1, :] = row
        rows[p, pl.ds(me, 1), :] = row

    def rows_to(p, count, t, out, sem):
        pltpu.make_async_remote_copy(
            src_ref=row_send.at[pl.ds(p, count), pl.ds(0, 1)], dst_ref=rows.at[pl.ds(p, count), pl.ds(me, 1)],
            send_sem=send.at[out], recv_sem=recv.at[sem],
            device_id=at(t), device_id_type=MESH).start()

    def each_peer(send):
        def body(i, _):
            send(i + jnp.where(i < me, 0, 1))
            return 0
        lax.fori_loop(0, ND - 1, body, 0, unroll=ND <= 64)

    take(4 * X * Y, load_sem.at[0])
    acc = looped(0, X, lambda x, a: tuple(add_rc(
        a, reg_e[x + DEEP, inner_rows], [r_e[c, x + DEEP, inner_rows] for c in range(3)])), zero_acc(ncr))
    make_row(0, acc)

    def inside(i, _):
        rows_to(0, 1, grp * GP + lax.rem(pos + i, GP), 0, 3)
        return 0

    lax.fori_loop(1, GP, inside, 0, unroll=GP <= 64)

    def halo(n, d):
        a, b = AROUND[d]
        e = BACK[d]
        return pltpu.make_async_remote_copy(
            src_ref=fields[n].at[part(n, d, False)], dst_ref=fields[n].at[part(n, e, True)],
            send_sem=send.at[0], recv_sem=recv.at[min(n, 1)],
            device_id=(wi + a, ni + b), device_id_type=MESH)

    def halo_c(d):
        a, b = AROUND[d]
        return pltpu.make_async_remote_copy(
            src_ref=call.at[here], dst_ref=c_in.at[BACK[d]],
            send_sem=send.at[1], recv_sem=recv.at[2],
            device_id=(wi + a, ni + b), device_id_type=MESH)

    loads[2].wait()
    loads[3].wait()

    for n in range(3):
        for d in range(8):
            @pl.when(has[d])
            def _():
                halo(n, d).start()

    def c_group(block, sem):
        for i in range(1, GP // 2):
            p = lax.rem(place + i, GP // 2)
            pltpu.make_async_remote_copy(
                src_ref=call.at[block], dst_ref=call.at[block],
                send_sem=send.at[2], recv_sem=recv.at[sem],
                device_id=(grp * GW + (p // nn) * 2 + half, lax.rem(p, nn)), device_id_type=MESH).start()

    c_group(here, 9)
    for d in range(8):
        if AROUND[d][0]:
            @pl.when(has[d])
            def _():
                halo_c(d).start()

    def c_column(group):
        pltpu.make_async_remote_copy(
            src_ref=call.at[here], dst_ref=call.at[here],
            send_sem=send.at[2], recv_sem=recv.at[5],
            device_id=column_of(group), device_id_type=MESH).start()

    for k in range(1, NG):
        @pl.when(grp >= k)
        def _():
            c_column(grp - k)

    def stiff_of(o):
        return jnp.where(o < 0, 0.0, soft_stiff + (bone_stiff - soft_stiff) * o.astype(f32))

    n2 = G * G

    def pairs(acc, first, seconds):
        out = list(acc)
        for g in range(G):
            t = None
            for label, value in seconds:
                v = jnp.where(label == g, value, 0.0)
                t = v if t is None else t + v
            for h in range(G):
                out[h * G + g] = acc[h * G + g] + fold(jnp.where(first == h, t, 0.0))
        return out

    row16 = lax.broadcasted_iota(jnp.int32, (Y, Z), 0)
    lane16 = lax.broadcasted_iota(jnp.int32, (Y, Z), 1)

    def own_pairs(i, carry):
        x = i + DEEP
        k, reg = stiff_of(occ_e[x, inner_rows]), reg_e[x, inner_rows]
        later = jnp.minimum(i + 1, X - 1) + DEEP
        kx_in = jnp.where(i < X - 1, 0.5 * (k + stiff_of(occ_e[later, inner_rows])), 0.0)
        ky_in = jnp.where(row16 == Y - 1, 0.0, 0.5 * (k + pltpu.roll(k, Y - 1, 0)))
        kz_in = jnp.where(lane16 == Z - 1, 0.0, 0.5 * (k + pltpu.roll(k, Z - 1, 1)))
        acc = pairs(carry[:n2], reg, ((reg_e[later, inner_rows], kx_in), (pltpu.roll(reg, Y - 1, 0), ky_in),
                                      (pltpu.roll(reg, Z - 1, 1), kz_in)))
        sums = [carry[n2 + g] + fold(jnp.where(reg == g, 0.25 * k, 0.0)) for g in range(G)]
        return tuple(acc) + tuple(sums)

    own_acc = lax.fori_loop(0, X, own_pairs, zero_acc(n2 + G), unroll=2)
    own_col = column(own_acc)

    def c_up(k):
        @pl.when(grp + k < NG)
        def _():
            pl.semaphore_wait(ready.at[k - 1], 1)
            c_column(grp + k)

    for k in range(1, NG):
        c_up(k)

    take(GP - 1, recv.at[3])
    mine = rows.at[0, pl.ds(pl.multiple_of(grp * GP, GP), GP)]

    def across(group):
        pltpu.make_async_remote_copy(
            src_ref=mine, dst_ref=mine, send_sem=send.at[0], recv_sem=recv.at[4],
            device_id=column_of(group), device_id_type=MESH).start()

    for k in range(1, NG):
        @pl.when(grp >= k)
        def _():
            across(grp - k)

    for k in range(1, NG):
        @pl.when(grp + k < NG)
        def _():
            across(grp + k)

    by_neighbours(lambda a, b: take(halo_rows(0, a, b), recv.at[0]))

    lane_id = lax.broadcasted_iota(jnp.int32, (Y + SUB, Z), 1)

    def stiffness(x, _):
        k_e[x] = stiff_of(occ_e[x])
        return 0

    lax.fori_loop(0, E, stiffness, 0, unroll=True)
    row8 = lax.broadcasted_iota(jnp.int32, (SUB, Z), 0)

    def coefficients(x):
        here = rows_from(-2, Y + SUB)
        k = k_e[x, here]
        low, high = k_e[x, rows_from(-3, Y + SUB)], k_e[x, rows_from(-1, Y + SUB)]
        back = jnp.where(lane_id == 0, 0.0, pltpu.roll(k, 1, 1))
        ahead = jnp.where(lane_id == Z - 1, 0.0, pltpu.roll(k, Z - 1, 1))
        xm = 0.5 * (k + k_e[x - 1, here])
        xp = 0.5 * (k + k_e[x + 1, here])
        ym = 0.5 * (k + low)
        yp = 0.5 * (k + high)
        zm = 0.5 * (k + back)
        zp = 0.5 * (k + ahead)
        diag = xm + xp + ym + yp + zm + zp + 0.5 * k
        kx[x, here] = xm
        kx[x + 1, here] = xp
        kyp[x, here] = yp
        kzm[x, here] = jnp.where(lane_id == 0, 0.0, zm)
        kzp[x, here] = jnp.where(lane_id == Z - 1, 0.0, zp)
        dg[x, here] = diag - 0.25 * k
        k4[x, here] = 0.25 * k
        invd[x, here] = jnp.where(k > 0.0, 1.0 / diag, 0.0)

    for x in (1, 2, DEEP + X, DEEP + X + 1):
        coefficients(x)

    def inner(i, sums):
        coefficients(i + DEEP)
        d, reg = dg[i + DEEP, inner_rows], reg_e[i + DEEP, inner_rows]
        return tuple(sums[g] + fold(jnp.where(reg == g, d, 0.0)) for g in range(G))

    sum_acc = lax.fori_loop(0, X, inner, zero_acc(G), unroll=4)

    by_neighbours(lambda a, b: take(halo_rows(1, a, b) + halo_rows(2, a, b), recv.at[1]))

    def side_rows(i, _):
        x = i + DEEP
        y_face[pl.ds(i, 1), :] = kyp[x, rows_from(Y - 1, 1), :]
        y_label[0, pl.ds(i, 1), :] = reg_e[x, rows_from(Y - 1, 1), :]
        y_label[1, pl.ds(i, 1), :] = reg_e[x, rows_from(Y, 1), :]
        return 0

    looped(0, X, side_rows, 0)
    top = DEEP + X - 1
    x_acc = pairs(zero_acc(n2), reg_e[top, inner_rows], ((reg_e[top + 1, inner_rows], kx[top + 1, inner_rows]),))
    y_acc = pairs(zero_acc(n2), y_label[0], ((y_label[1], y_face[...]),))
    rim_col = column(tuple(x_acc) + tuple(y_acc) + tuple(sum_acc))

    lane = lax.broadcasted_iota(jnp.int32, (n2, LANES), 1)
    pair = lax.broadcasted_iota(jnp.int32, (n2, LANES), 0)
    at_pair = jnp.logical_and(lane >= 3 * pair, lane < 3 * pair + 3)

    def lanes_of(col, mask):
        return jnp.sum(jnp.where(mask, col, 0.0), axis=0, keepdims=True)

    lane_g = lax.broadcasted_iota(jnp.int32, (G, LANES), 1)
    row_g = lax.broadcasted_iota(jnp.int32, (G, LANES), 0)
    diag_at, sum_at = 3 * (G + 1) * row_g, 3 * n2 + 9 * row_g
    at_diag = jnp.logical_and(lane_g >= diag_at, lane_g < diag_at + 3)
    at_sum = jnp.logical_and(lane_g >= sum_at, lane_g < sum_at + 9)
    ac_rows = (lanes_of(own_col[0:n2], at_pair) * -2.0 + lanes_of(rim_col[2 * n2:], at_diag)
               + lanes_of(own_col[n2:], at_sum),
               lanes_of(rim_col[0:n2], at_pair) * -2.0, lanes_of(rim_col[n2:2 * n2], at_pair) * -2.0)
    for n in range(3):
        row_send[n + 2, 0:1, :] = ac_rows[n]
        rows[n + 2, pl.ds(me, 1), :] = ac_rows[n]

    def coarse_vector(block):
        tiles = []
        for t in range(NC // LANES):
            lo = (LANES * t) // ncr // SUB * SUB
            hi = min(ND, -(-(-(-(LANES * (t + 1)) // ncr)) // SUB) * SUB)
            d = lax.broadcasted_iota(jnp.int32, (hi - lo, LANES), 0) + lo
            j = lax.broadcasted_iota(jnp.int32, (hi - lo, LANES), 1) + LANES * t
            m = (j >= d * ncr) & (j < d * ncr + ncr)
            tiles.append(jnp.sum(jnp.where(m, block[lo:hi, :], 0.0), axis=0, keepdims=True))
        return tiles

    def total(block, s):
        d = lax.broadcasted_iota(jnp.int32, (ND, LANES), 0)
        lane = lax.broadcasted_iota(jnp.int32, (ND, LANES), 1)
        m = lane == ((d * ncr + ncr + s) & (LANES - 1))
        v = jnp.sum(jnp.where(m, block, 0.0), axis=0, keepdims=True)
        return jnp.sum(v, axis=1, keepdims=True)

    def solve(tiles, block):
        s = block[:, 0:LANES] * tiles[0]
        for t in range(1, len(tiles)):
            s = s + block[:, t * LANES:(t + 1) * LANES] * tiles[t]
        return jnp.sum(s, axis=1, keepdims=True)

    def rows_of(d):
        a, b = AROUND[d]
        return c_in[d] if a else call[here + jnp.where(has[d], b * NG, 0)]

    def as_list(q):
        return [q[i:i + 1, :] for i in range(ncr)]

    take_c(NG - 1, recv.at[5])
    for k in range(1, NG):
        c_group(half * NH + place * NG + lax.rem(grp + k, NG), 6)

    take(ND - GP, recv.at[4])
    by_neighbours(lambda a, b: take_c(a + a * b, recv.at[2]))
    take_c(GP // 2 - 1, recv.at[9])
    tiles = coarse_vector(rows[0])
    q = as_list(solve(tiles, call[here]))
    qn = [as_list(solve(tiles, rows_of(d))) for d in range(8)]

    def either(hi, lo):
        return [jnp.where(row8 < SUB // 2, a, b) for a, b in zip(hi, lo)]

    def add_spread(x, q_in, q_out, inside):
        reg, inv = reg_e[x, inner_rows], invd[x, inner_rows]
        s = spread_over(reg, q_in, G, inside)
        reg_o[x, inner_rows] = reg
        for c in range(3):
            z_e[c, x, inner_rows] = r_e[c, x, inner_rows] * inv + s[c]
        reg, inv = both_sides(reg_e, Y, x), both_sides(invd, Y, x)
        s = spread_over(reg, q_out, G)
        some = SUB // 2
        reg_o[x, rows_from(Y, some)] = reg[0:some]
        reg_o[x, rows_from(-some, some)] = reg[some:SUB]
        for c in range(3):
            z = both_sides(r_e, Y, c, x) * inv + s[c]
            z_e[c, x, rows_from(Y, some)] = z[0:some]
            z_e[c, x, rows_from(-some, some)] = z[some:SUB]

    q_side = either(qn[3], qn[2])

    def spread_own(i, _):
        add_spread(i + DEEP, q, q_side, True)
        return 0

    looped(0, X, spread_own, 0)
    q_low, q_high = either(qn[5], qn[4]), either(qn[7], qn[6])
    for x in (1, 2):
        add_spread(x, qn[0], q_low, False)
    for x in (DEEP + X, DEEP + X + 1):
        add_spread(x, qn[1], q_high, False)

    faces = (kx, kyp, kzm, kzp, dg, k4)

    def dots(a, b):
        return fold(a[0] * b[0] + a[1] * b[1] + a[2] * b[2])

    def first(i, _):
        x, some = i + DEEP - 1, rows_from(-1, Y + SUB)
        _, a = apply(z_e, faces, x, -1, Y + SUB)
        for c in range(3):
            y_e[c, x, some] = a[c]
            g_e[c, x, some] = a[c] * invd[x, some]
        return 0

    lax.fori_loop(0, X + 2, first, 0, unroll=(X + 2) // 2)

    def own_of(ref, x):
        return [ref[c, x, inner_rows] for c in range(3)]

    def second(i, carry):
        x = i + DEEP
        w, a = apply(g_e, faces, x, 0, Y)
        for c in range(3):
            ag_o[c, i] = a[c]
        acc = add_rc(carry[:ncr], reg_e[x, inner_rows], a)
        return tuple(acc) + (carry[ncr] + dots(w, a),)

    acc2 = lax.fori_loop(0, X, second, zero_acc(ncr + 1), unroll=8)

    def third(i, carry):
        x = i + DEEP
        r, z, y, w = own_of(r_e, x), own_of(z_e, x), own_of(y_e, x), own_of(g_e, x)
        for c in range(3):
            r_o[c, i] = r[c]
        acc = add_rc(carry[:ncr], reg_e[x, inner_rows], y)
        return tuple(acc) + (carry[ncr] + dots(r, z), carry[ncr + 1] + dots(y, z), carry[ncr + 2] + dots(y, w))

    acc1 = lax.fori_loop(0, X, third, zero_acc(ncr + 3), unroll=8)
    make_row(1, tuple(acc1) + (acc2[ncr],) + tuple(acc2[:ncr]))
    each_peer(lambda t: rows_to(1, 4, t, 3, 7))

    rr = lax.broadcasted_iota(jnp.int32, (ncr, LANES), 0)
    ll = lax.broadcasted_iota(jnp.int32, (ncr, LANES), 1)
    m0, m1 = rr < 0, rr < 0
    for h in range(G):
        for g in range(G):
            for c in range(3):
                k = (h * G + g) * 3 + c
                m0 = jnp.logical_or(m0, (ll == k) & (rr == h * 3 + c))
                m1 = jnp.logical_or(m1, (ll == k) & (rr == g * 3 + c))
        for c in range(3):
            for e in range(3):
                k = 3 * n2 + h * 9 + c * 3 + e
                m0 = jnp.logical_or(m0, (ll == k) & (rr == h * 3 + c))
                m1 = jnp.logical_or(m1, (ll == k) & (rr == h * 3 + e))
    place_of[0] = jnp.where(m0, 1.0, 0.0)
    place_of[1] = jnp.where(m1, 1.0, 0.0)

    take_c((GP // 2 - 1) * (NG - 1), recv.at[6])
    swap_half = call.at[pl.ds(half * NH, NH)]
    swap = pltpu.make_async_remote_copy(
        src_ref=swap_half, dst_ref=swap_half, send_sem=send.at[2], recv_sem=recv.at[8],
        device_id=(wi + 1 - 2 * half, ni), device_id_type=MESH)
    swap.start()
    by_neighbours(lambda a, b: take(
        sum(halo_rows(n, a, b) for n in range(3)) + GP - 1 + (NG - 1) * GP, send.at[0]))
    by_neighbours(lambda a, b: take_c(a + a * b, send.at[1]))
    swap.wait_recv()
    take(4 * (ND - 1), recv.at[7])

    block = rows[1]
    b1 = coarse_vector(block)
    h1 = coarse_vector(pltpu.roll(block, LANES - ncr - 4, 1))
    lines = [jnp.zeros((ncr, LANES), f32) for _ in b1]
    for w in range(nw):
        for n in range(nn):
            d = w * nn + n
            q1 = solve(b1, call[w % 2 * NH + ((w % GW) // 2 * nn + n) * NG + w // GW])
            qpair[0, d:d + 1, :] = jnp.sum(place_of[0] * q1, axis=0, keepdims=True)
            qpair[1, d:d + 1, :] = jnp.sum(place_of[1] * q1, axis=0, keepdims=True)
            for t in range(d * ncr // LANES, (d * ncr + ncr - 1) // LANES + 1):
                lines[t] = jnp.where(ll + LANES * t == rr + d * ncr, q1, lines[t])
    lines = [jnp.sum(v, axis=0, keepdims=True) for v in lines]
    first_q, second_q = qpair[0], qpair[1]
    dev = lax.broadcasted_iota(jnp.int32, (ND, LANES), 0)
    next_x = jnp.where(dev < ND - nn, pltpu.roll(second_q, ND - nn, 0), 0.0)
    next_y = jnp.where(dev < ND - 1, pltpu.roll(second_q, ND - 1, 0), 0.0)
    energy = jnp.sum(first_q * (rows[2] * second_q + rows[3] * next_x + rows[4] * next_y), axis=0, keepdims=True)
    for t in range(len(b1)):
        energy = energy + 2.0 * h1[t] * lines[t]
    yv = b1[0] * lines[0]
    for t in range(1, len(b1)):
        yv = yv + b1[t] * lines[t]
    yv = total(block, 2) + jnp.sum(yv, axis=1, keepdims=True)
    vav = total(block, 3) + jnp.sum(energy, axis=1, keepdims=True)
    rz0, zy = total(block, 0), total(block, 1)
    alpha0 = rz0 / zy
    rz1 = alpha0 * alpha0 * yv - rz0
    zaz = zy - 2.0 * alpha0 * yv + alpha0 * alpha0 * vav
    beta = rz1 / rz0
    alpha1 = rz1 / (zaz - beta * rz1 / alpha0)
    a1b = alpha1 * beta
    for n, v in enumerate((alpha0 + a1b + alpha1, alpha1 * alpha0)):
        sc_o[n:n + 1, :] = jnp.broadcast_to(v, (1, LANES))
    q_o[0] = jnp.broadcast_to(solve(b1, call[here]), (ncr, LANES))
    for d in range(4):
        q_o[d + 1] = jnp.broadcast_to(solve(b1, rows_of(d)), (ncr, LANES))

    take(4 * (ND - 1), send.at[3])
    take_c(NG - 1 + (GP // 2 - 1) * NG + NH, send.at[2])


def finish(z_v, g_v, y_v, r_v, ag_v, reg_v, k4, dg, kx, kyp, kzm, kzp, q_v, sc_v, x_out, res_out, s_e, xb, rb, sem):
    a, b = sc_v[0:1, 0:1], sc_v[1:2, 0:1]
    E, YE, Z = reg_v.shape
    X, Y = E - 2 * DEEP, YE - 2 * SUB
    G = q_v.shape[1] // 3
    own = pl.ds(SUB, Y)
    row8 = lax.broadcasted_iota(jnp.int32, (SUB, Z), 0)
    q = [[q_v[d, i:i + 1, :] for i in range(3 * G)] for d in range(5)]
    side = [jnp.where(row8 < SUB // 2, hi, lo) for hi, lo in zip(q[4], q[3])]

    def fill(x, q_in, inside):
        s = spread_over(reg_v[x, own], q_in, G, inside)
        for c in range(3):
            s_e[c, x, own] = s[c]
        return s

    def fill_sides(x):
        s = spread_over(both_sides(reg_v, Y, x), side, G)
        some = SUB // 2
        for c in range(3):
            s_e[c, x, rows_from(Y, some)] = s[c][0:some]
            s_e[c, x, rows_from(-some, some)] = s[c][some:SUB]

    def fill_own(i, _):
        x = i + DEEP
        s = fill(x, q[0], True)
        fill_sides(x)
        for c in range(3):
            xb[c, i] = a * z_v[c, x, own] - b * (g_v[c, x, own] + s[c])
        return 0

    fill(DEEP - 1, q[1], False)
    fill(DEEP + X, q[2], False)
    faces = (kx, kyp, kzm, kzp, dg, k4)
    parts = 4
    step = X // parts

    def leave(m, src, dst, n):
        where = (slice(None), pl.ds(n * step, step))
        pltpu.make_async_copy(src.at[where], dst.at[where], sem.at[m]).start()

    def plane(i, _):
        u, w = apply(s_e, faces, i + DEEP, 0, Y)
        for c in range(3):
            rb[c, i] = r_v[c, i] - a * y_v[c, i + DEEP, own] + b * (ag_v[c, i] + w[c])
        return 0

    for n in range(parts):
        lax.fori_loop(n * step, (n + 1) * step, fill_own, 0, unroll=True)
        leave(0, xb, x_out, n)
    for n in range(parts):
        lax.fori_loop(n * step, (n + 1) * step, plane, 0, unroll=True)
        leave(1, rb, res_out, n)
    pltpu.make_async_copy(xb, x_out, sem.at[0]).wait()
    pltpu.make_async_copy(rb, res_out, sem.at[1]).wait()


def local_fast(nw, nn, right_side, occupancy, region, coarse_inverse):
    _, X, Y, Z = right_side.shape
    ncr, NC = coarse_inverse.shape
    ND = nw * nn
    f32, i32 = jnp.float32, jnp.int32
    V = pltpu.VMEM
    E, YE = X + 2 * DEEP, Y + 2 * SUB
    field, ext, scal = (3, X, Y, Z), (3, E, YE, Z), (E, YE, Z)
    ng = nw // group_of(nw)
    DMA = pltpu.SemaphoreType.DMA
    scratch = [
        V(scal, i32), V(scal, i32), V(ext, f32), V(scal, f32), V(scal, f32),
        V((ND, ncr, NC), f32), V((8, ncr, NC), f32), V((X, Z), f32), V((2, X, Z), i32), V((2, ND, LANES), f32), V((2, ncr, LANES), f32),
        V((5, SUB, LANES), f32), V((5, ND, LANES), f32), V((4 * X * Y, LANES), f32),
        DMA((3,)), DMA((4,)), DMA((10,)),
        pltpu.SemaphoreType.REGULAR((ng - 1,)),
    ]
    outs = (V(ext, f32),) * 3 + (V(field, f32),) * 2 + (V(scal, i32),) + (V(scal, f32),) * 6 + (V((5, ncr, LANES), f32), V((SUB, LANES), f32))
    parts = pl.pallas_call(
        functools.partial(kernel, nw, nn),
        out_shape=outs,
        in_specs=[pl.BlockSpec(memory_space=pltpu.HBM)] * 4,
        out_specs=(pl.BlockSpec(memory_space=pltpu.VMEM),) * len(outs),
        scratch_shapes=scratch,
        compiler_params=pltpu.CompilerParams(collective_id=0, has_side_effects=True, vmem_limit_bytes=32 * 1024 * 1024),
    )(*[pltpu.with_memory_space_constraint(a, pltpu.HBM) for a in (right_side, occupancy, region, coarse_inverse)])
    return pl.pallas_call(
        finish,
        out_shape=(jax.ShapeDtypeStruct(field, f32),) * 2,
        in_specs=[pl.BlockSpec(memory_space=pltpu.VMEM)] * len(outs),
        out_specs=(pl.BlockSpec(memory_space=pltpu.HBM),) * 2,
        scratch_shapes=[V(ext, f32), V(field, f32), V(field, f32), DMA((2,))],
        compiler_params=pltpu.CompilerParams(vmem_limit_bytes=24 * 1024 * 1024),
    )(*parts)


def local(nw, nn, right_side, occupancy, region, coarse_inverse):
    nc = coarse_inverse.shape[1]
    run = local_fast if group_of(nw) % 2 == 0 and nc * nc * 4 <= REPLICATED_BYTES else local_wide
    return run(nw, nn, right_side, occupancy, region, coarse_inverse)


def solution(mesh):
    return jax.shard_map(
        functools.partial(local, mesh.shape["wide"], mesh.shape["narrow"]),
        mesh=mesh,
        in_specs=(
            P(None, "wide", "narrow", None),
            P("wide", "narrow", None),
            P("wide", "narrow", None),
            P(("wide", "narrow"), None),
        ),
        out_specs=(P(None, "wide", "narrow", None), P(None, "wide", "narrow", None)),
        check_vma=False,
    )
```

```python
import functools

import jax
import jax.numpy as jnp
from jax import lax
from jax.experimental import pallas as pl
from jax.experimental.pallas import tpu as pltpu
from jax.sharding import PartitionSpec as P

LANES = 128
SUB = 8
UNROLL = 16
looped = functools.partial(lax.fori_loop, unroll=UNROLL)
MESH = pl.DeviceIdType.MESH
bone_stiff = 1.0
soft_stiff = 0.1


def kernel_wide(nw, nn, r_hbm, occ_hbm, reg_hbm, ci_hbm,
           z0_v, z1_v, r_v, az_v, y_v, sc_v,
            occ_v, reg_v, c_v, k_p, kx, kym, kyp, kzm, kzp, dg, invd,
           z_p, v_p, zy, vy,
           ix_in, iy_send, iy_in, c_in, wx_send, wx_in, wy_send, wy_in,
           row_send, rows, load_sem, hs_send, hs_recv, ag_send, ag_recv):
    X, Y, Z = occ_v.shape
    ncr, NC = c_v.shape
    G = ncr // 3
    ND = nw * nn
    wi = lax.axis_index("wide")
    ni = lax.axis_index("narrow")
    me = wi * nn + ni
    f32 = jnp.float32

    loads = [pltpu.make_async_copy(s, d, load_sem.at[i]) for i, (s, d) in enumerate(
        ((occ_hbm, occ_v), (reg_hbm, reg_v), (r_hbm, r_v), (ci_hbm, c_v)))]
    for l in loads:
        l.start()

    def peer(i):
        t = lax.rem(me + i, ND)
        return (t // nn, lax.rem(t, nn))

    barrier = pltpu.get_barrier_semaphore()

    def greet(i, _):
        pl.semaphore_signal(barrier, inc=1, device_id=peer(i), device_id_type=MESH)
        return 0

    lax.fori_loop(1, ND, greet, 0, unroll=ND <= 64)

    has = (wi > 0, wi < nw - 1, ni > 0, ni < nn - 1)
    to = ((wi - 1, ni), (wi + 1, ni), (wi, ni - 1), (wi, ni + 1))

    for d in range(4):
        @pl.when(jnp.logical_not(has[d]))
        def _():
            c_in[d] = jnp.zeros((ncr, NC), f32)
            for p in range(2):
                if d < 2:
                    wx_in[p, d] = jnp.zeros((3, Y, Z), f32)
                else:
                    wy_in[p, d - 2] = jnp.zeros((3, X, Z), f32)
            if d < 2:
                ix_in[d] = jnp.zeros((2, Y, Z), jnp.int32)
            else:
                iy_in[d - 2] = jnp.zeros((2, X, Z), jnp.int32)

    loads[0].wait()
    loads[1].wait()

    def pack_ints(x, _):
        iy_send[0, 0, pl.ds(x, 1), :] = occ_v[x, 0:1, :]
        iy_send[1, 0, pl.ds(x, 1), :] = occ_v[x, Y - 1:Y, :]
        iy_send[0, 1, pl.ds(x, 1), :] = reg_v[x, 0:1, :]
        iy_send[1, 1, pl.ds(x, 1), :] = reg_v[x, Y - 1:Y, :]
        return 0

    looped(0, X, pack_ints, 0)

    def fold(a):
        return jnp.sum(a.reshape(Y // SUB, SUB, Z), axis=0)

    def zero_acc(n):
        return tuple(jnp.zeros((SUB, Z), f32) for _ in range(n))

    def add_rc(acc, reg, u):
        out = list(acc)
        for g in range(G):
            m = reg == g
            for c in range(3):
                out[g * 3 + c] = acc[g * 3 + c] + fold(jnp.where(m, u[c], 0.0))
        return tuple(out)

    base = (me * ncr) % LANES

    def make_row(p, acc, first):
        a = jnp.concatenate([jnp.sum(b, axis=0, keepdims=True) for b in acc], axis=0)
        col = jnp.sum(a, axis=1, keepdims=True)
        n = len(acc)
        k = lax.broadcasted_iota(jnp.int32, (n, LANES), 0)
        lane = lax.broadcasted_iota(jnp.int32, (n, LANES), 1)
        target = (base + first + k) & (LANES - 1)
        row = jnp.sum(jnp.where(lane == target, col, 0.0), axis=0, keepdims=True)
        row_send[p, 0:1, :] = row
        rows[p, pl.ds(me, 1), :] = row

    def gather_start(p):
        def send(i, _):
            pltpu.make_async_remote_copy(
                src_ref=row_send.at[p, pl.ds(0, 1)], dst_ref=rows.at[p, pl.ds(me, 1)],
                send_sem=ag_send.at[p], recv_sem=ag_recv.at[p],
                device_id=peer(i), device_id_type=MESH).start()
            return 0
        lax.fori_loop(1, ND, send, 0, unroll=ND <= 64)

    def gather_wait(p, sem):
        part = rows.at[p, pl.ds(0, ND - 1)]
        pltpu.make_async_copy(part, part, sem.at[p]).wait()

    def coarse_vector(p):
        tiles = []
        for t in range(NC // LANES):
            lo = (LANES * t) // ncr // SUB * SUB
            hi = min(ND, -(-(-(-(LANES * (t + 1)) // ncr)) // SUB) * SUB)
            d = lax.broadcasted_iota(jnp.int32, (hi - lo, LANES), 0) + lo
            j = lax.broadcasted_iota(jnp.int32, (hi - lo, LANES), 1) + LANES * t
            m = (j >= d * ncr) & (j < d * ncr + ncr)
            tiles.append(jnp.sum(jnp.where(m, rows[p, lo:hi, :], 0.0), axis=0, keepdims=True))
        return tiles

    def total(p, s):
        d = lax.broadcasted_iota(jnp.int32, (ND, LANES), 0)
        lane = lax.broadcasted_iota(jnp.int32, (ND, LANES), 1)
        m = lane == ((d * ncr + ncr + s) & (LANES - 1))
        v = jnp.sum(jnp.where(m, rows[p], 0.0), axis=0, keepdims=True)
        return jnp.sum(v, axis=1, keepdims=True)

    def answers(tiles, ref):
        s = ref[:, 0:LANES] * tiles[0]
        for t in range(1, len(tiles)):
            s = s + ref[:, t * LANES:(t + 1) * LANES] * tiles[t]
        q = jnp.sum(s, axis=1, keepdims=True)
        return [q[i:i + 1, :] for i in range(ncr)]

    def spread(reg, q):
        masks = [reg == g for g in range(G)]
        out = []
        for c in range(3):
            s = jnp.zeros(reg.shape, f32)
            for g in range(G):
                s = jnp.where(masks[g], q[g * 3 + c], s)
            out.append(s)
        return out

    def halo(slot, d, src, dst):
        return pltpu.make_async_remote_copy(
            src_ref=src, dst_ref=dst, send_sem=hs_send.at[slot, d],
            recv_sem=hs_recv.at[slot, d ^ 1], device_id=to[d], device_id_type=MESH)

    def copies(kind, d):
        e = d ^ 1
        if kind == 0:
            if d < 2:
                x = 0 if d == 0 else X - 1
                return [halo(0, d, occ_v.at[x], ix_in.at[e, 0]),
                        halo(1, d, reg_v.at[x], ix_in.at[e, 1])]
            return [halo(0, d, iy_send.at[d - 2, 0], iy_in.at[e - 2, 0]),
                    halo(1, d, iy_send.at[d - 2, 1], iy_in.at[e - 2, 1])]
        if kind == 1:
            return [halo(2, d, c_v, c_in.at[e])]
        p = kind - 2
        if d < 2:
            return [halo(3 + p, d, wx_send.at[p, d], wx_in.at[p, e])]
        return [halo(3 + p, d, wy_send.at[p, d - 2], wy_in.at[p, e - 2])]

    def halo_start(kind):
        for d in range(4):
            @pl.when(has[d])
            def _():
                for c in copies(kind, d):
                    c.start()

    def halo_wait(kind):
        for d in range(4):
            @pl.when(has[d])
            def _():
                for c in copies(kind, d ^ 1):
                    c.wait_recv()

    def halo_done(kind):
        for d in range(4):
            @pl.when(has[d])
            def _():
                for c in copies(kind, d):
                    c.wait_send()

    loads[2].wait()
    acc = looped(0, X, lambda x, a: add_rc(a, reg_v[x], [r_v[c, x] for c in range(3)]),
                        zero_acc(ncr))
    make_row(0, acc, 0)
    loads[3].wait()

    pl.semaphore_wait(barrier, ND - 1)
    halo_start(0)
    gather_start(0)
    halo_start(1)

    def stiff_of(o):
        return soft_stiff + (bone_stiff - soft_stiff) * o.astype(f32)

    def own_k(x, _):
        k_p[x + 1] = stiff_of(occ_v[x])
        return 0

    looped(0, X, own_k, 0)
    halo_wait(0)
    for d in range(2):
        @pl.when(has[d])
        def _():
            k_p[0 if d == 0 else X + 1] = stiff_of(ix_in[d, 0])

        @pl.when(jnp.logical_not(has[d]))
        def _():
            k_p[0 if d == 0 else X + 1] = jnp.zeros((Y, Z), f32)

    row_id = lax.broadcasted_iota(jnp.int32, (Y, Z), 0)
    lane_id = lax.broadcasted_iota(jnp.int32, (Y, Z), 1)
    side_lo = jnp.where(has[2], 1.0, 0.0).astype(f32)
    side_hi = jnp.where(has[3], 1.0, 0.0).astype(f32)

    def yshift(u, lo, hi):
        down = jnp.where(row_id == 0, lo, pltpu.roll(u, 1, 0))
        up = jnp.where(row_id == Y - 1, hi, pltpu.roll(u, Y - 1, 0))
        return down, up

    def save_faces(p, x, w):
        for c in range(3):
            wy_send[p, 0, c, pl.ds(x, 1), :] = w[c][0:1, :]
            wy_send[p, 1, c, pl.ds(x, 1), :] = w[c][Y - 1:Y, :]

    def coefficients(x, _):
        k = k_p[x + 1]
        lo = stiff_of(iy_in[0, 0, pl.ds(x, 1), :]) * side_lo
        hi = stiff_of(iy_in[1, 0, pl.ds(x, 1), :]) * side_hi
        down, up = yshift(k, lo, hi)
        back = jnp.where(lane_id == 0, 0.0, pltpu.roll(k, 1, 1))
        ahead = jnp.where(lane_id == Z - 1, 0.0, pltpu.roll(k, Z - 1, 1))
        xm = 0.5 * (k + k_p[x])
        xp = 0.5 * (k + k_p[x + 2])
        ym = 0.5 * (k + down)
        yp = 0.5 * (k + up)
        zm = 0.5 * (k + back)
        zp = 0.5 * (k + ahead)
        diag = xm + xp + ym + yp + zm + zp + 0.5 * k
        inv = 1.0 / diag
        kx[x] = xm
        kx[x + 1] = xp
        kym[x] = ym
        kyp[x] = yp
        kzm[x] = jnp.where(lane_id == 0, 0.0, zm)
        kzp[x] = jnp.where(lane_id == Z - 1, 0.0, zp)
        dg[x] = diag - 0.25 * k
        invd[x] = inv
        w = [r_v[c, x] * inv for c in range(3)]
        for c in range(3):
            z_p[c, x + 1] = w[c]
        save_faces(0, x, w)
        return 0

    looped(0, X, coefficients, 0)
    for c in range(3):
        wx_send[0, 0, c] = z_p[c, 1]
        wx_send[0, 1, c] = z_p[c, X]
    halo_start(2)

    def edges(p, qs, pad, side):
        for d in range(2):
            s = spread(ix_in[d, 1], qs[d])
            for c in range(3):
                pad[c, 0 if d == 0 else X + 1] = wx_in[p, d, c] + s[c]
        for d in range(2):
            s = spread(iy_in[d, 1], qs[2 + d])
            for c in range(3):
                side[d, c] = wy_in[p, d, c] + s[c]

    def operate(pad, side, x):
        k = k_p[x + 1]
        u = [pad[c, x + 1] for c in range(3)]
        k4 = 0.25 * k * (u[0] + u[1] + u[2])
        out = []
        for c in range(3):
            down, up = yshift(u[c], side[0, c, pl.ds(x, 1), :], side[1, c, pl.ds(x, 1), :])
            a = dg[x] * u[c] + k4
            a = a - (kx[x] * pad[c, x] + kx[x + 1] * pad[c, x + 2])
            a = a - (kym[x] * down + kyp[x] * up)
            a = a - (kzm[x] * pltpu.roll(u[c], 1, 1) + kzp[x] * pltpu.roll(u[c], Z - 1, 1))
            out.append(a)
        return u, out

    gather_wait(0, ag_recv)
    halo_wait(1)
    tiles = coarse_vector(0)
    q = answers(tiles, c_v)
    qs = [answers(tiles, c_in.at[d]) for d in range(4)]

    def add_spread(x, _):
        s = spread(reg_v[x], q)
        for c in range(3):
            z = z_p[c, x + 1] + s[c]
            z_p[c, x + 1] = z
            z0_v[c, x] = z
        return 0

    looped(0, X, add_spread, 0)
    halo_wait(2)
    edges(0, qs, z_p, zy)

    def dots(a, b):
        return fold(a[0] * b[0] + a[1] * b[1] + a[2] * b[2])

    def first(x, carry):
        u, a = operate(z_p, zy, x)
        r = [r_v[c, x] for c in range(3)]
        w = []
        for c in range(3):
            y_v[c, x] = a[c]
            w.append(a[c] * invd[x])
            v_p[c, x + 1] = w[c]
        save_faces(1, x, w)
        acc = add_rc(carry[:ncr], reg_v[x], a)
        return acc + (carry[ncr] + dots(r, u), carry[ncr + 1] + dots(a, u))

    acc = looped(0, X, first, zero_acc(ncr + 2))
    make_row(1, acc, 0)
    gather_start(1)
    for c in range(3):
        wx_send[1, 0, c] = v_p[c, 1]
        wx_send[1, 1, c] = v_p[c, X]
    halo_start(3)
    halo_wait(3)
    gather_wait(1, ag_recv)
    tiles = coarse_vector(1)
    q = answers(tiles, c_v)
    qs = [answers(tiles, c_in.at[d]) for d in range(4)]
    rz0 = total(1, 0)
    alpha0 = rz0 / total(1, 1)

    def add_spread_v(x, _):
        s = spread(reg_v[x], q)
        for c in range(3):
            v_p[c, x + 1] = v_p[c, x + 1] + s[c]
        return 0

    looped(0, X, add_spread_v, 0)
    edges(1, qs, v_p, vy)

    def second(x, carry):
        u, a = operate(v_p, vy, x)
        r, z, az = [], [], []
        for c in range(3):
            y = y_v[c, x]
            r.append(r_v[c, x] - alpha0 * y)
            z.append(z_p[c, x + 1] - alpha0 * u[c])
            az.append(y - alpha0 * a[c])
            r_v[c, x] = r[c]
            z1_v[c, x] = z[c]
            az_v[c, x] = az[c]
        return (carry[0] + dots(r, z), carry[1] + dots(az, z))

    acc = looped(0, X, second, zero_acc(2))
    make_row(2, acc, ncr)
    gather_start(2)
    gather_wait(2, ag_recv)
    rz1 = total(2, 0)
    beta = rz1 / rz0
    alpha1 = rz1 / (total(2, 1) - beta * rz1 / alpha0)
    along = alpha0 + alpha1 * beta
    a1b = alpha1 * beta

    sc_v[0:1, :] = jnp.broadcast_to(along, (1, LANES))
    sc_v[1:2, :] = jnp.broadcast_to(alpha1, (1, LANES))
    sc_v[2:3, :] = jnp.broadcast_to(a1b, (1, LANES))
    for kind in range(4):
        halo_done(kind)
    for p in range(3):
        gather_wait(p, ag_send)


def finish_wide(z0_v, z1_v, r_v, az_v, y_v, sc_v, x_out, res_out, xb, rb, sem):
    along = sc_v[0:1, 0:1]
    alpha1 = sc_v[1:2, 0:1]
    a1b = sc_v[2:3, 0:1]
    X = z0_v.shape[1]
    copies = []
    for c in range(3):
        for x in range(X):
            xb[c, x] = along * z0_v[c, x] + alpha1 * z1_v[c, x]
            rb[c, x] = r_v[c, x] - alpha1 * az_v[c, x] - a1b * y_v[c, x]
        for n, (src, dst) in enumerate(((xb, x_out), (rb, res_out))):
            copies.append(pltpu.make_async_copy(src.at[c], dst.at[c], sem.at[n, c]))
            copies[-1].start()
    for copy in copies:
        copy.wait()


def local_wide(nw, nn, right_side, occupancy, region, coarse_inverse):
    _, X, Y, Z = right_side.shape
    ncr, NC = coarse_inverse.shape
    ND = nw * nn
    f32, i32 = jnp.float32, jnp.int32
    V = pltpu.VMEM
    field, pad, scal = (3, X, Y, Z), (3, X + 2, Y, Z), (X, Y, Z)
    scratch = [
        V(scal, i32), V(scal, i32), V((ncr, NC), f32),
        V((X + 2, Y, Z), f32), V((X + 1, Y, Z), f32),
        V(scal, f32), V(scal, f32), V(scal, f32), V(scal, f32), V(scal, f32), V(scal, f32),
        V(pad, f32), V(pad, f32),
        V((2, 3, X, Z), f32), V((2, 3, X, Z), f32),
        V((2, 2, Y, Z), i32), V((2, 2, X, Z), i32), V((2, 2, X, Z), i32),
        V((4, ncr, NC), f32),
        V((2, 2, 3, Y, Z), f32), V((2, 2, 3, Y, Z), f32),
        V((2, 2, 3, X, Z), f32), V((2, 2, 3, X, Z), f32),
        V((3, SUB, LANES), f32), V((3, ND, LANES), f32),
        pltpu.SemaphoreType.DMA((4,)),
        pltpu.SemaphoreType.DMA((5, 4)), pltpu.SemaphoreType.DMA((5, 4)),
        pltpu.SemaphoreType.DMA((3,)), pltpu.SemaphoreType.DMA((3,)),
    ]
    parts = pl.pallas_call(
        functools.partial(kernel_wide, nw, nn),
        out_shape=(V(field, f32),) * 5 + (V((SUB, LANES), f32),),
        in_specs=[pl.BlockSpec(memory_space=pltpu.HBM)] * 4,
        out_specs=(pl.BlockSpec(memory_space=pltpu.VMEM),) * 6,
        scratch_shapes=scratch,
        compiler_params=pltpu.CompilerParams(collective_id=0, has_side_effects=True, vmem_limit_bytes=32 * 1024 * 1024),
    )(*[pltpu.with_memory_space_constraint(a, pltpu.HBM) for a in (right_side, occupancy, region, coarse_inverse)])
    return pl.pallas_call(
        finish_wide,
        out_shape=(jax.ShapeDtypeStruct(field, f32),) * 2,
        in_specs=[pl.BlockSpec(memory_space=pltpu.VMEM)] * 6,
        out_specs=(pl.BlockSpec(memory_space=pltpu.HBM),) * 2,
        scratch_shapes=[V(field, f32), V(field, f32), pltpu.SemaphoreType.DMA((2, 3))],
        compiler_params=pltpu.CompilerParams(vmem_limit_bytes=16 * 1024 * 1024),
    )(*parts)


REPLICATED_BYTES = 4 * 1024 * 1024
DEEP = 3
AROUND = ((-1, 0), (1, 0), (0, -1), (0, 1), (-1, -1), (-1, 1), (1, -1), (1, 1))
BACK = tuple(AROUND.index((-a, -b)) for a, b in AROUND)


def group_of(n):
    return max(d for d in range(1, n + 1) if n % d == 0 and d * d <= n)


def spread_over(reg, q, G, inside=False):
    masks = [reg == g for g in range(G)]
    out = []
    for c in range(3):
        s = q[(G - 1) * 3 + c] if inside else jnp.where(masks[G - 1], q[(G - 1) * 3 + c], 0.0)
        for g in range(G - 1):
            s = jnp.where(masks[g], q[g * 3 + c], s)
        out.append(s)
    return out


def rows_from(low, count):
    return pl.ds(SUB + low, count)


def both_sides(ref, Y, *at):
    row = lax.broadcasted_iota(jnp.int32, (SUB, LANES), 0)
    return jnp.where(row < SUB // 2, ref[(*at, pl.ds(SUB + Y, SUB))], ref[(*at, pl.ds(0, SUB))])


def apply(ref, coefficients, x, low, count):
    kx, kyp, kzm, kzp, dg, k4 = coefficients
    here, down, up = rows_from(low, count), rows_from(low - 1, count), rows_from(low + 1, count)
    u = [ref[c, x, here] for c in range(3)]
    kk = k4[x, here] * (u[0] + u[1] + u[2])
    out = []
    for c in range(3):
        a = kx[x, here] * ref[c, x - 1, here] + kx[x + 1, here] * ref[c, x + 1, here]
        a = a + (kyp[x, down] * ref[c, x, down] + kyp[x, here] * ref[c, x, up])
        a = a + (kzm[x, here] * pltpu.roll(u[c], 1, 1) + kzp[x, here] * pltpu.roll(u[c], LANES - 1, 1))
        out.append(dg[x, here] * u[c] + kk - a)
    return u, out


def kernel(nw, nn, r_hbm, occ_hbm, reg_hbm, ci_hbm,
           z_e, g_e, y_e, r_o, ag_o, reg_o, k4, dg, kx, kyp, kzm, kzp, q_o, sc_o,
           occ_e, reg_e, r_e, k_e, invd,
           call, c_in, y_face, y_label, qpair, place_of, row_send, rows, sizes,
           load_sem, send, recv, ready):
    E, YE, Z = occ_e.shape
    X, Y = E - 2 * DEEP, YE - 2 * SUB
    ncr, NC = c_in.shape[1:]
    G = ncr // 3
    ND = nw * nn
    NH = ND // 2
    wi = lax.axis_index("wide")
    ni = lax.axis_index("narrow")
    me = wi * nn + ni
    f32 = jnp.float32
    GW = group_of(nw)
    GP = GW * nn
    NG = ND // GP
    grp, pos = me // GP, lax.rem(me, GP)
    half, place = lax.rem(wi, 2), (lax.rem(wi, GW) // 2) * nn + ni
    here = half * NH + place * NG + grp
    own, inner_rows = pl.ds(DEEP, X), pl.ds(SUB, Y)

    loads = [pltpu.make_async_copy(s, d, load_sem.at[i]) for s, d, i in (
        (reg_hbm, reg_e.at[own, inner_rows], 0), (r_hbm, r_e.at[:, own, inner_rows], 0),
        (occ_hbm, occ_e.at[own, inner_rows], 1), (ci_hbm, call.at[here], 2))]
    for l in loads:
        l.start()

    barrier = pltpu.get_barrier_semaphore()

    def at(t):
        return (t // nn, lax.rem(t, nn))

    def wait_for(sem, count):
        @pl.when(count > 0)
        def _():
            pl.semaphore_wait(sem, count)

    def column_of(group):
        return (wi + (group - grp) * GW, ni)

    at_low = jnp.logical_and(lax.rem(wi, GW) == 0, wi > 0)
    at_high = jnp.logical_and(lax.rem(wi, GW) == GW - 1, wi < nw - 1)
    aside = 1 + jnp.where(ni > 0, 1, 0) + jnp.where(ni < nn - 1, 1, 0)

    def touching(ahead, signal):
        @pl.when(at_high if ahead > 0 else at_low)
        def _():
            for b in (-1, 0, 1):
                @pl.when(jnp.logical_and(ni + b >= 0, ni + b < nn))
                def _():
                    signal((wi + ahead, ni + b))

    def say(sem):
        return lambda device: pl.semaphore_signal(sem, inc=1, device_id=device, device_id_type=MESH)

    for i in range(1, GP):
        say(barrier)(at(grp * GP + lax.rem(pos + i, GP)))
    touching(1, say(barrier))
    touching(-1, say(barrier))
    for k in range(1, NG):
        @pl.when(grp + k < NG)
        def _():
            say(barrier)(column_of(grp + k))

    def tell():
        for k in range(1, NG):
            @pl.when(grp >= k)
            def _():
                say(ready.at[k - 1])(column_of(grp - k))

    def take(rows_of, sem):
        some = sizes.at[pl.ds(0, rows_of)]
        pltpu.make_async_copy(some, some, sem).wait()

    def take_c(blocks, sem):
        some = call.at[pl.ds(0, blocks)]
        pltpu.make_async_copy(some, some, sem).wait()

    def by_neighbours(wait):
        nx = jnp.where(wi > 0, 1, 0) + jnp.where(wi < nw - 1, 1, 0)
        ny = jnp.where(ni > 0, 1, 0) + jnp.where(ni < nn - 1, 1, 0)
        for a in ((1,) if nw == 2 else (1, 2)):
            for b in (range(min(nn, 2)) if nn == 1 else (1,) if nn == 2 else (1, 2)):
                @pl.when(jnp.logical_and(nx == a, ny == b))
                def _():
                    wait(a, b)

    def halo_rows(n, a, b):
        deep, corner, count = ((DEEP, 2, 1), (2, 1, 1), (2, 1, 3))[n]
        return count * (a * deep * Y + b * deep * X + a * b * corner * corner)

    has = []
    for a, b in AROUND:
        h = jnp.logical_and(wi + a >= 0, wi + a < nw)
        has.append(jnp.logical_and(h, jnp.logical_and(ni + b >= 0, ni + b < nn)))

    def part(arr, d, into):
        a, b = AROUND[d]
        deep = {0: DEEP, 1: 2, 2: 2}[arr] if a == 0 or b == 0 else {0: 2, 1: 1, 2: 1}[arr]
        if into:
            xs = {-1: (DEEP - deep, deep), 0: (DEEP, X), 1: (DEEP + X, deep)}[a]
            ys = {-1: (SUB - deep, deep), 0: (SUB, Y), 1: (SUB + Y, deep)}[b]
        else:
            xs = {-1: (DEEP, deep), 0: (DEEP, X), 1: (DEEP + X - deep, deep)}[a]
            ys = {-1: (SUB, deep), 0: (SUB, Y), 1: (SUB + Y - deep, deep)}[b]
        xs, ys = pl.ds(*xs), pl.ds(*ys)
        return (slice(None), xs, ys) if arr == 2 else (xs, ys)

    fields = (occ_e, reg_e, r_e)
    for d in range(8):
        @pl.when(jnp.logical_not(has[d]))
        def _():
            for n, ref in enumerate(fields):
                where = part(n, d, True)
                v = ref[where]
                ref[where] = jnp.full(v.shape, (-1, -1, 0)[n], v.dtype)
            c_in[d] = jnp.zeros((ncr, NC), f32)

    wait_for(barrier, GP - 1 + grp + jnp.where(at_low, aside, 0) + jnp.where(at_high, aside, 0))
    tell()

    def fold(a):
        return jnp.sum(a.reshape(a.shape[0] // SUB, SUB, Z), axis=0)

    def zero_acc(n):
        return tuple(jnp.zeros((SUB, Z), f32) for _ in range(n))

    def add_rc(acc, reg, u):
        out = list(acc)
        for g in range(G):
            m = reg == g
            for c in range(3):
                out[g * 3 + c] = acc[g * 3 + c] + fold(jnp.where(m, u[c], 0.0))
        return out

    base = (me * ncr) % LANES

    def column(acc):
        a = jnp.concatenate([jnp.sum(b, axis=0, keepdims=True) for b in acc], axis=0)
        return jnp.sum(a, axis=1, keepdims=True)

    def make_row(p, acc):
        col = column(acc)
        n = len(acc)
        k = lax.broadcasted_iota(jnp.int32, (n, LANES), 0)
        lane = lax.broadcasted_iota(jnp.int32, (n, LANES), 1)
        target = (base + k) & (LANES - 1)
        row = jnp.sum(jnp.where(lane == target, col, 0.0), axis=0, keepdims=True)
        row_send[p, 0:1, :] = row
        rows[p, pl.ds(me, 1), :] = row

    def rows_to(p, count, t, out, sem):
        pltpu.make_async_remote_copy(
            src_ref=row_send.at[pl.ds(p, count), pl.ds(0, 1)], dst_ref=rows.at[pl.ds(p, count), pl.ds(me, 1)],
            send_sem=send.at[out], recv_sem=recv.at[sem],
            device_id=at(t), device_id_type=MESH).start()

    def each_peer(send):
        def body(i, _):
            send(i + jnp.where(i < me, 0, 1))
            return 0
        lax.fori_loop(0, ND - 1, body, 0, unroll=ND <= 64)

    take(4 * X * Y, load_sem.at[0])
    acc = looped(0, X, lambda x, a: tuple(add_rc(
        a, reg_e[x + DEEP, inner_rows], [r_e[c, x + DEEP, inner_rows] for c in range(3)])), zero_acc(ncr))
    make_row(0, acc)

    def inside(i, _):
        rows_to(0, 1, grp * GP + lax.rem(pos + i, GP), 0, 3)
        return 0

    lax.fori_loop(1, GP, inside, 0, unroll=GP <= 64)

    def halo(n, d):
        a, b = AROUND[d]
        e = BACK[d]
        return pltpu.make_async_remote_copy(
            src_ref=fields[n].at[part(n, d, False)], dst_ref=fields[n].at[part(n, e, True)],
            send_sem=send.at[0], recv_sem=recv.at[min(n, 1)],
            device_id=(wi + a, ni + b), device_id_type=MESH)

    def halo_c(d):
        a, b = AROUND[d]
        return pltpu.make_async_remote_copy(
            src_ref=call.at[here], dst_ref=c_in.at[BACK[d]],
            send_sem=send.at[1], recv_sem=recv.at[2],
            device_id=(wi + a, ni + b), device_id_type=MESH)

    loads[2].wait()
    loads[3].wait()

    for n in range(3):
        for d in range(8):
            @pl.when(has[d])
            def _():
                halo(n, d).start()

    def c_column(group):
        pltpu.make_async_remote_copy(
            src_ref=call.at[here], dst_ref=call.at[here],
            send_sem=send.at[2], recv_sem=recv.at[5],
            device_id=column_of(group), device_id_type=MESH).start()

    for k in range(1, NG):
        @pl.when(grp >= k)
        def _():
            c_column(grp - k)

    def c_group(block, sem):
        for i in range(1, GP // 2):
            p = lax.rem(place + i, GP // 2)
            pltpu.make_async_remote_copy(
                src_ref=call.at[block], dst_ref=call.at[block],
                send_sem=send.at[2], recv_sem=recv.at[sem],
                device_id=(grp * GW + (p // nn) * 2 + half, lax.rem(p, nn)), device_id_type=MESH).start()

    c_group(here, 9)
    for d in range(8):
        if AROUND[d][0]:
            @pl.when(has[d])
            def _():
                halo_c(d).start()

    def stiff_of(o):
        return jnp.where(o < 0, 0.0, soft_stiff + (bone_stiff - soft_stiff) * o.astype(f32))

    n2 = G * G

    def pairs(acc, first, seconds):
        out = list(acc)
        for g in range(G):
            t = None
            for label, value in seconds:
                v = jnp.where(label == g, value, 0.0)
                t = v if t is None else t + v
            for h in range(G):
                out[h * G + g] = acc[h * G + g] + fold(jnp.where(first == h, t, 0.0))
        return out

    row16 = lax.broadcasted_iota(jnp.int32, (Y, Z), 0)
    lane16 = lax.broadcasted_iota(jnp.int32, (Y, Z), 1)

    def own_pairs(i, carry):
        x = i + DEEP
        k, reg = stiff_of(occ_e[x, inner_rows]), reg_e[x, inner_rows]
        later = jnp.minimum(i + 1, X - 1) + DEEP
        kx_in = jnp.where(i < X - 1, 0.5 * (k + stiff_of(occ_e[later, inner_rows])), 0.0)
        ky_in = jnp.where(row16 == Y - 1, 0.0, 0.5 * (k + pltpu.roll(k, Y - 1, 0)))
        kz_in = jnp.where(lane16 == Z - 1, 0.0, 0.5 * (k + pltpu.roll(k, Z - 1, 1)))
        acc = pairs(carry[:n2], reg, ((reg_e[later, inner_rows], kx_in), (pltpu.roll(reg, Y - 1, 0), ky_in),
                                      (pltpu.roll(reg, Z - 1, 1), kz_in)))
        sums = [carry[n2 + g] + fold(jnp.where(reg == g, 0.25 * k, 0.0)) for g in range(G)]
        return tuple(acc) + tuple(sums)

    own_acc = lax.fori_loop(0, X, own_pairs, zero_acc(n2 + G), unroll=2)
    own_col = column(own_acc)

    def c_up(k):
        @pl.when(grp + k < NG)
        def _():
            pl.semaphore_wait(ready.at[k - 1], 1)
            c_column(grp + k)

    for k in range(1, NG):
        c_up(k)

    take(GP - 1, recv.at[3])
    mine = rows.at[0, pl.ds(pl.multiple_of(grp * GP, GP), GP)]

    def across(group):
        pltpu.make_async_remote_copy(
            src_ref=mine, dst_ref=mine, send_sem=send.at[0], recv_sem=recv.at[4],
            device_id=column_of(group), device_id_type=MESH).start()

    for k in range(1, NG):
        @pl.when(grp >= k)
        def _():
            across(grp - k)

    for k in range(1, NG):
        @pl.when(grp + k < NG)
        def _():
            across(grp + k)

    by_neighbours(lambda a, b: take(halo_rows(0, a, b), recv.at[0]))

    lane_id = lax.broadcasted_iota(jnp.int32, (Y + SUB, Z), 1)

    def stiffness(x, _):
        k_e[x] = stiff_of(occ_e[x])
        return 0

    lax.fori_loop(0, E, stiffness, 0, unroll=True)
    row8 = lax.broadcasted_iota(jnp.int32, (SUB, Z), 0)

    def coefficients(x):
        here = rows_from(-2, Y + SUB)
        k = k_e[x, here]
        low, high = k_e[x, rows_from(-3, Y + SUB)], k_e[x, rows_from(-1, Y + SUB)]
        back = jnp.where(lane_id == 0, 0.0, pltpu.roll(k, 1, 1))
        ahead = jnp.where(lane_id == Z - 1, 0.0, pltpu.roll(k, Z - 1, 1))
        xm = 0.5 * (k + k_e[x - 1, here])
        xp = 0.5 * (k + k_e[x + 1, here])
        ym = 0.5 * (k + low)
        yp = 0.5 * (k + high)
        zm = 0.5 * (k + back)
        zp = 0.5 * (k + ahead)
        diag = xm + xp + ym + yp + zm + zp + 0.5 * k
        kx[x, here] = xm
        kx[x + 1, here] = xp
        kyp[x, here] = yp
        kzm[x, here] = jnp.where(lane_id == 0, 0.0, zm)
        kzp[x, here] = jnp.where(lane_id == Z - 1, 0.0, zp)
        dg[x, here] = diag - 0.25 * k
        k4[x, here] = 0.25 * k
        invd[x, here] = jnp.where(k > 0.0, 1.0 / diag, 0.0)

    for x in (1, 2, DEEP + X, DEEP + X + 1):
        coefficients(x)

    def inner(i, sums):
        coefficients(i + DEEP)
        d, reg = dg[i + DEEP, inner_rows], reg_e[i + DEEP, inner_rows]
        return tuple(sums[g] + fold(jnp.where(reg == g, d, 0.0)) for g in range(G))

    sum_acc = lax.fori_loop(0, X, inner, zero_acc(G), unroll=4)

    take_c(NG - 1, recv.at[5])
    for k in range(1, NG):
        c_group(half * NH + place * NG + lax.rem(grp + k, NG), 6)

    by_neighbours(lambda a, b: take(halo_rows(1, a, b) + halo_rows(2, a, b), recv.at[1]))

    def side_rows(i, _):
        x = i + DEEP
        y_face[0, pl.ds(i, 1), :] = kyp[x, rows_from(Y - 1, 1), :]
        y_label[0, pl.ds(i, 1), :] = reg_e[x, rows_from(Y - 1, 1), :]
        y_label[1, pl.ds(i, 1), :] = reg_e[x, rows_from(Y, 1), :]
        return 0

    looped(0, X, side_rows, 0)
    top = DEEP + X - 1
    x_acc = pairs(zero_acc(n2), reg_e[top, inner_rows], ((reg_e[top + 1, inner_rows], kx[top + 1, inner_rows]),))
    y_acc = pairs(zero_acc(n2), y_label[0], ((y_label[1], y_face[0]),))
    rim_col = column(tuple(x_acc) + tuple(y_acc) + tuple(sum_acc))

    lane = lax.broadcasted_iota(jnp.int32, (n2, LANES), 1)
    pair = lax.broadcasted_iota(jnp.int32, (n2, LANES), 0)
    at_pair = jnp.logical_and(lane >= 3 * pair, lane < 3 * pair + 3)

    def lanes_of(col, mask):
        return jnp.sum(jnp.where(mask, col, 0.0), axis=0, keepdims=True)

    lane_g = lax.broadcasted_iota(jnp.int32, (G, LANES), 1)
    row_g = lax.broadcasted_iota(jnp.int32, (G, LANES), 0)
    diag_at, sum_at = 3 * (G + 1) * row_g, 3 * n2 + 9 * row_g
    at_diag = jnp.logical_and(lane_g >= diag_at, lane_g < diag_at + 3)
    at_sum = jnp.logical_and(lane_g >= sum_at, lane_g < sum_at + 9)
    ac_rows = (lanes_of(own_col[0:n2], at_pair) * -2.0 + lanes_of(rim_col[2 * n2:], at_diag)
               + lanes_of(own_col[n2:], at_sum),
               lanes_of(rim_col[0:n2], at_pair) * -2.0, lanes_of(rim_col[n2:2 * n2], at_pair) * -2.0)
    for n in range(3):
        row_send[n + 2, 0:1, :] = ac_rows[n]
        rows[n + 2, pl.ds(me, 1), :] = ac_rows[n]

    def coarse_vector(block):
        tiles = []
        for t in range(NC // LANES):
            lo = (LANES * t) // ncr // SUB * SUB
            hi = min(ND, -(-(-(-(LANES * (t + 1)) // ncr)) // SUB) * SUB)
            d = lax.broadcasted_iota(jnp.int32, (hi - lo, LANES), 0) + lo
            j = lax.broadcasted_iota(jnp.int32, (hi - lo, LANES), 1) + LANES * t
            m = (j >= d * ncr) & (j < d * ncr + ncr)
            tiles.append(jnp.sum(jnp.where(m, block[lo:hi, :], 0.0), axis=0, keepdims=True))
        return tiles

    def total(block, s):
        d = lax.broadcasted_iota(jnp.int32, (ND, LANES), 0)
        lane = lax.broadcasted_iota(jnp.int32, (ND, LANES), 1)
        m = lane == ((d * ncr + ncr + s) & (LANES - 1))
        v = jnp.sum(jnp.where(m, block, 0.0), axis=0, keepdims=True)
        return jnp.sum(v, axis=1, keepdims=True)

    def solve(tiles, block):
        s = block[:, 0:LANES] * tiles[0]
        for t in range(1, len(tiles)):
            s = s + block[:, t * LANES:(t + 1) * LANES] * tiles[t]
        return jnp.sum(s, axis=1, keepdims=True)

    def rows_of(d):
        a, b = AROUND[d]
        return c_in[d] if a else call[here + jnp.where(has[d], b * NG, 0)]

    def as_list(q):
        return [q[i:i + 1, :] for i in range(ncr)]

    take(ND - GP, recv.at[4])
    by_neighbours(lambda a, b: take_c(a + a * b, recv.at[2]))
    take_c(GP // 2 - 1, recv.at[9])
    tiles = coarse_vector(rows[0])
    q = as_list(solve(tiles, call[here]))
    qn = [as_list(solve(tiles, rows_of(d))) for d in range(8)]

    def either(hi, lo):
        return [jnp.where(row8 < SUB // 2, a, b) for a, b in zip(hi, lo)]

    def add_spread(x, q_in, q_out, inside):
        reg, inv = reg_e[x, inner_rows], invd[x, inner_rows]
        s = spread_over(reg, q_in, G, inside)
        reg_o[x, inner_rows] = reg
        for c in range(3):
            z_e[c, x, inner_rows] = r_e[c, x, inner_rows] * inv + s[c]
        reg, inv = both_sides(reg_e, Y, x), both_sides(invd, Y, x)
        s = spread_over(reg, q_out, G)
        some = SUB // 2
        reg_o[x, rows_from(Y, some)] = reg[0:some]
        reg_o[x, rows_from(-some, some)] = reg[some:SUB]
        for c in range(3):
            z = both_sides(r_e, Y, c, x) * inv + s[c]
            z_e[c, x, rows_from(Y, some)] = z[0:some]
            z_e[c, x, rows_from(-some, some)] = z[some:SUB]

    q_side = either(qn[3], qn[2])

    def spread_own(i, _):
        add_spread(i + DEEP, q, q_side, True)
        return 0

    looped(0, X, spread_own, 0)
    q_low, q_high = either(qn[5], qn[4]), either(qn[7], qn[6])
    for x in (1, 2):
        add_spread(x, qn[0], q_low, False)
    for x in (DEEP + X, DEEP + X + 1):
        add_spread(x, qn[1], q_high, False)

    faces = (kx, kyp, kzm, kzp, dg, k4)

    def dots(a, b):
        return fold(a[0] * b[0] + a[1] * b[1] + a[2] * b[2])

    def first(i, _):
        x, some = i + DEEP - 1, rows_from(-1, Y + SUB)
        _, a = apply(z_e, faces, x, -1, Y + SUB)
        for c in range(3):
            y_e[c, x, some] = a[c]
            g_e[c, x, some] = a[c] * invd[x, some]
        return 0

    lax.fori_loop(0, X + 2, first, 0, unroll=(X + 2) // 2)

    def own_of(ref, x):
        return [ref[c, x, inner_rows] for c in range(3)]

    def second(i, carry):
        x = i + DEEP
        w, a = apply(g_e, faces, x, 0, Y)
        for c in range(3):
            ag_o[c, i] = a[c]
        acc = add_rc(carry[:ncr], reg_e[x, inner_rows], a)
        return tuple(acc) + (carry[ncr] + dots(w, a),)

    acc2 = lax.fori_loop(0, X, second, zero_acc(ncr + 1), unroll=8)

    def third(i, carry):
        x = i + DEEP
        r, z, y, w = own_of(r_e, x), own_of(z_e, x), own_of(y_e, x), own_of(g_e, x)
        for c in range(3):
            r_o[c, i] = r[c]
        acc = add_rc(carry[:ncr], reg_e[x, inner_rows], y)
        return tuple(acc) + (carry[ncr] + dots(r, z), carry[ncr + 1] + dots(y, z), carry[ncr + 2] + dots(y, w))

    acc1 = lax.fori_loop(0, X, third, zero_acc(ncr + 3), unroll=8)
    make_row(1, tuple(acc1) + (acc2[ncr],) + tuple(acc2[:ncr]))
    each_peer(lambda t: rows_to(1, 4, t, 3, 7))

    rr = lax.broadcasted_iota(jnp.int32, (ncr, LANES), 0)
    ll = lax.broadcasted_iota(jnp.int32, (ncr, LANES), 1)
    m0, m1 = rr < 0, rr < 0
    for h in range(G):
        for g in range(G):
            for c in range(3):
                k = (h * G + g) * 3 + c
                m0 = jnp.logical_or(m0, (ll == k) & (rr == h * 3 + c))
                m1 = jnp.logical_or(m1, (ll == k) & (rr == g * 3 + c))
        for c in range(3):
            for e in range(3):
                k = 3 * n2 + h * 9 + c * 3 + e
                m0 = jnp.logical_or(m0, (ll == k) & (rr == h * 3 + c))
                m1 = jnp.logical_or(m1, (ll == k) & (rr == h * 3 + e))
    place_of[0] = jnp.where(m0, 1.0, 0.0)
    place_of[1] = jnp.where(m1, 1.0, 0.0)

    take_c((GP // 2 - 1) * (NG - 1), recv.at[6])
    swap_half = call.at[pl.ds(half * NH, NH)]
    swap = pltpu.make_async_remote_copy(
        src_ref=swap_half, dst_ref=swap_half, send_sem=send.at[2], recv_sem=recv.at[8],
        device_id=(wi + 1 - 2 * half, ni), device_id_type=MESH)
    swap.start()
    by_neighbours(lambda a, b: take(
        sum(halo_rows(n, a, b) for n in range(3)) + GP - 1 + (NG - 1) * GP, send.at[0]))
    by_neighbours(lambda a, b: take_c(a + a * b, send.at[1]))
    swap.wait_recv()
    take(4 * (ND - 1), recv.at[7])

    block = rows[1]
    b1 = coarse_vector(block)
    h1 = coarse_vector(pltpu.roll(block, LANES - ncr - 4, 1))
    lines = [jnp.zeros((ncr, LANES), f32) for _ in b1]
    for w in range(nw):
        for n in range(nn):
            d = w * nn + n
            q1 = solve(b1, call[w % 2 * NH + ((w % GW) // 2 * nn + n) * NG + w // GW])
            qpair[0, d:d + 1, :] = jnp.sum(place_of[0] * q1, axis=0, keepdims=True)
            qpair[1, d:d + 1, :] = jnp.sum(place_of[1] * q1, axis=0, keepdims=True)
            for t in range(d * ncr // LANES, (d * ncr + ncr - 1) // LANES + 1):
                lines[t] = jnp.where(ll + LANES * t == rr + d * ncr, q1, lines[t])
    lines = [jnp.sum(v, axis=0, keepdims=True) for v in lines]
    first_q, second_q = qpair[0], qpair[1]
    dev = lax.broadcasted_iota(jnp.int32, (ND, LANES), 0)
    next_x = jnp.where(dev < ND - nn, pltpu.roll(second_q, ND - nn, 0), 0.0)
    next_y = jnp.where(dev < ND - 1, pltpu.roll(second_q, ND - 1, 0), 0.0)
    energy = jnp.sum(first_q * (rows[2] * second_q + rows[3] * next_x + rows[4] * next_y), axis=0, keepdims=True)
    for t in range(len(b1)):
        energy = energy + 2.0 * h1[t] * lines[t]
    yv = b1[0] * lines[0]
    for t in range(1, len(b1)):
        yv = yv + b1[t] * lines[t]
    yv = total(block, 2) + jnp.sum(yv, axis=1, keepdims=True)
    vav = total(block, 3) + jnp.sum(energy, axis=1, keepdims=True)
    rz0, zy = total(block, 0), total(block, 1)
    alpha0 = rz0 / zy
    rz1 = alpha0 * alpha0 * yv - rz0
    zaz = zy - 2.0 * alpha0 * yv + alpha0 * alpha0 * vav
    beta = rz1 / rz0
    alpha1 = rz1 / (zaz - beta * rz1 / alpha0)
    a1b = alpha1 * beta
    for n, v in enumerate((alpha0 + a1b + alpha1, alpha1 * alpha0)):
        sc_o[n:n + 1, :] = jnp.broadcast_to(v, (1, LANES))
    q_o[0] = jnp.broadcast_to(solve(b1, call[here]), (ncr, LANES))
    for d in range(4):
        q_o[d + 1] = jnp.broadcast_to(solve(b1, rows_of(d)), (ncr, LANES))

    take(4 * (ND - 1), send.at[3])
    take_c(NG - 1 + (GP // 2 - 1) * NG + NH, send.at[2])


def finish(z_v, g_v, y_v, r_v, ag_v, reg_v, k4, dg, kx, kyp, kzm, kzp, q_v, sc_v, x_out, res_out, s_e, xb, rb, sem):
    a, b = sc_v[0:1, 0:1], sc_v[1:2, 0:1]
    E, YE, Z = reg_v.shape
    X, Y = E - 2 * DEEP, YE - 2 * SUB
    G = q_v.shape[1] // 3
    own = pl.ds(SUB, Y)
    row8 = lax.broadcasted_iota(jnp.int32, (SUB, Z), 0)
    q = [[q_v[d, i:i + 1, :] for i in range(3 * G)] for d in range(5)]
    side = [jnp.where(row8 < SUB // 2, hi, lo) for hi, lo in zip(q[4], q[3])]

    def fill(x, q_in, inside):
        s = spread_over(reg_v[x, own], q_in, G, inside)
        for c in range(3):
            s_e[c, x, own] = s[c]
        return s

    def fill_sides(x):
        s = spread_over(both_sides(reg_v, Y, x), side, G)
        some = SUB // 2
        for c in range(3):
            s_e[c, x, rows_from(Y, some)] = s[c][0:some]
            s_e[c, x, rows_from(-some, some)] = s[c][some:SUB]

    def fill_own(i, _):
        x = i + DEEP
        s = fill(x, q[0], True)
        fill_sides(x)
        for c in range(3):
            xb[c, i] = a * z_v[c, x, own] - b * (g_v[c, x, own] + s[c])
        return 0

    fill(DEEP - 1, q[1], False)
    fill(DEEP + X, q[2], False)
    faces = (kx, kyp, kzm, kzp, dg, k4)
    parts = 4
    step = X // parts

    def leave(m, src, dst, n):
        where = (slice(None), pl.ds(n * step, step))
        pltpu.make_async_copy(src.at[where], dst.at[where], sem.at[m]).start()

    def plane(i, _):
        u, w = apply(s_e, faces, i + DEEP, 0, Y)
        for c in range(3):
            rb[c, i] = r_v[c, i] - a * y_v[c, i + DEEP, own] + b * (ag_v[c, i] + w[c])
        return 0

    for n in range(parts):
        lax.fori_loop(n * step, (n + 1) * step, fill_own, 0, unroll=True)
        leave(0, xb, x_out, n)
    for n in range(parts):
        lax.fori_loop(n * step, (n + 1) * step, plane, 0, unroll=True)
        leave(1, rb, res_out, n)
    pltpu.make_async_copy(xb, x_out, sem.at[0]).wait()
    pltpu.make_async_copy(rb, res_out, sem.at[1]).wait()


def local_fast(nw, nn, right_side, occupancy, region, coarse_inverse):
    _, X, Y, Z = right_side.shape
    ncr, NC = coarse_inverse.shape
    ND = nw * nn
    f32, i32 = jnp.float32, jnp.int32
    V = pltpu.VMEM
    E, YE = X + 2 * DEEP, Y + 2 * SUB
    field, ext, scal = (3, X, Y, Z), (3, E, YE, Z), (E, YE, Z)
    ng = nw // group_of(nw)
    DMA = pltpu.SemaphoreType.DMA
    scratch = [
        V(scal, i32), V(scal, i32), V(ext, f32), V(scal, f32), V(scal, f32),
        V((ND, ncr, NC), f32), V((8, ncr, NC), f32), V((2, X, Z), f32), V((3, X, Z), i32), V((3, ND, LANES), f32), V((2, ncr, LANES), f32),
        V((5, SUB, LANES), f32), V((6, ND, LANES), f32), V((4 * X * Y, LANES), f32),
        DMA((3,)), DMA((4,)), DMA((10,)),
        pltpu.SemaphoreType.REGULAR((ng - 1,)),
    ]
    outs = (V(ext, f32),) * 3 + (V(field, f32),) * 2 + (V(scal, i32),) + (V(scal, f32),) * 6 + (V((5, ncr, LANES), f32), V((SUB, LANES), f32))
    parts = pl.pallas_call(
        functools.partial(kernel, nw, nn),
        out_shape=outs,
        in_specs=[pl.BlockSpec(memory_space=pltpu.HBM)] * 4,
        out_specs=(pl.BlockSpec(memory_space=pltpu.VMEM),) * len(outs),
        scratch_shapes=scratch,
        compiler_params=pltpu.CompilerParams(collective_id=0, has_side_effects=True, vmem_limit_bytes=32 * 1024 * 1024),
    )(*[pltpu.with_memory_space_constraint(a, pltpu.HBM) for a in (right_side, occupancy, region, coarse_inverse)])
    return pl.pallas_call(
        finish,
        out_shape=(jax.ShapeDtypeStruct(field, f32),) * 2,
        in_specs=[pl.BlockSpec(memory_space=pltpu.VMEM)] * len(outs),
        out_specs=(pl.BlockSpec(memory_space=pltpu.HBM),) * 2,
        scratch_shapes=[V(ext, f32), V(field, f32), V(field, f32), DMA((2,))],
        compiler_params=pltpu.CompilerParams(vmem_limit_bytes=24 * 1024 * 1024),
    )(*parts)


def local(nw, nn, right_side, occupancy, region, coarse_inverse):
    nc = coarse_inverse.shape[1]
    run = local_fast if group_of(nw) % 2 == 0 and nc * nc * 4 <= REPLICATED_BYTES else local_wide
    return run(nw, nn, right_side, occupancy, region, coarse_inverse)


def solution(mesh):
    return jax.shard_map(
        functools.partial(local, mesh.shape["wide"], mesh.shape["narrow"]),
        mesh=mesh,
        in_specs=(
            P(None, "wide", "narrow", None),
            P("wide", "narrow", None),
            P("wide", "narrow", None),
            P(("wide", "narrow"), None),
        ),
        out_specs=(P(None, "wide", "narrow", None), P(None, "wide", "narrow", None)),
        check_vma=False,
    )
```
